32 devices in a mesh: dp: 4 (over y, z), tp: 8 (over x, core).
Axes of the slice: x: 4, y: 2, z: 2, core: 2. Of those that a mesh axis runs over, the one named last changes fastest.
The devices are a block of a 4x4x8 slice.
Arguments:
- x_tokens: bfloat16 [12, 768, 5120], P('dp', 'tp'), parts along dimension 0
- e_time: float32 [12, 3, 5120], P('dp'), parts along dimension 0
- m_block: float32 [3, 5120], replicated
- w_q: bfloat16 [5120, 5120], P(None, 'tp')
- b_q: float32 [5120], P('tp')
- w_k: bfloat16 [5120, 5120], P(None, 'tp')
- b_k: float32 [5120], P('tp')
- w_v: bfloat16 [5120, 5120], P(None, 'tp')
- b_v: float32 [5120], P('tp')
- w_o: bfloat16 [5120, 5120], P('tp')
- b_o: float32 [5120], replicated
- g_q: float32 [5120], P('tp')
- g_k: float32 [5120], P('tp')
- positions: int32 [3072, 3], P('dp'), parts along dimension 0
- d_out: bfloat16 [12, 768, 5120], P('dp', 'tp'), parts along dimension 0
Outputs:
- output 1: bfloat16 [12, 768, 5120], P('dp', 'tp'), parts along dimension 0
- output 2: bfloat16 [12, 768, 5120], P('dp', 'tp'), parts along dimension 0
- output 3: float32 [12, 3, 5120], P('dp'), parts along dimension 0
- output 4: float32 [12, 5120], P('dp'), parts along dimension 0
- output 5: bfloat16 [20480, 5120], P('dp', 'tp'), parts along dimension 0
- output 6: bfloat16 [20480, 5120], P('dp', 'tp'), parts along dimension 0
- output 7: bfloat16 [20480, 5120], P('dp', 'tp'), parts along dimension 0
- output 8: bfloat16 [20480, 5120], P(('dp', 'tp')), parts along dimension 0
- output 9: float32 [20480], P(('dp', 'tp')), parts along dimension 0
- output 10: float32 [20480], P(('dp', 'tp')), parts along dimension 0
There are 4 independent parts. The reference program is written for one: setup_inputs(seed, part) draws one part's arguments, and reference() takes and returns one part's arrays. A program takes and returns all parts, laid end to end along the dimension named above; an argument that names none is the same for every part.
All inputs are finite; a program needn't handle non-finite values.
Results may differ from the reference program's by a relative error of at most 0.02.
Values are sent between devices in bfloat16 or wider.
A program may use at most 768 MiB of HBM per device.

```python
import jax
import jax.numpy as jnp
from jax import lax

NUM_BATCH = 3
SEQ_LEN = 768
NUM_HEADS = 40
HEAD_DIM = 128
MODEL_DIM = 5120
NUM_FRAMES = 21
NUM_ROWS = 45
NUM_COLS = 80

EPS_NORM = 1e-6
ROPE_BASE = 10000.0


def draw_positions(pos_key):
    coord_keys = jax.random.split(pos_key, 3)
    frame_ids = jax.random.randint(coord_keys[0], (SEQ_LEN,), 0, NUM_FRAMES)
    row_ids = jax.random.randint(coord_keys[1], (SEQ_LEN,), 0, NUM_ROWS)
    col_ids = jax.random.randint(coord_keys[2], (SEQ_LEN,), 0, NUM_COLS)
    grid_pos = jnp.stack([frame_ids, row_ids, col_ids], axis=1).astype(jnp.int32)
    corner_hi = jnp.array([NUM_FRAMES - 1, NUM_ROWS - 1, NUM_COLS - 1], dtype=jnp.int32)
    return grid_pos.at[0].set(corner_hi).at[1].set(jnp.zeros((3,), jnp.int32))


def setup_inputs(seed: int = 0, part: int = 0) -> dict:
    root_key = jax.random.key(seed)
    shared_keys = jax.random.split(root_key, 12)
    part_keys = jax.random.split(jax.random.fold_in(root_key, part), 4)
    fan_scale = MODEL_DIM ** -0.5
    head_ramp = 2.0 ** (2.0 * jnp.arange(NUM_HEADS, dtype=jnp.float32) / max(NUM_HEADS - 1, 1) - 1.0)
    col_scale = jnp.repeat(head_ramp, HEAD_DIM)
    sq_shape = (MODEL_DIM, MODEL_DIM)
    vec_shape = (MODEL_DIM,)
    tok_shape = (NUM_BATCH, SEQ_LEN, MODEL_DIM)
    return {
        'x_tokens': (0.5 * jax.random.normal(part_keys[0], tok_shape, jnp.float32)).astype(jnp.bfloat16),
        'e_time': 0.5 * jax.random.normal(part_keys[1], (NUM_BATCH, 3, MODEL_DIM), jnp.float32),
        'm_block': 0.5 * jax.random.normal(shared_keys[0], (3, MODEL_DIM), jnp.float32),
        'w_q': (jax.random.normal(shared_keys[1], sq_shape, jnp.float32) * fan_scale * col_scale).astype(jnp.bfloat16),
        'b_q': 0.5 * jax.random.normal(shared_keys[2], vec_shape, jnp.float32),
        'w_k': (jax.random.normal(shared_keys[3], sq_shape, jnp.float32) * fan_scale * col_scale).astype(jnp.bfloat16),
        'b_k': 0.5 * jax.random.normal(shared_keys[4], vec_shape, jnp.float32),
        'w_v': (jax.random.normal(shared_keys[5], sq_shape, jnp.float32) * (1.5 * fan_scale)).astype(jnp.bfloat16),
        'b_v': 0.5 * jax.random.normal(shared_keys[6], vec_shape, jnp.float32),
        'w_o': (jax.random.normal(shared_keys[7], sq_shape, jnp.float32) * fan_scale).astype(jnp.bfloat16),
        'b_o': 0.5 * jax.random.normal(shared_keys[8], vec_shape, jnp.float32),
        'g_q': jax.random.uniform(shared_keys[9], vec_shape, jnp.float32, 0.5, 1.5),
        'g_k': jax.random.uniform(shared_keys[10], vec_shape, jnp.float32, 0.5, 1.5),
        'positions': draw_positions(part_keys[3]),
        'd_out': jax.random.normal(part_keys[2], tok_shape, jnp.float32).astype(jnp.bfloat16),
    }


def rope_angles(positions):
    half_dim = HEAD_DIM // 2
    side_len = HEAD_DIM // 6
    first_len = half_dim - 2 * side_len
    pair_idx = jnp.arange(half_dim)
    section = (pair_idx >= first_len).astype(jnp.int32) + (pair_idx >= first_len + side_len).astype(jnp.int32)
    offset = jnp.where(section == 0, 0, jnp.where(section == 1, first_len, first_len + side_len))
    sec_width = jnp.where(section == 0, first_len, side_len)
    freq_vals = ROPE_BASE ** (-(pair_idx - offset).astype(jnp.float32) / sec_width.astype(jnp.float32))
    select = jnp.where(section[None, :] == jnp.arange(3)[:, None], freq_vals[None, :], 0.0)
    angles = jnp.sum(positions.astype(jnp.float32)[:, :, None] * select[None, :, :], axis=1)
    return jnp.cos(angles), jnp.sin(angles)


def rope_rotate(values, cos_part, sin_part):
    val_pairs = values.reshape(values.shape[:-1] + (values.shape[-1] // 2, 2))
    even_part = val_pairs[..., 0]
    odd_part = val_pairs[..., 1]
    rotated = jnp.stack([even_part * cos_part - odd_part * sin_part, even_part * sin_part + odd_part * cos_part], axis=-1)
    return rotated.reshape(values.shape)


def full_rms(values, gain):
    return values * lax.rsqrt(jnp.mean(values * values, axis=-1, keepdims=True) + EPS_NORM) * gain


def head_attention(operands):
    q_head, k_head, v_head = operands
    scores = jnp.einsum('bqd,bkd->bqk', q_head.astype(jnp.float32), k_head.astype(jnp.float32)) * HEAD_DIM ** -0.5
    attn_probs = jax.nn.softmax(scores, axis=-1).astype(jnp.bfloat16)
    return jnp.einsum('bqk,bkd->bqd', attn_probs.astype(jnp.float32), v_head.astype(jnp.float32)).astype(jnp.bfloat16)


def attention_block(x_tokens, e_time, m_block, w_q, b_q, w_k, b_k, w_v, b_v, w_o, b_o, g_q, g_k, cos_bcast, sin_bcast):
    head_shape = (NUM_BATCH, SEQ_LEN, NUM_HEADS, HEAD_DIM)
    mod_rows = m_block[None] + e_time
    shift_row = mod_rows[:, 0][:, None]
    scale_one = 1.0 + mod_rows[:, 1][:, None]
    gate_row = mod_rows[:, 2][:, None]
    x_float = x_tokens.astype(jnp.float32)
    centered = x_float - jnp.mean(x_float, axis=-1, keepdims=True)
    x_norm = centered * lax.rsqrt(jnp.mean(centered * centered, axis=-1, keepdims=True) + EPS_NORM)
    y_act = (x_norm * scale_one + shift_row).astype(jnp.bfloat16).reshape(NUM_BATCH * SEQ_LEN, MODEL_DIM)
    q_raw = jnp.dot(y_act, w_q, preferred_element_type=jnp.float32) + b_q
    k_raw = jnp.dot(y_act, w_k, preferred_element_type=jnp.float32) + b_k
    v_heads = (jnp.dot(y_act, w_v, preferred_element_type=jnp.float32) + b_v).astype(jnp.bfloat16).reshape(head_shape)
    q_rot = rope_rotate(full_rms(q_raw, g_q).reshape(head_shape), cos_bcast, sin_bcast).astype(jnp.bfloat16)
    k_rot = rope_rotate(full_rms(k_raw, g_k).reshape(head_shape), cos_bcast, sin_bcast).astype(jnp.bfloat16)
    o_heads = lax.map(jax.checkpoint(head_attention), (jnp.moveaxis(q_rot, 2, 0), jnp.moveaxis(k_rot, 2, 0), jnp.moveaxis(v_heads, 2, 0)))
    o_flat = jnp.moveaxis(o_heads, 0, 2).reshape(NUM_BATCH * SEQ_LEN, MODEL_DIM)
    proj_out = (jnp.dot(o_flat, w_o, preferred_element_type=jnp.float32) + b_o).reshape(NUM_BATCH, SEQ_LEN, MODEL_DIM)
    return (x_float + gate_row * proj_out).astype(jnp.bfloat16)


def reference(x_tokens, e_time, m_block, w_q, b_q, w_k, b_k, w_v, b_v, w_o, b_o, g_q, g_k, positions, d_out):
    cos_tab, sin_tab = rope_angles(positions)
    cos_bcast = cos_tab[None, :, None, :]
    sin_bcast = sin_tab[None, :, None, :]

    def block_fn(x_in, e_in, m_in, wq_in, wk_in, wv_in, wo_in, gq_in, gk_in):
        return attention_block(x_in, e_in, m_in, wq_in, b_q, wk_in, b_k, wv_in, b_v, wo_in, b_o, gq_in, gk_in, cos_bcast, sin_bcast)

    x_out, pull_back = jax.vjp(block_fn, x_tokens, e_time, m_block, w_q, w_k, w_v, w_o, g_q, g_k)
    d_x, d_e, d_m, d_wq, d_wk, d_wv, d_wo, d_gq, d_gk = pull_back(d_out)
    return (x_out, d_x, d_e, d_m, d_wq, d_wk, d_wv, d_wo, d_gq, d_gk)
```

```python
import functools

import jax
import jax.numpy as jnp
from jax import lax
from jax.experimental import pallas as pl
from jax.experimental.pallas import tpu as pltpu
from jax.sharding import PartitionSpec as P

HEAD_DIM = 128
EPS_NORM = 1e-6
ROPE_BASE = 10000.0
LOG2E = 1.4426950408889634
VMEM_LIMIT = 60 * 1024 * 1024
F32 = jnp.float32
BF16 = jnp.bfloat16
MESH_ID = pl.DeviceIdType.MESH
NT = (((1,), (1,)), ((), ()))
TN = (((0,), (0,)), ((), ()))


def params(*semantics, **kw):
    return pltpu.CompilerParams(dimension_semantics=semantics or None, vmem_limit_bytes=VMEM_LIMIT, **kw)


def cost(flops, nbytes):
    return pl.CostEstimate(flops=int(flops), bytes_accessed=int(nbytes), transcendentals=0)


def rope_tables(positions):
    half_dim = HEAD_DIM // 2
    side_len = HEAD_DIM // 6
    first_len = half_dim - 2 * side_len
    lane = jnp.arange(HEAD_DIM)
    pair_idx = lane // 2
    section = (pair_idx >= first_len).astype(jnp.int32) + (pair_idx >= first_len + side_len).astype(jnp.int32)
    offset = jnp.where(section == 0, 0, jnp.where(section == 1, first_len, first_len + side_len))
    sec_width = jnp.where(section == 0, first_len, side_len)
    freq_vals = ROPE_BASE ** (-(pair_idx - offset).astype(F32) / sec_width.astype(F32))
    select = jnp.where(section[None, :] == jnp.arange(3)[:, None], freq_vals[None, :], 0.0)
    angles = jnp.sum(positions.astype(F32)[:, :, None] * select[None, :, :], axis=1)
    return jnp.cos(angles), jnp.where((lane % 2 == 0)[None, :], -1.0, 1.0) * jnp.sin(angles)


def norm_stats(x):
    centered = x - jnp.mean(x, axis=-1, keepdims=True)
    inv_std = lax.rsqrt(jnp.mean(centered * centered, axis=-1, keepdims=True) + EPS_NORM)
    return centered * inv_std, inv_std


def ln_kernel(x_ref, m_ref, e_ref, y_ref):
    mod = m_ref[...] + e_ref[0]
    x_norm, _ = norm_stats(x_ref[0].astype(F32))
    y_ref[...] = (x_norm * (1.0 + mod[1:2]) + mod[0:1]).astype(BF16)


def ln_call(b, x_loc, m_block, e_loc):
    _, rows, dim = x_loc.shape
    return pl.pallas_call(
        ln_kernel, name=f"ln{b}", grid=(1,),
        out_shape=jax.ShapeDtypeStruct((rows, dim), BF16),
        in_specs=[pl.BlockSpec((1, rows, dim), lambda i: (b, 0, 0)), pl.BlockSpec((3, dim), lambda i: (0, 0)),
                  pl.BlockSpec((1, 3, dim), lambda i: (b, 0, 0))],
        out_specs=pl.BlockSpec((rows, dim), lambda i: (0, 0)),
        compiler_params=params("arbitrary"), cost_estimate=cost(rows * dim * 12, rows * dim * 4),
    )(x_loc, m_block, e_loc)


def gate_kernel(d_ref, m_ref, e_ref, o_ref):
    gate = m_ref[2:3] + e_ref[0, 2:3]
    o_ref[...] = (d_ref[0].astype(F32) * gate).astype(BF16)


def gate_call(b, dy_loc, m_block, e_loc):
    _, rows, dim = dy_loc.shape
    return pl.pallas_call(
        gate_kernel, name=f"gate{b}", grid=(1,),
        out_shape=jax.ShapeDtypeStruct((rows, dim), BF16),
        in_specs=[pl.BlockSpec((1, rows, dim), lambda i: (b, 0, 0)), pl.BlockSpec((3, dim), lambda i: (0, 0)),
                  pl.BlockSpec((1, 3, dim), lambda i: (b, 0, 0))],
        out_specs=pl.BlockSpec((rows, dim), lambda i: (0, 0)),
        compiler_params=params("arbitrary"), cost_estimate=cost(rows * dim * 4, rows * dim * 4),
    )(dy_loc, m_block, e_loc)


def to_row(acc):
    return jnp.sum(acc.T, axis=0, keepdims=True)


def lanes_of(row):
    return jnp.broadcast_to(row, (HEAD_DIM, row.shape[1])).T


def head_sum(values):
    out = values[:, :HEAD_DIM]
    for h in range(1, values.shape[1] // HEAD_DIM):
        out = out + values[:, h * HEAD_DIM:(h + 1) * HEAD_DIM]
    return out


def qkv_kernel(steps, y_ref, wq_ref, wk_ref, wv_ref, bq_ref, bk_ref, bv_ref, q_ref, k_ref, v_ref, ss_ref, acc):
    step = pl.program_id(0)
    cols = wq_ref.shape[1]

    @pl.when(step == 0)
    def _():
        acc[:, :cols] = jnp.broadcast_to(bq_ref[...], (acc.shape[0], cols))
        acc[:, cols:2 * cols] = jnp.broadcast_to(bk_ref[...], (acc.shape[0], cols))
        acc[:, 2 * cols:] = jnp.broadcast_to(bv_ref[...], (acc.shape[0], cols))

    w_all = jnp.concatenate([wq_ref[...], wk_ref[...], wv_ref[...]], axis=1)
    acc[...] += jnp.dot(y_ref[...], w_all, preferred_element_type=F32)

    @pl.when(step == steps - 1)
    def _():
        q = acc[:, :cols]
        k = acc[:, cols:2 * cols]
        q_ref[...] = q
        k_ref[...] = k
        v_ref[...] = acc[:, 2 * cols:].astype(BF16)
        row_q = to_row(head_sum(q * q))
        row_k = to_row(head_sum(k * k))
        ss_ref[...] = jnp.concatenate([row_q, row_k, jnp.zeros((6, row_q.shape[1]), F32)], axis=0)


def qkv_call(b, y, w_q, w_k, w_v, b_q, b_k, b_v):
    rows, dim = y.shape
    cols = w_q.shape[1]
    bk = min(512, dim)
    steps = dim // bk
    w_spec = pl.BlockSpec((bk, cols), lambda i: (i, 0))
    vec = pl.BlockSpec((1, cols), lambda i: (0, 0))
    full = pl.BlockSpec((rows, cols), lambda i: (0, 0))
    return pl.pallas_call(
        functools.partial(qkv_kernel, steps), name=f"qkv{b}", grid=(steps,),
        out_shape=[jax.ShapeDtypeStruct((rows, cols), F32), jax.ShapeDtypeStruct((rows, cols), F32),
                   jax.ShapeDtypeStruct((rows, cols), BF16), jax.ShapeDtypeStruct((8, rows), F32)],
        in_specs=[pl.BlockSpec((rows, bk), lambda i: (0, i)), w_spec, w_spec, w_spec, vec, vec, vec],
        out_specs=[full, full, full, pl.BlockSpec((8, rows), lambda i: (0, 0))],
        scratch_shapes=[pltpu.VMEM((rows, 3 * cols), F32)],
        compiler_params=params("arbitrary"),
        cost_estimate=cost(6 * rows * dim * cols, 2 * rows * dim + 6 * dim * cols + 10 * rows * cols),
    )(y, w_q, w_k, w_v, b_q[None], b_k[None], b_v[None])


def exchange_kernel(n, x_ref, o_ref, slots, send_sems, recv_sems):
    me = lax.axis_index('tp')
    barrier = pltpu.get_barrier_semaphore()
    for d in range(1, n):
        pl.semaphore_signal(barrier, inc=1, device_id={'tp': lax.rem(me + d, n)}, device_id_type=MESH_ID)
    pl.semaphore_wait(barrier, n - 1)
    copies = []
    for d in range(1, n):
        copy = pltpu.make_async_remote_copy(
            src_ref=x_ref, dst_ref=slots.at[me], send_sem=send_sems.at[d], recv_sem=recv_sems.at[me],
            device_id={'tp': lax.rem(me + d, n)}, device_id_type=MESH_ID)
        copy.start()
        copies.append(copy)
    slots[me] = x_ref[...]
    for copy in copies:
        copy.wait_send()
    for d in range(1, n):
        src = lax.rem(me + d, n)
        pltpu.make_async_remote_copy(
            src_ref=x_ref, dst_ref=slots.at[src], send_sem=send_sems.at[d], recv_sem=recv_sems.at[src],
            device_id={'tp': src}, device_id_type=MESH_ID).wait_recv()
    total = slots[0]
    for d in range(1, n):
        total = total + slots[d]
    o_ref[...] = total


def exchange_call(name, cid, n, x):
    spec = pl.BlockSpec(memory_space=pltpu.VMEM)
    return pl.pallas_call(
        functools.partial(exchange_kernel, n), name=name,
        out_shape=jax.ShapeDtypeStruct(x.shape, x.dtype), in_specs=[spec], out_specs=spec,
        scratch_shapes=[pltpu.VMEM((n,) + x.shape, x.dtype), pltpu.SemaphoreType.DMA((n,)), pltpu.SemaphoreType.DMA((n,))],
        compiler_params=pltpu.CompilerParams(collective_id=cid, has_side_effects=True),
        cost_estimate=cost(4_000_000_000, x.size * 4 * n),
    )(x)


def swap_pairs(x):
    lane = lax.broadcasted_iota(jnp.int32, x.shape, 1)
    return jnp.where(lane % 2 == 0, pltpu.roll(x, HEAD_DIM - 1, 1), pltpu.roll(x, 1, 1))


def attn_kernel(heads, dim, q_ref, k_ref, v_ref, do_ref, gq_ref, gk_ref, cos_ref, sin_ref, ss_ref,
                o_ref, dv_ref, dqs_ref, dks_ref, dgq_ref, dgk_ref, st_ref,
                inv_q, inv_k, acc_q, acc_k, p_all, ds_all, dq_all):
    head = pl.program_id(0)
    rows = q_ref.shape[0]
    blk = min(256, rows)
    scale = HEAD_DIM ** -0.5

    @pl.when(head == 0)
    def _():
        inv = lax.rsqrt(ss_ref[...] / dim + EPS_NORM)
        inv_q[...] = lanes_of(inv[0:1])
        inv_k[...] = lanes_of(inv[1:2])
        acc_q[...] = jnp.zeros_like(acc_q)
        acc_k[...] = jnp.zeros_like(acc_k)

    cos = cos_ref[...]
    sin = sin_ref[...]
    q_gain = q_ref[...] * inv_q[...] * gq_ref[...]
    k_gain = k_ref[...] * inv_k[...] * gk_ref[...]
    q_rot = (q_gain * cos + swap_pairs(q_gain) * sin).astype(BF16)
    k_rot = (k_gain * cos + swap_pairs(k_gain) * sin).astype(BF16)
    v = v_ref[...]
    do = do_ref[...]
    for i in range(rows // blk):
        sl = slice(i * blk, (i + 1) * blk)
        s = lax.dot_general(q_rot[sl], k_rot, NT, preferred_element_type=F32)
        top = jnp.max(s, axis=1, keepdims=True)
        p = jnp.exp2(s * (scale * LOG2E) - top * (scale * LOG2E))
        p = p * (1.0 / jnp.sum(p, axis=1, keepdims=True))
        p_bf = p.astype(BF16)
        p_all[sl] = p_bf
        o = jnp.dot(p_bf, v, preferred_element_type=F32)
        o_ref[sl] = o.astype(BF16)
        dp = lax.dot_general(do[sl], v, NT, preferred_element_type=F32)
        delta = jnp.sum(do[sl].astype(F32) * o, axis=1, keepdims=True)
        ds = (p * (dp - delta)).astype(BF16)
        ds_all[sl] = ds
        dq_all[sl] = jnp.dot(ds, k_rot, preferred_element_type=F32) * scale
    do_t = do.astype(F32).T.astype(BF16)
    q_t = q_rot.astype(F32).T.astype(BF16)
    dv_ref[...] = jnp.dot(do_t, p_all[...], preferred_element_type=F32).T.astype(BF16)
    dk_rot = (jnp.dot(q_t, ds_all[...], preferred_element_type=F32) * scale).T.astype(BF16).astype(F32)
    dq_rot = dq_all[...].astype(BF16).astype(F32)
    dq_hat = dq_rot * cos - swap_pairs(dq_rot) * sin
    dk_hat = dk_rot * cos - swap_pairs(dk_rot) * sin
    q_hat = q_ref[...] * inv_q[...]
    k_hat = k_ref[...] * inv_k[...]
    dgq_ref[...] = jnp.sum(dq_hat * q_hat, axis=0, keepdims=True)
    dgk_ref[...] = jnp.sum(dk_hat * k_hat, axis=0, keepdims=True)
    dq_s = dq_hat * gq_ref[...]
    dk_s = dk_hat * gk_ref[...]
    dqs_ref[...] = dq_s
    dks_ref[...] = dk_s
    acc_q[...] += dq_s * q_hat
    acc_k[...] += dk_s * k_hat

    @pl.when(head == heads - 1)
    def _():
        row_q = to_row(acc_q[...])
        row_k = to_row(acc_k[...])
        st_ref[...] = jnp.concatenate([row_q, row_k, jnp.zeros((6, row_q.shape[1]), F32)], axis=0)


def attn_call(b, dim, q, k, v, d_attn, g_q, g_k, cos_tab, sin_tab, ss):
    rows, cols = q.shape
    heads = cols // HEAD_DIM
    blk = pl.BlockSpec((rows, HEAD_DIM), lambda h: (0, h))
    vec = pl.BlockSpec((1, HEAD_DIM), lambda h: (0, h))
    tab = pl.BlockSpec((rows, HEAD_DIM), lambda h: (0, 0))
    small = pl.BlockSpec((8, rows), lambda h: (0, 0))
    shape = jax.ShapeDtypeStruct
    return pl.pallas_call(
        functools.partial(attn_kernel, heads, dim), name=f"attn{b}", grid=(heads,),
        out_shape=[shape((rows, cols), BF16), shape((rows, cols), BF16), shape((rows, cols), F32), shape((rows, cols), F32),
                   shape((1, cols), F32), shape((1, cols), F32), shape((8, rows), F32)],
        in_specs=[blk, blk, blk, blk, vec, vec, tab, tab, small],
        out_specs=[blk, blk, blk, blk, vec, vec, small],
        scratch_shapes=[pltpu.VMEM((rows, HEAD_DIM), F32)] * 4
        + [pltpu.VMEM((rows, rows), BF16)] * 2 + [pltpu.VMEM((rows, HEAD_DIM), F32)],
        compiler_params=params("arbitrary"),
        cost_estimate=cost(40 * rows * rows * cols, 24 * rows * cols),
    )(q, k, v, d_attn, g_q[None], g_k[None], cos_tab, sin_tab, ss)


def nn_kernel(a_ref, w_ref, o_ref):
    o_ref[...] = jnp.dot(a_ref[...], w_ref[...], preferred_element_type=F32).astype(BF16)


def nn_call(name, a, w):
    rows, depth = a.shape
    width = w.shape[1]
    bn = min(512, width)
    return pl.pallas_call(
        nn_kernel, name=name, grid=(width // bn,),
        out_shape=jax.ShapeDtypeStruct((rows, width), BF16),
        in_specs=[pl.BlockSpec((rows, depth), lambda i: (0, 0)), pl.BlockSpec((depth, bn), lambda i: (0, i))],
        out_specs=pl.BlockSpec((rows, bn), lambda i: (0, i)),
        compiler_params=params("arbitrary"),
        cost_estimate=cost(2 * rows * depth * width, 2 * (rows * depth + depth * width + rows * width)),
    )(a, w)


def nt_kernel(steps, a_ref, w_ref, o_ref, acc):
    step = pl.program_id(0)

    @pl.when(step == 0)
    def _():
        acc[...] = jnp.zeros_like(acc)

    acc[...] += lax.dot_general(a_ref[...], w_ref[...], NT, preferred_element_type=F32)

    @pl.when(step == steps - 1)
    def _():
        o_ref[...] = acc[...].astype(BF16)


def nt_call(name, a, w):
    rows, depth = a.shape
    width = w.shape[0]
    bk = min(512, depth)
    return pl.pallas_call(
        functools.partial(nt_kernel, depth // bk), name=name, grid=(depth // bk,),
        out_shape=jax.ShapeDtypeStruct((rows, width), BF16),
        in_specs=[pl.BlockSpec((rows, bk), lambda i: (0, i)), pl.BlockSpec((width, bk), lambda i: (0, i))],
        out_specs=pl.BlockSpec((rows, width), lambda i: (0, 0)),
        scratch_shapes=[pltpu.VMEM((rows, width), F32)],
        compiler_params=params("arbitrary"),
        cost_estimate=cost(2 * rows * depth * width, 2 * (rows * depth + depth * width + rows * width)),
    )(a, w)


def dy_kernel(dim, dqs_ref, dks_ref, q_ref, k_ref, dv_ref, ss_ref, st_ref, wq_ref, wk_ref, wv_ref, o_ref, g_ref):
    cols = dqs_ref.shape[1]

    @pl.when(pl.program_id(0) == 0)
    def _():
        inv = lax.rsqrt(ss_ref[...] / dim + EPS_NORM)
        for j, (d_ref, x_ref) in enumerate(((dqs_ref, q_ref), (dks_ref, k_ref))):
            inv_l = lanes_of(inv[j:j + 1])
            st_l = lanes_of(st_ref[j:j + 1] / dim)
            for h in range(cols // HEAD_DIM):
                sl = slice(h * HEAD_DIM, (h + 1) * HEAD_DIM)
                grad = inv_l * (d_ref[:, sl] - (x_ref[:, sl] * inv_l) * st_l)
                g_ref[:, j * cols + h * HEAD_DIM:j * cols + (h + 1) * HEAD_DIM] = grad.astype(BF16)
        g_ref[:, 2 * cols:] = dv_ref[...]

    w_all = jnp.concatenate([wq_ref[...], wk_ref[...], wv_ref[...]], axis=1)
    o_ref[...] = lax.dot_general(g_ref[...], w_all, NT, preferred_element_type=F32).astype(BF16)


def dy_call(b, dqs, dks, q, k, dv, ss, st, w_q, w_k, w_v):
    rows, cols = dqs.shape
    dim = w_q.shape[0]
    bn = min(512, dim)
    full = pl.BlockSpec((rows, cols), lambda i: (0, 0))
    small = pl.BlockSpec((8, rows), lambda i: (0, 0))
    w_spec = pl.BlockSpec((bn, cols), lambda i: (i, 0))
    return pl.pallas_call(
        functools.partial(dy_kernel, dim), name=f"dy{b}", grid=(dim // bn,),
        out_shape=[jax.ShapeDtypeStruct((rows, dim), BF16), jax.ShapeDtypeStruct((rows, 3 * cols), BF16)],
        in_specs=[full, full, full, full, full, small, small, w_spec, w_spec, w_spec],
        out_specs=[pl.BlockSpec((rows, bn), lambda i: (0, i)), pl.BlockSpec((rows, 3 * cols), lambda i: (0, 0))],
        compiler_params=params("arbitrary"),
        cost_estimate=cost(6 * rows * dim * cols, 2 * rows * dim + 6 * dim * cols + 20 * rows * cols),
    )(dqs, dks, q, k, dv, ss, st, w_q, w_k, w_v)


def dw_kernel(nb, *refs):
    y_refs, g_refs, outs = refs[:nb], refs[nb:2 * nb], refs[2 * nb:]
    acc = lax.dot_general(y_refs[0][...], g_refs[0][...], TN, preferred_element_type=F32)
    for b in range(1, nb):
        acc = acc + lax.dot_general(y_refs[b][...], g_refs[b][...], TN, preferred_element_type=F32)
    cols = outs[0].shape[1]
    for j, o_ref in enumerate(outs):
        o_ref[...] = acc[:, j * cols:(j + 1) * cols].astype(BF16)


def dw_call(ys, gs):
    nb = len(ys)
    rows, dim = ys[0].shape
    cols = gs[0].shape[1] // 3
    bm = min(512, dim)
    return pl.pallas_call(
        functools.partial(dw_kernel, nb), name="dw", grid=(dim // bm,),
        out_shape=[jax.ShapeDtypeStruct((dim, cols), BF16)] * 3,
        in_specs=[pl.BlockSpec((rows, bm), lambda i: (0, i))] * nb + [pl.BlockSpec((rows, 3 * cols), lambda i: (0, 0))] * nb,
        out_specs=[pl.BlockSpec((bm, cols), lambda i: (i, 0))] * 3,
        compiler_params=params("arbitrary"),
        cost_estimate=cost(6 * nb * rows * dim * cols, 2 * nb * rows * (dim + 3 * cols) + 6 * dim * cols),
    )(*ys, *gs)


def dwo_kernel(nb, *refs):
    o_refs, d_refs, out, turned = refs[:nb], refs[nb:2 * nb], refs[2 * nb], refs[2 * nb + 1]

    @pl.when(pl.program_id(0) == 0)
    def _():
        for b in range(nb):
            turned[b] = o_refs[b][...].T

    acc = jnp.dot(turned[0], d_refs[0][...], preferred_element_type=F32)
    for b in range(1, nb):
        acc = acc + jnp.dot(turned[b], d_refs[b][...], preferred_element_type=F32)
    out[...] = acc.astype(BF16)


def dwo_call(os, ds):
    nb = len(os)
    rows, cols = os[0].shape
    dim = ds[0].shape[1]
    bn = min(512, dim)
    return pl.pallas_call(
        functools.partial(dwo_kernel, nb), name="dwo", grid=(dim // bn,),
        out_shape=jax.ShapeDtypeStruct((cols, dim), BF16),
        in_specs=[pl.BlockSpec((rows, cols), lambda i: (0, 0))] * nb + [pl.BlockSpec((rows, bn), lambda i: (0, i))] * nb,
        out_specs=pl.BlockSpec((cols, bn), lambda i: (0, i)),
        scratch_shapes=[pltpu.VMEM((nb, cols, rows), BF16)],
        compiler_params=params("arbitrary"),
        cost_estimate=cost(2 * nb * rows * dim * cols, 2 * nb * rows * (dim + cols) + 2 * dim * cols),
    )(*os, *ds)


def out_kernel(x_ref, dy_ref, pr_ref, m_ref, e_ref, bo_ref, *rest):
    o_ref, dg_ref = rest[-2:]
    gate = m_ref[2:3] + e_ref[0, 2:3]
    proj = pr_ref[...].astype(F32) + bo_ref[...]
    o_ref[0] = (x_ref[0].astype(F32) + gate * proj).astype(BF16)
    dg_ref[...] = jnp.sum(dy_ref[0].astype(F32) * proj, axis=0, keepdims=True)


def dx_kernel(x_ref, dy_ref, g_ref, m_ref, e_ref, *rest):
    o_ref, dm_ref = rest[-2:]
    scale_one = 1.0 + (m_ref[1:2] + e_ref[0, 1:2])
    x_norm, inv_std = norm_stats(x_ref[0].astype(F32))
    d_y = g_ref[...].astype(F32)
    d_norm = d_y * scale_one
    d_x = dy_ref[0].astype(F32) + inv_std * (
        d_norm - jnp.mean(d_norm, axis=-1, keepdims=True) - x_norm * jnp.mean(d_norm * x_norm, axis=-1, keepdims=True))
    o_ref[0] = d_x.astype(BF16)
    dm_ref[0:1] = jnp.sum(d_y, axis=0, keepdims=True)
    dm_ref[1:2] = jnp.sum(d_y * x_norm, axis=0, keepdims=True)


def token_call(kernel, name, b, n_sums, x_loc, dy_loc, piece, m_block, e_loc, extra, whole):
    _, rows, dim = x_loc.shape
    row = pl.BlockSpec((1, rows, dim), lambda i: (b, 0, 0))
    specs = [row, row, pl.BlockSpec((rows, dim), lambda i: (0, 0)), pl.BlockSpec((3, dim), lambda i: (0, 0)),
             pl.BlockSpec((1, 3, dim), lambda i: (b, 0, 0))] + [pl.BlockSpec((1, dim), lambda i: (0, 0))] * len(extra)
    args = [x_loc, dy_loc, piece, m_block, e_loc, *extra]
    aliases = {}
    if whole is not None:
        aliases = {len(args): 0}
        specs.append(pl.BlockSpec(memory_space=pl.ANY))
        args.append(whole)
    return pl.pallas_call(
        kernel, name=f"{name}{b}", grid=(1,),
        out_shape=[jax.ShapeDtypeStruct(x_loc.shape, BF16), jax.ShapeDtypeStruct((n_sums, dim), F32)],
        in_specs=specs, out_specs=[row, pl.BlockSpec((n_sums, dim), lambda i: (0, 0))],
        input_output_aliases=aliases, compiler_params=params("arbitrary"),
        cost_estimate=cost(rows * dim * 20, rows * dim * 8),
    )(*args)


def solution(mesh):
    tp_size = mesh.shape['tp']

    def device_step(x_loc, e_loc, m_block, w_q, b_q, w_k, b_k, w_v, b_v, w_o, b_o, g_q, g_k, pos_part, dy_loc):
        nb, _, dim = x_loc.shape
        batch = range(nb)

        y_loc = [ln_call(b, x_loc, m_block, e_loc) for b in batch]
        dp_loc = [gate_call(b, dy_loc, m_block, e_loc) for b in batch]
        y_all = [lax.all_gather(y_loc[b], 'tp', axis=0, tiled=True) for b in batch]
        dp_all = [lax.all_gather(dp_loc[b], 'tp', axis=0, tiled=True) for b in batch]
        cos_tab, sin_tab = rope_tables(pos_part)

        qkv = []
        for b in batch:
            q, k, v, ss = qkv_call(b, y_all[b], w_q, w_k, w_v, b_q, b_k, b_v)
            qkv.append((q, k, v, exchange_call(f"sumsq{b}", b, tp_size, ss)))

        x_out, d_x = None, None
        o_all, grads, d_gq, d_gk, gate_sums, mod_sums, parts = [], [], [], [], [], [], []
        for b in batch:
            q, k, v, ss = qkv[b]
            d_attn = nt_call(f"dattn{b}", dp_all[b], w_o)
            o, dv, dqs, dks, dgq, dgk, st = attn_call(b, dim, q, k, v, d_attn, g_q, g_k, cos_tab, sin_tab, ss)
            o_all.append(o)
            d_gq.append(dgq)
            d_gk.append(dgk)
            part = nn_call(f"proj{b}", o, w_o)
            st, part = lax.optimization_barrier((st, part))
            st = exchange_call(f"stat{b}", nb + b, tp_size, st)
            dy_part, grad = dy_call(b, dqs, dks, q, k, dv, ss, st, w_q, w_k, w_v)
            grads.append(grad)
            parts.append((part, dy_part))
        d_wq, d_wk, d_wv = dw_call(y_all, grads)
        d_wo = dwo_call(o_all, dp_all)
        for b in batch:
            proj = lax.psum_scatter(parts[b][0], 'tp', scatter_dimension=0, tiled=True)
            if b:
                proj, mod_sums[b - 1] = lax.optimization_barrier((proj, mod_sums[b - 1]))
            x_out, dg = token_call(out_kernel, "xout", b, 1, x_loc, dy_loc, proj, m_block, e_loc, [b_o[None]], x_out)
            gate_sums.append(dg)
            d_y = lax.psum_scatter(parts[b][1], 'tp', scatter_dimension=0, tiled=True)
            d_x, dm = token_call(dx_kernel, "dx", b, 2, x_loc, dy_loc, d_y, m_block, e_loc, [], d_x)
            flat = jnp.concatenate([dm, gate_sums[b]], axis=0)
            mod_sums.append(exchange_call(f"dmod{b}", 2 * nb + b, tp_size, flat.reshape(8, -1)).reshape(3, dim))
        d_e = jnp.stack(mod_sums)
        return (x_out, d_x, d_e, jnp.sum(d_e, axis=0), d_wq, d_wk, d_wv, d_wo,
                sum(d_gq)[0], sum(d_gk)[0])

    in_specs = (P('dp', 'tp', None), P('dp', None, None), P(None, None), P(None, 'tp'), P('tp'), P(None, 'tp'), P('tp'),
                P(None, 'tp'), P('tp'), P('tp', None), P(None), P('tp'), P('tp'), P('dp', None), P('dp', 'tp', None))
    out_specs = (P('dp', 'tp', None), P('dp', 'tp', None), P('dp', None, None), P('dp', None), P('dp', 'tp'), P('dp', 'tp'),
                 P('dp', 'tp'), P(('dp', 'tp'), None), P(('dp', 'tp')), P(('dp', 'tp')))
    return jax.shard_map(device_step, mesh=mesh, in_specs=in_specs, out_specs=out_specs, check_vma=False)
```

```python
import functools

import jax
import jax.numpy as jnp
from jax import lax
from jax.experimental import pallas as pl
from jax.experimental.pallas import tpu as pltpu
from jax.sharding import PartitionSpec as P

HEAD_DIM = 128
EPS_NORM = 1e-6
ROPE_BASE = 10000.0
LOG2E = 1.4426950408889634
VMEM_LIMIT = 60 * 1024 * 1024
F32 = jnp.float32
BF16 = jnp.bfloat16
MESH_ID = pl.DeviceIdType.MESH
NT = (((1,), (1,)), ((), ()))
TN = (((0,), (0,)), ((), ()))


def params(*semantics, **kw):
    return pltpu.CompilerParams(dimension_semantics=semantics or None, vmem_limit_bytes=VMEM_LIMIT, **kw)


def cost(flops, nbytes):
    return pl.CostEstimate(flops=int(flops), bytes_accessed=int(nbytes), transcendentals=0)


def rope_tables(positions):
    half_dim = HEAD_DIM // 2
    side_len = HEAD_DIM // 6
    first_len = half_dim - 2 * side_len
    lane = jnp.arange(HEAD_DIM)
    pair_idx = lane // 2
    section = (pair_idx >= first_len).astype(jnp.int32) + (pair_idx >= first_len + side_len).astype(jnp.int32)
    offset = jnp.where(section == 0, 0, jnp.where(section == 1, first_len, first_len + side_len))
    sec_width = jnp.where(section == 0, first_len, side_len)
    freq_vals = ROPE_BASE ** (-(pair_idx - offset).astype(F32) / sec_width.astype(F32))
    select = jnp.where(section[None, :] == jnp.arange(3)[:, None], freq_vals[None, :], 0.0)
    angles = jnp.sum(positions.astype(F32)[:, :, None] * select[None, :, :], axis=1)
    return jnp.cos(angles), jnp.where((lane % 2 == 0)[None, :], -1.0, 1.0) * jnp.sin(angles)


def norm_stats(x):
    centered = x - jnp.mean(x, axis=-1, keepdims=True)
    inv_std = lax.rsqrt(jnp.mean(centered * centered, axis=-1, keepdims=True) + EPS_NORM)
    return centered * inv_std, inv_std


def to_row(acc):
    return jnp.sum(acc.T, axis=0, keepdims=True)


def lanes_of(row):
    return jnp.broadcast_to(row, (HEAD_DIM, row.shape[1])).T


def head_sum(values):
    out = values[:, :HEAD_DIM]
    for h in range(1, values.shape[1] // HEAD_DIM):
        out = out + values[:, h * HEAD_DIM:(h + 1) * HEAD_DIM]
    return out


class Place:
    def __init__(self, n):
        self.n = n
        self.me = lax.axis_index('tp')
        self.right = lax.rem(self.me + 2, n)
        self.left = lax.rem(self.me + n - 2, n)
        self.far = lax.rem(self.me + n // 2, n)
        self.chip = self.me // 2

    def partner(self, dev):
        return dev + 1 - 2 * lax.rem(dev, 2)

    def barrier(self, devices):
        sem = pltpu.get_barrier_semaphore()
        for dev in devices:
            pl.semaphore_signal(sem, inc=1, device_id={'tp': dev}, device_id_type=MESH_ID)
        pl.semaphore_wait(sem, len(devices))

    def everyone(self):
        return [lax.rem(self.me + d, self.n) for d in range(1, self.n)]

    def near(self):
        return [self.right, self.left, self.partner(self.me)]


class Gather:
    def __init__(self, place, full, rows, send, recv):
        self.at, self.full, self.rows, self.send, self.recv = place, full, rows, send, recv

    def part(self, b, dev, off, count):
        return self.full.at[b, pl.ds(pl.multiple_of(dev * self.rows + off, 16), count)]

    def copy(self, b, dev, off, count, s_idx, r_idx, target):
        ref = self.part(b, dev, off, count)
        return pltpu.make_async_remote_copy(src_ref=ref, dst_ref=ref, send_sem=self.send.at[b, s_idx], recv_sem=self.recv.at[b, r_idx],
                                            device_id={'tp': target}, device_id_type=MESH_ID)

    def start_own(self, b):
        p = self.at
        self.copy(b, p.me, 0, self.rows, 0, 0, p.right).start()
        self.copy(b, p.me, 0, self.rows, 1, 1, p.left).start()
        self.copy(b, p.me, 0, self.rows, 2, 4, p.partner(p.me)).start()

    def take_own(self, b):
        p = self.at
        self.copy(b, p.partner(p.me), 0, self.rows, 2, 4, p.me).wait_recv()

    def take_left(self, b):
        p, half = self.at, self.rows // 2
        self.copy(b, p.left, 0, self.rows, 0, 0, p.me).wait_recv()
        self.copy(b, p.left, 0, half, 3, 2, p.right).start()
        self.copy(b, p.left, 0, self.rows, 5, 5, p.partner(p.me)).start()
        self.copy(b, p.partner(p.left), 0, self.rows, 5, 5, p.me).wait_recv()

    def take_right(self, b):
        p, half = self.at, self.rows // 2
        self.copy(b, p.right, 0, self.rows, 1, 1, p.me).wait_recv()
        self.copy(b, p.right, half, half, 4, 3, p.left).start()
        self.copy(b, p.right, 0, self.rows, 6, 6, p.partner(p.me)).start()
        self.copy(b, p.partner(p.right), 0, self.rows, 6, 6, p.me).wait_recv()

    def take_far(self, b):
        p, half = self.at, self.rows // 2
        self.copy(b, p.far, 0, half, 3, 2, p.me).wait_recv()
        self.copy(b, p.far, 0, half, 7, 7, p.partner(p.me)).start()
        self.copy(b, p.far, half, half, 4, 3, p.me).wait_recv()
        self.copy(b, p.far, half, half, 8, 8, p.partner(p.me)).start()
        self.copy(b, p.partner(p.far), 0, half, 7, 7, p.me).wait_recv()
        self.copy(b, p.partner(p.far), half, half, 8, 8, p.me).wait_recv()

    def finish(self, b):
        p, half = self.at, self.rows // 2
        for s_idx, count in ((0, self.rows), (1, self.rows), (2, self.rows), (3, half), (4, half), (5, self.rows), (6, self.rows), (7, half), (8, half)):
            self.copy(b, p.me, 0, count, s_idx, s_idx, p.me).wait_send()

    def take_item(self, i, nb):
        j = i - nb
        b = jnp.where(i < nb, i, jnp.where(i < 3 * nb, j // 2, i - 3 * nb))
        is_left = (i >= nb) & (i < 3 * nb) & (lax.rem(j + 2 * nb, 2) == 0)
        is_right = (i >= nb) & (i < 3 * nb) & (lax.rem(j + 2 * nb, 2) == 1)
        pl.when(i < nb)(lambda: self.take_own(b))
        pl.when(is_left)(lambda: self.take_left(b))
        pl.when(is_right)(lambda: self.take_right(b))
        pl.when(i >= 3 * nb)(lambda: self.take_far(b))
        chips = self.at.n // 2
        off = jnp.where(i < nb, 0, jnp.where(is_left, chips - 1, jnp.where(is_right, 1, chips // 2)))
        chip = lax.rem(self.at.chip + off, chips)
        return b, pl.multiple_of(chip * (2 * self.rows), 32)


GATHER_SEMS = 9


def chunks_of(width, step):
    return [(c, min(c + step, width)) for c in range(0, width, step)]


def exchange(place, x_ref, slots, send_sems, recv_sems):
    n, me = place.n, place.me
    for d, dev in enumerate(place.everyone()):
        pltpu.make_async_remote_copy(src_ref=x_ref, dst_ref=slots.at[me], send_sem=send_sems.at[d], recv_sem=recv_sems.at[me],
                                     device_id={'tp': dev}, device_id_type=MESH_ID).start()
    slots[me] = x_ref[...]
    for d, dev in enumerate(place.everyone()):
        copy = pltpu.make_async_remote_copy(src_ref=x_ref, dst_ref=slots.at[dev], send_sem=send_sems.at[d], recv_sem=recv_sems.at[dev],
                                            device_id={'tp': dev}, device_id_type=MESH_ID)
        copy.wait_send()
        copy.wait_recv()
    total = slots[0]
    for d in range(1, n):
        total = total + slots[d]
    return total


def gather_qkv_kernel(n, x_ref, dy_ref, m_ref, e_ref, wq_ref, wk_ref, wv_ref, bias_ref,
                      y_full, d_full, q_out, k_out, v_out, ss_ref,
                      w_all, xin, stage, xbuf, zst, vst, sq, ss_row, slots,
                      w_sem, in_sem, st_sem, ld_sem, out_sem, g_send, g_recv, e_send, e_recv):
    nb, rows, dim = x_ref.shape
    cols = wq_ref.shape[1]
    place = Place(n)
    gather = Gather(place, y_full, rows, g_send, g_recv)
    w_copies = [pltpu.make_async_copy(w, w_all.at[:, pl.ds(j * cols, cols)], w_sem.at[j]) for j, w in enumerate((wq_ref, wk_ref, wv_ref))]
    load_x = pltpu.make_async_copy(x_ref, xin, in_sem)
    load_x.start()
    for c in w_copies:
        c.start()
    group = 16

    def mine(full, b):
        return full.at[b, pl.ds(pl.multiple_of(place.me * rows, 16), rows)]

    load_x.wait()
    place.barrier(place.everyone())

    def ln_step(b, _):
        shift = m_ref[0:1] + e_ref[b, 0:1]
        scale_one = 1.0 + (m_ref[1:2] + e_ref[b, 1:2])

        def ln_rows(r, _):
            sl = pl.ds(pl.multiple_of(r * group, group), group)
            x_norm, _ = norm_stats(xin[b, sl].astype(F32))
            stage[b, sl] = (x_norm * scale_one + shift).astype(BF16)
            return 0

        lax.fori_loop(0, rows // group, ln_rows, 0)
        out = pltpu.make_async_copy(stage.at[b], mine(y_full, b), st_sem)
        out.start()
        out.wait()
        gather.start_own(b)
        return 0

    lax.fori_loop(0, nb, ln_step, 0)
    load_dy = pltpu.make_async_copy(dy_ref, xin, in_sem)
    load_dy.start()

    def gate_step(b, _):
        gate = m_ref[2:3] + e_ref[b, 2:3]

        def gate_rows(r, _):
            sl = pl.ds(pl.multiple_of(r * group, group), group)
            stage[b, sl] = (xin[b, sl].astype(F32) * gate).astype(BF16)
            return 0

        lax.fori_loop(0, rows // group, gate_rows, 0)
        out = pltpu.make_async_copy(stage.at[b], mine(d_full, b), st_sem)
        out.start()
        out.wait()
        return 0

    for c in w_copies:
        c.wait()

    def outputs(b, row0, slot):
        dst = pl.ds(row0, 2 * rows)
        return [pltpu.make_async_copy(zst.at[slot, :, pl.ds(0, cols)], q_out.at[b, dst], out_sem.at[slot, 0]),
                pltpu.make_async_copy(zst.at[slot, :, pl.ds(cols, cols)], k_out.at[b, dst], out_sem.at[slot, 1]),
                pltpu.make_async_copy(vst.at[slot], v_out.at[b, dst], out_sem.at[slot, 2])]

    def item(i, _):
        b, row0 = gather.take_item(i, nb)
        slot = lax.rem(i, 2)
        load = pltpu.make_async_copy(y_full.at[b, pl.ds(row0, 2 * rows)], xbuf, ld_sem)
        load.start()

        @pl.when(i == nb)
        def _():
            load_dy.wait()
            lax.fori_loop(0, nb, gate_step, 0)

        @pl.when(i >= 2)
        def _():
            for c in outputs(0, 0, slot):
                c.wait()

        load.wait()
        for lo, hi in chunks_of(3 * cols, 512):
            zst[slot, :, lo:hi] = jnp.dot(xbuf[...], w_all[:, lo:hi], preferred_element_type=F32) + bias_ref[:, lo:hi]
        vst[slot] = zst[slot, :, 2 * cols:].astype(BF16)
        q = zst[slot, :, :cols]
        k = zst[slot, :, cols:2 * cols]
        sq[2 * b, pl.ds(row0, 2 * rows)] = head_sum(q * q)
        sq[2 * b + 1, pl.ds(row0, 2 * rows)] = head_sum(k * k)
        for c in outputs(b, row0, slot):
            c.start()
        return 0

    lax.fori_loop(0, 4 * nb, item, 0)
    ss_row[...] = jnp.zeros_like(ss_row)
    for j in range(2 * nb):
        ss_row[j:j + 1] = to_row(sq[j])
    for slot in range(2):
        for c in outputs(0, 0, slot):
            c.wait()
    for b in range(nb):
        gather.finish(b)
    ss_ref[...] = exchange(place, ss_row, slots, e_send, e_recv)


def gather_qkv_call(n, x_loc, dy_loc, m_block, e_loc, w_q, w_k, w_v, b_q, b_k, b_v):
    nb, rows, dim = x_loc.shape
    cols = w_q.shape[1]
    tokens = rows * n
    shape = jax.ShapeDtypeStruct
    any_spec = pl.BlockSpec(memory_space=pl.ANY)
    vmem = pl.BlockSpec(memory_space=pltpu.VMEM)
    dma = pltpu.SemaphoreType.DMA
    stat_rows = -(-2 * nb // 8) * 8
    return pl.pallas_call(
        functools.partial(gather_qkv_kernel, n), name="gather_qkv",
        out_shape=[shape((nb, tokens, dim), BF16), shape((nb, tokens, dim), BF16), shape((nb, tokens, cols), F32),
                   shape((nb, tokens, cols), F32), shape((nb, tokens, cols), BF16), shape((stat_rows, tokens), F32)],
        in_specs=[any_spec, any_spec, vmem, vmem, any_spec, any_spec, any_spec, vmem],
        out_specs=[any_spec] * 5 + [vmem],
        scratch_shapes=[
            pltpu.VMEM((dim, 3 * cols), BF16), pltpu.VMEM((nb, rows, dim), BF16), pltpu.VMEM((nb, rows, dim), BF16),
            pltpu.VMEM((2 * rows, dim), BF16), pltpu.VMEM((2, 2 * rows, 3 * cols), F32), pltpu.VMEM((2, 2 * rows, cols), BF16),
            pltpu.VMEM((2 * nb, tokens, HEAD_DIM), F32), pltpu.VMEM((stat_rows, tokens), F32), pltpu.VMEM((n, stat_rows, tokens), F32),
            dma((3,)), dma, dma, dma, dma((2, 3)), dma((nb, GATHER_SEMS)), dma((nb, GATHER_SEMS)), dma((n,)), dma((n,))],
        compiler_params=params(collective_id=0, has_side_effects=True),
        cost_estimate=cost(6 * nb * tokens * dim * cols, 6 * dim * cols + 14 * nb * tokens * cols),
    )(x_loc, dy_loc, m_block, e_loc, w_q, w_k, w_v, jnp.concatenate([b_q, b_k, b_v])[None])


def exchange_kernel(n, x_ref, o_ref, slots, send_sems, recv_sems):
    place = Place(n)
    place.barrier(place.everyone())
    o_ref[...] = exchange(place, x_ref, slots, send_sems, recv_sems)


def exchange_call(name, cid, n, x):
    spec = pl.BlockSpec(memory_space=pltpu.VMEM)
    return pl.pallas_call(
        functools.partial(exchange_kernel, n), name=name,
        out_shape=jax.ShapeDtypeStruct(x.shape, x.dtype), in_specs=[spec], out_specs=spec,
        scratch_shapes=[pltpu.VMEM((n,) + x.shape, x.dtype), pltpu.SemaphoreType.DMA((n,)), pltpu.SemaphoreType.DMA((n,))],
        compiler_params=pltpu.CompilerParams(collective_id=cid, has_side_effects=True),
        cost_estimate=cost(4_000_000_000, x.size * 4 * n),
    )(x)


def swap_pairs(x):
    lane = lax.broadcasted_iota(jnp.int32, x.shape, 1)
    return jnp.where(lane % 2 == 0, pltpu.roll(x, HEAD_DIM - 1, 1), pltpu.roll(x, 1, 1))


def rotate(x, cos, sin):
    return x * cos + swap_pairs(x) * sin


def softmax_block(s):
    c = HEAD_DIM ** -0.5 * LOG2E
    top = jnp.max(s, axis=1, keepdims=True)
    p = jnp.exp2(s * c - top * c)
    return p * (1.0 / jnp.sum(p, axis=1, keepdims=True))


def gather_attn_kernel(n, nb, heads, dim, q_ref, k_ref, v_ref, gq_ref, gk_ref, cos_ref, sin_ref, ss_ref, wo_ref, d_in,
                       d_full, o_out, da_out, dwo_out,
                       inv_q, inv_k, o_all, wo, xbuf, ast, turned, dbuf, acc, wst,
                       w_sem, ld_sem, out_sem, c_sem, o_sem, g_send, g_recv):
    step = pl.program_id(0)
    tokens = q_ref.shape[1]
    rows = tokens // n
    cols = heads * HEAD_DIM
    blk = min(256, tokens)
    place = Place(n)
    gather = Gather(place, d_full, rows, g_send, g_recv)
    load_w = pltpu.make_async_copy(wo_ref, wo, w_sem)

    @pl.when(step == 0)
    def _():
        load_w.start()
        place.barrier(place.near())

        def own(b, _):
            gather.start_own(b)
            return 0

        lax.fori_loop(0, nb, own, 0)

    @pl.when(step < nb * heads)
    def _():
        b = step // heads
        h = lax.rem(step, heads)

        @pl.when(h == 0)
        def _():
            inv_q[...] = lanes_of(lax.rsqrt(ss_ref[pl.ds(2 * b, 1)] / dim + EPS_NORM))
            inv_k[...] = lanes_of(lax.rsqrt(ss_ref[pl.ds(2 * b + 1, 1)] / dim + EPS_NORM))

        cos, sin = cos_ref[...], sin_ref[...]
        q_rot = rotate(q_ref[0] * inv_q[...] * gq_ref[...], cos, sin).astype(BF16)
        k_rot = rotate(k_ref[0] * inv_k[...] * gk_ref[...], cos, sin).astype(BF16)
        v = v_ref[0]
        lanes = pl.ds(pl.multiple_of(h * HEAD_DIM, HEAD_DIM), HEAD_DIM)
        for i in range(tokens // blk):
            s = lax.dot_general(q_rot[i * blk:(i + 1) * blk], k_rot, NT, preferred_element_type=F32)
            p = softmax_block(s).astype(BF16)
            o_all[b, i * blk:(i + 1) * blk, lanes] = jnp.dot(p, v, preferred_element_type=F32).astype(BF16)

    @pl.when(step == nb * heads)
    def _():
        o_copy = pltpu.make_async_copy(o_all, o_out, o_sem)
        o_copy.start()
        load_w.wait()
        bn = min(512, dim)
        n_chunks = dim // bn

        def outputs(b, row0, slot):
            return pltpu.make_async_copy(ast.at[slot], da_out.at[b, pl.ds(row0, 2 * rows)], out_sem.at[slot])

        def chunk(b, c):
            slot = lax.rem(c, 2)
            return pltpu.make_async_copy(d_full.at[b, :, pl.ds(pl.multiple_of(c * bn, bn), bn)], dbuf.at[slot], c_sem.at[slot])

        def item(i, _):
            b, row0 = gather.take_item(i, nb)
            slot = lax.rem(i, 2)
            load = pltpu.make_async_copy(d_full.at[b, pl.ds(row0, 2 * rows)], xbuf, ld_sem)
            load.start()

            @pl.when(i >= 2)
            def _():
                outputs(0, 0, slot).wait()

            load.wait()
            ast[slot] = lax.dot_general(xbuf[...], wo[...], NT, preferred_element_type=F32).astype(BF16)
            outputs(b, row0, slot).start()

            @pl.when(i >= 3 * nb)
            def _():
                chunk(b, 0).start()
                turned[...] = o_all[b].T

                def d_wo(c, _):
                    @pl.when(c + 1 < n_chunks)
                    def _():
                        chunk(b, c + 1).start()

                    chunk(b, c).wait()
                    sl = pl.ds(pl.multiple_of(c * bn, bn), bn)
                    part = jnp.dot(turned[...], dbuf[lax.rem(c, 2)], preferred_element_type=F32)

                    @pl.when(b == 0)
                    def _():
                        acc[:, sl] = part

                    @pl.when(b > 0)
                    def _():
                        acc[:, sl] += part

                    return 0

                lax.fori_loop(0, n_chunks, d_wo, 0)

            return 0

        lax.fori_loop(0, 4 * nb, item, 0)

        def flush(c, _):
            sl = pl.ds(pl.multiple_of(c * bn, bn), bn)
            slot = lax.rem(c, 2)

            @pl.when(c >= 2)
            def _():
                pltpu.make_async_copy(wst.at[slot], dwo_out.at[:, sl], c_sem.at[slot]).wait()

            wst[slot] = acc[:, sl].astype(BF16)
            pltpu.make_async_copy(wst.at[slot], dwo_out.at[:, sl], c_sem.at[slot]).start()
            return 0

        lax.fori_loop(0, n_chunks, flush, 0)
        for slot in range(min(2, n_chunks)):
            pltpu.make_async_copy(wst.at[slot], dwo_out.at[:, pl.ds(0, bn)], c_sem.at[slot]).wait()
        for slot in range(2):
            outputs(0, 0, slot).wait()
        o_copy.wait()
        for b in range(nb):
            gather.finish(b)


def gather_attn_call(n, q, k, v, g_q, g_k, cos_tab, sin_tab, ss, w_o, d_full):
    nb, tokens, cols = q.shape
    dim = w_o.shape[1]
    heads = cols // HEAD_DIM
    rows = tokens // n
    last = nb * heads - 1
    bn = min(512, dim)
    shape = jax.ShapeDtypeStruct
    dma = pltpu.SemaphoreType.DMA
    any_spec = pl.BlockSpec(memory_space=pl.ANY)

    def head_of(i):
        i = jnp.minimum(i, last)
        return i // heads, i % heads

    blk = pl.BlockSpec((1, tokens, HEAD_DIM), lambda i: (head_of(i)[0], 0, head_of(i)[1]))
    vec = pl.BlockSpec((1, HEAD_DIM), lambda i: (0, head_of(i)[1]))
    tab = pl.BlockSpec((tokens, HEAD_DIM), lambda i: (0, 0))
    return pl.pallas_call(
        functools.partial(gather_attn_kernel, n, nb, heads, dim), name="gather_attn", grid=(nb * heads + 1,),
        out_shape=[shape(d_full.shape, BF16), shape((nb, tokens, cols), BF16), shape((nb, tokens, cols), BF16), shape((cols, dim), BF16)],
        in_specs=[blk, blk, blk, vec, vec, tab, tab, pl.BlockSpec(ss.shape, lambda i: (0, 0)), any_spec, any_spec],
        out_specs=[any_spec] * 4,
        scratch_shapes=[
            pltpu.VMEM((tokens, HEAD_DIM), F32), pltpu.VMEM((tokens, HEAD_DIM), F32), pltpu.VMEM((nb, tokens, cols), BF16),
            pltpu.VMEM((cols, dim), BF16), pltpu.VMEM((2 * rows, dim), BF16), pltpu.VMEM((2, 2 * rows, cols), BF16),
            pltpu.VMEM((cols, tokens), BF16), pltpu.VMEM((2, tokens, bn), BF16), pltpu.VMEM((cols, dim), F32),
            pltpu.VMEM((2, cols, bn), BF16),
            dma, dma, dma((2,)), dma((2,)), dma, dma((nb, GATHER_SEMS)), dma((nb, GATHER_SEMS))],
        input_output_aliases={9: 0},
        compiler_params=params("arbitrary", collective_id=1, has_side_effects=True),
        cost_estimate=cost(4 * nb * tokens * dim * cols + 4 * nb * tokens * tokens * cols, 8 * nb * tokens * dim),
    )(q, k, v, g_q[None], g_k[None], cos_tab, sin_tab, ss, w_o, d_full)


def attn_bwd_kernel(heads, dim, q_ref, k_ref, v_ref, do_ref, gq_ref, gk_ref, cos_ref, sin_ref, ss_ref,
                    dv_ref, dqs_ref, dks_ref, dgq_ref, dgk_ref, st_ref,
                    inv_q, inv_k, acc_q, acc_k, p_all, ds_all, dq_all):
    b, head = pl.program_id(0), pl.program_id(1)
    tokens = q_ref.shape[1]
    blk = min(256, tokens)
    scale = HEAD_DIM ** -0.5

    @pl.when((head == 0) & (b == 0))
    def _():
        st_ref[...] = jnp.zeros_like(st_ref)

    @pl.when(head == 0)
    def _():
        inv_q[...] = lanes_of(lax.rsqrt(ss_ref[pl.ds(2 * b, 1)] / dim + EPS_NORM))
        inv_k[...] = lanes_of(lax.rsqrt(ss_ref[pl.ds(2 * b + 1, 1)] / dim + EPS_NORM))
        acc_q[...] = jnp.zeros_like(acc_q)
        acc_k[...] = jnp.zeros_like(acc_k)

    cos, sin = cos_ref[...], sin_ref[...]
    q_rot = rotate(q_ref[0] * inv_q[...] * gq_ref[...], cos, sin).astype(BF16)
    k_rot = rotate(k_ref[0] * inv_k[...] * gk_ref[...], cos, sin).astype(BF16)
    v = v_ref[0]
    do = do_ref[0]
    for i in range(tokens // blk):
        sl = slice(i * blk, (i + 1) * blk)
        p = softmax_block(lax.dot_general(q_rot[sl], k_rot, NT, preferred_element_type=F32))
        p_all[sl] = p.astype(BF16)
        dp = lax.dot_general(do[sl], v, NT, preferred_element_type=F32)
        delta = jnp.sum(dp * p, axis=1, keepdims=True)
        ds = (p * (dp - delta)).astype(BF16)
        ds_all[sl] = ds
        dq_all[sl] = jnp.dot(ds, k_rot, preferred_element_type=F32) * scale
    do_t = do.astype(F32).T.astype(BF16)
    q_t = q_rot.astype(F32).T.astype(BF16)
    dv_ref[0] = jnp.dot(do_t, p_all[...], preferred_element_type=F32).T.astype(BF16)
    dk_rot = (jnp.dot(q_t, ds_all[...], preferred_element_type=F32) * scale).T.astype(BF16).astype(F32)
    dq_rot = dq_all[...].astype(BF16).astype(F32)
    dq_hat = rotate(dq_rot, cos, -sin)
    dk_hat = rotate(dk_rot, cos, -sin)
    q_hat = q_ref[0] * inv_q[...]
    k_hat = k_ref[0] * inv_k[...]
    dgq_ref[0] = jnp.sum(dq_hat * q_hat, axis=0, keepdims=True)
    dgk_ref[0] = jnp.sum(dk_hat * k_hat, axis=0, keepdims=True)
    dq_s = dq_hat * gq_ref[...]
    dk_s = dk_hat * gk_ref[...]
    dqs_ref[0] = dq_s
    dks_ref[0] = dk_s
    acc_q[...] += dq_s * q_hat
    acc_k[...] += dk_s * k_hat

    @pl.when(head == heads - 1)
    def _():
        st_ref[pl.ds(2 * b, 1)] = to_row(acc_q[...])
        st_ref[pl.ds(2 * b + 1, 1)] = to_row(acc_k[...])


def attn_bwd_call(dim, q, k, v, d_attn, g_q, g_k, cos_tab, sin_tab, ss):
    nb, tokens, cols = q.shape
    heads = cols // HEAD_DIM
    blk = pl.BlockSpec((1, tokens, HEAD_DIM), lambda b, h: (b, 0, h))
    vec = pl.BlockSpec((1, HEAD_DIM), lambda b, h: (0, h))
    out_vec = pl.BlockSpec((1, 1, HEAD_DIM), lambda b, h: (b, 0, h))
    tab = pl.BlockSpec((tokens, HEAD_DIM), lambda b, h: (0, 0))
    small = pl.BlockSpec(ss.shape, lambda b, h: (0, 0))
    shape = jax.ShapeDtypeStruct
    whole = (nb, tokens, cols)
    return pl.pallas_call(
        functools.partial(attn_bwd_kernel, heads, dim), name="attn_bwd", grid=(nb, heads),
        out_shape=[shape(whole, BF16), shape(whole, F32), shape(whole, F32),
                   shape((nb, 1, cols), F32), shape((nb, 1, cols), F32), shape(ss.shape, F32)],
        in_specs=[blk, blk, blk, blk, vec, vec, tab, tab, small],
        out_specs=[blk, blk, blk, out_vec, out_vec, small],
        scratch_shapes=[pltpu.VMEM((tokens, HEAD_DIM), F32)] * 4
        + [pltpu.VMEM((tokens, tokens), BF16)] * 2 + [pltpu.VMEM((tokens, HEAD_DIM), F32)],
        compiler_params=params("arbitrary", "arbitrary"),
        cost_estimate=cost(36 * nb * tokens * tokens * cols, 24 * nb * tokens * cols),
    )(q, k, v, d_attn, g_q[None], g_k[None], cos_tab, sin_tab, ss)


def nn_kernel(a_ref, w_ref, o_ref):
    o_ref[...] = jnp.dot(a_ref[...], w_ref[...], preferred_element_type=F32).astype(BF16)


def nn_call(name, a, w):
    rows, depth = a.shape
    width = w.shape[1]
    bn = min(512, width)
    return pl.pallas_call(
        nn_kernel, name=name, grid=(width // bn,),
        out_shape=jax.ShapeDtypeStruct((rows, width), BF16),
        in_specs=[pl.BlockSpec((rows, depth), lambda i: (0, 0)), pl.BlockSpec((depth, bn), lambda i: (0, i))],
        out_specs=pl.BlockSpec((rows, bn), lambda i: (0, i)),
        compiler_params=params("arbitrary"),
        cost_estimate=cost(2 * rows * depth * width, 2 * (rows * depth + depth * width + rows * width)),
    )(a, w)


def dy_kernel(dim, dqs_ref, dks_ref, q_ref, k_ref, dv_ref, ss_ref, st_ref, wq_ref, wk_ref, wv_ref, o_ref, g_ref):
    b = pl.program_id(0)
    cols = dqs_ref.shape[2]

    @pl.when(pl.program_id(1) == 0)
    def _():
        for j, (d_ref, x_ref) in enumerate(((dqs_ref, q_ref), (dks_ref, k_ref))):
            inv_l = lanes_of(lax.rsqrt(ss_ref[pl.ds(2 * b + j, 1)] / dim + EPS_NORM))
            st_l = lanes_of(st_ref[pl.ds(2 * b + j, 1)] / dim)
            for h in range(cols // HEAD_DIM):
                sl = slice(h * HEAD_DIM, (h + 1) * HEAD_DIM)
                grad = inv_l * (d_ref[0, :, sl] - (x_ref[0, :, sl] * inv_l) * st_l)
                g_ref[0, :, j * cols + h * HEAD_DIM:j * cols + (h + 1) * HEAD_DIM] = grad.astype(BF16)
        g_ref[0, :, 2 * cols:] = dv_ref[0]

    w_all = jnp.concatenate([wq_ref[...], wk_ref[...], wv_ref[...]], axis=1)
    o_ref[0] = lax.dot_general(g_ref[0], w_all, NT, preferred_element_type=F32).astype(BF16)


def dy_call(dqs, dks, q, k, dv, ss, st, w_q, w_k, w_v):
    nb, rows, cols = dqs.shape
    dim = w_q.shape[0]
    bn = min(512, dim)
    full = pl.BlockSpec((1, rows, cols), lambda b, i: (b, 0, 0))
    small = pl.BlockSpec(ss.shape, lambda b, i: (0, 0))
    w_spec = pl.BlockSpec((bn, cols), lambda b, i: (i, 0))
    return pl.pallas_call(
        functools.partial(dy_kernel, dim), name="dy", grid=(nb, dim // bn),
        out_shape=[jax.ShapeDtypeStruct((nb, rows, dim), BF16), jax.ShapeDtypeStruct((nb, rows, 3 * cols), BF16)],
        in_specs=[full, full, full, full, full, small, small, w_spec, w_spec, w_spec],
        out_specs=[pl.BlockSpec((1, rows, bn), lambda b, i: (b, 0, i)), pl.BlockSpec((1, rows, 3 * cols), lambda b, i: (b, 0, 0))],
        compiler_params=params("arbitrary", "arbitrary"),
        cost_estimate=cost(6 * nb * rows * dim * cols, nb * (2 * rows * dim + 6 * dim * cols + 20 * rows * cols)),
    )(dqs, dks, q, k, dv, ss, st, w_q, w_k, w_v)


def dw_kernel(y_ref, g_ref, *outs):
    acc = lax.dot_general(y_ref[...], g_ref[...], TN, preferred_element_type=F32)
    cols = outs[0].shape[1]
    for j, o_ref in enumerate(outs):
        o_ref[...] = acc[:, j * cols:(j + 1) * cols].astype(BF16)


def dw_call(y, g):
    rows, dim = y.shape
    cols = g.shape[1] // 3
    bm = min(512, dim)
    return pl.pallas_call(
        dw_kernel, name="dw", grid=(dim // bm,),
        out_shape=[jax.ShapeDtypeStruct((dim, cols), BF16)] * 3,
        in_specs=[pl.BlockSpec((rows, bm), lambda i: (0, i)), pl.BlockSpec((rows, 3 * cols), lambda i: (0, 0))],
        out_specs=[pl.BlockSpec((bm, cols), lambda i: (i, 0))] * 3,
        compiler_params=params("arbitrary"),
        cost_estimate=cost(6 * rows * dim * cols, 2 * rows * (dim + 3 * cols) + 6 * dim * cols),
    )(y, g)


def out_kernel(x_ref, dy_ref, pr_ref, m_ref, e_ref, bo_ref, o_ref, dg_ref):
    gate = m_ref[2:3] + e_ref[0, 2:3]
    proj = pr_ref[0].astype(F32) + bo_ref[...]
    o_ref[0] = (x_ref[0].astype(F32) + gate * proj).astype(BF16)
    dg_ref[0] = jnp.sum(dy_ref[0].astype(F32) * proj, axis=0, keepdims=True)


def dx_kernel(x_ref, dy_ref, g_ref, m_ref, e_ref, o_ref, dm_ref):
    scale_one = 1.0 + (m_ref[1:2] + e_ref[0, 1:2])
    x_norm, inv_std = norm_stats(x_ref[0].astype(F32))
    d_y = g_ref[0].astype(F32)
    d_norm = d_y * scale_one
    d_x = dy_ref[0].astype(F32) + inv_std * (
        d_norm - jnp.mean(d_norm, axis=-1, keepdims=True) - x_norm * jnp.mean(d_norm * x_norm, axis=-1, keepdims=True))
    o_ref[0] = d_x.astype(BF16)
    dm_ref[0, 0:1] = jnp.sum(d_y, axis=0, keepdims=True)
    dm_ref[0, 1:2] = jnp.sum(d_y * x_norm, axis=0, keepdims=True)


def token_call(kernel, name, n_sums, x_loc, dy_loc, piece, m_block, e_loc, extra):
    nb, rows, dim = x_loc.shape
    row = pl.BlockSpec((1, rows, dim), lambda i: (i, 0, 0))
    specs = [row, row, row, pl.BlockSpec((3, dim), lambda i: (0, 0)),
             pl.BlockSpec((1, 3, dim), lambda i: (i, 0, 0))] + [pl.BlockSpec((1, dim), lambda i: (0, 0))] * len(extra)
    return pl.pallas_call(
        kernel, name=name, grid=(nb,),
        out_shape=[jax.ShapeDtypeStruct(x_loc.shape, BF16), jax.ShapeDtypeStruct((nb, n_sums, dim), F32)],
        in_specs=specs, out_specs=[row, pl.BlockSpec((1, n_sums, dim), lambda i: (i, 0, 0))],
        compiler_params=params("arbitrary"),
        cost_estimate=cost(nb * rows * dim * 20, nb * rows * dim * 8),
    )(x_loc, dy_loc, piece, m_block, e_loc, *extra)


def solution(mesh):
    tp_size = mesh.shape['tp']

    def device_step(x_loc, e_loc, m_block, w_q, b_q, w_k, b_k, w_v, b_v, w_o, b_o, g_q, g_k, pos_part, dy_loc):
        nb, _, dim = x_loc.shape
        cols = w_q.shape[1]
        cos_tab, sin_tab = rope_tables(pos_part)
        y_full, d_own, q, k, v, ss = gather_qkv_call(tp_size, x_loc, dy_loc, m_block, e_loc, w_q, w_k, w_v, b_q, b_k, b_v)
        d_full, o, d_attn, d_wo = gather_attn_call(tp_size, q, k, v, g_q, g_k, cos_tab, sin_tab, ss, w_o, d_own)
        rows_all = nb * q.shape[1]
        part = nn_call("proj", o.reshape(rows_all, cols), w_o).reshape(d_full.shape)
        proj = lax.psum_scatter(part, 'tp', scatter_dimension=1, tiled=True)
        d_attn, part = lax.optimization_barrier((d_attn, part))
        dv, dqs, dks, d_gq, d_gk, st = attn_bwd_call(dim, q, k, v, d_attn, g_q, g_k, cos_tab, sin_tab, ss)
        st = exchange_call("stat", 2, tp_size, st)
        dy_part, grad = dy_call(dqs, dks, q, k, dv, ss, st, w_q, w_k, w_v)
        dy_part, proj = lax.optimization_barrier((dy_part, proj))
        d_y = lax.psum_scatter(dy_part, 'tp', scatter_dimension=1, tiled=True)
        grad, dy_part = lax.optimization_barrier((grad, dy_part))
        d_wq, d_wk, d_wv = dw_call(y_full.reshape(rows_all, dim), grad.reshape(rows_all, 3 * cols))
        x_out, d_gate = token_call(out_kernel, "xout", 1, x_loc, dy_loc, proj, m_block, e_loc, [b_o[None]])
        d_x, d_mod = token_call(dx_kernel, "dx", 2, x_loc, dy_loc, d_y, m_block, e_loc, [])
        sums = jnp.concatenate([d_mod, d_gate], axis=1)
        d_e = exchange_call("dmod", 3, tp_size, sums.reshape(8, -1)).reshape(nb, 3, dim)
        return (x_out, d_x, d_e, jnp.sum(d_e, axis=0), d_wq, d_wk, d_wv, d_wo,
                jnp.sum(d_gq, axis=(0, 1)), jnp.sum(d_gk, axis=(0, 1)))

    in_specs = (P('dp', 'tp', None), P('dp', None, None), P(None, None), P(None, 'tp'), P('tp'), P(None, 'tp'), P('tp'),
                P(None, 'tp'), P('tp'), P('tp', None), P(None), P('tp'), P('tp'), P('dp', None), P('dp', 'tp', None))
    out_specs = (P('dp', 'tp', None), P('dp', 'tp', None), P('dp', None, None), P('dp', None), P('dp', 'tp'), P('dp', 'tp'),
                 P('dp', 'tp'), P(('dp', 'tp'), None), P(('dp', 'tp')), P(('dp', 'tp')))
    return jax.shard_map(device_step, mesh=mesh, in_specs=in_specs, out_specs=out_specs, check_vma=False)
```

```python
import functools

import jax
import jax.numpy as jnp
from jax import lax
from jax.experimental import pallas as pl
from jax.experimental.pallas import tpu as pltpu
from jax.sharding import PartitionSpec as P

HEAD_DIM = 128
EPS_NORM = 1e-6
ROPE_BASE = 10000.0
LOG2E = 1.4426950408889634
CHUNK = 512
VMEM_LIMIT = 60 * 1024 * 1024
F32 = jnp.float32
BF16 = jnp.bfloat16
MESH_ID = pl.DeviceIdType.MESH
NT = (((1,), (1,)), ((), ()))
TN = (((0,), (0,)), ((), ()))


def params(*semantics, **kw):
    return pltpu.CompilerParams(dimension_semantics=semantics or None, vmem_limit_bytes=VMEM_LIMIT, **kw)


def cost(flops, nbytes):
    return pl.CostEstimate(flops=int(flops), bytes_accessed=int(nbytes), transcendentals=0)


def rope_tables(positions):
    half_dim = HEAD_DIM // 2
    side_len = HEAD_DIM // 6
    first_len = half_dim - 2 * side_len
    lane = jnp.arange(HEAD_DIM)
    pair_idx = lane // 2
    section = (pair_idx >= first_len).astype(jnp.int32) + (pair_idx >= first_len + side_len).astype(jnp.int32)
    offset = jnp.where(section == 0, 0, jnp.where(section == 1, first_len, first_len + side_len))
    sec_width = jnp.where(section == 0, first_len, side_len)
    freq_vals = ROPE_BASE ** (-(pair_idx - offset).astype(F32) / sec_width.astype(F32))
    select = jnp.where(section[None, :] == jnp.arange(3)[:, None], freq_vals[None, :], 0.0)
    angles = jnp.sum(positions.astype(F32)[:, :, None] * select[None, :, :], axis=1)
    return jnp.cos(angles), jnp.where((lane % 2 == 0)[None, :], -1.0, 1.0) * jnp.sin(angles)


def norm_stats(x):
    centered = x - jnp.mean(x, axis=-1, keepdims=True)
    inv_std = lax.rsqrt(jnp.mean(centered * centered, axis=-1, keepdims=True) + EPS_NORM)
    return centered * inv_std, inv_std


def to_row(acc):
    return jnp.sum(acc.T, axis=0, keepdims=True)


def lanes_of(row):
    return jnp.broadcast_to(row, (HEAD_DIM, row.shape[1])).T


def head_sum(values):
    out = values[:, :HEAD_DIM]
    for h in range(1, values.shape[1] // HEAD_DIM):
        out = out + values[:, h * HEAD_DIM:(h + 1) * HEAD_DIM]
    return out


class Place:
    def __init__(self, n):
        self.n = n
        self.me = lax.axis_index('tp')
        self.right = lax.rem(self.me + 2, n)
        self.left = lax.rem(self.me + n - 2, n)
        self.far = lax.rem(self.me + n // 2, n)
        self.chip = self.me // 2

    def partner(self, dev):
        return dev + 1 - 2 * lax.rem(dev, 2)

    def barrier(self, devices):
        sem = pltpu.get_barrier_semaphore()
        for dev in devices:
            pl.semaphore_signal(sem, inc=1, device_id={'tp': dev}, device_id_type=MESH_ID)
        pl.semaphore_wait(sem, len(devices))

    def to_partner(self, src, dst, send_sem, recv_sem):
        return pltpu.make_async_remote_copy(src_ref=src, dst_ref=dst, send_sem=send_sem, recv_sem=recv_sem,
                                            device_id={'tp': self.partner(self.me)}, device_id_type=MESH_ID)

    def everyone(self):
        return [lax.rem(self.me + d, self.n) for d in range(1, self.n)]

    def near(self):
        return [self.right, self.left, self.partner(self.me)]


class Gather:
    def __init__(self, place, full, rows, send, recv):
        self.at, self.full, self.rows, self.send, self.recv = place, full, rows, send, recv

    def part(self, b, dev, off, count):
        return self.full.at[b, pl.ds(pl.multiple_of(dev * self.rows + off, 16), count)]

    def copy(self, b, dev, off, count, s_idx, r_idx, target):
        ref = self.part(b, dev, off, count)
        return pltpu.make_async_remote_copy(src_ref=ref, dst_ref=ref, send_sem=self.send.at[b, s_idx], recv_sem=self.recv.at[b, r_idx],
                                            device_id={'tp': target}, device_id_type=MESH_ID)

    def start_own(self, b):
        p = self.at
        self.copy(b, p.me, 0, self.rows, 0, 0, p.right).start()
        self.copy(b, p.me, 0, self.rows, 1, 1, p.left).start()
        self.copy(b, p.me, 0, self.rows, 2, 4, p.partner(p.me)).start()

    def take_own(self, b):
        p = self.at
        self.copy(b, p.partner(p.me), 0, self.rows, 2, 4, p.me).wait_recv()

    def take_left(self, b):
        p, half = self.at, self.rows // 2
        self.copy(b, p.left, 0, self.rows, 0, 0, p.me).wait_recv()
        self.copy(b, p.left, 0, half, 3, 2, p.right).start()
        self.copy(b, p.left, 0, self.rows, 5, 5, p.partner(p.me)).start()
        self.copy(b, p.partner(p.left), 0, self.rows, 5, 5, p.me).wait_recv()

    def take_right(self, b):
        p, half = self.at, self.rows // 2
        self.copy(b, p.right, 0, self.rows, 1, 1, p.me).wait_recv()
        self.copy(b, p.right, half, half, 4, 3, p.left).start()
        self.copy(b, p.right, 0, self.rows, 6, 6, p.partner(p.me)).start()
        self.copy(b, p.partner(p.right), 0, self.rows, 6, 6, p.me).wait_recv()

    def take_far(self, b):
        p, half = self.at, self.rows // 2
        self.copy(b, p.far, 0, half, 3, 2, p.me).wait_recv()
        self.copy(b, p.far, 0, half, 7, 7, p.partner(p.me)).start()
        self.copy(b, p.far, half, half, 4, 3, p.me).wait_recv()
        self.copy(b, p.far, half, half, 8, 8, p.partner(p.me)).start()
        self.copy(b, p.partner(p.far), 0, half, 7, 7, p.me).wait_recv()
        self.copy(b, p.partner(p.far), half, half, 8, 8, p.me).wait_recv()

    def finish(self, b):
        p, half = self.at, self.rows // 2
        for s_idx, count in ((0, self.rows), (1, self.rows), (2, self.rows), (3, half), (4, half), (5, self.rows), (6, self.rows), (7, half), (8, half)):
            self.copy(b, p.me, 0, count, s_idx, s_idx, p.me).wait_send()

    def item_place(self, i, nb):
        j = i - nb
        b = jnp.where(i < nb, i, jnp.where(i < 3 * nb, j // 2, i - 3 * nb))
        chips = self.at.n // 2
        side = jnp.where(lax.rem(j + 2 * nb, 2) == 0, chips - 1, 1)
        off = jnp.where(i < nb, 0, jnp.where(i < 3 * nb, side, chips // 2))
        return b, pl.multiple_of(lax.rem(self.at.chip + off, chips) * (2 * self.rows), 32)

    def take_item(self, i, nb):
        b, row0 = self.item_place(i, nb)
        odd = lax.rem(i + nb, 2)
        pl.when(i < nb)(lambda: self.take_own(b))
        pl.when((i >= nb) & (i < 3 * nb) & (odd == 0))(lambda: self.take_left(b))
        pl.when((i >= nb) & (i < 3 * nb) & (odd == 1))(lambda: self.take_right(b))
        pl.when(i >= 3 * nb)(lambda: self.take_far(b))
        return b, row0


GATHER_SEMS = 9


def chunks_of(width, step):
    return [(c, min(c + step, width)) for c in range(0, width, step)]


def exchange(place, x_ref, slots, send_sems, recv_sems):
    n, me = place.n, place.me
    for d, dev in enumerate(place.everyone()):
        pltpu.make_async_remote_copy(src_ref=x_ref, dst_ref=slots.at[me], send_sem=send_sems.at[d], recv_sem=recv_sems.at[me],
                                     device_id={'tp': dev}, device_id_type=MESH_ID).start()
    slots[me] = x_ref[...]
    for d, dev in enumerate(place.everyone()):
        copy = pltpu.make_async_remote_copy(src_ref=x_ref, dst_ref=slots.at[dev], send_sem=send_sems.at[d], recv_sem=recv_sems.at[dev],
                                            device_id={'tp': dev}, device_id_type=MESH_ID)
        copy.wait_send()
        copy.wait_recv()
    total = slots[0]
    for d in range(1, n):
        total = total + slots[d]
    return total


def gather_qkv_kernel(n, x_ref, dy_ref, m_ref, e_ref, wq_ref, wk_ref, wv_ref, bias_ref,
                      y_full, d_full, q_out, k_out, v_out, ss_ref,
                      w_all, xin, stage, xbuf, zst, vst, sq, ss_row, slots,
                      w_sem, in_sem, st_sem, ld_sem, out_sem, g_send, g_recv, e_send, e_recv):
    nb, rows, dim = x_ref.shape
    cols = wq_ref.shape[1]
    place = Place(n)
    gather = Gather(place, y_full, rows, g_send, g_recv)
    w_copies = [pltpu.make_async_copy(w, w_all.at[:, pl.ds(j * cols, cols)], w_sem.at[j]) for j, w in enumerate((wq_ref, wk_ref, wv_ref))]
    load_x = pltpu.make_async_copy(x_ref, xin, in_sem)
    load_x.start()
    for c in w_copies:
        c.start()
    group = 16

    def mine(full, b):
        return full.at[b, pl.ds(pl.multiple_of(place.me * rows, 16), rows)]

    load_x.wait()
    place.barrier(place.everyone())

    def ln_step(b, _):
        shift = m_ref[0:1] + e_ref[b, 0:1]
        scale_one = 1.0 + (m_ref[1:2] + e_ref[b, 1:2])

        def ln_rows(r, _):
            sl = pl.ds(pl.multiple_of(r * group, group), group)
            x_norm, _ = norm_stats(xin[b, sl].astype(F32))
            stage[b, sl] = (x_norm * scale_one + shift).astype(BF16)
            return 0

        lax.fori_loop(0, rows // group, ln_rows, 0)
        out = pltpu.make_async_copy(stage.at[b], mine(y_full, b), st_sem)
        out.start()
        out.wait()
        gather.start_own(b)
        return 0

    lax.fori_loop(0, nb, ln_step, 0)
    load_dy = pltpu.make_async_copy(dy_ref, xin, in_sem)
    load_dy.start()

    def gate_step(b, _):
        gate = m_ref[2:3] + e_ref[b, 2:3]

        def gate_rows(r, _):
            sl = pl.ds(pl.multiple_of(r * group, group), group)
            stage[b, sl] = (xin[b, sl].astype(F32) * gate).astype(BF16)
            return 0

        lax.fori_loop(0, rows // group, gate_rows, 0)
        out = pltpu.make_async_copy(stage.at[b], mine(d_full, b), st_sem)
        out.start()
        out.wait()
        return 0

    for c in w_copies:
        c.wait()

    def outputs(b, row0, slot):
        dst = pl.ds(row0, 2 * rows)
        return [pltpu.make_async_copy(zst.at[slot, :, pl.ds(0, cols)], q_out.at[b, dst], out_sem.at[slot, 0]),
                pltpu.make_async_copy(zst.at[slot, :, pl.ds(cols, cols)], k_out.at[b, dst], out_sem.at[slot, 1]),
                pltpu.make_async_copy(vst.at[slot], v_out.at[b, dst], out_sem.at[slot, 2])]

    def item(i, _):
        b, row0 = gather.take_item(i, nb)
        slot = lax.rem(i, 2)
        load = pltpu.make_async_copy(y_full.at[b, pl.ds(row0, 2 * rows)], xbuf, ld_sem)
        load.start()

        @pl.when(i == nb)
        def _():
            load_dy.wait()
            lax.fori_loop(0, nb, gate_step, 0)

        @pl.when(i >= 2)
        def _():
            for c in outputs(0, 0, slot):
                c.wait()

        load.wait()
        for lo, hi in chunks_of(3 * cols, 512):
            zst[slot, :, lo:hi] = jnp.dot(xbuf[...], w_all[:, lo:hi], preferred_element_type=F32) + bias_ref[:, lo:hi]
        vst[slot] = zst[slot, :, 2 * cols:].astype(BF16)
        q = zst[slot, :, :cols]
        k = zst[slot, :, cols:2 * cols]
        sq[2 * b, pl.ds(row0, 2 * rows)] = head_sum(q * q)
        sq[2 * b + 1, pl.ds(row0, 2 * rows)] = head_sum(k * k)
        for c in outputs(b, row0, slot):
            c.start()
        return 0

    lax.fori_loop(0, 4 * nb, item, 0)
    ss_row[...] = jnp.zeros_like(ss_row)
    for j in range(2 * nb):
        ss_row[j:j + 1] = to_row(sq[j])
    for slot in range(2):
        for c in outputs(0, 0, slot):
            c.wait()
    for b in range(nb):
        gather.finish(b)
    ss_ref[...] = exchange(place, ss_row, slots, e_send, e_recv)


def gather_qkv_call(n, x_loc, dy_loc, m_block, e_loc, w_q, w_k, w_v, b_q, b_k, b_v):
    nb, rows, dim = x_loc.shape
    cols = w_q.shape[1]
    tokens = rows * n
    shape = jax.ShapeDtypeStruct
    any_spec = pl.BlockSpec(memory_space=pl.ANY)
    vmem = pl.BlockSpec(memory_space=pltpu.VMEM)
    dma = pltpu.SemaphoreType.DMA
    stat_rows = -(-2 * nb // 8) * 8
    return pl.pallas_call(
        functools.partial(gather_qkv_kernel, n), name="gather_qkv",
        out_shape=[shape((nb, tokens, dim), BF16), shape((nb, tokens, dim), BF16), shape((nb, tokens, cols), F32),
                   shape((nb, tokens, cols), F32), shape((nb, tokens, cols), BF16), shape((stat_rows, tokens), F32)],
        in_specs=[any_spec, any_spec, vmem, vmem, any_spec, any_spec, any_spec, vmem],
        out_specs=[any_spec] * 5 + [vmem],
        scratch_shapes=[
            pltpu.VMEM((dim, 3 * cols), BF16), pltpu.VMEM((nb, rows, dim), BF16), pltpu.VMEM((nb, rows, dim), BF16),
            pltpu.VMEM((2 * rows, dim), BF16), pltpu.VMEM((2, 2 * rows, 3 * cols), F32), pltpu.VMEM((2, 2 * rows, cols), BF16),
            pltpu.VMEM((2 * nb, tokens, HEAD_DIM), F32), pltpu.VMEM((stat_rows, tokens), F32), pltpu.VMEM((n, stat_rows, tokens), F32),
            dma((3,)), dma, dma, dma, dma((2, 3)), dma((nb, GATHER_SEMS)), dma((nb, GATHER_SEMS)), dma((n,)), dma((n,))],
        compiler_params=params(collective_id=0, has_side_effects=True),
        cost_estimate=cost(6 * nb * tokens * dim * cols, 6 * dim * cols + 14 * nb * tokens * cols),
    )(x_loc, dy_loc, m_block, e_loc, w_q, w_k, w_v, jnp.concatenate([b_q, b_k, b_v])[None])


def all_sum_kernel(n, x_ref, o_ref, pieces, total, send_a, recv_a, send_b, recv_b):
    place = Place(n)
    me = place.me
    place.barrier(place.everyone())

    def first(d, dev, src):
        return pltpu.make_async_remote_copy(src_ref=x_ref.at[src], dst_ref=pieces.at[me], send_sem=send_a.at[d], recv_sem=recv_a.at[me],
                                            device_id={'tp': dev}, device_id_type=MESH_ID)

    for d, dev in enumerate(place.everyone()):
        first(d, dev, dev).start()
    pieces[me] = x_ref[me]
    for d, dev in enumerate(place.everyone()):
        pltpu.make_async_remote_copy(src_ref=x_ref.at[me], dst_ref=pieces.at[dev], send_sem=send_a.at[d], recv_sem=recv_a.at[dev],
                                     device_id={'tp': dev}, device_id_type=MESH_ID).wait_recv()
    acc = pieces[0]
    for d in range(1, n):
        acc = acc + pieces[d]
    total[...] = acc
    o_ref[me] = acc
    for d, dev in enumerate(place.everyone()):
        first(d, dev, dev).wait_send()
    for d, dev in enumerate(place.everyone()):
        pltpu.make_async_remote_copy(src_ref=total, dst_ref=o_ref.at[me], send_sem=send_b.at[d], recv_sem=recv_b.at[me],
                                     device_id={'tp': dev}, device_id_type=MESH_ID).start()
    for d, dev in enumerate(place.everyone()):
        copy = pltpu.make_async_remote_copy(src_ref=total, dst_ref=o_ref.at[dev], send_sem=send_b.at[d], recv_sem=recv_b.at[dev],
                                            device_id={'tp': dev}, device_id_type=MESH_ID)
        copy.wait_send()
        copy.wait_recv()


def all_sum_call(n, x):
    spec = pl.BlockSpec(memory_space=pltpu.VMEM)
    dma = pltpu.SemaphoreType.DMA
    return pl.pallas_call(
        functools.partial(all_sum_kernel, n), name="all_sum",
        out_shape=jax.ShapeDtypeStruct(x.shape, x.dtype), in_specs=[spec], out_specs=spec,
        scratch_shapes=[pltpu.VMEM(x.shape, x.dtype), pltpu.VMEM(x.shape[1:], x.dtype), dma((n,)), dma((n,)), dma((n,)), dma((n,))],
        compiler_params=pltpu.CompilerParams(collective_id=4, has_side_effects=True, vmem_limit_bytes=4 * 1024 * 1024),
        cost_estimate=cost(4_000_000_000, x.size * 8),
    )(x)


def swap_pairs(x):
    lane = lax.broadcasted_iota(jnp.int32, x.shape, 1)
    return jnp.where(lane % 2 == 0, pltpu.roll(x, HEAD_DIM - 1, 1), pltpu.roll(x, 1, 1))


def rotate(x, cos, sin):
    return x * cos + swap_pairs(x) * sin


def softmax_block(s):
    c = HEAD_DIM ** -0.5 * LOG2E
    top = jnp.max(s, axis=1, keepdims=True)
    p = jnp.exp2(s * c - top * c)
    return p * (1.0 / jnp.sum(p, axis=1, keepdims=True))


def gather_attn_kernel(n, nb, heads, dim, q_ref, k_ref, v_ref, gq_ref, gk_ref, cos_ref, sin_ref, ss_ref,
                       wq_ref, wk_ref, wv_ref, wo_ref, d_in,
                       d_full, o_out, o_p, da_out, wq_p, wk_p, wv_p, wo_p,
                       inv_q, inv_k, o_all, wo, xbuf, ast,
                       w_sem, ld_sem, out_sem, o_sem, g_send, g_recv, t_send, t_recv):
    step = pl.program_id(0)
    tokens = q_ref.shape[1]
    rows = tokens // n
    blk = min(256, tokens)
    place = Place(n)
    gather = Gather(place, d_full, rows, g_send, g_recv)
    pairs = ((wo_ref, wo_p), (wq_ref, wq_p), (wk_ref, wk_p), (wv_ref, wv_p), (o_out, o_p))

    def trade(j):
        return place.to_partner(*pairs[j], t_send.at[j], t_recv.at[j])


    @pl.when(step == 0)
    def _():
        pltpu.make_async_copy(wo_ref, wo, w_sem).start()
        place.barrier(place.near())

        def own(b, _):
            gather.start_own(b)
            return 0

        lax.fori_loop(0, nb, own, 0)
        for j in range(4):
            trade(j).start()

    @pl.when(step < nb * heads)
    def _():
        b = step // heads
        h = lax.rem(step, heads)

        @pl.when(h == 0)
        def _():
            inv_q[...] = lanes_of(lax.rsqrt(ss_ref[pl.ds(2 * b, 1)] / dim + EPS_NORM))
            inv_k[...] = lanes_of(lax.rsqrt(ss_ref[pl.ds(2 * b + 1, 1)] / dim + EPS_NORM))

        cos, sin = cos_ref[...], sin_ref[...]
        q_rot = rotate(q_ref[0] * inv_q[...] * gq_ref[...], cos, sin).astype(BF16)
        k_rot = rotate(k_ref[0] * inv_k[...] * gk_ref[...], cos, sin).astype(BF16)
        v = v_ref[0]
        lanes = pl.ds(pl.multiple_of(h * HEAD_DIM, HEAD_DIM), HEAD_DIM)
        for i in range(tokens // blk):
            s = lax.dot_general(q_rot[i * blk:(i + 1) * blk], k_rot, NT, preferred_element_type=F32)
            p = softmax_block(s).astype(BF16)
            o_all[b, i * blk:(i + 1) * blk, lanes] = jnp.dot(p, v, preferred_element_type=F32).astype(BF16)

    @pl.when(step == nb * heads)
    def _():
        o_copy = pltpu.make_async_copy(o_all, o_out, o_sem)
        o_copy.start()
        pltpu.make_async_copy(wo_ref, wo, w_sem).wait()

        def outputs(b, row0, slot):
            return pltpu.make_async_copy(ast.at[slot], da_out.at[b, pl.ds(row0, 2 * rows)], out_sem.at[slot])

        def load(b, row0, slot):
            return pltpu.make_async_copy(d_full.at[b, pl.ds(row0, 2 * rows)], xbuf.at[slot], ld_sem.at[slot])

        def take(i):
            b, row0 = gather.take_item(i, nb)
            load(b, row0, lax.rem(i, 2)).start()

        take(0)

        def item(i, _):
            slot = lax.rem(i, 2)

            @pl.when(i + 1 < 3 * nb)
            def _():
                take(i + 1)

            @pl.when(i >= 2)
            def _():
                outputs(0, 0, slot).wait()

            load(0, 0, slot).wait()
            ast[slot] = lax.dot_general(xbuf[slot], wo[...], NT, preferred_element_type=F32).astype(BF16)
            b, row0 = gather.item_place(i, nb)
            outputs(b, row0, slot).start()

            @pl.when(i == 0)
            def _():
                o_copy.wait()
                trade(4).start()

            @pl.when((i + 1 >= 3 * nb) & (i + 1 < 4 * nb))
            def _():
                take(i + 1)

            return 0

        lax.fori_loop(0, 4 * nb, item, 0)
        for slot in range(2):
            outputs(0, 0, slot).wait()
        for b in range(nb):
            gather.finish(b)
        for j in range(5):
            trade(j).wait()


def gather_attn_call(n, q, k, v, g_q, g_k, cos_tab, sin_tab, ss, w_q, w_k, w_v, w_o, d_full):
    nb, tokens, cols = q.shape
    dim = w_o.shape[1]
    heads = cols // HEAD_DIM
    rows = tokens // n
    last = nb * heads - 1
    shape = jax.ShapeDtypeStruct
    dma = pltpu.SemaphoreType.DMA
    any_spec = pl.BlockSpec(memory_space=pl.ANY)

    def head_of(i):
        i = jnp.minimum(i, last)
        return i // heads, i % heads

    blk = pl.BlockSpec((1, tokens, HEAD_DIM), lambda i: (head_of(i)[0], 0, head_of(i)[1]))
    vec = pl.BlockSpec((1, HEAD_DIM), lambda i: (0, head_of(i)[1]))
    tab = pl.BlockSpec((tokens, HEAD_DIM), lambda i: (0, 0))
    head_arr = shape((nb, tokens, cols), BF16)
    return pl.pallas_call(
        functools.partial(gather_attn_kernel, n, nb, heads, dim), name="gather_attn", grid=(nb * heads + 1,),
        out_shape=[shape(d_full.shape, BF16), head_arr, head_arr, head_arr] + [shape(w.shape, BF16) for w in (w_q, w_k, w_v, w_o)],
        in_specs=[blk, blk, blk, vec, vec, tab, tab, pl.BlockSpec(ss.shape, lambda i: (0, 0))] + [any_spec] * 5,
        out_specs=[any_spec] * 8,
        scratch_shapes=[
            pltpu.VMEM((tokens, HEAD_DIM), F32), pltpu.VMEM((tokens, HEAD_DIM), F32), pltpu.VMEM((nb, tokens, cols), BF16),
            pltpu.VMEM((cols, dim), BF16), pltpu.VMEM((2, 2 * rows, dim), BF16), pltpu.VMEM((2, 2 * rows, cols), BF16),
            dma, dma((2,)), dma((2,)), dma, dma((nb, GATHER_SEMS)), dma((nb, GATHER_SEMS)), dma((5,)), dma((5,))],
        input_output_aliases={12: 0},
        compiler_params=params("arbitrary", collective_id=1, has_side_effects=True),
        cost_estimate=cost(2 * nb * tokens * dim * cols + 4 * nb * tokens * tokens * cols, 8 * nb * tokens * dim),
    )(q, k, v, g_q[None], g_k[None], cos_tab, sin_tab, ss, w_q, w_k, w_v, w_o, d_full)


class Scatter:
    def __init__(self, place, part, recv_far, recv_side, send, recv):
        self.at, self.part, self.far, self.side, self.send, self.recv = place, part, recv_far, recv_side, send, recv
        self.rows = part.shape[2]
        self.half = self.rows // 2

    def copy(self, j, idx, src, dst, target):
        return pltpu.make_async_remote_copy(src_ref=src, dst_ref=dst, send_sem=self.send.at[j, idx], recv_sem=self.recv.at[j, idx],
                                            device_id={'tp': target}, device_id_type=MESH_ID)

    def message(self, j, idx):
        p, part, far, side = self.at, self.part, self.far, self.side
        first, second = pl.ds(0, self.half), pl.ds(self.half, self.rows - self.half)
        src, dst, target = (
            lambda: (part.at[j, 0, first], far.at[j, 0], p.right),
            lambda: (part.at[j, 0, second], far.at[j, 1], p.left),
            lambda: (part.at[j, 1, second], side.at[j, 0, second], p.right),
            lambda: (part.at[j, 2, first], side.at[j, 1, first], p.left),
            lambda: (part.at[j, 1, first], side.at[j, 0, first], p.right),
            lambda: (part.at[j, 2, second], side.at[j, 1, second], p.left))[idx]()
        return self.copy(j, idx, src, dst, target)

    def start(self, j):
        for idx in range(4):
            self.message(j, idx).start()

    def sums(self, j):
        h = self.half
        self.message(j, 0).wait_recv()
        self.part[j, 1, :h] = (self.part[j, 1, :h].astype(F32) + self.far[j, 0].astype(F32)).astype(BF16)
        self.message(j, 1).wait_recv()
        self.part[j, 2, h:] = (self.part[j, 2, h:].astype(F32) + self.far[j, 1].astype(F32)).astype(BF16)
        self.message(j, 4).start()
        self.message(j, 5).start()

    def final(self, j):
        for idx in range(2, 6):
            self.message(j, idx).wait_recv()
        total = self.part[j, 3].astype(F32) + self.side[j, 0].astype(F32) + self.side[j, 1].astype(F32)
        self.part[j, 3] = total.astype(BF16)

    def finish(self, j):
        for idx in range(6):
            self.message(j, idx).wait_send()

    @staticmethod
    def scratch(rows, dim):
        nc, dma = dim // CHUNK, pltpu.SemaphoreType.DMA
        return [pltpu.VMEM((nc, 4, rows, CHUNK), BF16), pltpu.VMEM((nc, 2, rows // 2, CHUNK), BF16),
                pltpu.VMEM((nc, 2, rows, CHUNK), BF16), dma((nc, 6)), dma((nc, 6))]


def scatter_outputs(part, out, sem, j):
    nb, rows, _ = out.shape
    cs = pl.ds(pl.multiple_of(j * CHUNK, CHUNK), CHUNK)
    return [pltpu.make_async_copy(part.at[j, 3, pl.ds(b * rows, rows)], out.at[b, :, cs], sem.at[b]) for b in range(nb)]


def scatter_end(scatter, out, sem, nc):
    def last(j, _):
        scatter.final(j)
        for c in scatter_outputs(scatter.part, out, sem, j):
            c.start()
        return 0

    lax.fori_loop(0, nc, last, 0)

    def drain(j, _):
        for c in scatter_outputs(scatter.part, out, sem, j):
            c.wait()
        scatter.finish(j)
        return 0

    lax.fori_loop(0, nc, drain, 0)


def pair_rows(place, nb, rows, mine, theirs, lhs, sem):
    width = mine.shape[2]
    out = []
    for d, dev in enumerate((place.far, place.right, place.left, place.me)):
        src_rows = pl.ds(pl.multiple_of(dev * rows, 16), rows)
        for b in range(nb):
            dst_rows = pl.ds((d * nb + b) * rows, rows)
            for j, src in enumerate((mine, theirs)):
                out.append(pltpu.make_async_copy(src.at[b, src_rows], lhs.at[dst_rows, pl.ds(j * width, width)], sem))
    return out


def proj_bwd_kernel(n, nb, heads, dim, q_ref, k_ref, v_ref, do_ref, gq_ref, gk_ref, cos_ref, sin_ref, ss_ref,
                    q_hbm, k_hbm, o_hbm, o_p, wo_hbm, wo_p, d_full,
                    proj_out, g_out, g_p, dqs_out, dks_out, dwo_out, dgq_ref, dgk_ref,
                    part, recv_far, recv_side, s_send, s_recv,
                    inv_q, inv_k, acc_q, acc_k, p_all, ds_all, dq_all, qs_st, ks_st, v_st, st_row, st_sum, slots,
                    ld_sem, w_sem, fl_sem, g_sem, go_sem, out_sem, e_send, e_recv, t_send, t_recv):
    step = pl.program_id(0)
    tokens = q_ref.shape[1]
    rows = tokens // n
    cols = heads * HEAD_DIM
    blk = min(256, tokens)
    nc = dim // CHUNK
    steps = nb * heads
    scale = HEAD_DIM ** -0.5
    place = Place(n)
    scatter = Scatter(place, part, recv_far, recv_side, s_send, s_recv)

    @pl.when(step == 0)
    def _():
        def project(lhs, wbuf):
            loads = pair_rows(place, nb, rows, o_hbm, o_p, lhs, ld_sem.at[0])
            for c in loads:
                c.start()

            def chunk(j):
                cs = pl.ds(pl.multiple_of(j * CHUNK, CHUNK), CHUNK)
                slot = lax.rem(j, 2)
                return [pltpu.make_async_copy(wo_hbm.at[:, cs], wbuf.at[slot, pl.ds(0, cols)], w_sem.at[slot, 0]),
                        pltpu.make_async_copy(wo_p.at[:, cs], wbuf.at[slot, pl.ds(cols, cols)], w_sem.at[slot, 1])]

            for c in chunk(0):
                c.start()
            place.barrier(place.everyone())
            for c in loads:
                c.wait()

            def body(j, _):
                @pl.when(j + 1 < nc)
                def _():
                    for c in chunk(j + 1):
                        c.start()

                for c in chunk(j):
                    c.wait()
                w = wbuf[lax.rem(j, 2)]
                half = 2 * nb * rows
                for d in range(2):
                    z = jnp.dot(lhs[d * half:(d + 1) * half], w, preferred_element_type=F32).astype(BF16)
                    part[j, 2 * d] = z[:half // 2]
                    part[j, 2 * d + 1] = z[half // 2:]
                scatter.start(j)
                return 0

            lax.fori_loop(0, nc, body, 0)

        pl.run_scoped(project, pltpu.VMEM((4 * nb * rows, 2 * cols), BF16), pltpu.VMEM((2, 2 * cols, CHUNK), BF16))

    def flush(b, h, slot):
        lanes = pl.ds(pl.multiple_of(h * HEAD_DIM, HEAD_DIM), HEAD_DIM)
        v_lanes = pl.ds(pl.multiple_of(2 * cols + h * HEAD_DIM, HEAD_DIM), HEAD_DIM)
        return [pltpu.make_async_copy(qs_st.at[slot], dqs_out.at[b, :, lanes], fl_sem.at[slot, 0]),
                pltpu.make_async_copy(ks_st.at[slot], dks_out.at[b, :, lanes], fl_sem.at[slot, 1]),
                pltpu.make_async_copy(v_st.at[slot], g_out.at[b, :, v_lanes], fl_sem.at[slot, 2])]

    for j in range(nc):
        at_step = 1 + j * (steps - 1) // max(nc - 1, 1)
        pl.when(step == at_step)(functools.partial(scatter.sums, j))

    @pl.when((step >= 1) & (step <= steps))
    def _():
        b = (step - 1) // heads
        head = lax.rem(step - 1, heads)
        slot = lax.rem(step, 2)

        @pl.when(step == 1)
        def _():
            st_row[...] = jnp.zeros_like(st_row)

        @pl.when(head == 0)
        def _():
            inv_q[...] = lanes_of(lax.rsqrt(ss_ref[pl.ds(2 * b, 1)] / dim + EPS_NORM))
            inv_k[...] = lanes_of(lax.rsqrt(ss_ref[pl.ds(2 * b + 1, 1)] / dim + EPS_NORM))
            acc_q[...] = jnp.zeros_like(acc_q)
            acc_k[...] = jnp.zeros_like(acc_k)

        @pl.when(step >= 3)
        def _():
            for c in flush(0, 0, slot):
                c.wait()

        cos, sin = cos_ref[...], sin_ref[...]
        q_rot = rotate(q_ref[0] * inv_q[...] * gq_ref[...], cos, sin).astype(BF16)
        k_rot = rotate(k_ref[0] * inv_k[...] * gk_ref[...], cos, sin).astype(BF16)
        v = v_ref[0]
        do = do_ref[0]
        for i in range(tokens // blk):
            sl = slice(i * blk, (i + 1) * blk)
            p = softmax_block(lax.dot_general(q_rot[sl], k_rot, NT, preferred_element_type=F32))
            p_all[sl] = p.astype(BF16)
            dp = lax.dot_general(do[sl], v, NT, preferred_element_type=F32)
            delta = jnp.sum(dp * p, axis=1, keepdims=True)
            ds = (p * (dp - delta)).astype(BF16)
            ds_all[sl] = ds
            dq_all[sl] = jnp.dot(ds, k_rot, preferred_element_type=F32) * scale
        do_t = do.astype(F32).T.astype(BF16)
        q_t = q_rot.astype(F32).T.astype(BF16)
        v_st[slot] = jnp.dot(do_t, p_all[...], preferred_element_type=F32).T.astype(BF16)
        dk_rot = (jnp.dot(q_t, ds_all[...], preferred_element_type=F32) * scale).T.astype(BF16).astype(F32)
        dq_rot = dq_all[...].astype(BF16).astype(F32)
        dq_hat = rotate(dq_rot, cos, -sin)
        dk_hat = rotate(dk_rot, cos, -sin)
        q_hat = q_ref[0] * inv_q[...]
        k_hat = k_ref[0] * inv_k[...]
        dgq_ref[0] = jnp.sum(dq_hat * q_hat, axis=0, keepdims=True)
        dgk_ref[0] = jnp.sum(dk_hat * k_hat, axis=0, keepdims=True)
        dq_s = dq_hat * gq_ref[...]
        dk_s = dk_hat * gk_ref[...]
        qs_st[slot] = dq_s
        ks_st[slot] = dk_s
        acc_q[...] += dq_s * q_hat
        acc_k[...] += dk_s * k_hat
        for c in flush(b, head, slot):
            c.start()

        @pl.when(head == heads - 1)
        def _():
            st_row[pl.ds(2 * b, 1)] = to_row(acc_q[...])
            st_row[pl.ds(2 * b + 1, 1)] = to_row(acc_k[...])

    @pl.when(step == steps + 1)
    def _():
        for s in (steps - 1, steps):
            for c in flush(0, 0, s % 2):
                c.wait()
        st_sum[...] = exchange(place, st_row, slots, e_send, e_recv)
        rb = min(256, tokens)
        per = tokens // rb
        trade = place.to_partner(g_out, g_p, t_send, t_recv)

        def norm_grad(fbuf, gbuf):
            def loads(i, slot):
                b, r0 = i // per, pl.multiple_of(lax.rem(i, per) * rb, rb)
                return [pltpu.make_async_copy(src.at[b, pl.ds(r0, rb)], fbuf.at[slot, m], g_sem.at[slot, m])
                        for m, src in enumerate((dqs_out, q_hbm, dks_out, k_hbm))]

            def store(i, slot):
                b, r0 = i // per, pl.multiple_of(lax.rem(i, per) * rb, rb)
                return pltpu.make_async_copy(gbuf.at[slot], g_out.at[b, pl.ds(r0, rb), pl.ds(0, 2 * cols)], go_sem.at[slot])

            for c in loads(0, 0):
                c.start()

            def body(i, _):
                slot = lax.rem(i, 2)
                b, r0 = i // per, pl.multiple_of(lax.rem(i, per) * rb, rb)

                @pl.when(i + 1 < nb * per)
                def _():
                    for c in loads(i + 1, lax.rem(i + 1, 2)):
                        c.start()

                @pl.when(r0 == 0)
                def _():
                    inv_q[...] = lanes_of(lax.rsqrt(ss_ref[pl.ds(2 * b, 1)] / dim + EPS_NORM))
                    inv_k[...] = lanes_of(lax.rsqrt(ss_ref[pl.ds(2 * b + 1, 1)] / dim + EPS_NORM))
                    acc_q[...] = lanes_of(st_sum[pl.ds(2 * b, 1)] / dim)
                    acc_k[...] = lanes_of(st_sum[pl.ds(2 * b + 1, 1)] / dim)

                @pl.when(i >= 2)
                def _():
                    store(0, slot).wait()

                for c in loads(i, slot):
                    c.wait()
                sl = pl.ds(r0, rb)
                for m, (inv, st) in enumerate(((inv_q, acc_q), (inv_k, acc_k))):
                    inv_l, st_l = inv[sl], st[sl]
                    for h in range(heads):
                        hs = slice(h * HEAD_DIM, (h + 1) * HEAD_DIM)
                        grad = inv_l * (fbuf[slot, 2 * m, :, hs] - (fbuf[slot, 2 * m + 1, :, hs] * inv_l) * st_l)
                        gbuf[slot, :, m * cols + h * HEAD_DIM:m * cols + (h + 1) * HEAD_DIM] = grad.astype(BF16)
                store(i, slot).start()
                return 0

            lax.fori_loop(0, nb * per, body, 0)
            for s in range(min(2, nb * per)):
                store(0, s).wait()

        pl.run_scoped(norm_grad, pltpu.VMEM((2, 4, rb, cols), F32), pltpu.VMEM((2, rb, 2 * cols), BF16))
        trade.start()

        def weight_grad(turned, obuf, dbuf, wst):
            bn = min(512, dim)
            n_chunks = dim // bn

            def chunk(c):
                slot = lax.rem(c, 2)
                return pltpu.make_async_copy(d_full.at[:, :, pl.ds(pl.multiple_of(c * bn, bn), bn)], dbuf.at[slot], go_sem.at[slot])

            def store(c):
                slot = lax.rem(c, 2)
                return pltpu.make_async_copy(wst.at[slot], dwo_out.at[:, pl.ds(pl.multiple_of(c * bn, bn), bn)], w_sem.at[slot, 0])

            load_o = pltpu.make_async_copy(o_hbm, obuf, ld_sem.at[0])
            load_o.start()
            chunk(0).start()
            load_o.wait()
            for b in range(nb):
                turned[:, b * tokens:(b + 1) * tokens] = obuf[b].T

            def body(c, _):
                slot = lax.rem(c, 2)

                @pl.when(c + 1 < n_chunks)
                def _():
                    chunk(c + 1).start()

                @pl.when(c >= 2)
                def _():
                    store(c).wait()

                chunk(c).wait()
                d = dbuf[slot].reshape(nb * tokens, bn)
                wst[slot] = jnp.dot(turned[...], d, preferred_element_type=F32).astype(BF16)
                store(c).start()
                return 0

            lax.fori_loop(0, n_chunks, body, 0)
            for s in range(min(2, n_chunks)):
                store(s).wait()

        bn = min(512, dim)
        pl.run_scoped(weight_grad, pltpu.VMEM((cols, nb * tokens), BF16), pltpu.VMEM((nb, tokens, cols), BF16),
                      pltpu.VMEM((2, nb, tokens, bn), BF16), pltpu.VMEM((2, cols, bn), BF16))
        scatter_end(scatter, proj_out, out_sem, nc)
        trade.wait()


def proj_bwd_call(n, q, k, v, d_attn, g_q, g_k, cos_tab, sin_tab, ss, o, o_p, w_o, wo_p, d_full):
    nb, tokens, cols = q.shape
    dim = w_o.shape[1]
    heads = cols // HEAD_DIM
    rows = tokens // n
    steps = nb * heads
    shape = jax.ShapeDtypeStruct
    dma = pltpu.SemaphoreType.DMA
    any_spec = pl.BlockSpec(memory_space=pl.ANY)

    def head_of(i):
        i = jnp.clip(i - 1, 0, steps - 1)
        return i // heads, i % heads

    blk = pl.BlockSpec((1, tokens, HEAD_DIM), lambda i: (head_of(i)[0], 0, head_of(i)[1]))
    vec = pl.BlockSpec((1, HEAD_DIM), lambda i: (0, head_of(i)[1]))
    out_vec = pl.BlockSpec((1, 1, HEAD_DIM), lambda i: (head_of(i)[0], 0, head_of(i)[1]))
    tab = pl.BlockSpec((tokens, HEAD_DIM), lambda i: (0, 0))
    whole = (nb, tokens, cols)
    lane_tile = pltpu.VMEM((tokens, HEAD_DIM), F32)
    return pl.pallas_call(
        functools.partial(proj_bwd_kernel, n, nb, heads, dim), name="proj_bwd", grid=(steps + 2,),
        out_shape=[shape((nb, rows, dim), BF16), shape((nb, tokens, 3 * cols), BF16), shape((nb, tokens, 3 * cols), BF16),
                   shape(whole, F32), shape(whole, F32), shape((cols, dim), BF16), shape((nb, 1, cols), F32), shape((nb, 1, cols), F32)],
        in_specs=[blk, blk, blk, blk, vec, vec, tab, tab, pl.BlockSpec(ss.shape, lambda i: (0, 0))] + [any_spec] * 7,
        out_specs=[any_spec] * 6 + [out_vec, out_vec],
        scratch_shapes=Scatter.scratch(nb * rows, dim) + [lane_tile] * 4 + [pltpu.VMEM((tokens, tokens), BF16)] * 2 + [
            lane_tile, pltpu.VMEM((2, tokens, HEAD_DIM), F32), pltpu.VMEM((2, tokens, HEAD_DIM), F32),
            pltpu.VMEM((2, tokens, HEAD_DIM), BF16), pltpu.VMEM(ss.shape, F32), pltpu.VMEM(ss.shape, F32), pltpu.VMEM((n,) + ss.shape, F32),
            dma((1,)), dma((2, 2)), dma((2, 3)), dma((2, 4)), dma((2,)), dma((nb,)), dma((n,)), dma((n,)), dma, dma],
        compiler_params=params("arbitrary", collective_id=2, has_side_effects=True),
        cost_estimate=cost(4 * nb * tokens * dim * cols + 36 * nb * tokens * tokens * cols, 30 * nb * tokens * cols),
    )(q, k, v, d_attn, g_q[None], g_k[None], cos_tab, sin_tab, ss, q, k, o, o_p, w_o, wo_p, d_full)


def dy_dw_kernel(n, nb, dim, g_hbm, g_p, wq_hbm, wk_hbm, wv_hbm, wq_p, wk_p, wv_p, y_full,
                 dy_out, dwq_out, dwk_out, dwv_out,
                 part, recv_far, recv_side, s_send, s_recv, ld_sem, w_sem, y_sem, o_sem, out_sem):
    tokens = g_hbm.shape[1]
    rows = tokens // n
    cols = g_hbm.shape[2] // 3
    nc = dim // CHUNK
    place = Place(n)
    scatter = Scatter(place, part, recv_far, recv_side, s_send, s_recv)
    lag = 2

    def chain(lhs, wbuf):
        loads = pair_rows(place, nb, rows, g_hbm, g_p, lhs, ld_sem)
        for c in loads:
            c.start()

        def chunk(j):
            slot = lax.rem(j, 2)
            src = pl.ds(pl.multiple_of(j * CHUNK, CHUNK), CHUNK)
            return [pltpu.make_async_copy(w.at[src], wbuf.at[slot, :, pl.ds(m * cols, cols)], w_sem.at[slot, m])
                    for m, w in enumerate((wq_hbm, wk_hbm, wv_hbm, wq_p, wk_p, wv_p))]

        for c in chunk(0):
            c.start()
        place.barrier(place.near()[:2])
        for c in loads:
            c.wait()

        def body(j, _):
            @pl.when(j + 1 < nc)
            def _():
                for c in chunk(j + 1):
                    c.start()

            for c in chunk(j):
                c.wait()
            w = wbuf[lax.rem(j, 2)]
            half = 2 * nb * rows
            for d in range(2):
                z = lax.dot_general(lhs[d * half:(d + 1) * half], w, NT, preferred_element_type=F32).astype(BF16)
                part[j, 2 * d] = z[:half // 2]
                part[j, 2 * d + 1] = z[half // 2:]
            scatter.start(j)

            @pl.when(j >= lag)
            def _():
                scatter.sums(j - lag)

            return 0

        lax.fori_loop(0, nc, body, 0)

    pl.run_scoped(chain, pltpu.VMEM((4 * nb * rows, 6 * cols), BF16), pltpu.VMEM((2, CHUNK, 6 * cols), BF16))

    def weight_grad(g, ybuf, wst):
        bm = min(512, dim)
        n_chunks = dim // bm

        def chunk(c):
            slot = lax.rem(c, 2)
            return pltpu.make_async_copy(y_full.at[:, :, pl.ds(pl.multiple_of(c * bm, bm), bm)], ybuf.at[slot], y_sem.at[slot])

        def store(c):
            slot = lax.rem(c, 2)
            dst = pl.ds(pl.multiple_of(c * bm, bm), bm)
            return [pltpu.make_async_copy(wst.at[slot, :, pl.ds(m * cols, cols)], out.at[dst], o_sem.at[slot, m])
                    for m, out in enumerate((dwq_out, dwk_out, dwv_out))]

        load_g = pltpu.make_async_copy(g_hbm, g, ld_sem)
        load_g.start()
        chunk(0).start()
        load_g.wait()

        def body(c, _):
            slot = lax.rem(c, 2)

            @pl.when(c + 1 < n_chunks)
            def _():
                chunk(c + 1).start()

            @pl.when(c >= 2)
            def _():
                for s in store(c):
                    s.wait()

            chunk(c).wait()
            for m in range(lag):
                late = nc - lag + m
                pl.when(c == min(1 + 2 * m, n_chunks - 1))(functools.partial(scatter.sums, max(late, 0)) if late >= 0 else (lambda: None))
            wst[slot] = lax.dot_general(ybuf[slot].reshape(nb * tokens, bm), g[...].reshape(nb * tokens, 3 * cols), TN,
                                        preferred_element_type=F32).astype(BF16)
            for s in store(c):
                s.start()
            return 0

        lax.fori_loop(0, n_chunks, body, 0)
        for s in range(min(2, n_chunks)):
            for c in store(s):
                c.wait()

    bm = min(512, dim)
    pl.run_scoped(weight_grad, pltpu.VMEM((nb, tokens, 3 * cols), BF16), pltpu.VMEM((2, nb, tokens, bm), BF16),
                  pltpu.VMEM((2, bm, 3 * cols), BF16))
    scatter_end(scatter, dy_out, out_sem, nc)


def dy_dw_call(n, g, g_p, w_q, w_k, w_v, wq_p, wk_p, wv_p, y_full):
    nb, tokens, wide = g.shape
    dim = y_full.shape[2]
    cols = wide // 3
    rows = tokens // n
    shape = jax.ShapeDtypeStruct
    dma = pltpu.SemaphoreType.DMA
    any_spec = pl.BlockSpec(memory_space=pl.ANY)
    return pl.pallas_call(
        functools.partial(dy_dw_kernel, n, nb, dim), name="dy_dw",
        out_shape=[shape((nb, rows, dim), BF16)] + [shape((dim, cols), BF16)] * 3,
        in_specs=[any_spec] * 9, out_specs=[any_spec] * 4,
        scratch_shapes=Scatter.scratch(nb * rows, dim) + [dma, dma((2, 6)), dma((2,)), dma((2, 3)), dma((nb,))],
        compiler_params=params(collective_id=3, has_side_effects=True),
        cost_estimate=cost(12 * nb * tokens * dim * cols, 30 * nb * tokens * cols),
    )(g, g_p, w_q, w_k, w_v, wq_p, wk_p, wv_p, y_full)


def token_kernel(x_ref, dy_ref, pr_ref, g_ref, m_ref, e_ref, bo_ref, xo_ref, dx_ref, dm_ref):
    mod = m_ref[...] + e_ref[0]
    x = x_ref[0].astype(F32)
    d_out = dy_ref[0].astype(F32)
    proj = pr_ref[0].astype(F32) + bo_ref[...]
    xo_ref[0] = (x + mod[2:3] * proj).astype(BF16)
    x_norm, inv_std = norm_stats(x)
    d_y = g_ref[0].astype(F32)
    d_norm = d_y * (1.0 + mod[1:2])
    d_x = d_out + inv_std * (
        d_norm - jnp.mean(d_norm, axis=-1, keepdims=True) - x_norm * jnp.mean(d_norm * x_norm, axis=-1, keepdims=True))
    dx_ref[0] = d_x.astype(BF16)
    dm_ref[0, 0:1] = jnp.sum(d_y, axis=0, keepdims=True)
    dm_ref[0, 1:2] = jnp.sum(d_y * x_norm, axis=0, keepdims=True)
    dm_ref[0, 2:3] = jnp.sum(d_out * proj, axis=0, keepdims=True)


def token_call(x_loc, dy_loc, proj, d_y, m_block, e_loc, b_o):
    nb, rows, dim = x_loc.shape
    row = pl.BlockSpec((1, rows, dim), lambda i: (i, 0, 0))
    mod = pl.BlockSpec((1, 3, dim), lambda i: (i, 0, 0))
    return pl.pallas_call(
        token_kernel, name="tokens", grid=(nb,),
        out_shape=[jax.ShapeDtypeStruct(x_loc.shape, BF16), jax.ShapeDtypeStruct(x_loc.shape, BF16),
                   jax.ShapeDtypeStruct((nb, 3, dim), F32)],
        in_specs=[row, row, row, row, pl.BlockSpec((3, dim), lambda i: (0, 0)), mod, pl.BlockSpec((1, dim), lambda i: (0, 0))],
        out_specs=[row, row, mod],
        compiler_params=params("arbitrary"),
        cost_estimate=cost(nb * rows * dim * 30, nb * rows * dim * 12),
    )(x_loc, dy_loc, proj, d_y, m_block, e_loc, b_o[None])


def solution(mesh):
    tp_size = mesh.shape['tp']

    def device_step(x_loc, e_loc, m_block, w_q, b_q, w_k, b_k, w_v, b_v, w_o, b_o, g_q, g_k, pos_part, dy_loc):
        nb, _, dim = x_loc.shape
        cos_tab, sin_tab = rope_tables(pos_part)
        y_full, d_own, q, k, v, ss = gather_qkv_call(tp_size, x_loc, dy_loc, m_block, e_loc, w_q, w_k, w_v, b_q, b_k, b_v)
        d_full, o, o_p, d_attn, wq_p, wk_p, wv_p, wo_p = gather_attn_call(
            tp_size, q, k, v, g_q, g_k, cos_tab, sin_tab, ss, w_q, w_k, w_v, w_o, d_own)
        proj, g, g_p, _, _, d_wo, d_gq, d_gk = proj_bwd_call(
            tp_size, q, k, v, d_attn, g_q, g_k, cos_tab, sin_tab, ss, o, o_p, w_o, wo_p, d_full)
        d_y, d_wq, d_wk, d_wv = dy_dw_call(tp_size, g, g_p, w_q, w_k, w_v, wq_p, wk_p, wv_p, y_full)
        x_out, d_x, d_mod = token_call(x_loc, dy_loc, proj, d_y, m_block, e_loc, b_o)
        d_e = all_sum_call(tp_size, d_mod.reshape(tp_size, -1, HEAD_DIM)).reshape(nb, 3, dim)
        return (x_out, d_x, d_e, jnp.sum(d_e, axis=0), d_wq, d_wk, d_wv, d_wo,
                jnp.sum(d_gq, axis=(0, 1)), jnp.sum(d_gk, axis=(0, 1)))

    in_specs = (P('dp', 'tp', None), P('dp', None, None), P(None, None), P(None, 'tp'), P('tp'), P(None, 'tp'), P('tp'),
                P(None, 'tp'), P('tp'), P('tp', None), P(None), P('tp'), P('tp'), P('dp', None), P('dp', 'tp', None))
    out_specs = (P('dp', 'tp', None), P('dp', 'tp', None), P('dp', None, None), P('dp', None), P('dp', 'tp'), P('dp', 'tp'),
                 P('dp', 'tp'), P(('dp', 'tp'), None), P(('dp', 'tp')), P(('dp', 'tp')))
    return jax.shard_map(device_step, mesh=mesh, in_specs=in_specs, out_specs=out_specs, check_vma=False)
```

```python
import functools

import jax
import jax.numpy as jnp
import numpy as np
from jax import lax
from jax.experimental import pallas as pl
from jax.experimental.pallas import tpu as pltpu
from jax.sharding import PartitionSpec as P

HEAD_DIM = 128
EPS_NORM = 1e-6
ROPE_BASE = 10000.0
LOG2E = 1.4426950408889634
CHUNK = 512
VMEM_LIMIT = 60 * 1024 * 1024
F32 = jnp.float32
BF16 = jnp.bfloat16
MESH_ID = pl.DeviceIdType.MESH
NT = (((1,), (1,)), ((), ()))
TN = (((0,), (0,)), ((), ()))


def params(*semantics, **kw):
    return pltpu.CompilerParams(dimension_semantics=semantics or None, vmem_limit_bytes=VMEM_LIMIT, **kw)


def cost(flops, nbytes):
    return pl.CostEstimate(flops=int(flops), bytes_accessed=int(nbytes), transcendentals=0)


def rope_freqs():
    half_dim = HEAD_DIM // 2
    side_len = HEAD_DIM // 6
    first_len = half_dim - 2 * side_len
    pair_idx = np.arange(HEAD_DIM) // 2
    section = (pair_idx >= first_len).astype(np.int32) + (pair_idx >= first_len + side_len).astype(np.int32)
    offset = np.where(section == 0, 0, np.where(section == 1, first_len, first_len + side_len))
    sec_width = np.where(section == 0, first_len, side_len)
    exponent = -(pair_idx - offset).astype(np.float32) / sec_width.astype(np.float32)
    freq_vals = np.power(np.float32(ROPE_BASE), exponent)
    return np.where(section[None, :] == np.arange(3)[:, None], freq_vals[None, :], np.float32(0.0)).astype(np.float32)


def norm_stats(x):
    centered = x - jnp.mean(x, axis=-1, keepdims=True)
    inv_std = lax.rsqrt(jnp.mean(centered * centered, axis=-1, keepdims=True) + EPS_NORM)
    return centered * inv_std, inv_std


def to_row(acc):
    return jnp.sum(acc.T, axis=0, keepdims=True)


def lanes_of(row):
    return jnp.broadcast_to(row, (HEAD_DIM, row.shape[1])).T


def head_sum(values):
    out = values[:, :HEAD_DIM]
    for h in range(1, values.shape[1] // HEAD_DIM):
        out = out + values[:, h * HEAD_DIM:(h + 1) * HEAD_DIM]
    return out


class Place:
    def __init__(self, n):
        self.n = n
        self.me = lax.axis_index('tp')
        self.right = lax.rem(self.me + 2, n)
        self.left = lax.rem(self.me + n - 2, n)
        self.far = lax.rem(self.me + n // 2, n)
        self.chip = self.me // 2

    def partner(self, dev):
        return dev + 1 - 2 * lax.rem(dev, 2)

    def barrier(self, devices):
        sem = pltpu.get_barrier_semaphore()
        for dev in devices:
            pl.semaphore_signal(sem, inc=1, device_id={'tp': dev}, device_id_type=MESH_ID)
        pl.semaphore_wait(sem, len(devices))

    def to_partner(self, src, dst, send_sem, recv_sem):
        return pltpu.make_async_remote_copy(src_ref=src, dst_ref=dst, send_sem=send_sem, recv_sem=recv_sem,
                                            device_id={'tp': self.partner(self.me)}, device_id_type=MESH_ID)

    def everyone(self):
        return [lax.rem(self.me + d, self.n) for d in range(1, self.n)]

    def near(self):
        return [self.right, self.left, self.partner(self.me)]


class Gather:
    def __init__(self, place, full, rows, send, recv):
        self.at, self.full, self.rows, self.send, self.recv = place, full, rows, send, recv

    def part(self, b, dev, off, count):
        return self.full.at[b, pl.ds(pl.multiple_of(dev * self.rows + off, 16), count)]

    def copy(self, b, dev, off, count, s_idx, r_idx, target):
        ref = self.part(b, dev, off, count)
        return pltpu.make_async_remote_copy(src_ref=ref, dst_ref=ref, send_sem=self.send.at[b, s_idx], recv_sem=self.recv.at[b, r_idx],
                                            device_id={'tp': target}, device_id_type=MESH_ID)

    def start_own(self, b):
        p = self.at
        self.copy(b, p.me, 0, self.rows, 0, 0, p.right).start()
        self.copy(b, p.me, 0, self.rows, 1, 1, p.left).start()
        self.copy(b, p.me, 0, self.rows, 2, 4, p.partner(p.me)).start()

    def take_own(self, b):
        p = self.at
        self.copy(b, p.partner(p.me), 0, self.rows, 2, 4, p.me).wait_recv()

    def take_left(self, b):
        p, half = self.at, self.rows // 2
        self.copy(b, p.left, 0, self.rows, 0, 0, p.me).wait_recv()
        self.copy(b, p.left, 0, half, 3, 2, p.right).start()
        self.copy(b, p.left, 0, self.rows, 5, 5, p.partner(p.me)).start()
        self.copy(b, p.partner(p.left), 0, self.rows, 5, 5, p.me).wait_recv()

    def take_right(self, b):
        p, half = self.at, self.rows // 2
        self.copy(b, p.right, 0, self.rows, 1, 1, p.me).wait_recv()
        self.copy(b, p.right, half, half, 4, 3, p.left).start()
        self.copy(b, p.right, 0, self.rows, 6, 6, p.partner(p.me)).start()
        self.copy(b, p.partner(p.right), 0, self.rows, 6, 6, p.me).wait_recv()

    def take_far(self, b):
        p, half = self.at, self.rows // 2
        self.copy(b, p.far, 0, half, 3, 2, p.me).wait_recv()
        self.copy(b, p.far, 0, half, 7, 7, p.partner(p.me)).start()
        self.copy(b, p.far, half, half, 4, 3, p.me).wait_recv()
        self.copy(b, p.far, half, half, 8, 8, p.partner(p.me)).start()
        self.copy(b, p.partner(p.far), 0, half, 7, 7, p.me).wait_recv()
        self.copy(b, p.partner(p.far), half, half, 8, 8, p.me).wait_recv()

    def finish(self, b):
        p, half = self.at, self.rows // 2
        for s_idx, count in ((0, self.rows), (1, self.rows), (2, self.rows), (3, half), (4, half), (5, self.rows), (6, self.rows), (7, half), (8, half)):
            self.copy(b, p.me, 0, count, s_idx, s_idx, p.me).wait_send()

    def item_place(self, i, nb):
        j = i - nb
        b = jnp.where(i < nb, i, jnp.where(i < 3 * nb, j // 2, i - 3 * nb))
        chips = self.at.n // 2
        side = jnp.where(lax.rem(j + 2 * nb, 2) == 0, chips - 1, 1)
        off = jnp.where(i < nb, 0, jnp.where(i < 3 * nb, side, chips // 2))
        return b, pl.multiple_of(lax.rem(self.at.chip + off, chips) * (2 * self.rows), 32)

    def take_item(self, i, nb):
        b, row0 = self.item_place(i, nb)
        odd = lax.rem(i + nb, 2)
        pl.when(i < nb)(lambda: self.take_own(b))
        pl.when((i >= nb) & (i < 3 * nb) & (odd == 0))(lambda: self.take_left(b))
        pl.when((i >= nb) & (i < 3 * nb) & (odd == 1))(lambda: self.take_right(b))
        pl.when(i >= 3 * nb)(lambda: self.take_far(b))
        return b, row0


GATHER_SEMS = 9


def chunks_of(width, step):
    return [(c, min(c + step, width)) for c in range(0, width, step)]


class Exchange:
    def __init__(self, place, x_ref, slots, send_sems, recv_sems):
        self.at, self.x, self.slots, self.send, self.recv = place, x_ref, slots, send_sems, recv_sems

    def copy(self, d, dev, src):
        return pltpu.make_async_remote_copy(src_ref=self.x, dst_ref=self.slots.at[src], send_sem=self.send.at[d], recv_sem=self.recv.at[src],
                                            device_id={'tp': dev}, device_id_type=MESH_ID)

    def start(self):
        for d, dev in enumerate(self.at.everyone()):
            self.copy(d, dev, self.at.me).start()
        self.slots[self.at.me] = self.x[...]

    def finish(self):
        for d, dev in enumerate(self.at.everyone()):
            self.copy(d, dev, dev).wait()
        total = self.slots[0]
        for d in range(1, self.at.n):
            total = total + self.slots[d]
        return total


def gather_qkv_kernel(n, x_ref, dy_ref, m_ref, e_ref, wq_ref, wk_ref, wv_ref, bq_ref, bk_ref, bv_ref, gq_ref, gk_ref, pos_ref, freq_ref,
                      y_full, d_full, q_out, k_out, v_out, ss_ref, cos_ref, sin_ref, gain_ref,
                      bias_ref, w_all, xin, stage, xbuf, zst, vst, sq, ss_row, slots,
                      w_sem, in_sem, st_sem, ld_sem, out_sem, g_send, g_recv, e_send, e_recv):
    nb, rows, dim = x_ref.shape
    cols = wq_ref.shape[1]
    place = Place(n)
    gather = Gather(place, y_full, rows, g_send, g_recv)
    w_copies = [pltpu.make_async_copy(w, w_all.at[:, pl.ds(j * cols, cols)], w_sem.at[j]) for j, w in enumerate((wq_ref, wk_ref, wv_ref))]
    load_x = pltpu.make_async_copy(x_ref, xin, in_sem)
    load_x.start()
    for c in w_copies:
        c.start()
    group = 16

    def mine(full, b):
        return full.at[b, pl.ds(pl.multiple_of(place.me * rows, 16), rows)]

    load_x.wait()
    place.barrier(place.everyone())

    def ln_step(b, _):
        shift = m_ref[0:1] + e_ref[b, 0:1]
        scale_one = 1.0 + (m_ref[1:2] + e_ref[b, 1:2])

        def ln_rows(r, _):
            sl = pl.ds(pl.multiple_of(r * group, group), group)
            x_norm, _ = norm_stats(xin[b, sl].astype(F32))
            stage[b, sl] = (x_norm * scale_one + shift).astype(BF16)
            return 0

        lax.fori_loop(0, rows // group, ln_rows, 0)
        out = pltpu.make_async_copy(stage.at[b], mine(y_full, b), st_sem)
        out.start()
        out.wait()
        gather.start_own(b)
        return 0

    lax.fori_loop(0, nb, ln_step, 0)
    load_dy = pltpu.make_async_copy(dy_ref, xin, in_sem)
    load_dy.start()
    for j, ref in enumerate((bq_ref, bk_ref, bv_ref)):
        bias_ref[:, j * cols:(j + 1) * cols] = ref[...].reshape(1, cols)
    for j, ref in enumerate((gq_ref, gk_ref)):
        gain_ref[j:j + 1] = ref[...].reshape(1, cols)

    def tables():
        lane = lax.broadcasted_iota(jnp.int32, (128, HEAD_DIM), 1)

        def rows_of(r, _):
            sl = pl.ds(pl.multiple_of(r * 128, 128), 128)
            pos = pos_ref[sl].astype(F32)
            angle = pos[:, 0:1] * freq_ref[0:1] + pos[:, 1:2] * freq_ref[1:2] + pos[:, 2:3] * freq_ref[2:3]
            cos_ref[sl] = jnp.cos(angle)
            sin_ref[sl] = jnp.where(lane % 2 == 0, -1.0, 1.0) * jnp.sin(angle)
            return 0

        lax.fori_loop(0, pos_ref.shape[0] // 128, rows_of, 0)

    def gate_step(b, _):
        gate = m_ref[2:3] + e_ref[b, 2:3]

        def gate_rows(r, _):
            sl = pl.ds(pl.multiple_of(r * group, group), group)
            stage[b, sl] = (xin[b, sl].astype(F32) * gate).astype(BF16)
            return 0

        lax.fori_loop(0, rows // group, gate_rows, 0)
        out = pltpu.make_async_copy(stage.at[b], mine(d_full, b), st_sem)
        out.start()
        out.wait()
        return 0

    for c in w_copies:
        c.wait()

    def outputs(b, row0, slot):
        dst = pl.ds(row0, 2 * rows)
        return [pltpu.make_async_copy(zst.at[slot, :, pl.ds(0, cols)], q_out.at[b, dst], out_sem.at[slot, 0]),
                pltpu.make_async_copy(zst.at[slot, :, pl.ds(cols, cols)], k_out.at[b, dst], out_sem.at[slot, 1]),
                pltpu.make_async_copy(vst.at[slot], v_out.at[b, dst], out_sem.at[slot, 2])]

    def item(i, _):
        b, row0 = gather.take_item(i, nb)
        slot = lax.rem(i, 2)
        load = pltpu.make_async_copy(y_full.at[b, pl.ds(row0, 2 * rows)], xbuf, ld_sem)
        load.start()

        @pl.when(i == nb)
        def _():
            load_dy.wait()
            lax.fori_loop(0, nb, gate_step, 0)
            tables()

        @pl.when(i >= 2)
        def _():
            for c in outputs(0, 0, slot):
                c.wait()

        load.wait()
        for lo, hi in chunks_of(3 * cols, 512):
            zst[slot, :, lo:hi] = jnp.dot(xbuf[...], w_all[:, lo:hi], preferred_element_type=F32) + bias_ref[:, lo:hi]
        vst[slot] = zst[slot, :, 2 * cols:].astype(BF16)
        q = zst[slot, :, :cols]
        k = zst[slot, :, cols:2 * cols]
        sq[2 * b, pl.ds(row0, 2 * rows)] = head_sum(q * q)
        sq[2 * b + 1, pl.ds(row0, 2 * rows)] = head_sum(k * k)
        for c in outputs(b, row0, slot):
            c.start()
        return 0

    lax.fori_loop(0, 4 * nb, item, 0)
    ss_row[...] = jnp.zeros_like(ss_row)
    for j in range(2 * nb):
        ss_row[j:j + 1] = to_row(sq[j])
    sums = Exchange(place, ss_row, slots, e_send, e_recv)
    sums.start()
    for slot in range(2):
        for c in outputs(0, 0, slot):
            c.wait()
    for b in range(nb):
        gather.finish(b)
    ss_ref[...] = sums.finish()


def gather_qkv_call(n, x_loc, dy_loc, m_block, e_loc, w_q, w_k, w_v, b_q, b_k, b_v, g_q, g_k, positions):
    nb, rows, dim = x_loc.shape
    cols = w_q.shape[1]
    tokens = rows * n
    shape = jax.ShapeDtypeStruct
    any_spec = pl.BlockSpec(memory_space=pl.ANY)
    vmem = pl.BlockSpec(memory_space=pltpu.VMEM)
    dma = pltpu.SemaphoreType.DMA
    stat_rows = -(-2 * nb // 8) * 8
    return pl.pallas_call(
        functools.partial(gather_qkv_kernel, n), name="gather_qkv",
        out_shape=[shape((nb, tokens, dim), BF16), shape((nb, tokens, dim), BF16), shape((nb, tokens, cols), F32),
                   shape((nb, tokens, cols), F32), shape((nb, tokens, cols), BF16), shape((stat_rows, tokens), F32),
                   shape((tokens, HEAD_DIM), F32), shape((tokens, HEAD_DIM), F32), shape((2, cols), F32)],
        in_specs=[any_spec, any_spec, vmem, vmem, any_spec, any_spec, any_spec] + [vmem] * 7,
        out_specs=[any_spec] * 5 + [vmem] * 4,
        scratch_shapes=[
            pltpu.VMEM((1, 3 * cols), F32),
            pltpu.VMEM((dim, 3 * cols), BF16), pltpu.VMEM((nb, rows, dim), BF16), pltpu.VMEM((nb, rows, dim), BF16),
            pltpu.VMEM((2 * rows, dim), BF16), pltpu.VMEM((2, 2 * rows, 3 * cols), F32), pltpu.VMEM((2, 2 * rows, cols), BF16),
            pltpu.VMEM((2 * nb, tokens, HEAD_DIM), F32), pltpu.VMEM((stat_rows, tokens), F32), pltpu.VMEM((n, stat_rows, tokens), F32),
            dma((3,)), dma, dma, dma, dma((2, 3)), dma((nb, GATHER_SEMS)), dma((nb, GATHER_SEMS)), dma((n,)), dma((n,))],
        compiler_params=params(collective_id=0, has_side_effects=True),
        cost_estimate=cost(6 * nb * tokens * dim * cols, 6 * dim * cols + 14 * nb * tokens * cols),
    )(x_loc, dy_loc, m_block, e_loc, w_q, w_k, w_v, b_q, b_k, b_v, g_q, g_k, positions, jnp.asarray(rope_freqs()))


def all_sum_kernel(n, x_ref, o_ref, pieces, total, send_a, recv_a, send_b, recv_b):
    place = Place(n)
    me = place.me
    place.barrier(place.everyone())

    def first(d, dev, src):
        return pltpu.make_async_remote_copy(src_ref=x_ref.at[src], dst_ref=pieces.at[me], send_sem=send_a.at[d], recv_sem=recv_a.at[me],
                                            device_id={'tp': dev}, device_id_type=MESH_ID)

    for d, dev in enumerate(place.everyone()):
        first(d, dev, dev).start()
    pieces[me] = x_ref[me]
    for d, dev in enumerate(place.everyone()):
        pltpu.make_async_remote_copy(src_ref=x_ref.at[me], dst_ref=pieces.at[dev], send_sem=send_a.at[d], recv_sem=recv_a.at[dev],
                                     device_id={'tp': dev}, device_id_type=MESH_ID).wait_recv()
    acc = pieces[0]
    for d in range(1, n):
        acc = acc + pieces[d]
    total[...] = acc
    o_ref[me] = acc
    for d, dev in enumerate(place.everyone()):
        first(d, dev, dev).wait_send()
    for d, dev in enumerate(place.everyone()):
        pltpu.make_async_remote_copy(src_ref=total, dst_ref=o_ref.at[me], send_sem=send_b.at[d], recv_sem=recv_b.at[me],
                                     device_id={'tp': dev}, device_id_type=MESH_ID).start()
    for d, dev in enumerate(place.everyone()):
        copy = pltpu.make_async_remote_copy(src_ref=total, dst_ref=o_ref.at[dev], send_sem=send_b.at[d], recv_sem=recv_b.at[dev],
                                            device_id={'tp': dev}, device_id_type=MESH_ID)
        copy.wait_send()
        copy.wait_recv()


def all_sum_call(n, x):
    spec = pl.BlockSpec(memory_space=pltpu.VMEM)
    dma = pltpu.SemaphoreType.DMA
    return pl.pallas_call(
        functools.partial(all_sum_kernel, n), name="all_sum",
        out_shape=jax.ShapeDtypeStruct(x.shape, x.dtype), in_specs=[spec], out_specs=spec,
        scratch_shapes=[pltpu.VMEM(x.shape, x.dtype), pltpu.VMEM(x.shape[1:], x.dtype), dma((n,)), dma((n,)), dma((n,)), dma((n,))],
        compiler_params=pltpu.CompilerParams(collective_id=4, has_side_effects=True, vmem_limit_bytes=4 * 1024 * 1024),
        cost_estimate=cost(4_000_000_000, x.size * 8),
    )(x)


def swap_pairs(x):
    lane = lax.broadcasted_iota(jnp.int32, x.shape, 1)
    return jnp.where(lane % 2 == 0, pltpu.roll(x, HEAD_DIM - 1, 1), pltpu.roll(x, 1, 1))


def rotate(x, cos, sin):
    return x * cos + swap_pairs(x) * sin


def softmax_block(s):
    c = HEAD_DIM ** -0.5 * LOG2E
    top = jnp.max(s, axis=1, keepdims=True)
    p = jnp.exp2(s * c - top * c)
    return p * (1.0 / jnp.sum(p, axis=1, keepdims=True))


def gather_attn_kernel(n, nb, heads, dim, q_ref, k_ref, v_ref, gain_ref, cos_ref, sin_ref, ss_ref,
                       wq_ref, wk_ref, wv_ref, wo_ref, d_in,
                       d_full, o_out, o_p, da_out, wq_p, wk_p, wv_p, wo_p,
                       inv_q, inv_k, o_all, wo, xbuf, ast,
                       w_sem, ld_sem, out_sem, o_sem, g_send, g_recv, t_send, t_recv):
    step = pl.program_id(0)
    tokens = q_ref.shape[1]
    rows = tokens // n
    blk = min(256, tokens)
    place = Place(n)
    gather = Gather(place, d_full, rows, g_send, g_recv)
    pairs = ((wo_ref, wo_p), (wq_ref, wq_p), (wk_ref, wk_p), (wv_ref, wv_p), (o_out, o_p))

    def trade(j):
        return place.to_partner(*pairs[j], t_send.at[j], t_recv.at[j])


    @pl.when(step == 0)
    def _():
        pltpu.make_async_copy(wo_ref, wo, w_sem).start()
        place.barrier(place.near())

        def own(b, _):
            gather.start_own(b)
            return 0

        lax.fori_loop(0, nb, own, 0)
        for j in range(4):
            trade(j).start()

    @pl.when(step < nb * heads)
    def _():
        b = step // heads
        h = lax.rem(step, heads)

        @pl.when(h == 0)
        def _():
            inv_q[...] = lanes_of(lax.rsqrt(ss_ref[pl.ds(2 * b, 1)] / dim + EPS_NORM))
            inv_k[...] = lanes_of(lax.rsqrt(ss_ref[pl.ds(2 * b + 1, 1)] / dim + EPS_NORM))

        cos, sin = cos_ref[...], sin_ref[...]
        q_rot = rotate(q_ref[0] * inv_q[...] * gain_ref[0:1], cos, sin).astype(BF16)
        k_rot = rotate(k_ref[0] * inv_k[...] * gain_ref[1:2], cos, sin).astype(BF16)
        v = v_ref[0]
        lanes = pl.ds(pl.multiple_of(h * HEAD_DIM, HEAD_DIM), HEAD_DIM)
        for i in range(tokens // blk):
            s = lax.dot_general(q_rot[i * blk:(i + 1) * blk], k_rot, NT, preferred_element_type=F32)
            p = softmax_block(s).astype(BF16)
            o_all[b, i * blk:(i + 1) * blk, lanes] = jnp.dot(p, v, preferred_element_type=F32).astype(BF16)

    @pl.when(step == nb * heads)
    def _():
        o_copy = pltpu.make_async_copy(o_all, o_out, o_sem)
        o_copy.start()
        pltpu.make_async_copy(wo_ref, wo, w_sem).wait()

        def outputs(b, row0, slot):
            return pltpu.make_async_copy(ast.at[slot], da_out.at[b, pl.ds(row0, 2 * rows)], out_sem.at[slot])

        def load(b, row0, slot):
            return pltpu.make_async_copy(d_full.at[b, pl.ds(row0, 2 * rows)], xbuf.at[slot], ld_sem.at[slot])

        def take(i):
            b, row0 = gather.take_item(i, nb)
            load(b, row0, lax.rem(i, 2)).start()

        take(0)

        def item(i, _):
            slot = lax.rem(i, 2)

            @pl.when(i + 1 < 3 * nb)
            def _():
                take(i + 1)

            @pl.when(i >= 2)
            def _():
                outputs(0, 0, slot).wait()

            load(0, 0, slot).wait()
            ast[slot] = lax.dot_general(xbuf[slot], wo[...], NT, preferred_element_type=F32).astype(BF16)
            b, row0 = gather.item_place(i, nb)
            outputs(b, row0, slot).start()

            @pl.when(i == 0)
            def _():
                o_copy.wait()
                trade(4).start()

            @pl.when((i + 1 >= 3 * nb) & (i + 1 < 4 * nb))
            def _():
                take(i + 1)

            return 0

        lax.fori_loop(0, 4 * nb, item, 0)
        for slot in range(2):
            outputs(0, 0, slot).wait()
        for b in range(nb):
            gather.finish(b)
        for j in range(5):
            trade(j).wait()


def gather_attn_call(n, q, k, v, gains, cos_tab, sin_tab, ss, w_q, w_k, w_v, w_o, d_full):
    nb, tokens, cols = q.shape
    dim = w_o.shape[1]
    heads = cols // HEAD_DIM
    rows = tokens // n
    last = nb * heads - 1
    shape = jax.ShapeDtypeStruct
    dma = pltpu.SemaphoreType.DMA
    any_spec = pl.BlockSpec(memory_space=pl.ANY)

    def head_of(i):
        i = jnp.minimum(i, last)
        return i // heads, i % heads

    blk = pl.BlockSpec((1, tokens, HEAD_DIM), lambda i: (head_of(i)[0], 0, head_of(i)[1]))
    vec = pl.BlockSpec((2, HEAD_DIM), lambda i: (0, head_of(i)[1]))
    tab = pl.BlockSpec((tokens, HEAD_DIM), lambda i: (0, 0))
    head_arr = shape((nb, tokens, cols), BF16)
    return pl.pallas_call(
        functools.partial(gather_attn_kernel, n, nb, heads, dim), name="gather_attn", grid=(nb * heads + 1,),
        out_shape=[shape(d_full.shape, BF16), head_arr, head_arr, head_arr] + [shape(w.shape, BF16) for w in (w_q, w_k, w_v, w_o)],
        in_specs=[blk, blk, blk, vec, tab, tab, pl.BlockSpec(ss.shape, lambda i: (0, 0))] + [any_spec] * 5,
        out_specs=[any_spec] * 8,
        scratch_shapes=[
            pltpu.VMEM((tokens, HEAD_DIM), F32), pltpu.VMEM((tokens, HEAD_DIM), F32), pltpu.VMEM((nb, tokens, cols), BF16),
            pltpu.VMEM((cols, dim), BF16), pltpu.VMEM((2, 2 * rows, dim), BF16), pltpu.VMEM((2, 2 * rows, cols), BF16),
            dma, dma((2,)), dma((2,)), dma, dma((nb, GATHER_SEMS)), dma((nb, GATHER_SEMS)), dma((5,)), dma((5,))],
        input_output_aliases={11: 0},
        compiler_params=params("arbitrary", collective_id=1, has_side_effects=True),
        cost_estimate=cost(2 * nb * tokens * dim * cols + 4 * nb * tokens * tokens * cols, 8 * nb * tokens * dim),
    )(q, k, v, gains, cos_tab, sin_tab, ss, w_q, w_k, w_v, w_o, d_full)


class Scatter:
    def __init__(self, place, part, recv_far, recv_side, send, recv):
        self.at, self.part, self.far, self.side, self.send, self.recv = place, part, recv_far, recv_side, send, recv
        self.rows = part.shape[2]
        self.half = self.rows // 2

    def copy(self, j, idx, src, dst, target):
        return pltpu.make_async_remote_copy(src_ref=src, dst_ref=dst, send_sem=self.send.at[j, idx], recv_sem=self.recv.at[j, idx],
                                            device_id={'tp': target}, device_id_type=MESH_ID)

    def message(self, j, idx):
        p, part, far, side = self.at, self.part, self.far, self.side
        first, second = pl.ds(0, self.half), pl.ds(self.half, self.rows - self.half)
        src, dst, target = (
            lambda: (part.at[j, 0, first], far.at[j, 0], p.right),
            lambda: (part.at[j, 0, second], far.at[j, 1], p.left),
            lambda: (part.at[j, 1, second], side.at[j, 0, second], p.right),
            lambda: (part.at[j, 2, first], side.at[j, 1, first], p.left),
            lambda: (part.at[j, 1, first], side.at[j, 0, first], p.right),
            lambda: (part.at[j, 2, second], side.at[j, 1, second], p.left))[idx]()
        return self.copy(j, idx, src, dst, target)

    def start_far(self, j):
        for idx in (0, 1):
            self.message(j, idx).start()

    def start_side(self, j, _):
        for idx in (2, 3):
            self.message(j, idx).start()
        return 0

    def sums(self, j):
        h = self.half
        self.message(j, 0).wait_recv()
        self.part[j, 1, :h] = (self.part[j, 1, :h].astype(F32) + self.far[j, 0].astype(F32)).astype(BF16)
        self.message(j, 1).wait_recv()
        self.part[j, 2, h:] = (self.part[j, 2, h:].astype(F32) + self.far[j, 1].astype(F32)).astype(BF16)
        self.message(j, 4).start()
        self.message(j, 5).start()

    def final(self, j):
        for idx in range(2, 6):
            self.message(j, idx).wait_recv()
        total = self.part[j, 3].astype(F32) + self.side[j, 0].astype(F32) + self.side[j, 1].astype(F32)
        self.part[j, 3] = total.astype(BF16)

    def finish(self, j):
        for idx in range(6):
            self.message(j, idx).wait_send()

    @staticmethod
    def scratch(rows, dim):
        nc, dma = dim // CHUNK, pltpu.SemaphoreType.DMA
        return [pltpu.VMEM((nc, 4, rows, CHUNK), BF16), pltpu.VMEM((nc, 2, rows // 2, CHUNK), BF16),
                pltpu.VMEM((nc, 2, rows, CHUNK), BF16), dma((nc, 6)), dma((nc, 6))]


def scatter_outputs(part, out, sem, j):
    nb, rows, _ = out.shape
    cs = pl.ds(pl.multiple_of(j * CHUNK, CHUNK), CHUNK)
    return [pltpu.make_async_copy(part.at[j, 3, pl.ds(b * rows, rows)], out.at[b, :, cs], sem.at[b]) for b in range(nb)]


def scatter_end(scatter, out, sem, nc):
    def last(j, _):
        scatter.final(j)
        for c in scatter_outputs(scatter.part, out, sem, j):
            c.start()
        return 0

    lax.fori_loop(0, nc, last, 0)

    def drain(j, _):
        for c in scatter_outputs(scatter.part, out, sem, j):
            c.wait()
        scatter.finish(j)
        return 0

    lax.fori_loop(0, nc, drain, 0)


def pair_rows(place, nb, rows, mine, theirs, lhs, sem):
    width = mine.shape[2]
    out = []
    for d, dev in enumerate((place.far, place.right, place.left, place.me)):
        src_rows = pl.ds(pl.multiple_of(dev * rows, 16), rows)
        for b in range(nb):
            dst_rows = pl.ds((d * nb + b) * rows, rows)
            for j, src in enumerate((mine, theirs)):
                out.append(pltpu.make_async_copy(src.at[b, src_rows], lhs.at[dst_rows, pl.ds(j * width, width)], sem))
    return out


def proj_bwd_kernel(n, nb, heads, dim, q_ref, k_ref, v_ref, do_ref, gain_ref, cos_ref, sin_ref, ss_ref,
                    q_hbm, k_hbm, o_hbm, o_p, wo_hbm, wo_p, d_full,
                    proj_out, g_out, g_p, dqs_out, dks_out, dwo_out, dgq_ref, dgk_ref,
                    part, recv_far, recv_side, s_send, s_recv,
                    inv_q, inv_k, acc_q, acc_k, p_all, ds_all, dq_all, qs_st, ks_st, v_st, st_row, st_sum, slots,
                    ld_sem, w_sem, fl_sem, g_sem, go_sem, out_sem, e_send, e_recv, t_send, t_recv):
    step = pl.program_id(0)
    tokens = q_ref.shape[1]
    rows = tokens // n
    cols = heads * HEAD_DIM
    blk = min(256, tokens)
    nc = dim // CHUNK
    steps = nb * heads
    scale = HEAD_DIM ** -0.5
    place = Place(n)
    scatter = Scatter(place, part, recv_far, recv_side, s_send, s_recv)

    @pl.when(step == 0)
    def _():
        def project(lhs, wbuf):
            loads = pair_rows(place, nb, rows, o_hbm, o_p, lhs, ld_sem.at[0])
            for c in loads:
                c.start()

            def chunk(j):
                cs = pl.ds(pl.multiple_of(j * CHUNK, CHUNK), CHUNK)
                slot = lax.rem(j, 2)
                return [pltpu.make_async_copy(wo_hbm.at[:, cs], wbuf.at[slot, pl.ds(0, cols)], w_sem.at[slot, 0]),
                        pltpu.make_async_copy(wo_p.at[:, cs], wbuf.at[slot, pl.ds(cols, cols)], w_sem.at[slot, 1])]

            for c in chunk(0):
                c.start()
            place.barrier(place.everyone())
            for c in loads:
                c.wait()

            def body(j, _):
                @pl.when(j + 1 < nc)
                def _():
                    for c in chunk(j + 1):
                        c.start()

                for c in chunk(j):
                    c.wait()
                w = wbuf[lax.rem(j, 2)]
                half = 2 * nb * rows
                for d in range(2):
                    z = jnp.dot(lhs[d * half:(d + 1) * half], w, preferred_element_type=F32).astype(BF16)
                    part[j, 2 * d] = z[:half // 2]
                    part[j, 2 * d + 1] = z[half // 2:]
                scatter.start_far(j)
                return 0

            lax.fori_loop(0, nc, body, 0)

        pl.run_scoped(project, pltpu.VMEM((4 * nb * rows, 2 * cols), BF16), pltpu.VMEM((2, 2 * cols, CHUNK), BF16))

    def flush(b, h, slot):
        lanes = pl.ds(pl.multiple_of(h * HEAD_DIM, HEAD_DIM), HEAD_DIM)
        v_lanes = pl.ds(pl.multiple_of(2 * cols + h * HEAD_DIM, HEAD_DIM), HEAD_DIM)
        return [pltpu.make_async_copy(qs_st.at[slot], dqs_out.at[b, :, lanes], fl_sem.at[slot, 0]),
                pltpu.make_async_copy(ks_st.at[slot], dks_out.at[b, :, lanes], fl_sem.at[slot, 1]),
                pltpu.make_async_copy(v_st.at[slot], g_out.at[b, :, v_lanes], fl_sem.at[slot, 2])]

    for j in range(nc):
        at_step = 1 + j * (steps - 1) // max(nc - 1, 1)
        pl.when(step == at_step)(functools.partial(scatter.sums, j))

    @pl.when((step >= 1) & (step <= steps))
    def _():
        b = (step - 1) // heads
        head = lax.rem(step - 1, heads)
        slot = lax.rem(step, 2)

        @pl.when(step == 1)
        def _():
            st_row[...] = jnp.zeros_like(st_row)

        @pl.when(head == 0)
        def _():
            inv_q[...] = lanes_of(lax.rsqrt(ss_ref[pl.ds(2 * b, 1)] / dim + EPS_NORM))
            inv_k[...] = lanes_of(lax.rsqrt(ss_ref[pl.ds(2 * b + 1, 1)] / dim + EPS_NORM))
            acc_q[...] = jnp.zeros_like(acc_q)
            acc_k[...] = jnp.zeros_like(acc_k)

        @pl.when(step >= 3)
        def _():
            for c in flush(0, 0, slot):
                c.wait()

        cos, sin = cos_ref[...], sin_ref[...]
        q_rot = rotate(q_ref[0] * inv_q[...] * gain_ref[0:1], cos, sin).astype(BF16)
        k_rot = rotate(k_ref[0] * inv_k[...] * gain_ref[1:2], cos, sin).astype(BF16)
        v = v_ref[0]
        do = do_ref[0]
        for i in range(tokens // blk):
            sl = slice(i * blk, (i + 1) * blk)
            p = softmax_block(lax.dot_general(q_rot[sl], k_rot, NT, preferred_element_type=F32))
            p_all[sl] = p.astype(BF16)
            dp = lax.dot_general(do[sl], v, NT, preferred_element_type=F32)
            delta = jnp.sum(dp * p, axis=1, keepdims=True)
            ds = (p * (dp - delta)).astype(BF16)
            ds_all[sl] = ds
            dq_all[sl] = jnp.dot(ds, k_rot, preferred_element_type=F32) * scale
        do_t = do.astype(F32).T.astype(BF16)
        q_t = q_rot.astype(F32).T.astype(BF16)
        v_st[slot] = jnp.dot(do_t, p_all[...], preferred_element_type=F32).T.astype(BF16)
        dk_rot = (jnp.dot(q_t, ds_all[...], preferred_element_type=F32) * scale).T.astype(BF16).astype(F32)
        dq_rot = dq_all[...].astype(BF16).astype(F32)
        dq_hat = rotate(dq_rot, cos, -sin)
        dk_hat = rotate(dk_rot, cos, -sin)
        q_hat = q_ref[0] * inv_q[...]
        k_hat = k_ref[0] * inv_k[...]
        dgq_ref[0] = jnp.sum(dq_hat * q_hat, axis=0, keepdims=True)
        dgk_ref[0] = jnp.sum(dk_hat * k_hat, axis=0, keepdims=True)
        dq_s = dq_hat * gain_ref[0:1]
        dk_s = dk_hat * gain_ref[1:2]
        qs_st[slot] = dq_s
        ks_st[slot] = dk_s
        acc_q[...] += dq_s * q_hat
        acc_k[...] += dk_s * k_hat
        for c in flush(b, head, slot):
            c.start()

        @pl.when(head == heads - 1)
        def _():
            st_row[pl.ds(2 * b, 1)] = to_row(acc_q[...])
            st_row[pl.ds(2 * b + 1, 1)] = to_row(acc_k[...])

    @pl.when(step == steps + 1)
    def _():
        for s in (steps - 1, steps):
            for c in flush(0, 0, s % 2):
                c.wait()
        stats = Exchange(place, st_row, slots, e_send, e_recv)
        stats.start()
        lax.fori_loop(0, nc, scatter.start_side, 0)
        st_sum[...] = stats.finish()
        rb = min(256, tokens)
        per = tokens // rb
        trade = place.to_partner(g_out, g_p, t_send, t_recv)

        def norm_grad(fbuf, gbuf):
            def loads(i, slot):
                b, r0 = i // per, pl.multiple_of(lax.rem(i, per) * rb, rb)
                return [pltpu.make_async_copy(src.at[b, pl.ds(r0, rb)], fbuf.at[slot, m], g_sem.at[slot, m])
                        for m, src in enumerate((dqs_out, q_hbm, dks_out, k_hbm))]

            def store(i, slot):
                b, r0 = i // per, pl.multiple_of(lax.rem(i, per) * rb, rb)
                return pltpu.make_async_copy(gbuf.at[slot], g_out.at[b, pl.ds(r0, rb), pl.ds(0, 2 * cols)], go_sem.at[slot])

            for c in loads(0, 0):
                c.start()

            def body(i, _):
                slot = lax.rem(i, 2)
                b, r0 = i // per, pl.multiple_of(lax.rem(i, per) * rb, rb)

                @pl.when(i + 1 < nb * per)
                def _():
                    for c in loads(i + 1, lax.rem(i + 1, 2)):
                        c.start()

                @pl.when(r0 == 0)
                def _():
                    inv_q[...] = lanes_of(lax.rsqrt(ss_ref[pl.ds(2 * b, 1)] / dim + EPS_NORM))
                    inv_k[...] = lanes_of(lax.rsqrt(ss_ref[pl.ds(2 * b + 1, 1)] / dim + EPS_NORM))
                    acc_q[...] = lanes_of(st_sum[pl.ds(2 * b, 1)] / dim)
                    acc_k[...] = lanes_of(st_sum[pl.ds(2 * b + 1, 1)] / dim)

                @pl.when(i >= 2)
                def _():
                    store(0, slot).wait()

                for c in loads(i, slot):
                    c.wait()
                sl = pl.ds(r0, rb)
                for m, (inv, st) in enumerate(((inv_q, acc_q), (inv_k, acc_k))):
                    inv_l, st_l = inv[sl], st[sl]
                    for h in range(heads):
                        hs = slice(h * HEAD_DIM, (h + 1) * HEAD_DIM)
                        grad = inv_l * (fbuf[slot, 2 * m, :, hs] - (fbuf[slot, 2 * m + 1, :, hs] * inv_l) * st_l)
                        gbuf[slot, :, m * cols + h * HEAD_DIM:m * cols + (h + 1) * HEAD_DIM] = grad.astype(BF16)
                store(i, slot).start()
                return 0

            lax.fori_loop(0, nb * per, body, 0)
            for s in range(min(2, nb * per)):
                store(0, s).wait()

        pl.run_scoped(norm_grad, pltpu.VMEM((2, 4, rb, cols), F32), pltpu.VMEM((2, rb, 2 * cols), BF16))
        trade.start()

        def weight_grad(turned, obuf, dbuf, wst):
            bn = min(512, dim)
            n_chunks = dim // bn

            def chunk(c):
                slot = lax.rem(c, 2)
                return pltpu.make_async_copy(d_full.at[:, :, pl.ds(pl.multiple_of(c * bn, bn), bn)], dbuf.at[slot], go_sem.at[slot])

            def store(c):
                slot = lax.rem(c, 2)
                return pltpu.make_async_copy(wst.at[slot], dwo_out.at[:, pl.ds(pl.multiple_of(c * bn, bn), bn)], w_sem.at[slot, 0])

            load_o = pltpu.make_async_copy(o_hbm, obuf, ld_sem.at[0])
            load_o.start()
            chunk(0).start()
            load_o.wait()
            for b in range(nb):
                turned[:, b * tokens:(b + 1) * tokens] = obuf[b].T

            def body(c, _):
                slot = lax.rem(c, 2)

                @pl.when(c + 1 < n_chunks)
                def _():
                    chunk(c + 1).start()

                @pl.when(c >= 2)
                def _():
                    store(c).wait()

                chunk(c).wait()
                d = dbuf[slot].reshape(nb * tokens, bn)
                wst[slot] = jnp.dot(turned[...], d, preferred_element_type=F32).astype(BF16)
                store(c).start()
                return 0

            lax.fori_loop(0, n_chunks, body, 0)
            for s in range(min(2, n_chunks)):
                store(s).wait()

        bn = min(512, dim)
        pl.run_scoped(weight_grad, pltpu.VMEM((cols, nb * tokens), BF16), pltpu.VMEM((nb, tokens, cols), BF16),
                      pltpu.VMEM((2, nb, tokens, bn), BF16), pltpu.VMEM((2, cols, bn), BF16))
        scatter_end(scatter, proj_out, out_sem, nc)
        trade.wait()


def proj_bwd_call(n, q, k, v, d_attn, gains, cos_tab, sin_tab, ss, o, o_p, w_o, wo_p, d_full):
    nb, tokens, cols = q.shape
    dim = w_o.shape[1]
    heads = cols // HEAD_DIM
    rows = tokens // n
    steps = nb * heads
    shape = jax.ShapeDtypeStruct
    dma = pltpu.SemaphoreType.DMA
    any_spec = pl.BlockSpec(memory_space=pl.ANY)

    def head_of(i):
        i = jnp.clip(i - 1, 0, steps - 1)
        return i // heads, i % heads

    blk = pl.BlockSpec((1, tokens, HEAD_DIM), lambda i: (head_of(i)[0], 0, head_of(i)[1]))
    vec = pl.BlockSpec((2, HEAD_DIM), lambda i: (0, head_of(i)[1]))
    out_vec = pl.BlockSpec((1, 1, HEAD_DIM), lambda i: (head_of(i)[0], 0, head_of(i)[1]))
    tab = pl.BlockSpec((tokens, HEAD_DIM), lambda i: (0, 0))
    whole = (nb, tokens, cols)
    lane_tile = pltpu.VMEM((tokens, HEAD_DIM), F32)
    return pl.pallas_call(
        functools.partial(proj_bwd_kernel, n, nb, heads, dim), name="proj_bwd", grid=(steps + 2,),
        out_shape=[shape((nb, rows, dim), BF16), shape((nb, tokens, 3 * cols), BF16), shape((nb, tokens, 3 * cols), BF16),
                   shape(whole, F32), shape(whole, F32), shape((cols, dim), BF16), shape((nb, 1, cols), F32), shape((nb, 1, cols), F32)],
        in_specs=[blk, blk, blk, blk, vec, tab, tab, pl.BlockSpec(ss.shape, lambda i: (0, 0))] + [any_spec] * 7,
        out_specs=[any_spec] * 6 + [out_vec, out_vec],
        scratch_shapes=Scatter.scratch(nb * rows, dim) + [lane_tile] * 4 + [pltpu.VMEM((tokens, tokens), BF16)] * 2 + [
            lane_tile, pltpu.VMEM((2, tokens, HEAD_DIM), F32), pltpu.VMEM((2, tokens, HEAD_DIM), F32),
            pltpu.VMEM((2, tokens, HEAD_DIM), BF16), pltpu.VMEM(ss.shape, F32), pltpu.VMEM(ss.shape, F32), pltpu.VMEM((n,) + ss.shape, F32),
            dma((1,)), dma((2, 2)), dma((2, 3)), dma((2, 4)), dma((2,)), dma((nb,)), dma((n,)), dma((n,)), dma, dma],
        compiler_params=params("arbitrary", collective_id=2, has_side_effects=True),
        cost_estimate=cost(4 * nb * tokens * dim * cols + 36 * nb * tokens * tokens * cols, 30 * nb * tokens * cols),
    )(q, k, v, d_attn, gains, cos_tab, sin_tab, ss, q, k, o, o_p, w_o, wo_p, d_full)


def dy_dw_kernel(n, nb, dim, g_hbm, g_p, wq_hbm, wk_hbm, wv_hbm, wq_p, wk_p, wv_p, y_full,
                 dy_out, dwq_out, dwk_out, dwv_out,
                 part, recv_far, recv_side, s_send, s_recv, ld_sem, w_sem, y_sem, o_sem, out_sem):
    tokens = g_hbm.shape[1]
    rows = tokens // n
    cols = g_hbm.shape[2] // 3
    nc = dim // CHUNK
    place = Place(n)
    scatter = Scatter(place, part, recv_far, recv_side, s_send, s_recv)
    lag = 4

    def chain(lhs, wbuf):
        loads = pair_rows(place, nb, rows, g_hbm, g_p, lhs, ld_sem)
        for c in loads:
            c.start()

        def chunk(j):
            slot = lax.rem(j, 2)
            src = pl.ds(pl.multiple_of(j * CHUNK, CHUNK), CHUNK)
            return [pltpu.make_async_copy(w.at[src], wbuf.at[slot, :, pl.ds(m * cols, cols)], w_sem.at[slot, m])
                    for m, w in enumerate((wq_hbm, wk_hbm, wv_hbm, wq_p, wk_p, wv_p))]

        for c in chunk(0):
            c.start()
        place.barrier(place.near()[:2])
        for c in loads:
            c.wait()

        def body(j, _):
            @pl.when(j + 1 < nc)
            def _():
                for c in chunk(j + 1):
                    c.start()

            for c in chunk(j):
                c.wait()
            w = wbuf[lax.rem(j, 2)]
            half = 2 * nb * rows
            for d in range(2):
                z = lax.dot_general(lhs[d * half:(d + 1) * half], w, NT, preferred_element_type=F32).astype(BF16)
                part[j, 2 * d] = z[:half // 2]
                part[j, 2 * d + 1] = z[half // 2:]
            scatter.start_far(j)

            @pl.when(j >= lag)
            def _():
                scatter.sums(j - lag)

            return 0

        lax.fori_loop(0, nc, body, 0)
        lax.fori_loop(0, nc, scatter.start_side, 0)

    pl.run_scoped(chain, pltpu.VMEM((4 * nb * rows, 6 * cols), BF16), pltpu.VMEM((2, CHUNK, 6 * cols), BF16))

    def weight_grad(g, ybuf, wst):
        bm = min(512, dim)
        n_chunks = dim // bm

        def chunk(c):
            slot = lax.rem(c, 2)
            return pltpu.make_async_copy(y_full.at[:, :, pl.ds(pl.multiple_of(c * bm, bm), bm)], ybuf.at[slot], y_sem.at[slot])

        def store(c):
            slot = lax.rem(c, 2)
            dst = pl.ds(pl.multiple_of(c * bm, bm), bm)
            return [pltpu.make_async_copy(wst.at[slot, :, pl.ds(m * cols, cols)], out.at[dst], o_sem.at[slot, m])
                    for m, out in enumerate((dwq_out, dwk_out, dwv_out))]

        load_g = pltpu.make_async_copy(g_hbm, g, ld_sem)
        load_g.start()
        chunk(0).start()
        load_g.wait()

        def body(c, _):
            slot = lax.rem(c, 2)

            @pl.when(c + 1 < n_chunks)
            def _():
                chunk(c + 1).start()

            @pl.when(c >= 2)
            def _():
                for s in store(c):
                    s.wait()

            chunk(c).wait()
            for m in range(lag):
                late = nc - lag + m
                pl.when(c == min(m, n_chunks - 1))(functools.partial(scatter.sums, max(late, 0)) if late >= 0 else (lambda: None))
            wst[slot] = lax.dot_general(ybuf[slot].reshape(nb * tokens, bm), g[...].reshape(nb * tokens, 3 * cols), TN,
                                        preferred_element_type=F32).astype(BF16)
            for s in store(c):
                s.start()
            return 0

        lax.fori_loop(0, n_chunks, body, 0)
        for s in range(min(2, n_chunks)):
            for c in store(s):
                c.wait()

    bm = min(512, dim)
    pl.run_scoped(weight_grad, pltpu.VMEM((nb, tokens, 3 * cols), BF16), pltpu.VMEM((2, nb, tokens, bm), BF16),
                  pltpu.VMEM((2, bm, 3 * cols), BF16))
    scatter_end(scatter, dy_out, out_sem, nc)


def dy_dw_call(n, g, g_p, w_q, w_k, w_v, wq_p, wk_p, wv_p, y_full):
    nb, tokens, wide = g.shape
    dim = y_full.shape[2]
    cols = wide // 3
    rows = tokens // n
    shape = jax.ShapeDtypeStruct
    dma = pltpu.SemaphoreType.DMA
    any_spec = pl.BlockSpec(memory_space=pl.ANY)
    return pl.pallas_call(
        functools.partial(dy_dw_kernel, n, nb, dim), name="dy_dw",
        out_shape=[shape((nb, rows, dim), BF16)] + [shape((dim, cols), BF16)] * 3,
        in_specs=[any_spec] * 9, out_specs=[any_spec] * 4,
        scratch_shapes=Scatter.scratch(nb * rows, dim) + [dma, dma((2, 6)), dma((2,)), dma((2, 3)), dma((nb,))],
        compiler_params=params(collective_id=3, has_side_effects=True),
        cost_estimate=cost(12 * nb * tokens * dim * cols, 30 * nb * tokens * cols),
    )(g, g_p, w_q, w_k, w_v, wq_p, wk_p, wv_p, y_full)


def token_kernel(n_copies, x_ref, dy_ref, pr_ref, g_ref, m_ref, e_ref, bo_ref, *refs):
    srcs, (xo_ref, dx_ref, dm_ref), dsts = refs[:4], refs[4:7], refs[7:11]
    bufs, (acc, in_sem, out_sem) = refs[11:15], refs[15:]
    group = 16
    step = pl.program_id(0)
    rows = x_ref.shape[1]
    groups = rows // group
    depth = bufs[0].shape[0]
    lag = depth - 1

    def move(c, out):
        copies = []
        for j, (src, dst, buf) in enumerate(zip(srcs, dsts, bufs)):
            size = buf.shape[1]
            sl = pl.ds(pl.multiple_of(c * size, 16), size)
            slot = lax.rem(c, depth)
            copies.append(pltpu.make_async_copy(buf.at[slot], dst.at[sl], out_sem.at[slot, j]) if out
                          else pltpu.make_async_copy(src.at[sl], buf.at[slot], in_sem.at[slot, j]))
        return copies

    def advance(i):
        @pl.when(i < n_copies)
        def _():
            @pl.when(i >= depth)
            def _():
                for c in move(i - depth, True):
                    c.wait()

            for c in move(i, False):
                c.start()

        @pl.when((i >= lag) & (i < n_copies + lag))
        def _():
            for c in move(i - lag, False):
                c.wait()
            for c in move(i - lag, True):
                c.start()

    mod = m_ref[...] + e_ref[0]
    shift_bo = bo_ref[...].reshape(1, bo_ref.shape[0])
    acc[...] = jnp.zeros_like(acc)

    def body(r, _):
        advance(step * groups + r)
        sl = pl.ds(pl.multiple_of(r * group, group), group)
        x = x_ref[0, sl].astype(F32)
        d_out = dy_ref[0, sl].astype(F32)
        proj = pr_ref[0, sl].astype(F32) + shift_bo
        xo_ref[0, sl] = (x + mod[2:3] * proj).astype(BF16)
        gate_part = d_out * proj
        x_norm, inv_std = norm_stats(x)
        d_y = g_ref[0, sl].astype(F32)
        d_norm = d_y * (1.0 + mod[1:2])
        d_x = d_out + inv_std * (
            d_norm - jnp.mean(d_norm, axis=-1, keepdims=True) - x_norm * jnp.mean(d_norm * x_norm, axis=-1, keepdims=True))
        dx_ref[0, sl] = d_x.astype(BF16)
        scale_part = d_y * x_norm
        acc[0] += d_y[:8] + d_y[8:]
        acc[1] += scale_part[:8] + scale_part[8:]
        acc[2] += gate_part[:8] + gate_part[8:]
        return 0

    lax.fori_loop(0, groups, body, 0)
    for j in range(3):
        dm_ref[0, j:j + 1] = jnp.sum(acc[j], axis=0, keepdims=True)

    @pl.when(step == pl.num_programs(0) - 1)
    def _():
        total = pl.num_programs(0) * groups

        def rest(i, _):
            advance(i)
            return 0

        lax.fori_loop(total, jnp.maximum(total, n_copies + lag), rest, 0)
        for c in range(max(n_copies - depth, 0), n_copies):
            for copy in move(c, True):
                copy.wait()


def token_call(x_loc, dy_loc, proj, d_y, m_block, e_loc, b_o, grads):
    nb, rows, dim = x_loc.shape
    n_copies = dim // min(512, dim)
    row = pl.BlockSpec((1, rows, dim), lambda i: (i, 0, 0))
    mod = pl.BlockSpec((1, 3, dim), lambda i: (i, 0, 0))
    any_spec = pl.BlockSpec(memory_space=pl.ANY)
    dma = pltpu.SemaphoreType.DMA
    depth = 4
    return pl.pallas_call(
        functools.partial(token_kernel, n_copies), name="tokens", grid=(nb,),
        out_shape=[jax.ShapeDtypeStruct(x_loc.shape, BF16), jax.ShapeDtypeStruct(x_loc.shape, BF16),
                   jax.ShapeDtypeStruct((nb, 3, dim), F32)] + [jax.ShapeDtypeStruct(w.shape, BF16) for w in grads],
        in_specs=[row, row, row, row, pl.BlockSpec((3, dim), lambda i: (0, 0)), mod, pl.BlockSpec(memory_space=pltpu.VMEM)] + [any_spec] * 4,
        out_specs=[row, row, mod] + [any_spec] * 4,
        scratch_shapes=[pltpu.VMEM((depth, w.shape[0] // n_copies, w.shape[1]), BF16) for w in grads]
        + [pltpu.VMEM((3, 8, dim), F32), dma((depth, 4)), dma((depth, 4))],
        compiler_params=params("arbitrary"),
        cost_estimate=cost(nb * rows * dim * 30, nb * rows * dim * 12),
    )(x_loc, dy_loc, proj, d_y, m_block, e_loc, b_o, *grads)


def solution(mesh):
    tp_size = mesh.shape['tp']

    def device_step(x_loc, e_loc, m_block, w_q, b_q, w_k, b_k, w_v, b_v, w_o, b_o, g_q, g_k, pos_part, dy_loc):
        nb, _, dim = x_loc.shape
        y_full, d_own, q, k, v, ss, cos_tab, sin_tab, gains = gather_qkv_call(
            tp_size, x_loc, dy_loc, m_block, e_loc, w_q, w_k, w_v, b_q, b_k, b_v, g_q, g_k, pos_part)
        d_full, o, o_p, d_attn, wq_p, wk_p, wv_p, wo_p = gather_attn_call(
            tp_size, q, k, v, gains, cos_tab, sin_tab, ss, w_q, w_k, w_v, w_o, d_own)
        proj, g, g_p, _, _, d_wo, d_gq, d_gk = proj_bwd_call(
            tp_size, q, k, v, d_attn, gains, cos_tab, sin_tab, ss, o, o_p, w_o, wo_p, d_full)
        d_y, d_wq, d_wk, d_wv = dy_dw_call(tp_size, g, g_p, w_q, w_k, w_v, wq_p, wk_p, wv_p, y_full)
        x_out, d_x, d_mod, d_wq, d_wk, d_wv, d_wo = token_call(
            x_loc, dy_loc, proj, d_y, m_block, e_loc, b_o, (d_wq, d_wk, d_wv, d_wo))
        d_e = all_sum_call(tp_size, d_mod.reshape(tp_size, -1, HEAD_DIM)).reshape(nb, 3, dim)
        return (x_out, d_x, d_e, jnp.sum(d_e, axis=0), d_wq, d_wk, d_wv, d_wo,
                jnp.sum(d_gq, axis=(0, 1)), jnp.sum(d_gk, axis=(0, 1)))

    in_specs = (P('dp', 'tp', None), P('dp', None, None), P(None, None), P(None, 'tp'), P('tp'), P(None, 'tp'), P('tp'),
                P(None, 'tp'), P('tp'), P('tp', None), P(None), P('tp'), P('tp'), P('dp', None), P('dp', 'tp', None))
    out_specs = (P('dp', 'tp', None), P('dp', 'tp', None), P('dp', None, None), P('dp', None), P('dp', 'tp'), P('dp', 'tp'),
                 P('dp', 'tp'), P(('dp', 'tp'), None), P(('dp', 'tp')), P(('dp', 'tp')))
    return jax.shard_map(device_step, mesh=mesh, in_specs=in_specs, out_specs=out_specs, check_vma=False)
```

```python
import functools

import jax
import jax.numpy as jnp
import numpy as np
from jax import lax
from jax.experimental import pallas as pl
from jax.experimental.pallas import tpu as pltpu
from jax.sharding import PartitionSpec as P

HEAD_DIM = 128
EPS_NORM = 1e-6
ROPE_BASE = 10000.0
LOG2E = 1.4426950408889634
CHUNK = 512
VMEM_LIMIT = 60 * 1024 * 1024
F32 = jnp.float32
BF16 = jnp.bfloat16
MESH_ID = pl.DeviceIdType.MESH
NT = (((1,), (1,)), ((), ()))
TN = (((0,), (0,)), ((), ()))


def params(*semantics, **kw):
    return pltpu.CompilerParams(dimension_semantics=semantics or None, vmem_limit_bytes=VMEM_LIMIT, **kw)


def cost(flops, nbytes):
    return pl.CostEstimate(flops=int(flops), bytes_accessed=int(nbytes), transcendentals=0)


def rope_freqs():
    half_dim = HEAD_DIM // 2
    side_len = HEAD_DIM // 6
    first_len = half_dim - 2 * side_len
    pair_idx = np.arange(HEAD_DIM) // 2
    section = (pair_idx >= first_len).astype(np.int32) + (pair_idx >= first_len + side_len).astype(np.int32)
    offset = np.where(section == 0, 0, np.where(section == 1, first_len, first_len + side_len))
    sec_width = np.where(section == 0, first_len, side_len)
    exponent = -(pair_idx - offset).astype(np.float32) / sec_width.astype(np.float32)
    freq_vals = np.power(np.float32(ROPE_BASE), exponent)
    return np.where(section[None, :] == np.arange(3)[:, None], freq_vals[None, :], np.float32(0.0)).astype(np.float32)


def norm_stats(x):
    centered = x - jnp.mean(x, axis=-1, keepdims=True)
    inv_std = lax.rsqrt(jnp.mean(centered * centered, axis=-1, keepdims=True) + EPS_NORM)
    return centered * inv_std, inv_std


def to_row(acc):
    return jnp.sum(acc.T, axis=0, keepdims=True)


def lanes_of(row):
    return jnp.broadcast_to(row, (HEAD_DIM, row.shape[1])).T


def head_sum(values):
    out = values[:, :HEAD_DIM]
    for h in range(1, values.shape[1] // HEAD_DIM):
        out = out + values[:, h * HEAD_DIM:(h + 1) * HEAD_DIM]
    return out


class Place:
    def __init__(self, n):
        self.n = n
        self.me = lax.axis_index('tp')
        self.right = lax.rem(self.me + 2, n)
        self.left = lax.rem(self.me + n - 2, n)
        self.far = lax.rem(self.me + n // 2, n)
        self.chip = self.me // 2

    def partner(self, dev):
        return dev + 1 - 2 * lax.rem(dev, 2)

    def barrier(self, devices):
        sem = pltpu.get_barrier_semaphore()
        for dev in devices:
            pl.semaphore_signal(sem, inc=1, device_id={'tp': dev}, device_id_type=MESH_ID)
        pl.semaphore_wait(sem, len(devices))

    def to_partner(self, src, dst, send_sem, recv_sem):
        return pltpu.make_async_remote_copy(src_ref=src, dst_ref=dst, send_sem=send_sem, recv_sem=recv_sem,
                                            device_id={'tp': self.partner(self.me)}, device_id_type=MESH_ID)

    def everyone(self):
        return [lax.rem(self.me + d, self.n) for d in range(1, self.n)]

    def near(self):
        return [self.right, self.left, self.partner(self.me)]


class Gather:
    def __init__(self, place, full, rows, send, recv, early=0):
        self.at, self.full, self.rows, self.send, self.recv, self.early = place, full, rows, send, recv, early

    def part(self, b, dev, off, count):
        return self.full.at[b, pl.ds(pl.multiple_of(dev * self.rows + off, 16), count)]

    def copy(self, b, dev, off, count, s_idx, r_idx, target):
        ref = self.part(b, dev, off, count)
        return pltpu.make_async_remote_copy(src_ref=ref, dst_ref=ref, send_sem=self.send.at[b, s_idx], recv_sem=self.recv.at[b, r_idx],
                                            device_id={'tp': target}, device_id_type=MESH_ID)

    def start_own(self, b):
        p = self.at
        self.copy(b, p.me, 0, self.rows, 0, 0, p.right).start()
        self.copy(b, p.me, 0, self.rows, 1, 1, p.left).start()
        self.copy(b, p.me, 0, self.rows, 2, 4, p.partner(p.me)).start()

    def whole_blocks_in(self, b):
        p = self.at
        self.copy(b, p.partner(p.me), 0, self.rows, 2, 4, p.me).wait_recv()
        self.copy(b, p.left, 0, self.rows, 0, 0, p.me).wait_recv()
        self.copy(b, p.right, 0, self.rows, 1, 1, p.me).wait_recv()
        for s_idx in range(3):
            self.copy(b, p.me, 0, self.rows, s_idx, s_idx, p.me).wait_send()

    def pass_left(self, b):
        p, half = self.at, self.rows // 2
        self.copy(b, p.left, 0, half, 3, 2, p.right).start()
        self.copy(b, p.left, 0, self.rows, 5, 5, p.partner(p.me)).start()

    def pass_right(self, b):
        p, half = self.at, self.rows // 2
        self.copy(b, p.right, half, half, 4, 3, p.left).start()
        self.copy(b, p.right, 0, self.rows, 6, 6, p.partner(p.me)).start()

    def take_own(self, b):
        p = self.at

        @pl.when(b >= self.early)
        def _():
            self.copy(b, p.partner(p.me), 0, self.rows, 2, 4, p.me).wait_recv()

    def take_left(self, b):
        p = self.at

        @pl.when(b >= self.early)
        def _():
            self.copy(b, p.left, 0, self.rows, 0, 0, p.me).wait_recv()
            self.pass_left(b)

        self.copy(b, p.partner(p.left), 0, self.rows, 5, 5, p.me).wait_recv()

    def take_right(self, b):
        p = self.at

        @pl.when(b >= self.early)
        def _():
            self.copy(b, p.right, 0, self.rows, 1, 1, p.me).wait_recv()
            self.pass_right(b)

        self.copy(b, p.partner(p.right), 0, self.rows, 6, 6, p.me).wait_recv()

    def take_far(self, b):
        p, half = self.at, self.rows // 2
        self.copy(b, p.far, 0, half, 3, 2, p.me).wait_recv()
        self.copy(b, p.far, 0, half, 7, 7, p.partner(p.me)).start()
        self.copy(b, p.far, half, half, 4, 3, p.me).wait_recv()
        self.copy(b, p.far, half, half, 8, 8, p.partner(p.me)).start()
        self.copy(b, p.partner(p.far), 0, half, 7, 7, p.me).wait_recv()
        self.copy(b, p.partner(p.far), half, half, 8, 8, p.me).wait_recv()

    def finish(self, b):
        p, half = self.at, self.rows // 2
        counts = (self.rows, self.rows, self.rows, half, half, self.rows, self.rows, half, half)
        for s_idx, count in list(enumerate(counts))[3 if b < self.early else 0:]:
            self.copy(b, p.me, 0, count, s_idx, s_idx, p.me).wait_send()

    def item_place(self, i, nb):
        j = i - nb
        b = jnp.where(i < nb, i, jnp.where(i < 3 * nb, j // 2, i - 3 * nb))
        chips = self.at.n // 2
        side = jnp.where(lax.rem(j + 2 * nb, 2) == 0, chips - 1, 1)
        off = jnp.where(i < nb, 0, jnp.where(i < 3 * nb, side, chips // 2))
        return b, pl.multiple_of(lax.rem(self.at.chip + off, chips) * (2 * self.rows), 32)

    def take_item(self, i, nb):
        b, row0 = self.item_place(i, nb)
        odd = lax.rem(i + nb, 2)
        pl.when(i < nb)(lambda: self.take_own(b))
        pl.when((i >= nb) & (i < 3 * nb) & (odd == 0))(lambda: self.take_left(b))
        pl.when((i >= nb) & (i < 3 * nb) & (odd == 1))(lambda: self.take_right(b))
        pl.when(i >= 3 * nb)(lambda: self.take_far(b))
        return b, row0


GATHER_SEMS = 9
EARLY_ROWS = 1
EARLY_CHUNKS = 4


def chunks_of(width, step):
    return [(c, min(c + step, width)) for c in range(0, width, step)]


class Exchange:
    def __init__(self, place, x_ref, slots, send_sems, recv_sems):
        self.at, self.x, self.slots, self.send, self.recv = place, x_ref, slots, send_sems, recv_sems

    def copy(self, d, dev, src):
        return pltpu.make_async_remote_copy(src_ref=self.x, dst_ref=self.slots.at[src], send_sem=self.send.at[d], recv_sem=self.recv.at[src],
                                            device_id={'tp': dev}, device_id_type=MESH_ID)

    def start(self):
        for d, dev in enumerate(self.at.everyone()):
            self.copy(d, dev, self.at.me).start()
        self.slots[self.at.me] = self.x[...]

    def finish(self):
        for d, dev in enumerate(self.at.everyone()):
            self.copy(d, dev, dev).wait()
        total = self.slots[0]
        for d in range(1, self.at.n):
            total = total + self.slots[d]
        return total


def gather_qkv_kernel(n, x_ref, dy_ref, m_ref, e_ref, wq_ref, wk_ref, wv_ref, bq_ref, bk_ref, bv_ref, gq_ref, gk_ref, pos_ref, freq_ref,
                      y_full, d_full, q_out, k_out, v_out, ss_ref, cos_ref, sin_ref, gain_ref,
                      bias_ref, w_all, xin, stage, xbuf, zst, vst, sq, ss_row, slots,
                      w_sem, in_sem, st_sem, ld_sem, out_sem, g_send, g_recv, d_send, d_recv, e_send, e_recv):
    nb, rows, dim = x_ref.shape
    cols = wq_ref.shape[1]
    place = Place(n)
    gather = Gather(place, y_full, rows, g_send, g_recv)
    gather_d = Gather(place, d_full, rows, d_send, d_recv)
    w_copies = [pltpu.make_async_copy(w, w_all.at[:, pl.ds(j * cols, cols)], w_sem.at[j]) for j, w in enumerate((wq_ref, wk_ref, wv_ref))]
    load_x = pltpu.make_async_copy(x_ref, xin, in_sem)
    load_x.start()
    for c in w_copies:
        c.start()
    group = 16

    def mine(full, b):
        return full.at[b, pl.ds(pl.multiple_of(place.me * rows, 16), rows)]

    load_x.wait()
    place.barrier(place.everyone())

    def ln_step(b, _):
        shift = m_ref[0:1] + e_ref[b, 0:1]
        scale_one = 1.0 + (m_ref[1:2] + e_ref[b, 1:2])

        def ln_rows(r, _):
            sl = pl.ds(pl.multiple_of(r * group, group), group)
            x_norm, _ = norm_stats(xin[b, sl].astype(F32))
            stage[b, sl] = (x_norm * scale_one + shift).astype(BF16)
            return 0

        lax.fori_loop(0, rows // group, ln_rows, 0)
        out = pltpu.make_async_copy(stage.at[b], mine(y_full, b), st_sem)
        out.start()
        out.wait()
        gather.start_own(b)
        return 0

    lax.fori_loop(0, nb, ln_step, 0)
    load_dy = pltpu.make_async_copy(dy_ref, xin, in_sem)
    load_dy.start()
    for j, ref in enumerate((bq_ref, bk_ref, bv_ref)):
        bias_ref[:, j * cols:(j + 1) * cols] = ref[...].reshape(1, cols)
    for j, ref in enumerate((gq_ref, gk_ref)):
        gain_ref[j:j + 1] = ref[...].reshape(1, cols)

    def tables():
        lane = lax.broadcasted_iota(jnp.int32, (128, HEAD_DIM), 1)

        def rows_of(r, _):
            sl = pl.ds(pl.multiple_of(r * 128, 128), 128)
            pos = pos_ref[sl].astype(F32)
            angle = pos[:, 0:1] * freq_ref[0:1] + pos[:, 1:2] * freq_ref[1:2] + pos[:, 2:3] * freq_ref[2:3]
            cos_ref[sl] = jnp.cos(angle)
            sin_ref[sl] = jnp.where(lane % 2 == 0, -1.0, 1.0) * jnp.sin(angle)
            return 0

        lax.fori_loop(0, pos_ref.shape[0] // 128, rows_of, 0)

    def gate_step(b, _):
        gate = m_ref[2:3] + e_ref[b, 2:3]

        def gate_rows(r, _):
            sl = pl.ds(pl.multiple_of(r * group, group), group)
            stage[b, sl] = (xin[b, sl].astype(F32) * gate).astype(BF16)
            return 0

        lax.fori_loop(0, rows // group, gate_rows, 0)
        out = pltpu.make_async_copy(stage.at[b], mine(d_full, b), st_sem)
        out.start()
        out.wait()
        return 0

    for c in w_copies:
        c.wait()

    def outputs(b, row0, slot):
        dst = pl.ds(row0, 2 * rows)
        return [pltpu.make_async_copy(zst.at[slot, :, pl.ds(0, cols)], q_out.at[b, dst], out_sem.at[slot, 0]),
                pltpu.make_async_copy(zst.at[slot, :, pl.ds(cols, cols)], k_out.at[b, dst], out_sem.at[slot, 1]),
                pltpu.make_async_copy(vst.at[slot], v_out.at[b, dst], out_sem.at[slot, 2])]

    def item(i, _):
        b, row0 = gather.take_item(i, nb)
        slot = lax.rem(i, 2)
        load = pltpu.make_async_copy(y_full.at[b, pl.ds(row0, 2 * rows)], xbuf, ld_sem)
        load.start()

        @pl.when(i == 3 * nb - 1)
        def _():
            for d in range(EARLY_ROWS):
                gather_d.start_own(d)

        @pl.when(i == nb)
        def _():
            load_dy.wait()
            lax.fori_loop(0, nb, gate_step, 0)
            tables()

        @pl.when(i >= 2)
        def _():
            for c in outputs(0, 0, slot):
                c.wait()

        load.wait()
        for lo, hi in chunks_of(3 * cols, 512):
            zst[slot, :, lo:hi] = jnp.dot(xbuf[...], w_all[:, lo:hi], preferred_element_type=F32) + bias_ref[:, lo:hi]
        vst[slot] = zst[slot, :, 2 * cols:].astype(BF16)
        q = zst[slot, :, :cols]
        k = zst[slot, :, cols:2 * cols]
        sq[2 * b, pl.ds(row0, 2 * rows)] = head_sum(q * q)
        sq[2 * b + 1, pl.ds(row0, 2 * rows)] = head_sum(k * k)
        for c in outputs(b, row0, slot):
            c.start()
        return 0

    lax.fori_loop(0, 4 * nb, item, 0)
    ss_row[...] = jnp.zeros_like(ss_row)
    for j in range(2 * nb):
        ss_row[j:j + 1] = to_row(sq[j])
    sums = Exchange(place, ss_row, slots, e_send, e_recv)
    sums.start()
    for slot in range(2):
        for c in outputs(0, 0, slot):
            c.wait()
    for b in range(nb):
        gather.finish(b)
    for d in range(EARLY_ROWS):
        gather_d.whole_blocks_in(d)
    ss_ref[...] = sums.finish()


def gather_qkv_call(n, x_loc, dy_loc, m_block, e_loc, w_q, w_k, w_v, b_q, b_k, b_v, g_q, g_k, positions):
    nb, rows, dim = x_loc.shape
    cols = w_q.shape[1]
    tokens = rows * n
    shape = jax.ShapeDtypeStruct
    any_spec = pl.BlockSpec(memory_space=pl.ANY)
    vmem = pl.BlockSpec(memory_space=pltpu.VMEM)
    dma = pltpu.SemaphoreType.DMA
    stat_rows = -(-2 * nb // 8) * 8
    return pl.pallas_call(
        functools.partial(gather_qkv_kernel, n), name="gather_qkv",
        out_shape=[shape((nb, tokens, dim), BF16), shape((nb, tokens, dim), BF16), shape((nb, tokens, cols), F32),
                   shape((nb, tokens, cols), F32), shape((nb, tokens, cols), BF16), shape((stat_rows, tokens), F32),
                   shape((tokens, HEAD_DIM), F32), shape((tokens, HEAD_DIM), F32), shape((2, cols), F32)],
        in_specs=[any_spec, any_spec, vmem, vmem, any_spec, any_spec, any_spec] + [vmem] * 7,
        out_specs=[any_spec] * 5 + [vmem] * 4,
        scratch_shapes=[
            pltpu.VMEM((1, 3 * cols), F32),
            pltpu.VMEM((dim, 3 * cols), BF16), pltpu.VMEM((nb, rows, dim), BF16), pltpu.VMEM((nb, rows, dim), BF16),
            pltpu.VMEM((2 * rows, dim), BF16), pltpu.VMEM((2, 2 * rows, 3 * cols), F32), pltpu.VMEM((2, 2 * rows, cols), BF16),
            pltpu.VMEM((2 * nb, tokens, HEAD_DIM), F32), pltpu.VMEM((stat_rows, tokens), F32), pltpu.VMEM((n, stat_rows, tokens), F32),
            dma((3,)), dma, dma, dma, dma((2, 3)), dma((nb, GATHER_SEMS)), dma((nb, GATHER_SEMS)),
            dma((EARLY_ROWS, GATHER_SEMS)), dma((EARLY_ROWS, GATHER_SEMS)), dma((n,)), dma((n,))],
        compiler_params=params(collective_id=0, has_side_effects=True),
        cost_estimate=cost(6 * nb * tokens * dim * cols, 6 * dim * cols + 14 * nb * tokens * cols),
    )(x_loc, dy_loc, m_block, e_loc, w_q, w_k, w_v, b_q, b_k, b_v, g_q, g_k, positions, jnp.asarray(rope_freqs()))


def all_sum_kernel(n, x_ref, o_ref, pieces, total, send_a, recv_a, send_b, recv_b):
    place = Place(n)
    me = place.me
    place.barrier(place.everyone())

    def first(d, dev, src):
        return pltpu.make_async_remote_copy(src_ref=x_ref.at[src], dst_ref=pieces.at[me], send_sem=send_a.at[d], recv_sem=recv_a.at[me],
                                            device_id={'tp': dev}, device_id_type=MESH_ID)

    for d, dev in enumerate(place.everyone()):
        first(d, dev, dev).start()
    pieces[me] = x_ref[me]
    for d, dev in enumerate(place.everyone()):
        pltpu.make_async_remote_copy(src_ref=x_ref.at[me], dst_ref=pieces.at[dev], send_sem=send_a.at[d], recv_sem=recv_a.at[dev],
                                     device_id={'tp': dev}, device_id_type=MESH_ID).wait_recv()
    acc = pieces[0]
    for d in range(1, n):
        acc = acc + pieces[d]
    total[...] = acc
    o_ref[me] = acc
    for d, dev in enumerate(place.everyone()):
        first(d, dev, dev).wait_send()
    for d, dev in enumerate(place.everyone()):
        pltpu.make_async_remote_copy(src_ref=total, dst_ref=o_ref.at[me], send_sem=send_b.at[d], recv_sem=recv_b.at[me],
                                     device_id={'tp': dev}, device_id_type=MESH_ID).start()
    for d, dev in enumerate(place.everyone()):
        copy = pltpu.make_async_remote_copy(src_ref=total, dst_ref=o_ref.at[dev], send_sem=send_b.at[d], recv_sem=recv_b.at[dev],
                                            device_id={'tp': dev}, device_id_type=MESH_ID)
        copy.wait_send()
        copy.wait_recv()


def all_sum_call(n, x):
    spec = pl.BlockSpec(memory_space=pltpu.VMEM)
    dma = pltpu.SemaphoreType.DMA
    return pl.pallas_call(
        functools.partial(all_sum_kernel, n), name="all_sum",
        out_shape=jax.ShapeDtypeStruct(x.shape, x.dtype), in_specs=[spec], out_specs=spec,
        scratch_shapes=[pltpu.VMEM(x.shape, x.dtype), pltpu.VMEM(x.shape[1:], x.dtype), dma((n,)), dma((n,)), dma((n,)), dma((n,))],
        compiler_params=pltpu.CompilerParams(collective_id=4, has_side_effects=True, vmem_limit_bytes=4 * 1024 * 1024),
        cost_estimate=cost(4_000_000_000, x.size * 8),
    )(x)


def swap_pairs(x):
    lane = lax.broadcasted_iota(jnp.int32, x.shape, 1)
    return jnp.where(lane % 2 == 0, pltpu.roll(x, HEAD_DIM - 1, 1), pltpu.roll(x, 1, 1))


def rotate(x, cos, sin):
    return x * cos + swap_pairs(x) * sin


def softmax_block(s):
    c = HEAD_DIM ** -0.5 * LOG2E
    top = jnp.max(s, axis=1, keepdims=True)
    p = jnp.exp2(s * c - top * c)
    return p * (1.0 / jnp.sum(p, axis=1, keepdims=True))


class Scatter:
    def __init__(self, place, part, recv_far, recv_side, send, recv, far_src=None, early=0):
        self.at, self.part, self.far, self.side, self.send, self.recv = place, part, recv_far, recv_side, send, recv
        self.far_src, self.early = part if far_src is None else far_src, early
        self.rows = part.shape[2]
        self.half = self.rows // 2

    def copy(self, j, idx, src, dst, target):
        return pltpu.make_async_remote_copy(src_ref=src, dst_ref=dst, send_sem=self.send.at[j, idx], recv_sem=self.recv.at[j, idx],
                                            device_id={'tp': target}, device_id_type=MESH_ID)

    def message(self, j, idx):
        p, part, far, side = self.at, self.part, self.far, self.side
        first, second = pl.ds(0, self.half), pl.ds(self.half, self.rows - self.half)
        src, dst, target = (
            lambda: (self.far_src.at[j, 0, first], far.at[j, 0], p.right),
            lambda: (self.far_src.at[j, 0, second], far.at[j, 1], p.left),
            lambda: (part.at[j, 1, second], side.at[j, 0, second], p.right),
            lambda: (part.at[j, 2, first], side.at[j, 1, first], p.left),
            lambda: (part.at[j, 1, first], side.at[j, 0, first], p.right),
            lambda: (part.at[j, 2, second], side.at[j, 1, second], p.left))[idx]()
        return self.copy(j, idx, src, dst, target)

    def start_far(self, j, _=0):
        for idx in (0, 1):
            self.message(j, idx).start()
        return 0

    def start_side(self, j, _):
        for idx in (2, 3):
            self.message(j, idx).start()
        return 0

    def sums(self, j):
        h = self.half
        arrived = isinstance(j, int) and j < self.early
        if not arrived:
            self.message(j, 0).wait_recv()
        self.part[j, 1, :h] = (self.part[j, 1, :h].astype(F32) + self.far[j, 0].astype(F32)).astype(BF16)
        if not arrived:
            self.message(j, 1).wait_recv()
        self.part[j, 2, h:] = (self.part[j, 2, h:].astype(F32) + self.far[j, 1].astype(F32)).astype(BF16)
        self.message(j, 4).start()
        self.message(j, 5).start()

    def final(self, j):
        for idx in range(2, 6):
            self.message(j, idx).wait_recv()
        total = self.part[j, 3].astype(F32) + self.side[j, 0].astype(F32) + self.side[j, 1].astype(F32)
        self.part[j, 3] = total.astype(BF16)

    def finish(self, j):
        @pl.when(j >= self.early)
        def _():
            for idx in range(2):
                self.message(j, idx).wait_send()

        for idx in range(2, 6):
            self.message(j, idx).wait_send()

    @staticmethod
    def scratch(rows, dim):
        nc, dma = dim // CHUNK, pltpu.SemaphoreType.DMA
        return [pltpu.VMEM((nc, 4, rows, CHUNK), BF16), pltpu.VMEM((nc, 2, rows // 2, CHUNK), BF16),
                pltpu.VMEM((nc, 2, rows, CHUNK), BF16), dma((nc, 6)), dma((nc, 6))]


def scatter_outputs(part, out, sem, j):
    nb, rows, _ = out.shape
    cs = pl.ds(pl.multiple_of(j * CHUNK, CHUNK), CHUNK)
    return [pltpu.make_async_copy(part.at[j, 3, pl.ds(b * rows, rows)], out.at[b, :, cs], sem.at[b]) for b in range(nb)]


def scatter_end(scatter, out, sem, nc):
    def last(j, _):
        scatter.final(j)
        for c in scatter_outputs(scatter.part, out, sem, j):
            c.start()
        return 0

    lax.fori_loop(0, nc, last, 0)

    def drain(j, _):
        for c in scatter_outputs(scatter.part, out, sem, j):
            c.wait()
        scatter.finish(j)
        return 0

    lax.fori_loop(0, nc, drain, 0)


def pair_rows(place, nb, rows, mine, theirs, lhs, sem):
    width = mine.shape[2]
    out = []
    for d, dev in enumerate((place.far, place.right, place.left, place.me)):
        src_rows = pl.ds(pl.multiple_of(dev * rows, 16), rows)
        for b in range(nb):
            dst_rows = pl.ds((d * nb + b) * rows, rows)
            for j, src in enumerate((mine, theirs)):
                out.append(pltpu.make_async_copy(src.at[b, src_rows], lhs.at[dst_rows, pl.ds(j * width, width)], sem))
    return out


def gather_attn_kernel(n, nb, heads, dim, q_ref, k_ref, v_ref, gain_ref, cos_ref, sin_ref, ss_ref,
                       wq_ref, wk_ref, wv_ref, wo_ref, d_in,
                       d_full, o_out, o_p, da_out, wq_p, wk_p, wv_p, wo_p, part_out, far_in,
                       inv_q, inv_k, o_all, wo, xbuf, ast,
                       w_sem, ld_sem, out_sem, o_sem, p_sem, l_sem, g_send, g_recv, t_send, t_recv, s_send, s_recv):
    step = pl.program_id(0)
    tokens = q_ref.shape[1]
    rows = tokens // n
    blk = min(256, tokens)
    place = Place(n)
    gather = Gather(place, d_full, rows, g_send, g_recv, early=EARLY_ROWS)
    cols = heads * HEAD_DIM
    nc = dim // CHUNK
    early_chunks = min(EARLY_CHUNKS, nc)
    scatter = Scatter(place, part_out, far_in, None, s_send, s_recv)
    pairs = ((wo_ref, wo_p), (wq_ref, wq_p), (wk_ref, wk_p), (wv_ref, wv_p), (o_out, o_p))

    def trade(j):
        return place.to_partner(*pairs[j], t_send.at[j], t_recv.at[j])


    @pl.when(step == 0)
    def _():
        pltpu.make_async_copy(wo_ref, wo, w_sem).start()
        place.barrier(place.near())

        for b in range(EARLY_ROWS):
            gather.pass_left(b)
            gather.pass_right(b)

        def own(b, _):
            gather.start_own(b)
            return 0

        lax.fori_loop(EARLY_ROWS, nb, own, 0)
        for j in range(4):
            trade(j).start()

    @pl.when(step < nb * heads)
    def _():
        b = step // heads
        h = lax.rem(step, heads)

        @pl.when(h == 0)
        def _():
            inv_q[...] = lanes_of(lax.rsqrt(ss_ref[pl.ds(2 * b, 1)] / dim + EPS_NORM))
            inv_k[...] = lanes_of(lax.rsqrt(ss_ref[pl.ds(2 * b + 1, 1)] / dim + EPS_NORM))

        cos, sin = cos_ref[...], sin_ref[...]
        q_rot = rotate(q_ref[0] * inv_q[...] * gain_ref[0:1], cos, sin).astype(BF16)
        k_rot = rotate(k_ref[0] * inv_k[...] * gain_ref[1:2], cos, sin).astype(BF16)
        v = v_ref[0]
        lanes = pl.ds(pl.multiple_of(h * HEAD_DIM, HEAD_DIM), HEAD_DIM)
        for i in range(tokens // blk):
            s = lax.dot_general(q_rot[i * blk:(i + 1) * blk], k_rot, NT, preferred_element_type=F32)
            p = softmax_block(s).astype(BF16)
            o_all[b, i * blk:(i + 1) * blk, lanes] = jnp.dot(p, v, preferred_element_type=F32).astype(BF16)

    @pl.when(step == nb * heads)
    def _():
        o_copy = pltpu.make_async_copy(o_all, o_out, o_sem)
        o_copy.start()
        pltpu.make_async_copy(wo_ref, wo, w_sem).wait()

        def outputs(b, row0, slot):
            return pltpu.make_async_copy(ast.at[slot], da_out.at[b, pl.ds(row0, 2 * rows)], out_sem.at[slot])

        def load(b, row0, slot):
            return pltpu.make_async_copy(d_full.at[b, pl.ds(row0, 2 * rows)], xbuf.at[slot], ld_sem.at[slot])

        def project(lhs, wbuf, stage):
            loads = pair_rows(place, nb, rows, o_out, o_p, lhs, l_sem.at[0])
            for c in loads:
                c.start()

            def chunk(j):
                cs = pl.ds(pl.multiple_of(j * CHUNK, CHUNK), CHUNK)
                slot = lax.rem(j, 2)
                return [pltpu.make_async_copy(wo_ref.at[:, cs], wbuf.at[slot, pl.ds(0, cols)], p_sem.at[slot, 0]),
                        pltpu.make_async_copy(wo_p.at[:, cs], wbuf.at[slot, pl.ds(cols, cols)], p_sem.at[slot, 1])]

            def store(j):
                slot = lax.rem(j, 2)
                return pltpu.make_async_copy(stage.at[slot], part_out.at[j], p_sem.at[slot, 2])

            def stored(j):
                store(j).wait()

                @pl.when(j < early_chunks)
                def _():
                    scatter.start_far(j)

            for c in chunk(0):
                c.start()
            for c in loads:
                c.wait()

            def body(j, _):
                slot = lax.rem(j, 2)

                @pl.when(j + 1 < nc)
                def _():
                    for c in chunk(j + 1):
                        c.start()

                for c in chunk(j):
                    c.wait()
                half = 2 * nb * rows
                for d in range(2):
                    z = jnp.dot(lhs[d * half:(d + 1) * half], wbuf[slot], preferred_element_type=F32).astype(BF16)
                    stage[slot, 2 * d] = z[:half // 2]
                    stage[slot, 2 * d + 1] = z[half // 2:]
                store(j).start()

                @pl.when(j >= 1)
                def _():
                    stored(j - 1)

                return 0

            lax.fori_loop(0, nc, body, 0)
            stored(nc - 1)

        def take(i):
            b, row0 = gather.take_item(i, nb)
            load(b, row0, lax.rem(i, 2)).start()

        take(0)

        def item(i, _):
            slot = lax.rem(i, 2)

            @pl.when(i + 1 < 3 * nb)
            def _():
                take(i + 1)

            @pl.when(i >= 2)
            def _():
                outputs(0, 0, slot).wait()

            load(0, 0, slot).wait()
            ast[slot] = lax.dot_general(xbuf[slot], wo[...], NT, preferred_element_type=F32).astype(BF16)
            b, row0 = gather.item_place(i, nb)
            outputs(b, row0, slot).start()

            @pl.when(i == 0)
            def _():
                o_copy.wait()
                trade(4).start()

            @pl.when(i + 1 == 3 * nb)
            def _():
                trade(4).wait_recv()
                trade(0).wait_recv()
                pl.run_scoped(project, pltpu.VMEM((4 * nb * rows, 2 * cols), BF16), pltpu.VMEM((2, 2 * cols, CHUNK), BF16),
                              pltpu.VMEM((2, 4, nb * rows, CHUNK), BF16))

            @pl.when((i + 1 >= 3 * nb) & (i + 1 < 4 * nb))
            def _():
                take(i + 1)

            return 0

        lax.fori_loop(0, 4 * nb, item, 0)
        for slot in range(2):
            outputs(0, 0, slot).wait()
        for b in range(nb):
            gather.finish(b)
        trade(0).wait_send()
        trade(4).wait_send()
        for j in range(1, 4):
            trade(j).wait()
        for j in range(early_chunks):
            for idx in (0, 1):
                scatter.message(j, idx).wait()


def gather_attn_call(n, q, k, v, gains, cos_tab, sin_tab, ss, w_q, w_k, w_v, w_o, d_full):
    nb, tokens, cols = q.shape
    dim = w_o.shape[1]
    heads = cols // HEAD_DIM
    rows = tokens // n
    last = nb * heads - 1
    nc = dim // CHUNK
    early = min(EARLY_CHUNKS, nc)
    shape = jax.ShapeDtypeStruct
    dma = pltpu.SemaphoreType.DMA
    any_spec = pl.BlockSpec(memory_space=pl.ANY)

    def head_of(i):
        i = jnp.minimum(i, last)
        return i // heads, i % heads

    blk = pl.BlockSpec((1, tokens, HEAD_DIM), lambda i: (head_of(i)[0], 0, head_of(i)[1]))
    vec = pl.BlockSpec((2, HEAD_DIM), lambda i: (0, head_of(i)[1]))
    tab = pl.BlockSpec((tokens, HEAD_DIM), lambda i: (0, 0))
    head_arr = shape((nb, tokens, cols), BF16)
    return pl.pallas_call(
        functools.partial(gather_attn_kernel, n, nb, heads, dim), name="gather_attn", grid=(nb * heads + 1,),
        out_shape=[shape(d_full.shape, BF16), head_arr, head_arr, head_arr] + [shape(w.shape, BF16) for w in (w_q, w_k, w_v, w_o)]
        + [shape((nc, 4, nb * rows, CHUNK), BF16), shape((early, 2, nb * rows // 2, CHUNK), BF16)],
        in_specs=[blk, blk, blk, vec, tab, tab, pl.BlockSpec(ss.shape, lambda i: (0, 0))] + [any_spec] * 5,
        out_specs=[any_spec] * 10,
        scratch_shapes=[
            pltpu.VMEM((tokens, HEAD_DIM), F32), pltpu.VMEM((tokens, HEAD_DIM), F32), pltpu.VMEM((nb, tokens, cols), BF16),
            pltpu.VMEM((cols, dim), BF16), pltpu.VMEM((2, 2 * rows, dim), BF16), pltpu.VMEM((2, 2 * rows, cols), BF16),
            dma, dma((2,)), dma((2,)), dma, dma((2, 3)), dma((1,)), dma((nb, GATHER_SEMS)), dma((nb, GATHER_SEMS)), dma((5,)), dma((5,)),
            dma((early, 6)), dma((early, 6))],
        input_output_aliases={11: 0},
        compiler_params=params("arbitrary", collective_id=1, has_side_effects=True),
        cost_estimate=cost(4 * nb * tokens * dim * cols + 4 * nb * tokens * tokens * cols, 8 * nb * tokens * dim),
    )(q, k, v, gains, cos_tab, sin_tab, ss, w_q, w_k, w_v, w_o, d_full)


def attn_bwd_kernel(n, nb, heads, dim, q_ref, k_ref, v_ref, do_ref, gain_ref, cos_ref, sin_ref, ss_ref,
                    q_hbm, k_hbm, o_hbm, part_in, far_in, d_full,
                    proj_out, g_out, g_p, dqs_out, dks_out, dwo_out, dgq_ref, dgk_ref,
                    part, recv_far, recv_side, s_send, s_recv,
                    inv_q, inv_k, acc_q, acc_k, p_all, ds_all, dq_all, qs_st, ks_st, v_st, st_row, st_sum, slots,
                    ld_sem, w_sem, fl_sem, g_sem, go_sem, out_sem, e_send, e_recv, t_send, t_recv):
    step = pl.program_id(0)
    tokens = q_ref.shape[1]
    rows = tokens // n
    cols = heads * HEAD_DIM
    blk = min(256, tokens)
    nc = dim // CHUNK
    steps = nb * heads
    scale = HEAD_DIM ** -0.5
    place = Place(n)
    early = far_in.shape[0]
    scatter = Scatter(place, part, recv_far, recv_side, s_send, s_recv, far_src=part_in, early=early)

    def stored():
        return [pltpu.make_async_copy(part_in, part, ld_sem.at[0]),
                pltpu.make_async_copy(far_in, recv_far.at[pl.ds(0, early)], ld_sem.at[1])]

    @pl.when(step == 0)
    def _():
        place.barrier(place.everyone())
        lax.fori_loop(early, nc, scatter.start_far, 0)
        for c in stored():
            c.start()

    @pl.when(step == 1)
    def _():
        for c in stored():
            c.wait()

    def flush(b, h, slot):
        lanes = pl.ds(pl.multiple_of(h * HEAD_DIM, HEAD_DIM), HEAD_DIM)
        v_lanes = pl.ds(pl.multiple_of(2 * cols + h * HEAD_DIM, HEAD_DIM), HEAD_DIM)
        return [pltpu.make_async_copy(qs_st.at[slot], dqs_out.at[b, :, lanes], fl_sem.at[slot, 0]),
                pltpu.make_async_copy(ks_st.at[slot], dks_out.at[b, :, lanes], fl_sem.at[slot, 1]),
                pltpu.make_async_copy(v_st.at[slot], g_out.at[b, :, v_lanes], fl_sem.at[slot, 2])]

    for j in range(nc):
        at_step = 1 + j * (steps - 2) // max(nc - 1, 1)
        pl.when(step == at_step)(functools.partial(scatter.sums, j))

    @pl.when(step < steps)
    def _():
        b = step // heads
        head = lax.rem(step, heads)
        slot = lax.rem(step, 2)

        @pl.when(step == 0)
        def _():
            st_row[...] = jnp.zeros_like(st_row)

        @pl.when(head == 0)
        def _():
            inv_q[...] = lanes_of(lax.rsqrt(ss_ref[pl.ds(2 * b, 1)] / dim + EPS_NORM))
            inv_k[...] = lanes_of(lax.rsqrt(ss_ref[pl.ds(2 * b + 1, 1)] / dim + EPS_NORM))
            acc_q[...] = jnp.zeros_like(acc_q)
            acc_k[...] = jnp.zeros_like(acc_k)

        @pl.when(step >= 2)
        def _():
            for c in flush(0, 0, slot):
                c.wait()

        cos, sin = cos_ref[...], sin_ref[...]
        q_rot = rotate(q_ref[0] * inv_q[...] * gain_ref[0:1], cos, sin).astype(BF16)
        k_rot = rotate(k_ref[0] * inv_k[...] * gain_ref[1:2], cos, sin).astype(BF16)
        v = v_ref[0]
        do = do_ref[0]
        for i in range(tokens // blk):
            sl = slice(i * blk, (i + 1) * blk)
            p = softmax_block(lax.dot_general(q_rot[sl], k_rot, NT, preferred_element_type=F32))
            p_all[sl] = p.astype(BF16)
            dp = lax.dot_general(do[sl], v, NT, preferred_element_type=F32)
            delta = jnp.sum(dp * p, axis=1, keepdims=True)
            ds = (p * (dp - delta)).astype(BF16)
            ds_all[sl] = ds
            dq_all[sl] = jnp.dot(ds, k_rot, preferred_element_type=F32) * scale
        do_t = do.astype(F32).T.astype(BF16)
        q_t = q_rot.astype(F32).T.astype(BF16)
        v_st[slot] = jnp.dot(do_t, p_all[...], preferred_element_type=F32).T.astype(BF16)
        dk_rot = (jnp.dot(q_t, ds_all[...], preferred_element_type=F32) * scale).T.astype(BF16).astype(F32)
        dq_rot = dq_all[...].astype(BF16).astype(F32)
        dq_hat = rotate(dq_rot, cos, -sin)
        dk_hat = rotate(dk_rot, cos, -sin)
        q_hat = q_ref[0] * inv_q[...]
        k_hat = k_ref[0] * inv_k[...]
        dgq_ref[0] = jnp.sum(dq_hat * q_hat, axis=0, keepdims=True)
        dgk_ref[0] = jnp.sum(dk_hat * k_hat, axis=0, keepdims=True)
        dq_s = dq_hat * gain_ref[0:1]
        dk_s = dk_hat * gain_ref[1:2]
        qs_st[slot] = dq_s
        ks_st[slot] = dk_s
        acc_q[...] += dq_s * q_hat
        acc_k[...] += dk_s * k_hat
        for c in flush(b, head, slot):
            c.start()

        @pl.when(head == heads - 1)
        def _():
            st_row[pl.ds(2 * b, 1)] = to_row(acc_q[...])
            st_row[pl.ds(2 * b + 1, 1)] = to_row(acc_k[...])

    @pl.when(step == steps)
    def _():
        for s in range(2):
            for c in flush(0, 0, s):
                c.wait()
        stats = Exchange(place, st_row, slots, e_send, e_recv)
        stats.start()
        lax.fori_loop(0, nc, scatter.start_side, 0)
        st_sum[...] = stats.finish()
        rb = min(256, tokens)
        per = tokens // rb
        trade = place.to_partner(g_out, g_p, t_send, t_recv)

        def norm_grad(fbuf, gbuf):
            def loads(i, slot):
                b, r0 = i // per, pl.multiple_of(lax.rem(i, per) * rb, rb)
                return [pltpu.make_async_copy(src.at[b, pl.ds(r0, rb)], fbuf.at[slot, m], g_sem.at[slot, m])
                        for m, src in enumerate((dqs_out, q_hbm, dks_out, k_hbm))]

            def store(i, slot):
                b, r0 = i // per, pl.multiple_of(lax.rem(i, per) * rb, rb)
                return pltpu.make_async_copy(gbuf.at[slot], g_out.at[b, pl.ds(r0, rb), pl.ds(0, 2 * cols)], go_sem.at[slot])

            for c in loads(0, 0):
                c.start()

            def body(i, _):
                slot = lax.rem(i, 2)
                b, r0 = i // per, pl.multiple_of(lax.rem(i, per) * rb, rb)

                @pl.when(i + 1 < nb * per)
                def _():
                    for c in loads(i + 1, lax.rem(i + 1, 2)):
                        c.start()

                @pl.when(r0 == 0)
                def _():
                    inv_q[...] = lanes_of(lax.rsqrt(ss_ref[pl.ds(2 * b, 1)] / dim + EPS_NORM))
                    inv_k[...] = lanes_of(lax.rsqrt(ss_ref[pl.ds(2 * b + 1, 1)] / dim + EPS_NORM))
                    acc_q[...] = lanes_of(st_sum[pl.ds(2 * b, 1)] / dim)
                    acc_k[...] = lanes_of(st_sum[pl.ds(2 * b + 1, 1)] / dim)

                @pl.when(i >= 2)
                def _():
                    store(0, slot).wait()

                for c in loads(i, slot):
                    c.wait()
                sl = pl.ds(r0, rb)
                for m, (inv, st) in enumerate(((inv_q, acc_q), (inv_k, acc_k))):
                    inv_l, st_l = inv[sl], st[sl]
                    for h in range(heads):
                        hs = slice(h * HEAD_DIM, (h + 1) * HEAD_DIM)
                        grad = inv_l * (fbuf[slot, 2 * m, :, hs] - (fbuf[slot, 2 * m + 1, :, hs] * inv_l) * st_l)
                        gbuf[slot, :, m * cols + h * HEAD_DIM:m * cols + (h + 1) * HEAD_DIM] = grad.astype(BF16)
                store(i, slot).start()
                return 0

            lax.fori_loop(0, nb * per, body, 0)
            for s in range(min(2, nb * per)):
                store(0, s).wait()

        pl.run_scoped(norm_grad, pltpu.VMEM((2, 4, rb, cols), F32), pltpu.VMEM((2, rb, 2 * cols), BF16))
        trade.start()

        def weight_grad(turned, obuf, dbuf, wst):
            bn = min(512, dim)
            n_chunks = dim // bn

            def chunk(c):
                slot = lax.rem(c, 2)
                return pltpu.make_async_copy(d_full.at[:, :, pl.ds(pl.multiple_of(c * bn, bn), bn)], dbuf.at[slot], go_sem.at[slot])

            def store(c):
                slot = lax.rem(c, 2)
                return pltpu.make_async_copy(wst.at[slot], dwo_out.at[:, pl.ds(pl.multiple_of(c * bn, bn), bn)], w_sem.at[slot, 0])

            load_o = pltpu.make_async_copy(o_hbm, obuf, ld_sem.at[0])
            load_o.start()
            chunk(0).start()
            load_o.wait()
            for b in range(nb):
                turned[:, b * tokens:(b + 1) * tokens] = obuf[b].T

            def body(c, _):
                slot = lax.rem(c, 2)

                @pl.when(c + 1 < n_chunks)
                def _():
                    chunk(c + 1).start()

                @pl.when(c >= 2)
                def _():
                    store(c).wait()

                chunk(c).wait()
                d = dbuf[slot].reshape(nb * tokens, bn)
                wst[slot] = jnp.dot(turned[...], d, preferred_element_type=F32).astype(BF16)
                store(c).start()
                return 0

            lax.fori_loop(0, n_chunks, body, 0)
            for s in range(min(2, n_chunks)):
                store(s).wait()

        bn = min(512, dim)
        pl.run_scoped(weight_grad, pltpu.VMEM((cols, nb * tokens), BF16), pltpu.VMEM((nb, tokens, cols), BF16),
                      pltpu.VMEM((2, nb, tokens, bn), BF16), pltpu.VMEM((2, cols, bn), BF16))
        scatter_end(scatter, proj_out, out_sem, nc)
        trade.wait()


def attn_bwd_call(n, q, k, v, d_attn, gains, cos_tab, sin_tab, ss, o, part, far, d_full):
    nb, tokens, cols = q.shape
    dim = d_full.shape[2]
    heads = cols // HEAD_DIM
    rows = tokens // n
    steps = nb * heads
    shape = jax.ShapeDtypeStruct
    dma = pltpu.SemaphoreType.DMA
    any_spec = pl.BlockSpec(memory_space=pl.ANY)

    def head_of(i):
        i = jnp.minimum(i, steps - 1)
        return i // heads, i % heads

    blk = pl.BlockSpec((1, tokens, HEAD_DIM), lambda i: (head_of(i)[0], 0, head_of(i)[1]))
    vec = pl.BlockSpec((2, HEAD_DIM), lambda i: (0, head_of(i)[1]))
    out_vec = pl.BlockSpec((1, 1, HEAD_DIM), lambda i: (head_of(i)[0], 0, head_of(i)[1]))
    tab = pl.BlockSpec((tokens, HEAD_DIM), lambda i: (0, 0))
    whole = (nb, tokens, cols)
    lane_tile = pltpu.VMEM((tokens, HEAD_DIM), F32)
    return pl.pallas_call(
        functools.partial(attn_bwd_kernel, n, nb, heads, dim), name="attn_bwd", grid=(steps + 1,),
        out_shape=[shape((nb, rows, dim), BF16), shape((nb, tokens, 3 * cols), BF16), shape((nb, tokens, 3 * cols), BF16),
                   shape(whole, F32), shape(whole, F32), shape((cols, dim), BF16), shape((nb, 1, cols), F32), shape((nb, 1, cols), F32)],
        in_specs=[blk, blk, blk, blk, vec, tab, tab, pl.BlockSpec(ss.shape, lambda i: (0, 0))] + [any_spec] * 6,
        out_specs=[any_spec] * 6 + [out_vec, out_vec],
        scratch_shapes=Scatter.scratch(nb * rows, dim) + [lane_tile] * 4 + [pltpu.VMEM((tokens, tokens), BF16)] * 2 + [
            lane_tile, pltpu.VMEM((2, tokens, HEAD_DIM), F32), pltpu.VMEM((2, tokens, HEAD_DIM), F32),
            pltpu.VMEM((2, tokens, HEAD_DIM), BF16), pltpu.VMEM(ss.shape, F32), pltpu.VMEM(ss.shape, F32), pltpu.VMEM((n,) + ss.shape, F32),
            dma((2,)), dma((2, 2)), dma((2, 3)), dma((2, 4)), dma((2,)), dma((nb,)), dma((n,)), dma((n,)), dma, dma],
        compiler_params=params("arbitrary", collective_id=2, has_side_effects=True),
        cost_estimate=cost(4 * nb * tokens * dim * cols + 36 * nb * tokens * tokens * cols, 30 * nb * tokens * cols),
    )(q, k, v, d_attn, gains, cos_tab, sin_tab, ss, q, k, o, part, far, d_full)


def dy_dw_kernel(n, nb, dim, g_hbm, g_p, wq_hbm, wk_hbm, wv_hbm, wq_p, wk_p, wv_p, y_full,
                 dy_out, dwq_out, dwk_out, dwv_out,
                 part, recv_far, recv_side, s_send, s_recv, ld_sem, w_sem, y_sem, o_sem, out_sem):
    tokens = g_hbm.shape[1]
    rows = tokens // n
    cols = g_hbm.shape[2] // 3
    nc = dim // CHUNK
    place = Place(n)
    scatter = Scatter(place, part, recv_far, recv_side, s_send, s_recv)
    lag = 4

    def chain(lhs, wbuf):
        loads = pair_rows(place, nb, rows, g_hbm, g_p, lhs, ld_sem)
        for c in loads:
            c.start()

        def chunk(j):
            slot = lax.rem(j, 2)
            src = pl.ds(pl.multiple_of(j * CHUNK, CHUNK), CHUNK)
            return [pltpu.make_async_copy(w.at[src], wbuf.at[slot, :, pl.ds(m * cols, cols)], w_sem.at[slot, m])
                    for m, w in enumerate((wq_hbm, wk_hbm, wv_hbm, wq_p, wk_p, wv_p))]

        for c in chunk(0):
            c.start()
        place.barrier(place.near()[:2])
        for c in loads:
            c.wait()

        def body(j, _):
            @pl.when(j + 1 < nc)
            def _():
                for c in chunk(j + 1):
                    c.start()

            for c in chunk(j):
                c.wait()
            w = wbuf[lax.rem(j, 2)]
            half = 2 * nb * rows
            for d in range(2):
                z = lax.dot_general(lhs[d * half:(d + 1) * half], w, NT, preferred_element_type=F32).astype(BF16)
                part[j, 2 * d] = z[:half // 2]
                part[j, 2 * d + 1] = z[half // 2:]
            scatter.start_far(j)

            @pl.when(j >= lag)
            def _():
                scatter.sums(j - lag)

            return 0

        lax.fori_loop(0, nc, body, 0)
        lax.fori_loop(0, nc, scatter.start_side, 0)

    pl.run_scoped(chain, pltpu.VMEM((4 * nb * rows, 6 * cols), BF16), pltpu.VMEM((2, CHUNK, 6 * cols), BF16))

    def weight_grad(g, ybuf, wst):
        bm = min(512, dim)
        n_chunks = dim // bm

        def chunk(c):
            slot = lax.rem(c, 2)
            return pltpu.make_async_copy(y_full.at[:, :, pl.ds(pl.multiple_of(c * bm, bm), bm)], ybuf.at[slot], y_sem.at[slot])

        def store(c):
            slot = lax.rem(c, 2)
            dst = pl.ds(pl.multiple_of(c * bm, bm), bm)
            return [pltpu.make_async_copy(wst.at[slot, :, pl.ds(m * cols, cols)], out.at[dst], o_sem.at[slot, m])
                    for m, out in enumerate((dwq_out, dwk_out, dwv_out))]

        load_g = pltpu.make_async_copy(g_hbm, g, ld_sem)
        load_g.start()
        chunk(0).start()
        load_g.wait()

        def body(c, _):
            slot = lax.rem(c, 2)

            @pl.when(c + 1 < n_chunks)
            def _():
                chunk(c + 1).start()

            @pl.when(c >= 2)
            def _():
                for s in store(c):
                    s.wait()

            chunk(c).wait()
            for m in range(lag):
                late = nc - lag + m
                pl.when(c == min(m, n_chunks - 1))(functools.partial(scatter.sums, max(late, 0)) if late >= 0 else (lambda: None))
            wst[slot] = lax.dot_general(ybuf[slot].reshape(nb * tokens, bm), g[...].reshape(nb * tokens, 3 * cols), TN,
                                        preferred_element_type=F32).astype(BF16)
            for s in store(c):
                s.start()
            return 0

        lax.fori_loop(0, n_chunks, body, 0)
        for s in range(min(2, n_chunks)):
            for c in store(s):
                c.wait()

    bm = min(512, dim)
    pl.run_scoped(weight_grad, pltpu.VMEM((nb, tokens, 3 * cols), BF16), pltpu.VMEM((2, nb, tokens, bm), BF16),
                  pltpu.VMEM((2, bm, 3 * cols), BF16))
    scatter_end(scatter, dy_out, out_sem, nc)


def dy_dw_call(n, g, g_p, w_q, w_k, w_v, wq_p, wk_p, wv_p, y_full):
    nb, tokens, wide = g.shape
    dim = y_full.shape[2]
    cols = wide // 3
    rows = tokens // n
    shape = jax.ShapeDtypeStruct
    dma = pltpu.SemaphoreType.DMA
    any_spec = pl.BlockSpec(memory_space=pl.ANY)
    return pl.pallas_call(
        functools.partial(dy_dw_kernel, n, nb, dim), name="dy_dw",
        out_shape=[shape((nb, rows, dim), BF16)] + [shape((dim, cols), BF16)] * 3,
        in_specs=[any_spec] * 9, out_specs=[any_spec] * 4,
        scratch_shapes=Scatter.scratch(nb * rows, dim) + [dma, dma((2, 6)), dma((2,)), dma((2, 3)), dma((nb,))],
        compiler_params=params(collective_id=3, has_side_effects=True),
        cost_estimate=cost(12 * nb * tokens * dim * cols, 30 * nb * tokens * cols),
    )(g, g_p, w_q, w_k, w_v, wq_p, wk_p, wv_p, y_full)


def token_kernel(n_copies, x_ref, dy_ref, pr_ref, g_ref, m_ref, e_ref, bo_ref, *refs):
    srcs, (xo_ref, dx_ref, dm_ref), dsts = refs[:4], refs[4:7], refs[7:11]
    bufs, (acc, in_sem, out_sem) = refs[11:15], refs[15:]
    group = 16
    step = pl.program_id(0)
    rows = x_ref.shape[1]
    groups = rows // group
    depth = bufs[0].shape[0]
    lag = depth - 1

    def move(c, out):
        copies = []
        for j, (src, dst, buf) in enumerate(zip(srcs, dsts, bufs)):
            size = buf.shape[1]
            sl = pl.ds(pl.multiple_of(c * size, 16), size)
            slot = lax.rem(c, depth)
            copies.append(pltpu.make_async_copy(buf.at[slot], dst.at[sl], out_sem.at[slot, j]) if out
                          else pltpu.make_async_copy(src.at[sl], buf.at[slot], in_sem.at[slot, j]))
        return copies

    def advance(i):
        @pl.when(i < n_copies)
        def _():
            @pl.when(i >= depth)
            def _():
                for c in move(i - depth, True):
                    c.wait()

            for c in move(i, False):
                c.start()

        @pl.when((i >= lag) & (i < n_copies + lag))
        def _():
            for c in move(i - lag, False):
                c.wait()
            for c in move(i - lag, True):
                c.start()

    mod = m_ref[...] + e_ref[0]
    shift_bo = bo_ref[...].reshape(1, bo_ref.shape[0])
    acc[...] = jnp.zeros_like(acc)

    def body(r, _):
        advance(step * groups + r)
        sl = pl.ds(pl.multiple_of(r * group, group), group)
        x = x_ref[0, sl].astype(F32)
        d_out = dy_ref[0, sl].astype(F32)
        proj = pr_ref[0, sl].astype(F32) + shift_bo
        xo_ref[0, sl] = (x + mod[2:3] * proj).astype(BF16)
        gate_part = d_out * proj
        x_norm, inv_std = norm_stats(x)
        d_y = g_ref[0, sl].astype(F32)
        d_norm = d_y * (1.0 + mod[1:2])
        d_x = d_out + inv_std * (
            d_norm - jnp.mean(d_norm, axis=-1, keepdims=True) - x_norm * jnp.mean(d_norm * x_norm, axis=-1, keepdims=True))
        dx_ref[0, sl] = d_x.astype(BF16)
        scale_part = d_y * x_norm
        acc[0] += d_y[:8] + d_y[8:]
        acc[1] += scale_part[:8] + scale_part[8:]
        acc[2] += gate_part[:8] + gate_part[8:]
        return 0

    lax.fori_loop(0, groups, body, 0)
    for j in range(3):
        dm_ref[0, j:j + 1] = jnp.sum(acc[j], axis=0, keepdims=True)

    @pl.when(step == pl.num_programs(0) - 1)
    def _():
        total = pl.num_programs(0) * groups

        def rest(i, _):
            advance(i)
            return 0

        lax.fori_loop(total, jnp.maximum(total, n_copies + lag), rest, 0)
        for c in range(max(n_copies - depth, 0), n_copies):
            for copy in move(c, True):
                copy.wait()


def token_call(x_loc, dy_loc, proj, d_y, m_block, e_loc, b_o, grads):
    nb, rows, dim = x_loc.shape
    n_copies = dim // min(512, dim)
    row = pl.BlockSpec((1, rows, dim), lambda i: (i, 0, 0))
    mod = pl.BlockSpec((1, 3, dim), lambda i: (i, 0, 0))
    any_spec = pl.BlockSpec(memory_space=pl.ANY)
    dma = pltpu.SemaphoreType.DMA
    depth = 4
    return pl.pallas_call(
        functools.partial(token_kernel, n_copies), name="tokens", grid=(nb,),
        out_shape=[jax.ShapeDtypeStruct(x_loc.shape, BF16), jax.ShapeDtypeStruct(x_loc.shape, BF16),
                   jax.ShapeDtypeStruct((nb, 3, dim), F32)] + [jax.ShapeDtypeStruct(w.shape, BF16) for w in grads],
        in_specs=[row, row, row, row, pl.BlockSpec((3, dim), lambda i: (0, 0)), mod, pl.BlockSpec(memory_space=pltpu.VMEM)] + [any_spec] * 4,
        out_specs=[row, row, mod] + [any_spec] * 4,
        scratch_shapes=[pltpu.VMEM((depth, w.shape[0] // n_copies, w.shape[1]), BF16) for w in grads]
        + [pltpu.VMEM((3, 8, dim), F32), dma((depth, 4)), dma((depth, 4))],
        compiler_params=params("arbitrary"),
        cost_estimate=cost(nb * rows * dim * 30, nb * rows * dim * 12),
    )(x_loc, dy_loc, proj, d_y, m_block, e_loc, b_o, *grads)


def solution(mesh):
    tp_size = mesh.shape['tp']

    def device_step(x_loc, e_loc, m_block, w_q, b_q, w_k, b_k, w_v, b_v, w_o, b_o, g_q, g_k, pos_part, dy_loc):
        nb, _, dim = x_loc.shape
        y_full, d_own, q, k, v, ss, cos_tab, sin_tab, gains = gather_qkv_call(
            tp_size, x_loc, dy_loc, m_block, e_loc, w_q, w_k, w_v, b_q, b_k, b_v, g_q, g_k, pos_part)
        d_full, o, _, d_attn, wq_p, wk_p, wv_p, _, part, far = gather_attn_call(
            tp_size, q, k, v, gains, cos_tab, sin_tab, ss, w_q, w_k, w_v, w_o, d_own)
        proj, g, g_p, _, _, d_wo, d_gq, d_gk = attn_bwd_call(
            tp_size, q, k, v, d_attn, gains, cos_tab, sin_tab, ss, o, part, far, d_full)
        d_y, d_wq, d_wk, d_wv = dy_dw_call(tp_size, g, g_p, w_q, w_k, w_v, wq_p, wk_p, wv_p, y_full)
        x_out, d_x, d_mod, d_wq, d_wk, d_wv, d_wo = token_call(
            x_loc, dy_loc, proj, d_y, m_block, e_loc, b_o, (d_wq, d_wk, d_wv, d_wo))
        d_e = all_sum_call(tp_size, d_mod.reshape(tp_size, -1, HEAD_DIM)).reshape(nb, 3, dim)
        return (x_out, d_x, d_e, jnp.sum(d_e, axis=0), d_wq, d_wk, d_wv, d_wo,
                jnp.sum(d_gq, axis=(0, 1)), jnp.sum(d_gk, axis=(0, 1)))

    in_specs = (P('dp', 'tp', None), P('dp', None, None), P(None, None), P(None, 'tp'), P('tp'), P(None, 'tp'), P('tp'),
                P(None, 'tp'), P('tp'), P('tp', None), P(None), P('tp'), P('tp'), P('dp', None), P('dp', 'tp', None))
    out_specs = (P('dp', 'tp', None), P('dp', 'tp', None), P('dp', None, None), P('dp', None), P('dp', 'tp'), P('dp', 'tp'),
                 P('dp', 'tp'), P(('dp', 'tp'), None), P(('dp', 'tp')), P(('dp', 'tp')))
    return jax.shard_map(device_step, mesh=mesh, in_specs=in_specs, out_specs=out_specs, check_vma=False)
```

```python
import functools

import jax
import jax.numpy as jnp
import numpy as np
from jax import lax
from jax.experimental import pallas as pl
from jax.experimental.pallas import tpu as pltpu
from jax.sharding import PartitionSpec as P

HEAD_DIM = 128
EPS_NORM = 1e-6
ROPE_BASE = 10000.0
LOG2E = 1.4426950408889634
CHUNK = 512
VMEM_LIMIT = 60 * 1024 * 1024
F32 = jnp.float32
BF16 = jnp.bfloat16
MESH_ID = pl.DeviceIdType.MESH
NT = (((1,), (1,)), ((), ()))
TN = (((0,), (0,)), ((), ()))


def params(*semantics, **kw):
    return pltpu.CompilerParams(dimension_semantics=semantics or None, vmem_limit_bytes=VMEM_LIMIT, **kw)


def cost(flops, nbytes):
    return pl.CostEstimate(flops=int(flops), bytes_accessed=int(nbytes), transcendentals=0)


def rope_freqs():
    half_dim = HEAD_DIM // 2
    side_len = HEAD_DIM // 6
    first_len = half_dim - 2 * side_len
    pair_idx = np.arange(HEAD_DIM) // 2
    section = (pair_idx >= first_len).astype(np.int32) + (pair_idx >= first_len + side_len).astype(np.int32)
    offset = np.where(section == 0, 0, np.where(section == 1, first_len, first_len + side_len))
    sec_width = np.where(section == 0, first_len, side_len)
    exponent = -(pair_idx - offset).astype(np.float32) / sec_width.astype(np.float32)
    freq_vals = np.power(np.float32(ROPE_BASE), exponent)
    return np.where(section[None, :] == np.arange(3)[:, None], freq_vals[None, :], np.float32(0.0)).astype(np.float32)


def norm_stats(x):
    centered = x - jnp.mean(x, axis=-1, keepdims=True)
    inv_std = lax.rsqrt(jnp.mean(centered * centered, axis=-1, keepdims=True) + EPS_NORM)
    return centered * inv_std, inv_std


def to_row(acc):
    return jnp.sum(acc.T, axis=0, keepdims=True)


def lanes_of(row):
    return jnp.broadcast_to(row, (HEAD_DIM, row.shape[1])).T


def head_sum(values):
    out = values[:, :HEAD_DIM]
    for h in range(1, values.shape[1] // HEAD_DIM):
        out = out + values[:, h * HEAD_DIM:(h + 1) * HEAD_DIM]
    return out


class Place:
    def __init__(self, n):
        self.n = n
        self.me = lax.axis_index('tp')
        self.right = lax.rem(self.me + 2, n)
        self.left = lax.rem(self.me + n - 2, n)
        self.far = lax.rem(self.me + n // 2, n)
        self.chip = self.me // 2

    def partner(self, dev):
        return dev + 1 - 2 * lax.rem(dev, 2)

    def arrive(self, devices):
        for dev in devices:
            pl.semaphore_signal(pltpu.get_barrier_semaphore(), inc=1, device_id={'tp': dev}, device_id_type=MESH_ID)

    def barrier(self, devices):
        self.arrive(devices)
        pl.semaphore_wait(pltpu.get_barrier_semaphore(), len(devices))

    def to_partner(self, src, dst, send_sem, recv_sem):
        return pltpu.make_async_remote_copy(src_ref=src, dst_ref=dst, send_sem=send_sem, recv_sem=recv_sem,
                                            device_id={'tp': self.partner(self.me)}, device_id_type=MESH_ID)

    def everyone(self):
        return [lax.rem(self.me + d, self.n) for d in range(1, self.n)]

    def near(self):
        return [self.right, self.left, self.partner(self.me)]


class Gather:
    def __init__(self, place, full, rows, send, recv, early=0):
        self.at, self.full, self.rows, self.send, self.recv, self.early = place, full, rows, send, recv, early

    def part(self, b, dev, off, count):
        return self.full.at[b, pl.ds(pl.multiple_of(dev * self.rows + off, 16), count)]

    def copy(self, b, dev, off, count, s_idx, r_idx, target):
        ref = self.part(b, dev, off, count)
        return pltpu.make_async_remote_copy(src_ref=ref, dst_ref=ref, send_sem=self.send.at[b, s_idx], recv_sem=self.recv.at[b, r_idx],
                                            device_id={'tp': target}, device_id_type=MESH_ID)

    def start_own(self, b):
        p = self.at
        self.copy(b, p.me, 0, self.rows, 0, 0, p.right).start()
        self.copy(b, p.me, 0, self.rows, 1, 1, p.left).start()
        self.copy(b, p.me, 0, self.rows, 2, 4, p.partner(p.me)).start()

    def whole_blocks_in(self, b):
        p = self.at
        self.copy(b, p.partner(p.me), 0, self.rows, 2, 4, p.me).wait_recv()
        self.copy(b, p.left, 0, self.rows, 0, 0, p.me).wait_recv()
        self.copy(b, p.right, 0, self.rows, 1, 1, p.me).wait_recv()
        for s_idx in range(3):
            self.copy(b, p.me, 0, self.rows, s_idx, s_idx, p.me).wait_send()

    def pass_left(self, b):
        p, half = self.at, self.rows // 2
        self.copy(b, p.left, 0, half, 3, 2, p.right).start()
        self.copy(b, p.left, 0, self.rows, 5, 5, p.partner(p.me)).start()

    def pass_right(self, b):
        p, half = self.at, self.rows // 2
        self.copy(b, p.right, half, half, 4, 3, p.left).start()
        self.copy(b, p.right, 0, self.rows, 6, 6, p.partner(p.me)).start()

    def take_own(self, b):
        p = self.at

        @pl.when(b >= self.early)
        def _():
            self.copy(b, p.partner(p.me), 0, self.rows, 2, 4, p.me).wait_recv()

    def take_left(self, b):
        p = self.at

        @pl.when(b >= self.early)
        def _():
            self.copy(b, p.left, 0, self.rows, 0, 0, p.me).wait_recv()
            self.pass_left(b)

        self.copy(b, p.partner(p.left), 0, self.rows, 5, 5, p.me).wait_recv()

    def take_right(self, b):
        p = self.at

        @pl.when(b >= self.early)
        def _():
            self.copy(b, p.right, 0, self.rows, 1, 1, p.me).wait_recv()
            self.pass_right(b)

        self.copy(b, p.partner(p.right), 0, self.rows, 6, 6, p.me).wait_recv()

    def take_far(self, b):
        p, half = self.at, self.rows // 2
        self.copy(b, p.far, 0, half, 3, 2, p.me).wait_recv()
        self.copy(b, p.far, 0, half, 7, 7, p.partner(p.me)).start()
        self.copy(b, p.far, half, half, 4, 3, p.me).wait_recv()
        self.copy(b, p.far, half, half, 8, 8, p.partner(p.me)).start()
        self.copy(b, p.partner(p.far), 0, half, 7, 7, p.me).wait_recv()
        self.copy(b, p.partner(p.far), half, half, 8, 8, p.me).wait_recv()

    def finish(self, b):
        p, half = self.at, self.rows // 2
        counts = (self.rows, self.rows, self.rows, half, half, self.rows, self.rows, half, half)
        for s_idx, count in list(enumerate(counts))[3 if b < self.early else 0:]:
            self.copy(b, p.me, 0, count, s_idx, s_idx, p.me).wait_send()

    def item_place(self, i, nb):
        j = i - nb
        b = jnp.where(i < nb, i, jnp.where(i < 3 * nb, j // 2, i - 3 * nb))
        chips = self.at.n // 2
        side = jnp.where(lax.rem(j + 2 * nb, 2) == 0, chips - 1, 1)
        off = jnp.where(i < nb, 0, jnp.where(i < 3 * nb, side, chips // 2))
        return b, pl.multiple_of(lax.rem(self.at.chip + off, chips) * (2 * self.rows), 32)

    def take_item(self, i, nb):
        b, row0 = self.item_place(i, nb)
        odd = lax.rem(i + nb, 2)
        pl.when(i < nb)(lambda: self.take_own(b))
        pl.when((i >= nb) & (i < 3 * nb) & (odd == 0))(lambda: self.take_left(b))
        pl.when((i >= nb) & (i < 3 * nb) & (odd == 1))(lambda: self.take_right(b))
        pl.when(i >= 3 * nb)(lambda: self.take_far(b))
        return b, row0


class RowTrade:
    def __init__(self, place, src, dst, rows, send, recv):
        self.at, self.src, self.dst, self.rows, self.send, self.recv = place, src, dst, rows, send, recv

    def copies(self, parity):
        p = self.at
        for b in range(self.src.shape[0]):
            for k in range(p.n // 2):
                sl = pl.ds(pl.multiple_of((2 * k + parity) * self.rows, 16), self.rows)
                yield p.to_partner(self.src.at[b, sl], self.dst.at[b, sl], self.send.at[b, k], self.recv.at[b, k])

    def start(self):
        for c in self.copies(1 - lax.rem(self.at.me, 2)):
            c.start()

    def wait_recv(self):
        for c in self.copies(lax.rem(self.at.me, 2)):
            c.wait_recv()

    def wait_send(self):
        for c in self.copies(1 - lax.rem(self.at.me, 2)):
            c.wait_send()


GATHER_SEMS = 9
EARLY_ROWS = 1
EARLY_CHUNKS = 4


def chunks_of(width, step):
    return [(c, min(c + step, width)) for c in range(0, width, step)]


class Exchange:
    def __init__(self, place, x_ref, slots, send_sems, recv_sems):
        self.at, self.x, self.slots, self.send, self.recv = place, x_ref, slots, send_sems, recv_sems

    def copy(self, d, dev, src):
        return pltpu.make_async_remote_copy(src_ref=self.x, dst_ref=self.slots.at[src], send_sem=self.send.at[d], recv_sem=self.recv.at[src],
                                            device_id={'tp': dev}, device_id_type=MESH_ID)

    def start(self):
        for d, dev in enumerate(self.at.everyone()):
            self.copy(d, dev, self.at.me).start()
        self.slots[self.at.me] = self.x[...]

    def finish(self):
        for d, dev in enumerate(self.at.everyone()):
            self.copy(d, dev, dev).wait()
        total = self.slots[0]
        for d in range(1, self.at.n):
            total = total + self.slots[d]
        return total


def gather_qkv_kernel(n, x_ref, dy_ref, m_ref, e_ref, wq_ref, wk_ref, wv_ref, wo_ref, bq_ref, bk_ref, bv_ref, gq_ref, gk_ref, pos_ref,
                      freq_ref, y_full, d_full, q_out, k_out, v_out, wo_p, ss_ref, cos_ref, sin_ref, gain_ref,
                      bias_ref, w_all, xin, stage, xbuf, zst, vst, sq, ss_row, slots,
                      w_sem, in_sem, st_sem, ld_sem, out_sem, g_send, g_recv, d_send, d_recv, e_send, e_recv, t_send, t_recv):
    nb, rows, dim = x_ref.shape
    cols = wq_ref.shape[1]
    place = Place(n)
    gather = Gather(place, y_full, rows, g_send, g_recv)
    gather_d = Gather(place, d_full, rows, d_send, d_recv)
    w_copies = [pltpu.make_async_copy(w, w_all.at[:, pl.ds(j * cols, cols)], w_sem.at[j]) for j, w in enumerate((wq_ref, wk_ref, wv_ref))]
    place.arrive(place.everyone())
    trade = place.to_partner(wo_ref, wo_p, t_send, t_recv)

    def load_x(b):
        return pltpu.make_async_copy(x_ref.at[b], xin.at[b], in_sem.at[b])

    for b in range(nb):
        load_x(b).start()
    for c in w_copies:
        c.start()
    group = 16

    def mine(full, b):
        return full.at[b, pl.ds(pl.multiple_of(place.me * rows, 16), rows)]

    def ln_step(b, _):
        load_x(b).wait()
        shift = m_ref[0:1] + e_ref[b, 0:1]
        scale_one = 1.0 + (m_ref[1:2] + e_ref[b, 1:2])

        def ln_rows(r, _):
            sl = pl.ds(pl.multiple_of(r * group, group), group)
            x_norm, _ = norm_stats(xin[b, sl].astype(F32))
            stage[b, sl] = (x_norm * scale_one + shift).astype(BF16)
            return 0

        lax.fori_loop(0, rows // group, ln_rows, 0)
        out = pltpu.make_async_copy(stage.at[b], mine(y_full, b), st_sem)
        out.start()

        @pl.when(b == 0)
        def _():
            pl.semaphore_wait(pltpu.get_barrier_semaphore(), n - 1)

        out.wait()
        gather.start_own(b)
        return 0

    lax.fori_loop(0, nb, ln_step, 0)
    load_dy = pltpu.make_async_copy(dy_ref, xin, in_sem.at[0])
    load_dy.start()
    for j, ref in enumerate((bq_ref, bk_ref, bv_ref)):
        bias_ref[:, j * cols:(j + 1) * cols] = ref[...].reshape(1, cols)
    for j, ref in enumerate((gq_ref, gk_ref)):
        gain_ref[j:j + 1] = ref[...].reshape(1, cols)

    def tables():
        lane = lax.broadcasted_iota(jnp.int32, (128, HEAD_DIM), 1)

        def rows_of(r, _):
            sl = pl.ds(pl.multiple_of(r * 128, 128), 128)
            pos = [lanes_of(pos_ref[m:m + 1, sl].astype(F32)) for m in range(3)]
            angle = pos[0] * freq_ref[0:1] + pos[1] * freq_ref[1:2] + pos[2] * freq_ref[2:3]
            cos_ref[sl] = jnp.cos(angle)
            sin_ref[sl] = jnp.where(lane % 2 == 0, -1.0, 1.0) * jnp.sin(angle)
            return 0

        lax.fori_loop(0, pos_ref.shape[1] // 128, rows_of, 0)

    def gate_step(b, _):
        gate = m_ref[2:3] + e_ref[b, 2:3]

        def gate_rows(r, _):
            sl = pl.ds(pl.multiple_of(r * group, group), group)
            stage[b, sl] = (xin[b, sl].astype(F32) * gate).astype(BF16)
            return 0

        lax.fori_loop(0, rows // group, gate_rows, 0)
        out = pltpu.make_async_copy(stage.at[b], mine(d_full, b), st_sem)
        out.start()
        out.wait()
        return 0

    for c in w_copies:
        c.wait()

    def outputs(b, row0, slot):
        dst = pl.ds(row0, 2 * rows)
        return [pltpu.make_async_copy(zst.at[slot, :, pl.ds(0, cols)], q_out.at[b, dst], out_sem.at[slot, 0]),
                pltpu.make_async_copy(zst.at[slot, :, pl.ds(cols, cols)], k_out.at[b, dst], out_sem.at[slot, 1]),
                pltpu.make_async_copy(vst.at[slot], v_out.at[b, dst], out_sem.at[slot, 2])]

    def item(i, _):
        b, row0 = gather.take_item(i, nb)
        slot = lax.rem(i, 2)
        load = pltpu.make_async_copy(y_full.at[b, pl.ds(row0, 2 * rows)], xbuf, ld_sem)
        load.start()

        @pl.when(i == 3 * nb - 1)
        def _():
            for d in range(EARLY_ROWS):
                gather_d.start_own(d)

        @pl.when(i == nb)
        def _():
            load_dy.wait()
            trade.start()
            lax.fori_loop(0, nb, gate_step, 0)
            tables()

        @pl.when(i >= 2)
        def _():
            for c in outputs(0, 0, slot):
                c.wait()

        load.wait()
        for lo, hi in chunks_of(3 * cols, 512):
            zst[slot, :, lo:hi] = jnp.dot(xbuf[...], w_all[:, lo:hi], preferred_element_type=F32) + bias_ref[:, lo:hi]
        vst[slot] = zst[slot, :, 2 * cols:].astype(BF16)
        q = zst[slot, :, :cols]
        k = zst[slot, :, cols:2 * cols]
        sq[2 * b, pl.ds(row0, 2 * rows)] = head_sum(q * q)
        sq[2 * b + 1, pl.ds(row0, 2 * rows)] = head_sum(k * k)
        for c in outputs(b, row0, slot):
            c.start()
        return 0

    lax.fori_loop(0, 4 * nb, item, 0)
    ss_row[...] = jnp.zeros_like(ss_row)
    for j in range(2 * nb):
        ss_row[j:j + 1] = to_row(sq[j])
    sums = Exchange(place, ss_row, slots, e_send, e_recv)
    sums.start()
    for slot in range(2):
        for c in outputs(0, 0, slot):
            c.wait()
    for b in range(nb):
        gather.finish(b)
    for d in range(EARLY_ROWS):
        gather_d.whole_blocks_in(d)
    trade.wait()
    ss_ref[...] = sums.finish()


def gather_qkv_call(n, x_loc, dy_loc, m_block, e_loc, w_q, w_k, w_v, w_o, b_q, b_k, b_v, g_q, g_k, positions):
    nb, rows, dim = x_loc.shape
    cols = w_q.shape[1]
    tokens = rows * n
    shape = jax.ShapeDtypeStruct
    any_spec = pl.BlockSpec(memory_space=pl.ANY)
    vmem = pl.BlockSpec(memory_space=pltpu.VMEM)
    dma = pltpu.SemaphoreType.DMA
    stat_rows = -(-2 * nb // 8) * 8
    return pl.pallas_call(
        functools.partial(gather_qkv_kernel, n), name="gather_qkv",
        out_shape=[shape((nb, tokens, dim), BF16), shape((nb, tokens, dim), BF16), shape((nb, tokens, cols), F32),
                   shape((nb, tokens, cols), F32), shape((nb, tokens, cols), BF16), shape(w_o.shape, BF16), shape((stat_rows, tokens), F32),
                   shape((tokens, HEAD_DIM), F32), shape((tokens, HEAD_DIM), F32), shape((2, cols), F32)],
        in_specs=[any_spec, any_spec, vmem, vmem] + [any_spec] * 4 + [vmem] * 7,
        out_specs=[any_spec] * 6 + [vmem] * 4,
        scratch_shapes=[
            pltpu.VMEM((1, 3 * cols), F32),
            pltpu.VMEM((dim, 3 * cols), BF16), pltpu.VMEM((nb, rows, dim), BF16), pltpu.VMEM((nb, rows, dim), BF16),
            pltpu.VMEM((2 * rows, dim), BF16), pltpu.VMEM((2, 2 * rows, 3 * cols), F32), pltpu.VMEM((2, 2 * rows, cols), BF16),
            pltpu.VMEM((2 * nb, tokens, HEAD_DIM), F32), pltpu.VMEM((stat_rows, tokens), F32), pltpu.VMEM((n, stat_rows, tokens), F32),
            dma((3,)), dma((nb,)), dma, dma, dma((2, 3)), dma((nb, GATHER_SEMS)), dma((nb, GATHER_SEMS)),
            dma((EARLY_ROWS, GATHER_SEMS)), dma((EARLY_ROWS, GATHER_SEMS)), dma((n,)), dma((n,)), dma, dma],
        compiler_params=params(collective_id=0, has_side_effects=True),
        cost_estimate=cost(6 * nb * tokens * dim * cols, 6 * dim * cols + 14 * nb * tokens * cols),
    )(x_loc, dy_loc, m_block, e_loc, w_q, w_k, w_v, w_o, b_q, b_k, b_v, g_q, g_k, positions.T, jnp.asarray(rope_freqs()))


def all_sum_kernel(n, x_ref, o_ref, pieces, total, send_a, recv_a, send_b, recv_b):
    place = Place(n)
    me = place.me
    place.barrier(place.everyone())

    def first(d, dev, src):
        return pltpu.make_async_remote_copy(src_ref=x_ref.at[src], dst_ref=pieces.at[me], send_sem=send_a.at[d], recv_sem=recv_a.at[me],
                                            device_id={'tp': dev}, device_id_type=MESH_ID)

    for d, dev in enumerate(place.everyone()):
        first(d, dev, dev).start()
    pieces[me] = x_ref[me]
    for d, dev in enumerate(place.everyone()):
        pltpu.make_async_remote_copy(src_ref=x_ref.at[me], dst_ref=pieces.at[dev], send_sem=send_a.at[d], recv_sem=recv_a.at[dev],
                                     device_id={'tp': dev}, device_id_type=MESH_ID).wait_recv()
    acc = pieces[0]
    for d in range(1, n):
        acc = acc + pieces[d]
    total[...] = acc
    o_ref[me] = acc
    for d, dev in enumerate(place.everyone()):
        first(d, dev, dev).wait_send()
    for d, dev in enumerate(place.everyone()):
        pltpu.make_async_remote_copy(src_ref=total, dst_ref=o_ref.at[me], send_sem=send_b.at[d], recv_sem=recv_b.at[me],
                                     device_id={'tp': dev}, device_id_type=MESH_ID).start()
    for d, dev in enumerate(place.everyone()):
        copy = pltpu.make_async_remote_copy(src_ref=total, dst_ref=o_ref.at[dev], send_sem=send_b.at[d], recv_sem=recv_b.at[dev],
                                            device_id={'tp': dev}, device_id_type=MESH_ID)
        copy.wait_send()
        copy.wait_recv()


def all_sum_call(n, x):
    spec = pl.BlockSpec(memory_space=pltpu.VMEM)
    dma = pltpu.SemaphoreType.DMA
    return pl.pallas_call(
        functools.partial(all_sum_kernel, n), name="all_sum",
        out_shape=jax.ShapeDtypeStruct(x.shape, x.dtype), in_specs=[spec], out_specs=spec,
        scratch_shapes=[pltpu.VMEM(x.shape, x.dtype), pltpu.VMEM(x.shape[1:], x.dtype), dma((n,)), dma((n,)), dma((n,)), dma((n,))],
        compiler_params=pltpu.CompilerParams(collective_id=4, has_side_effects=True, vmem_limit_bytes=4 * 1024 * 1024),
        cost_estimate=cost(4_000_000_000, x.size * 8),
    )(x)


def swap_pairs(x):
    lane = lax.broadcasted_iota(jnp.int32, x.shape, 1)
    return jnp.where(lane % 2 == 0, pltpu.roll(x, HEAD_DIM - 1, 1), pltpu.roll(x, 1, 1))


def rotate(x, cos, sin):
    return x * cos + swap_pairs(x) * sin


def softmax_block(s):
    c = HEAD_DIM ** -0.5 * LOG2E
    top = jnp.max(s, axis=1, keepdims=True)
    p = jnp.exp2(s * c - top * c)
    return p * (1.0 / jnp.sum(p, axis=1, keepdims=True))


class Scatter:
    def __init__(self, place, part, recv_far, recv_side, send, recv, far_src=None, early=0):
        self.at, self.part, self.far, self.side, self.send, self.recv = place, part, recv_far, recv_side, send, recv
        self.far_src, self.early = part if far_src is None else far_src, early
        self.rows = part.shape[2]
        self.half = self.rows // 2

    def copy(self, j, idx, src, dst, target):
        return pltpu.make_async_remote_copy(src_ref=src, dst_ref=dst, send_sem=self.send.at[j, idx], recv_sem=self.recv.at[j, idx],
                                            device_id={'tp': target}, device_id_type=MESH_ID)

    def message(self, j, idx):
        p, part, far, side = self.at, self.part, self.far, self.side
        first, second = pl.ds(0, self.half), pl.ds(self.half, self.rows - self.half)
        src, dst, target = (
            lambda: (self.far_src.at[j, 0, first], far.at[j, 0], p.right),
            lambda: (self.far_src.at[j, 0, second], far.at[j, 1], p.left),
            lambda: (part.at[j, 1, second], side.at[j, 0, second], p.right),
            lambda: (part.at[j, 2, first], side.at[j, 1, first], p.left),
            lambda: (part.at[j, 1, first], side.at[j, 0, first], p.right),
            lambda: (part.at[j, 2, second], side.at[j, 1, second], p.left))[idx]()
        return self.copy(j, idx, src, dst, target)

    def start_far(self, j, _=0):
        for idx in (0, 1):
            self.message(j, idx).start()
        return 0

    def start_side(self, j, _):
        for idx in (2, 3):
            self.message(j, idx).start()
        return 0

    def sums(self, j):
        h = self.half
        arrived = isinstance(j, int) and j < self.early
        if not arrived:
            self.message(j, 0).wait_recv()
        self.part[j, 1, :h] = (self.part[j, 1, :h].astype(F32) + self.far[j, 0].astype(F32)).astype(BF16)
        if not arrived:
            self.message(j, 1).wait_recv()
        self.part[j, 2, h:] = (self.part[j, 2, h:].astype(F32) + self.far[j, 1].astype(F32)).astype(BF16)
        self.message(j, 4).start()
        self.message(j, 5).start()

    def final(self, j):
        for idx in range(2, 6):
            self.message(j, idx).wait_recv()
        total = self.part[j, 3].astype(F32) + self.side[j, 0].astype(F32) + self.side[j, 1].astype(F32)
        self.part[j, 3] = total.astype(BF16)

    def finish(self, j):
        @pl.when(j >= self.early)
        def _():
            for idx in range(2):
                self.message(j, idx).wait_send()

        for idx in range(2, 6):
            self.message(j, idx).wait_send()

    @staticmethod
    def scratch(rows, dim):
        nc, dma = dim // CHUNK, pltpu.SemaphoreType.DMA
        return [pltpu.VMEM((nc, 4, rows, CHUNK), BF16), pltpu.VMEM((nc, 2, rows // 2, CHUNK), BF16),
                pltpu.VMEM((nc, 2, rows, CHUNK), BF16), dma((nc, 6)), dma((nc, 6))]


def scatter_outputs(part, out, sem, j):
    nb, rows, _ = out.shape
    cs = pl.ds(pl.multiple_of(j * CHUNK, CHUNK), CHUNK)
    return [pltpu.make_async_copy(part.at[j, 3, pl.ds(b * rows, rows)], out.at[b, :, cs], sem.at[b]) for b in range(nb)]


def scatter_end(scatter, out, sem, nc):
    def last(j, _):
        scatter.final(j)
        for c in scatter_outputs(scatter.part, out, sem, j):
            c.start()
        return 0

    lax.fori_loop(0, nc, last, 0)

    def drain(j, _):
        for c in scatter_outputs(scatter.part, out, sem, j):
            c.wait()
        scatter.finish(j)
        return 0

    lax.fori_loop(0, nc, drain, 0)


def pair_rows(place, nb, rows, mine, theirs, lhs, sem):
    width = mine.shape[2]
    out = []
    for d, dev in enumerate((place.far, place.right, place.left, place.me)):
        src_rows = pl.ds(pl.multiple_of(dev * rows, 16), rows)
        for b in range(nb):
            dst_rows = pl.ds((d * nb + b) * rows, rows)
            for j, src in enumerate((mine, theirs)):
                out.append(pltpu.make_async_copy(src.at[b, src_rows], lhs.at[dst_rows, pl.ds(j * width, width)], sem.at[d // 2]))
    return out


def gather_attn_kernel(n, nb, heads, dim, q_ref, k_ref, v_ref, gain_ref, cos_ref, sin_ref, ss_ref,
                       wq_ref, wo_ref, wo_p, d_in,
                       d_full, o_out, o_p, da_out, wq_p, part_out, far_in,
                       inv_q, inv_k, o_all, wo, xbuf, ast,
                       w_sem, ld_sem, out_sem, o_sem, p_sem, l_sem, g_send, g_recv, t_send, t_recv, r_send, r_recv, s_send, s_recv):
    step = pl.program_id(0)
    tokens = q_ref.shape[1]
    rows = tokens // n
    blk = min(256, tokens)
    place = Place(n)
    gather = Gather(place, d_full, rows, g_send, g_recv, early=EARLY_ROWS)
    cols = heads * HEAD_DIM
    nc = dim // CHUNK
    early_chunks = min(EARLY_CHUNKS, nc)
    scatter = Scatter(place, part_out, far_in, None, s_send, s_recv)
    trade_o = RowTrade(place, o_out, o_p, rows, r_send, r_recv)

    def trade_w():
        return place.to_partner(wq_ref, wq_p, t_send, t_recv)


    @pl.when(step == 0)
    def _():
        pltpu.make_async_copy(wo_ref, wo, w_sem).start()
        place.barrier(place.near())

        for b in range(EARLY_ROWS):
            gather.pass_left(b)
            gather.pass_right(b)

        def own(b, _):
            gather.start_own(b)
            return 0

        lax.fori_loop(EARLY_ROWS, nb, own, 0)
        trade_w().start()

    @pl.when(step < nb * heads)
    def _():
        b = step // heads
        h = lax.rem(step, heads)

        @pl.when(h == 0)
        def _():
            inv_q[...] = lanes_of(lax.rsqrt(ss_ref[pl.ds(2 * b, 1)] / dim + EPS_NORM))
            inv_k[...] = lanes_of(lax.rsqrt(ss_ref[pl.ds(2 * b + 1, 1)] / dim + EPS_NORM))

        cos, sin = cos_ref[...], sin_ref[...]
        q_rot = rotate(q_ref[0] * inv_q[...] * gain_ref[0:1], cos, sin).astype(BF16)
        k_rot = rotate(k_ref[0] * inv_k[...] * gain_ref[1:2], cos, sin).astype(BF16)
        v = v_ref[0]
        lanes = pl.ds(pl.multiple_of(h * HEAD_DIM, HEAD_DIM), HEAD_DIM)
        for i in range(tokens // blk):
            s = lax.dot_general(q_rot[i * blk:(i + 1) * blk], k_rot, NT, preferred_element_type=F32)
            p = softmax_block(s).astype(BF16)
            o_all[b, i * blk:(i + 1) * blk, lanes] = jnp.dot(p, v, preferred_element_type=F32).astype(BF16)

    @pl.when(step == nb * heads)
    def _():
        o_copy = pltpu.make_async_copy(o_all, o_out, o_sem)
        o_copy.start()
        pltpu.make_async_copy(wo_ref, wo, w_sem).wait()

        def outputs(b, row0, slot):
            return pltpu.make_async_copy(ast.at[slot], da_out.at[b, pl.ds(row0, 2 * rows)], out_sem.at[slot])

        def load(b, row0, slot):
            return pltpu.make_async_copy(d_full.at[b, pl.ds(row0, 2 * rows)], xbuf.at[slot], ld_sem.at[slot])

        def project(lhs, wbuf, stage):
            loads = pair_rows(place, nb, rows, o_out, o_p, lhs, l_sem)
            for c in loads:
                c.start()

            def chunk(j):
                cs = pl.ds(pl.multiple_of(j * CHUNK, CHUNK), CHUNK)
                slot = lax.rem(j, 2)
                return [pltpu.make_async_copy(wo_ref.at[:, cs], wbuf.at[slot, pl.ds(0, cols)], p_sem.at[slot, 0]),
                        pltpu.make_async_copy(wo_p.at[:, cs], wbuf.at[slot, pl.ds(cols, cols)], p_sem.at[slot, 1])]

            def store(j):
                slot = lax.rem(j, 2)
                return pltpu.make_async_copy(stage.at[slot], part_out.at[j], p_sem.at[slot, 2])

            def stored(j):
                store(j).wait()

                @pl.when(j < early_chunks)
                def _():
                    scatter.start_far(j)

            for c in chunk(0):
                c.start()
            for c in loads:
                c.wait()

            def body(j, _):
                slot = lax.rem(j, 2)

                @pl.when(j + 1 < nc)
                def _():
                    for c in chunk(j + 1):
                        c.start()

                for c in chunk(j):
                    c.wait()
                half = 2 * nb * rows
                for d in range(2):
                    z = jnp.dot(lhs[d * half:(d + 1) * half], wbuf[slot], preferred_element_type=F32).astype(BF16)
                    stage[slot, 2 * d] = z[:half // 2]
                    stage[slot, 2 * d + 1] = z[half // 2:]
                store(j).start()

                @pl.when(j >= 1)
                def _():
                    stored(j - 1)

                return 0

            lax.fori_loop(0, nc, body, 0)
            stored(nc - 1)

        def take(i):
            b, row0 = gather.take_item(i, nb)
            load(b, row0, lax.rem(i, 2)).start()

        take(0)

        def item(i, _):
            slot = lax.rem(i, 2)

            @pl.when(i + 1 < 3 * nb)
            def _():
                take(i + 1)

            @pl.when(i >= 2)
            def _():
                outputs(0, 0, slot).wait()

            load(0, 0, slot).wait()
            ast[slot] = lax.dot_general(xbuf[slot], wo[...], NT, preferred_element_type=F32).astype(BF16)
            b, row0 = gather.item_place(i, nb)
            outputs(b, row0, slot).start()

            @pl.when(i == 0)
            def _():
                o_copy.wait()
                trade_o.start()

            @pl.when(i + 1 == 3 * nb)
            def _():
                trade_o.wait_recv()
                pl.run_scoped(project, pltpu.VMEM((4 * nb * rows, 2 * cols), BF16), pltpu.VMEM((2, 2 * cols, CHUNK), BF16),
                              pltpu.VMEM((2, 4, nb * rows, CHUNK), BF16))

            @pl.when((i + 1 >= 3 * nb) & (i + 1 < 4 * nb))
            def _():
                take(i + 1)

            return 0

        lax.fori_loop(0, 4 * nb, item, 0)
        for slot in range(2):
            outputs(0, 0, slot).wait()
        for b in range(nb):
            gather.finish(b)
        trade_o.wait_send()
        trade_w().wait()
        for j in range(early_chunks):
            for idx in (0, 1):
                scatter.message(j, idx).wait()


def gather_attn_call(n, q, k, v, gains, cos_tab, sin_tab, ss, w_q, w_o, wo_p, d_full):
    nb, tokens, cols = q.shape
    dim = w_o.shape[1]
    heads = cols // HEAD_DIM
    rows = tokens // n
    last = nb * heads - 1
    nc = dim // CHUNK
    early = min(EARLY_CHUNKS, nc)
    shape = jax.ShapeDtypeStruct
    dma = pltpu.SemaphoreType.DMA
    any_spec = pl.BlockSpec(memory_space=pl.ANY)

    def head_of(i):
        i = jnp.minimum(i, last)
        return i // heads, i % heads

    blk = pl.BlockSpec((1, tokens, HEAD_DIM), lambda i: (head_of(i)[0], 0, head_of(i)[1]))
    vec = pl.BlockSpec((2, HEAD_DIM), lambda i: (0, head_of(i)[1]))
    tab = pl.BlockSpec((tokens, HEAD_DIM), lambda i: (0, 0))
    head_arr = shape((nb, tokens, cols), BF16)
    return pl.pallas_call(
        functools.partial(gather_attn_kernel, n, nb, heads, dim), name="gather_attn", grid=(nb * heads + 1,),
        out_shape=[shape(d_full.shape, BF16), head_arr, head_arr, head_arr, shape(w_q.shape, BF16)]
        + [shape((nc, 4, nb * rows, CHUNK), BF16), shape((early, 2, nb * rows // 2, CHUNK), BF16)],
        in_specs=[blk, blk, blk, vec, tab, tab, pl.BlockSpec(ss.shape, lambda i: (0, 0))] + [any_spec] * 4,
        out_specs=[any_spec] * 7,
        scratch_shapes=[
            pltpu.VMEM((tokens, HEAD_DIM), F32), pltpu.VMEM((tokens, HEAD_DIM), F32), pltpu.VMEM((nb, tokens, cols), BF16),
            pltpu.VMEM((cols, dim), BF16), pltpu.VMEM((2, 2 * rows, dim), BF16), pltpu.VMEM((2, 2 * rows, cols), BF16),
            dma, dma((2,)), dma((2,)), dma, dma((2, 3)), dma((2,)), dma((nb, GATHER_SEMS)), dma((nb, GATHER_SEMS)), dma, dma,
            dma((nb, n // 2)), dma((nb, n // 2)), dma((early, 6)), dma((early, 6))],
        input_output_aliases={10: 0},
        compiler_params=params("arbitrary", collective_id=1, has_side_effects=True),
        cost_estimate=cost(4 * nb * tokens * dim * cols + 4 * nb * tokens * tokens * cols, 8 * nb * tokens * dim),
    )(q, k, v, gains, cos_tab, sin_tab, ss, w_q, w_o, wo_p, d_full)


def attn_bwd_kernel(n, nb, heads, dim, q_ref, k_ref, v_ref, do_ref, gain_ref, cos_ref, sin_ref, ss_ref,
                    q_hbm, k_hbm, o_hbm, part_in, far_in, d_full, wk_hbm, wv_hbm,
                    proj_out, g_out, g_p, dqs_out, dks_out, dwo_out, wk_p, wv_p, dgq_ref, dgk_ref,
                    part, recv_far, recv_side, s_send, s_recv,
                    inv_q, inv_k, acc_q, acc_k, p_all, ds_all, dq_all, qs_st, ks_st, v_st, st_row, st_sum, slots,
                    ld_sem, w_sem, fl_sem, g_sem, go_sem, out_sem, e_send, e_recv, t_send, t_recv, r_send, r_recv):
    step = pl.program_id(0)
    tokens = q_ref.shape[1]
    rows = tokens // n
    cols = heads * HEAD_DIM
    blk = min(256, tokens)
    nc = dim // CHUNK
    steps = nb * heads
    scale = HEAD_DIM ** -0.5
    place = Place(n)
    early = far_in.shape[0]
    scatter = Scatter(place, part, recv_far, recv_side, s_send, s_recv, far_src=part_in, early=early)

    def stored():
        return [pltpu.make_async_copy(part_in, part, ld_sem.at[0]),
                pltpu.make_async_copy(far_in, recv_far.at[pl.ds(0, early)], ld_sem.at[1])]

    def trade_w(j):
        return place.to_partner((wk_hbm, wv_hbm)[j], (wk_p, wv_p)[j], t_send.at[j], t_recv.at[j])

    @pl.when(step == 0)
    def _():
        place.barrier(place.everyone())
        lax.fori_loop(early, nc, scatter.start_far, 0)
        for c in stored():
            c.start()
        for j in range(2):
            trade_w(j).start()

    @pl.when(step == 1)
    def _():
        for c in stored():
            c.wait()

    def flush(b, h, slot):
        lanes = pl.ds(pl.multiple_of(h * HEAD_DIM, HEAD_DIM), HEAD_DIM)
        v_lanes = pl.ds(pl.multiple_of(2 * cols + h * HEAD_DIM, HEAD_DIM), HEAD_DIM)
        return [pltpu.make_async_copy(qs_st.at[slot], dqs_out.at[b, :, lanes], fl_sem.at[slot, 0]),
                pltpu.make_async_copy(ks_st.at[slot], dks_out.at[b, :, lanes], fl_sem.at[slot, 1]),
                pltpu.make_async_copy(v_st.at[slot], g_out.at[b, :, v_lanes], fl_sem.at[slot, 2])]

    for j in range(nc):
        at_step = 1 + j * (steps - 2) // max(nc - 1, 1)
        pl.when(step == at_step)(functools.partial(scatter.sums, j))

    @pl.when(step < steps)
    def _():
        b = step // heads
        head = lax.rem(step, heads)
        slot = lax.rem(step, 2)

        @pl.when(step == 0)
        def _():
            st_row[...] = jnp.zeros_like(st_row)

        @pl.when(head == 0)
        def _():
            inv_q[...] = lanes_of(lax.rsqrt(ss_ref[pl.ds(2 * b, 1)] / dim + EPS_NORM))
            inv_k[...] = lanes_of(lax.rsqrt(ss_ref[pl.ds(2 * b + 1, 1)] / dim + EPS_NORM))
            acc_q[...] = jnp.zeros_like(acc_q)
            acc_k[...] = jnp.zeros_like(acc_k)

        @pl.when(step >= 2)
        def _():
            for c in flush(0, 0, slot):
                c.wait()

        cos, sin = cos_ref[...], sin_ref[...]
        q_rot = rotate(q_ref[0] * inv_q[...] * gain_ref[0:1], cos, sin).astype(BF16)
        k_rot = rotate(k_ref[0] * inv_k[...] * gain_ref[1:2], cos, sin).astype(BF16)
        v = v_ref[0]
        do = do_ref[0]
        for i in range(tokens // blk):
            sl = slice(i * blk, (i + 1) * blk)
            p = softmax_block(lax.dot_general(q_rot[sl], k_rot, NT, preferred_element_type=F32))
            p_all[sl] = p.astype(BF16)
            dp = lax.dot_general(do[sl], v, NT, preferred_element_type=F32)
            delta = jnp.sum(dp * p, axis=1, keepdims=True)
            ds = (p * (dp - delta)).astype(BF16)
            ds_all[sl] = ds
            dq_all[sl] = jnp.dot(ds, k_rot, preferred_element_type=F32) * scale
        do_t = do.astype(F32).T.astype(BF16)
        q_t = q_rot.astype(F32).T.astype(BF16)
        v_st[slot] = jnp.dot(do_t, p_all[...], preferred_element_type=F32).T.astype(BF16)
        dk_rot = (jnp.dot(q_t, ds_all[...], preferred_element_type=F32) * scale).T.astype(BF16).astype(F32)
        dq_rot = dq_all[...].astype(BF16).astype(F32)
        dq_hat = rotate(dq_rot, cos, -sin)
        dk_hat = rotate(dk_rot, cos, -sin)
        q_hat = q_ref[0] * inv_q[...]
        k_hat = k_ref[0] * inv_k[...]
        dgq_ref[0] = jnp.sum(dq_hat * q_hat, axis=0, keepdims=True)
        dgk_ref[0] = jnp.sum(dk_hat * k_hat, axis=0, keepdims=True)
        dq_s = dq_hat * gain_ref[0:1]
        dk_s = dk_hat * gain_ref[1:2]
        qs_st[slot] = dq_s
        ks_st[slot] = dk_s
        acc_q[...] += dq_s * q_hat
        acc_k[...] += dk_s * k_hat
        for c in flush(b, head, slot):
            c.start()

        @pl.when(head == heads - 1)
        def _():
            st_row[pl.ds(2 * b, 1)] = to_row(acc_q[...])
            st_row[pl.ds(2 * b + 1, 1)] = to_row(acc_k[...])

    @pl.when(step == steps)
    def _():
        for s in range(2):
            for c in flush(0, 0, s):
                c.wait()
        stats = Exchange(place, st_row, slots, e_send, e_recv)
        stats.start()
        lax.fori_loop(0, nc, scatter.start_side, 0)
        st_sum[...] = stats.finish()
        rb = min(256, tokens)
        per = tokens // rb
        trade = RowTrade(place, g_out, g_p, rows, r_send, r_recv)

        def norm_grad(fbuf, gbuf):
            def loads(i, slot):
                b, r0 = i // per, pl.multiple_of(lax.rem(i, per) * rb, rb)
                return [pltpu.make_async_copy(src.at[b, pl.ds(r0, rb)], fbuf.at[slot, m], g_sem.at[slot, m])
                        for m, src in enumerate((dqs_out, q_hbm, dks_out, k_hbm))]

            def store(i, slot):
                b, r0 = i // per, pl.multiple_of(lax.rem(i, per) * rb, rb)
                return pltpu.make_async_copy(gbuf.at[slot], g_out.at[b, pl.ds(r0, rb), pl.ds(0, 2 * cols)], go_sem.at[slot])

            for c in loads(0, 0):
                c.start()

            def body(i, _):
                slot = lax.rem(i, 2)
                b, r0 = i // per, pl.multiple_of(lax.rem(i, per) * rb, rb)

                @pl.when(i + 1 < nb * per)
                def _():
                    for c in loads(i + 1, lax.rem(i + 1, 2)):
                        c.start()

                @pl.when(r0 == 0)
                def _():
                    inv_q[...] = lanes_of(lax.rsqrt(ss_ref[pl.ds(2 * b, 1)] / dim + EPS_NORM))
                    inv_k[...] = lanes_of(lax.rsqrt(ss_ref[pl.ds(2 * b + 1, 1)] / dim + EPS_NORM))
                    acc_q[...] = lanes_of(st_sum[pl.ds(2 * b, 1)] / dim)
                    acc_k[...] = lanes_of(st_sum[pl.ds(2 * b + 1, 1)] / dim)

                @pl.when(i >= 2)
                def _():
                    store(0, slot).wait()

                for c in loads(i, slot):
                    c.wait()
                sl = pl.ds(r0, rb)
                for m, (inv, st) in enumerate(((inv_q, acc_q), (inv_k, acc_k))):
                    inv_l, st_l = inv[sl], st[sl]
                    for h in range(heads):
                        hs = slice(h * HEAD_DIM, (h + 1) * HEAD_DIM)
                        grad = inv_l * (fbuf[slot, 2 * m, :, hs] - (fbuf[slot, 2 * m + 1, :, hs] * inv_l) * st_l)
                        gbuf[slot, :, m * cols + h * HEAD_DIM:m * cols + (h + 1) * HEAD_DIM] = grad.astype(BF16)
                store(i, slot).start()
                return 0

            lax.fori_loop(0, nb * per, body, 0)
            for s in range(min(2, nb * per)):
                store(0, s).wait()

        pl.run_scoped(norm_grad, pltpu.VMEM((2, 4, rb, cols), F32), pltpu.VMEM((2, rb, 2 * cols), BF16))
        trade.start()

        def weight_grad(turned, obuf, dbuf, wst):
            bn = min(512, dim)
            n_chunks = dim // bn

            def chunk(c):
                slot = lax.rem(c, 2)
                return pltpu.make_async_copy(d_full.at[:, :, pl.ds(pl.multiple_of(c * bn, bn), bn)], dbuf.at[slot], go_sem.at[slot])

            def store(c):
                slot = lax.rem(c, 2)
                return pltpu.make_async_copy(wst.at[slot], dwo_out.at[:, pl.ds(pl.multiple_of(c * bn, bn), bn)], w_sem.at[slot, 0])

            load_o = pltpu.make_async_copy(o_hbm, obuf, ld_sem.at[0])
            load_o.start()
            chunk(0).start()
            load_o.wait()
            for b in range(nb):
                turned[:, b * tokens:(b + 1) * tokens] = obuf[b].T

            def body(c, _):
                slot = lax.rem(c, 2)

                @pl.when(c + 1 < n_chunks)
                def _():
                    chunk(c + 1).start()

                @pl.when(c >= 2)
                def _():
                    store(c).wait()

                chunk(c).wait()
                d = dbuf[slot].reshape(nb * tokens, bn)
                wst[slot] = jnp.dot(turned[...], d, preferred_element_type=F32).astype(BF16)
                store(c).start()
                return 0

            lax.fori_loop(0, n_chunks, body, 0)
            for s in range(min(2, n_chunks)):
                store(s).wait()

        bn = min(512, dim)
        pl.run_scoped(weight_grad, pltpu.VMEM((cols, nb * tokens), BF16), pltpu.VMEM((nb, tokens, cols), BF16),
                      pltpu.VMEM((2, nb, tokens, bn), BF16), pltpu.VMEM((2, cols, bn), BF16))
        scatter_end(scatter, proj_out, out_sem, nc)
        trade.wait_recv()
        trade.wait_send()
        for j in range(2):
            trade_w(j).wait()


def attn_bwd_call(n, q, k, v, d_attn, gains, cos_tab, sin_tab, ss, o, part, far, d_full, w_k, w_v):
    nb, tokens, cols = q.shape
    dim = d_full.shape[2]
    heads = cols // HEAD_DIM
    rows = tokens // n
    steps = nb * heads
    shape = jax.ShapeDtypeStruct
    dma = pltpu.SemaphoreType.DMA
    any_spec = pl.BlockSpec(memory_space=pl.ANY)

    def head_of(i):
        i = jnp.minimum(i, steps - 1)
        return i // heads, i % heads

    blk = pl.BlockSpec((1, tokens, HEAD_DIM), lambda i: (head_of(i)[0], 0, head_of(i)[1]))
    vec = pl.BlockSpec((2, HEAD_DIM), lambda i: (0, head_of(i)[1]))
    out_vec = pl.BlockSpec((1, 1, HEAD_DIM), lambda i: (head_of(i)[0], 0, head_of(i)[1]))
    tab = pl.BlockSpec((tokens, HEAD_DIM), lambda i: (0, 0))
    whole = (nb, tokens, cols)
    lane_tile = pltpu.VMEM((tokens, HEAD_DIM), F32)
    return pl.pallas_call(
        functools.partial(attn_bwd_kernel, n, nb, heads, dim), name="attn_bwd", grid=(steps + 1,),
        out_shape=[shape((nb, rows, dim), BF16), shape((nb, tokens, 3 * cols), BF16), shape((nb, tokens, 3 * cols), BF16),
                   shape(whole, F32), shape(whole, F32), shape((cols, dim), BF16),
                   shape(w_k.shape, BF16), shape(w_v.shape, BF16), shape((nb, 1, cols), F32), shape((nb, 1, cols), F32)],
        in_specs=[blk, blk, blk, blk, vec, tab, tab, pl.BlockSpec(ss.shape, lambda i: (0, 0))] + [any_spec] * 8,
        out_specs=[any_spec] * 8 + [out_vec, out_vec],
        scratch_shapes=Scatter.scratch(nb * rows, dim) + [lane_tile] * 4 + [pltpu.VMEM((tokens, tokens), BF16)] * 2 + [
            lane_tile, pltpu.VMEM((2, tokens, HEAD_DIM), F32), pltpu.VMEM((2, tokens, HEAD_DIM), F32),
            pltpu.VMEM((2, tokens, HEAD_DIM), BF16), pltpu.VMEM(ss.shape, F32), pltpu.VMEM(ss.shape, F32), pltpu.VMEM((n,) + ss.shape, F32),
            dma((2,)), dma((2, 2)), dma((2, 3)), dma((2, 4)), dma((2,)), dma((nb,)), dma((n,)), dma((n,)), dma((2,)), dma((2,)),
            dma((nb, n // 2)), dma((nb, n // 2))],
        compiler_params=params("arbitrary", collective_id=2, has_side_effects=True),
        cost_estimate=cost(4 * nb * tokens * dim * cols + 36 * nb * tokens * tokens * cols, 30 * nb * tokens * cols),
    )(q, k, v, d_attn, gains, cos_tab, sin_tab, ss, q, k, o, part, far, d_full, w_k, w_v)


def dy_dw_kernel(n, nb, dim, g_hbm, g_p, wq_hbm, wk_hbm, wv_hbm, wq_p, wk_p, wv_p, y_full,
                 dy_out, dwq_out, dwk_out, dwv_out,
                 part, recv_far, recv_side, s_send, s_recv, ld_sem, w_sem, y_sem, o_sem, out_sem):
    tokens = g_hbm.shape[1]
    rows = tokens // n
    cols = g_hbm.shape[2] // 3
    nc = dim // CHUNK
    place = Place(n)
    scatter = Scatter(place, part, recv_far, recv_side, s_send, s_recv)
    lag = 4

    def chain(lhs, wbuf):
        loads = pair_rows(place, nb, rows, g_hbm, g_p, lhs, ld_sem)
        for c in loads:
            c.start()

        def chunk(j):
            slot = lax.rem(j, 2)
            src = pl.ds(pl.multiple_of(j * CHUNK, CHUNK), CHUNK)
            return [pltpu.make_async_copy(w.at[src], wbuf.at[slot, :, pl.ds(m * cols, cols)], w_sem.at[slot, m])
                    for m, w in enumerate((wq_hbm, wk_hbm, wv_hbm, wq_p, wk_p, wv_p))]

        for c in chunk(0):
            c.start()
        place.barrier(place.near()[:2])

        def body(j, _):
            @pl.when(j + 1 < nc)
            def _():
                for c in chunk(j + 1):
                    c.start()

            for c in chunk(j):
                c.wait()
            slot = lax.rem(j, 2)
            half = 2 * nb * rows
            for d in range(2):
                @pl.when(j == 0)
                def _(d=d):
                    for c in loads[d * len(loads) // 2:(d + 1) * len(loads) // 2]:
                        c.wait()

                z = lax.dot_general(lhs[d * half:(d + 1) * half], wbuf[slot], NT, preferred_element_type=F32).astype(BF16)
                part[j, 2 * d] = z[:half // 2]
                part[j, 2 * d + 1] = z[half // 2:]
                if d == 0:
                    scatter.start_far(j)

            @pl.when(j >= lag)
            def _():
                scatter.sums(j - lag)

            return 0

        lax.fori_loop(0, nc, body, 0)
        lax.fori_loop(0, nc, scatter.start_side, 0)

    pl.run_scoped(chain, pltpu.VMEM((4 * nb * rows, 6 * cols), BF16), pltpu.VMEM((2, CHUNK, 6 * cols), BF16))

    def weight_grad(g, ybuf, wst):
        bm = min(512, dim)
        n_chunks = dim // bm

        def chunk(c):
            slot = lax.rem(c, 2)
            return pltpu.make_async_copy(y_full.at[:, :, pl.ds(pl.multiple_of(c * bm, bm), bm)], ybuf.at[slot], y_sem.at[slot])

        def store(c):
            slot = lax.rem(c, 2)
            dst = pl.ds(pl.multiple_of(c * bm, bm), bm)
            return [pltpu.make_async_copy(wst.at[slot, :, pl.ds(m * cols, cols)], out.at[dst], o_sem.at[slot, m])
                    for m, out in enumerate((dwq_out, dwk_out, dwv_out))]

        load_g = pltpu.make_async_copy(g_hbm, g, ld_sem.at[0])
        load_g.start()
        chunk(0).start()
        load_g.wait()

        def body(c, _):
            slot = lax.rem(c, 2)

            @pl.when(c + 1 < n_chunks)
            def _():
                chunk(c + 1).start()

            @pl.when(c >= 2)
            def _():
                for s in store(c):
                    s.wait()

            chunk(c).wait()
            for m in range(lag):
                late = nc - lag + m
                pl.when(c == min(m, n_chunks - 1))(functools.partial(scatter.sums, max(late, 0)) if late >= 0 else (lambda: None))
            wst[slot] = lax.dot_general(ybuf[slot].reshape(nb * tokens, bm), g[...].reshape(nb * tokens, 3 * cols), TN,
                                        preferred_element_type=F32).astype(BF16)
            for s in store(c):
                s.start()
            return 0

        lax.fori_loop(0, n_chunks, body, 0)
        for s in range(min(2, n_chunks)):
            for c in store(s):
                c.wait()

    bm = min(512, dim)
    pl.run_scoped(weight_grad, pltpu.VMEM((nb, tokens, 3 * cols), BF16), pltpu.VMEM((2, nb, tokens, bm), BF16),
                  pltpu.VMEM((2, bm, 3 * cols), BF16))
    scatter_end(scatter, dy_out, out_sem, nc)


def dy_dw_call(n, g, g_p, w_q, w_k, w_v, wq_p, wk_p, wv_p, y_full):
    nb, tokens, wide = g.shape
    dim = y_full.shape[2]
    cols = wide // 3
    rows = tokens // n
    shape = jax.ShapeDtypeStruct
    dma = pltpu.SemaphoreType.DMA
    any_spec = pl.BlockSpec(memory_space=pl.ANY)
    return pl.pallas_call(
        functools.partial(dy_dw_kernel, n, nb, dim), name="dy_dw",
        out_shape=[shape((nb, rows, dim), BF16)] + [shape((dim, cols), BF16)] * 3,
        in_specs=[any_spec] * 9, out_specs=[any_spec] * 4,
        scratch_shapes=Scatter.scratch(nb * rows, dim) + [dma((2,)), dma((2, 6)), dma((2,)), dma((2, 3)), dma((nb,))],
        compiler_params=params(collective_id=3, has_side_effects=True),
        cost_estimate=cost(12 * nb * tokens * dim * cols, 30 * nb * tokens * cols),
    )(g, g_p, w_q, w_k, w_v, wq_p, wk_p, wv_p, y_full)


def token_kernel(n_copies, x_ref, dy_ref, pr_ref, g_ref, m_ref, e_ref, bo_ref, gq_ref, gk_ref, *refs):
    srcs, (xo_ref, dx_ref, dm_ref, dgq_ref, dgk_ref), dsts = refs[:4], refs[4:9], refs[9:13]
    bufs, (acc, in_sem, out_sem) = refs[13:17], refs[17:]
    group = 16
    step = pl.program_id(0)
    rows = x_ref.shape[1]
    groups = rows // group
    depth = bufs[0].shape[0]
    lag = depth - 1

    def move(c, out):
        copies = []
        for j, (src, dst, buf) in enumerate(zip(srcs, dsts, bufs)):
            size = buf.shape[1]
            sl = pl.ds(pl.multiple_of(c * size, 16), size)
            slot = lax.rem(c, depth)
            copies.append(pltpu.make_async_copy(buf.at[slot], dst.at[sl], out_sem.at[slot, j]) if out
                          else pltpu.make_async_copy(src.at[sl], buf.at[slot], in_sem.at[slot, j]))
        return copies

    def advance(i):
        @pl.when(i < n_copies)
        def _():
            @pl.when(i >= depth)
            def _():
                for c in move(i - depth, True):
                    c.wait()

            for c in move(i, False):
                c.start()

        @pl.when((i >= lag) & (i < n_copies + lag))
        def _():
            for c in move(i - lag, False):
                c.wait()
            for c in move(i - lag, True):
                c.start()

    mod = m_ref[...] + e_ref[0]
    for src, dst in ((gq_ref, dgq_ref), (gk_ref, dgk_ref)):
        dst[...] = jnp.sum(src[...], axis=(0, 1))
    shift_bo = bo_ref[...].reshape(1, bo_ref.shape[0])
    acc[...] = jnp.zeros_like(acc)

    def body(r, _):
        advance(step * groups + r)
        sl = pl.ds(pl.multiple_of(r * group, group), group)
        x = x_ref[0, sl].astype(F32)
        d_out = dy_ref[0, sl].astype(F32)
        proj = pr_ref[0, sl].astype(F32) + shift_bo
        xo_ref[0, sl] = (x + mod[2:3] * proj).astype(BF16)
        gate_part = d_out * proj
        x_norm, inv_std = norm_stats(x)
        d_y = g_ref[0, sl].astype(F32)
        d_norm = d_y * (1.0 + mod[1:2])
        d_x = d_out + inv_std * (
            d_norm - jnp.mean(d_norm, axis=-1, keepdims=True) - x_norm * jnp.mean(d_norm * x_norm, axis=-1, keepdims=True))
        dx_ref[0, sl] = d_x.astype(BF16)
        scale_part = d_y * x_norm
        acc[0] += d_y[:8] + d_y[8:]
        acc[1] += scale_part[:8] + scale_part[8:]
        acc[2] += gate_part[:8] + gate_part[8:]
        return 0

    lax.fori_loop(0, groups, body, 0)
    for j in range(3):
        dm_ref[0, j:j + 1] = jnp.sum(acc[j], axis=0, keepdims=True)

    @pl.when(step == pl.num_programs(0) - 1)
    def _():
        total = pl.num_programs(0) * groups

        def rest(i, _):
            advance(i)
            return 0

        lax.fori_loop(total, jnp.maximum(total, n_copies + lag), rest, 0)
        for c in range(max(n_copies - depth, 0), n_copies):
            for copy in move(c, True):
                copy.wait()


def token_call(x_loc, dy_loc, proj, d_y, m_block, e_loc, b_o, d_gq, d_gk, grads):
    nb, rows, dim = x_loc.shape
    n_copies = dim // min(512, dim)
    row = pl.BlockSpec((1, rows, dim), lambda i: (i, 0, 0))
    mod = pl.BlockSpec((1, 3, dim), lambda i: (i, 0, 0))
    any_spec = pl.BlockSpec(memory_space=pl.ANY)
    dma = pltpu.SemaphoreType.DMA
    depth = 4
    return pl.pallas_call(
        functools.partial(token_kernel, n_copies), name="tokens", grid=(nb,),
        out_shape=[jax.ShapeDtypeStruct(x_loc.shape, BF16), jax.ShapeDtypeStruct(x_loc.shape, BF16),
                   jax.ShapeDtypeStruct((nb, 3, dim), F32)] + [jax.ShapeDtypeStruct(d_gq.shape[2:], F32)] * 2 + [jax.ShapeDtypeStruct(w.shape, BF16) for w in grads],
        in_specs=[row, row, row, row, pl.BlockSpec((3, dim), lambda i: (0, 0)), mod] + [pl.BlockSpec(memory_space=pltpu.VMEM)] * 3 + [any_spec] * 4,
        out_specs=[row, row, mod] + [pl.BlockSpec(memory_space=pltpu.VMEM)] * 2 + [any_spec] * 4,
        scratch_shapes=[pltpu.VMEM((depth, w.shape[0] // n_copies, w.shape[1]), BF16) for w in grads]
        + [pltpu.VMEM((3, 8, dim), F32), dma((depth, 4)), dma((depth, 4))],
        compiler_params=params("arbitrary"),
        cost_estimate=cost(nb * rows * dim * 30, nb * rows * dim * 12),
    )(x_loc, dy_loc, proj, d_y, m_block, e_loc, b_o, d_gq, d_gk, *grads)


def solution(mesh):
    tp_size = mesh.shape['tp']

    def device_step(x_loc, e_loc, m_block, w_q, b_q, w_k, b_k, w_v, b_v, w_o, b_o, g_q, g_k, pos_part, dy_loc):
        nb, _, dim = x_loc.shape
        y_full, d_own, q, k, v, wo_p, ss, cos_tab, sin_tab, gains = gather_qkv_call(
            tp_size, x_loc, dy_loc, m_block, e_loc, w_q, w_k, w_v, w_o, b_q, b_k, b_v, g_q, g_k, pos_part)
        d_full, o, _, d_attn, wq_p, part, far = gather_attn_call(
            tp_size, q, k, v, gains, cos_tab, sin_tab, ss, w_q, w_o, wo_p, d_own)
        proj, g, g_p, _, _, d_wo, wk_p, wv_p, d_gq, d_gk = attn_bwd_call(
            tp_size, q, k, v, d_attn, gains, cos_tab, sin_tab, ss, o, part, far, d_full, w_k, w_v)
        d_y, d_wq, d_wk, d_wv = dy_dw_call(tp_size, g, g_p, w_q, w_k, w_v, wq_p, wk_p, wv_p, y_full)
        x_out, d_x, d_mod, d_gq, d_gk, d_wq, d_wk, d_wv, d_wo = token_call(
            x_loc, dy_loc, proj, d_y, m_block, e_loc, b_o, d_gq, d_gk, (d_wq, d_wk, d_wv, d_wo))
        d_e = all_sum_call(tp_size, d_mod.reshape(tp_size, -1, HEAD_DIM)).reshape(nb, 3, dim)
        return x_out, d_x, d_e, jnp.sum(d_e, axis=0), d_wq, d_wk, d_wv, d_wo, d_gq, d_gk

    in_specs = (P('dp', 'tp', None), P('dp', None, None), P(None, None), P(None, 'tp'), P('tp'), P(None, 'tp'), P('tp'),
                P(None, 'tp'), P('tp'), P('tp', None), P(None), P('tp'), P('tp'), P('dp', None), P('dp', 'tp', None))
    out_specs = (P('dp', 'tp', None), P('dp', 'tp', None), P('dp', None, None), P('dp', None), P('dp', 'tp'), P('dp', 'tp'),
                 P('dp', 'tp'), P(('dp', 'tp'), None), P(('dp', 'tp')), P(('dp', 'tp')))
    return jax.shard_map(device_step, mesh=mesh, in_specs=in_specs, out_specs=out_specs, check_vma=False)
```

```python
import functools

import jax
import jax.numpy as jnp
import numpy as np
from jax import lax
from jax.experimental import pallas as pl
from jax.experimental.pallas import tpu as pltpu
from jax.sharding import PartitionSpec as P

HEAD_DIM = 128
EPS_NORM = 1e-6
ROPE_BASE = 10000.0
LOG2E = 1.4426950408889634
CHUNK = 512
VMEM_LIMIT = 60 * 1024 * 1024
F32 = jnp.float32
BF16 = jnp.bfloat16
MESH_ID = pl.DeviceIdType.MESH
NT = (((1,), (1,)), ((), ()))
TN = (((0,), (0,)), ((), ()))


def params(*semantics, **kw):
    return pltpu.CompilerParams(dimension_semantics=semantics or None, vmem_limit_bytes=VMEM_LIMIT, **kw)


def cost(flops, nbytes):
    return pl.CostEstimate(flops=int(flops), bytes_accessed=int(nbytes), transcendentals=0)


def rope_freqs():
    half_dim = HEAD_DIM // 2
    side_len = HEAD_DIM // 6
    first_len = half_dim - 2 * side_len
    pair_idx = np.arange(HEAD_DIM) // 2
    section = (pair_idx >= first_len).astype(np.int32) + (pair_idx >= first_len + side_len).astype(np.int32)
    offset = np.where(section == 0, 0, np.where(section == 1, first_len, first_len + side_len))
    sec_width = np.where(section == 0, first_len, side_len)
    exponent = -(pair_idx - offset).astype(np.float32) / sec_width.astype(np.float32)
    freq_vals = np.power(np.float32(ROPE_BASE), exponent)
    return np.where(section[None, :] == np.arange(3)[:, None], freq_vals[None, :], np.float32(0.0)).astype(np.float32)


def norm_stats(x):
    centered = x - jnp.mean(x, axis=-1, keepdims=True)
    inv_std = lax.rsqrt(jnp.mean(centered * centered, axis=-1, keepdims=True) + EPS_NORM)
    return centered * inv_std, inv_std


def to_row(acc):
    return jnp.sum(acc.T, axis=0, keepdims=True)


def lanes_of(row):
    return jnp.broadcast_to(row, (HEAD_DIM, row.shape[1])).T


def head_sum(values):
    out = values[:, :HEAD_DIM]
    for h in range(1, values.shape[1] // HEAD_DIM):
        out = out + values[:, h * HEAD_DIM:(h + 1) * HEAD_DIM]
    return out


class Place:
    def __init__(self, n):
        self.n = n
        self.me = lax.axis_index('tp')
        self.right = lax.rem(self.me + 2, n)
        self.left = lax.rem(self.me + n - 2, n)
        self.far = lax.rem(self.me + n // 2, n)
        self.chip = self.me // 2

    def partner(self, dev):
        return dev + 1 - 2 * lax.rem(dev, 2)

    def arrive(self, devices):
        for dev in devices:
            pl.semaphore_signal(pltpu.get_barrier_semaphore(), inc=1, device_id={'tp': dev}, device_id_type=MESH_ID)

    def barrier(self, devices):
        self.arrive(devices)
        pl.semaphore_wait(pltpu.get_barrier_semaphore(), len(devices))

    def to_partner(self, src, dst, send_sem, recv_sem):
        return pltpu.make_async_remote_copy(src_ref=src, dst_ref=dst, send_sem=send_sem, recv_sem=recv_sem,
                                            device_id={'tp': self.partner(self.me)}, device_id_type=MESH_ID)

    def everyone(self):
        return [lax.rem(self.me + d, self.n) for d in range(1, self.n)]

    def near(self):
        return [self.right, self.left, self.partner(self.me)]


class Gather:
    def __init__(self, place, full, rows, send, recv, early=0):
        self.at, self.full, self.rows, self.send, self.recv, self.early = place, full, rows, send, recv, early

    def part(self, b, dev, off, count):
        return self.full.at[b, pl.ds(pl.multiple_of(dev * self.rows + off, 16), count)]

    def copy(self, b, dev, off, count, s_idx, r_idx, target):
        ref = self.part(b, dev, off, count)
        return pltpu.make_async_remote_copy(src_ref=ref, dst_ref=ref, send_sem=self.send.at[b, s_idx], recv_sem=self.recv.at[b, r_idx],
                                            device_id={'tp': target}, device_id_type=MESH_ID)

    def start_own(self, b):
        p = self.at
        self.copy(b, p.me, 0, self.rows, 0, 0, p.right).start()
        self.copy(b, p.me, 0, self.rows, 1, 1, p.left).start()
        self.copy(b, p.me, 0, self.rows, 2, 4, p.partner(p.me)).start()

    def whole_blocks_in(self, b):
        p = self.at
        self.copy(b, p.partner(p.me), 0, self.rows, 2, 4, p.me).wait_recv()
        self.copy(b, p.left, 0, self.rows, 0, 0, p.me).wait_recv()
        self.copy(b, p.right, 0, self.rows, 1, 1, p.me).wait_recv()
        for s_idx in range(3):
            self.copy(b, p.me, 0, self.rows, s_idx, s_idx, p.me).wait_send()

    def pass_left(self, b):
        p, half = self.at, self.rows // 2
        self.copy(b, p.left, 0, half, 3, 2, p.right).start()
        self.copy(b, p.left, 0, self.rows, 5, 5, p.partner(p.me)).start()

    def pass_right(self, b):
        p, half = self.at, self.rows // 2
        self.copy(b, p.right, half, half, 4, 3, p.left).start()
        self.copy(b, p.right, 0, self.rows, 6, 6, p.partner(p.me)).start()

    def take_own(self, b):
        p = self.at

        @pl.when(b >= self.early)
        def _():
            self.copy(b, p.partner(p.me), 0, self.rows, 2, 4, p.me).wait_recv()

    def take_left(self, b):
        p = self.at

        @pl.when(b >= self.early)
        def _():
            self.copy(b, p.left, 0, self.rows, 0, 0, p.me).wait_recv()
            self.pass_left(b)

        self.copy(b, p.partner(p.left), 0, self.rows, 5, 5, p.me).wait_recv()

    def take_right(self, b):
        p = self.at

        @pl.when(b >= self.early)
        def _():
            self.copy(b, p.right, 0, self.rows, 1, 1, p.me).wait_recv()
            self.pass_right(b)

        self.copy(b, p.partner(p.right), 0, self.rows, 6, 6, p.me).wait_recv()

    def take_far(self, b):
        p, half = self.at, self.rows // 2
        self.copy(b, p.far, 0, half, 3, 2, p.me).wait_recv()
        self.copy(b, p.far, 0, half, 7, 7, p.partner(p.me)).start()
        self.copy(b, p.far, half, half, 4, 3, p.me).wait_recv()
        self.copy(b, p.far, half, half, 8, 8, p.partner(p.me)).start()
        self.copy(b, p.partner(p.far), 0, half, 7, 7, p.me).wait_recv()
        self.copy(b, p.partner(p.far), half, half, 8, 8, p.me).wait_recv()

    def finish(self, b):
        p, half = self.at, self.rows // 2
        counts = (self.rows, self.rows, self.rows, half, half, self.rows, self.rows, half, half)
        for s_idx, count in list(enumerate(counts))[3 if b < self.early else 0:]:
            self.copy(b, p.me, 0, count, s_idx, s_idx, p.me).wait_send()

    def item_place(self, i, nb):
        j = i - nb
        b = jnp.where(i < nb, i, jnp.where(i < 3 * nb, j // 2, i - 3 * nb))
        chips = self.at.n // 2
        side = jnp.where(lax.rem(j + 2 * nb, 2) == 0, chips - 1, 1)
        off = jnp.where(i < nb, 0, jnp.where(i < 3 * nb, side, chips // 2))
        return b, pl.multiple_of(lax.rem(self.at.chip + off, chips) * (2 * self.rows), 32)

    def take_item(self, i, nb):
        b, row0 = self.item_place(i, nb)
        odd = lax.rem(i + nb, 2)
        pl.when(i < nb)(lambda: self.take_own(b))
        pl.when((i >= nb) & (i < 3 * nb) & (odd == 0))(lambda: self.take_left(b))
        pl.when((i >= nb) & (i < 3 * nb) & (odd == 1))(lambda: self.take_right(b))
        pl.when(i >= 3 * nb)(lambda: self.take_far(b))
        return b, row0


class RowTrade:
    def __init__(self, place, src, dst, rows, send, recv):
        self.at, self.src, self.dst, self.rows, self.send, self.recv = place, src, dst, rows, send, recv

    def copies(self, parity):
        p = self.at
        for b in range(self.src.shape[0]):
            for k in range(p.n // 2):
                sl = pl.ds(pl.multiple_of((2 * k + parity) * self.rows, 16), self.rows)
                yield p.to_partner(self.src.at[b, sl], self.dst.at[b, sl], self.send.at[b, k], self.recv.at[b, k])

    def start(self):
        for c in self.copies(1 - lax.rem(self.at.me, 2)):
            c.start()

    def wait_recv(self):
        for c in self.copies(lax.rem(self.at.me, 2)):
            c.wait_recv()

    def wait_send(self):
        for c in self.copies(1 - lax.rem(self.at.me, 2)):
            c.wait_send()


GATHER_SEMS = 9
EARLY_ROWS = 1
EARLY_CHUNKS = 4
EARLY_DY = 4


def chunks_of(width, step):
    return [(c, min(c + step, width)) for c in range(0, width, step)]


class Exchange:
    def __init__(self, place, x_ref, slots, send_sems, recv_sems):
        self.at, self.x, self.slots, self.send, self.recv = place, x_ref, slots, send_sems, recv_sems

    def copy(self, d, dev, src):
        return pltpu.make_async_remote_copy(src_ref=self.x, dst_ref=self.slots.at[src], send_sem=self.send.at[d], recv_sem=self.recv.at[src],
                                            device_id={'tp': dev}, device_id_type=MESH_ID)

    def start(self):
        for d, dev in enumerate(self.at.everyone()):
            self.copy(d, dev, self.at.me).start()
        self.slots[self.at.me] = self.x[...]

    def finish(self):
        for d, dev in enumerate(self.at.everyone()):
            self.copy(d, dev, dev).wait()
        total = self.slots[0]
        for d in range(1, self.at.n):
            total = total + self.slots[d]
        return total


def gather_qkv_kernel(n, x_ref, dy_ref, m_ref, e_ref, wq_ref, wk_ref, wv_ref, wo_ref, bq_ref, bk_ref, bv_ref, gq_ref, gk_ref, pos_ref,
                      freq_ref, y_full, d_full, q_out, k_out, v_out, wo_p, wo_t, ss_ref, cos_ref, sin_ref, gain_ref,
                      bias_ref, w_all, xin, stage, xbuf, zst, vst, sq, ss_row, slots, wo_in, wo_st, wo_sem,
                      w_sem, in_sem, st_sem, ld_sem, out_sem, g_send, g_recv, d_send, d_recv, e_send, e_recv, t_send, t_recv):
    nb, rows, dim = x_ref.shape
    cols = wq_ref.shape[1]
    place = Place(n)
    gather = Gather(place, y_full, rows, g_send, g_recv)
    gather_d = Gather(place, d_full, rows, d_send, d_recv)
    w_copies = [pltpu.make_async_copy(w, w_all.at[:, pl.ds(j * cols, cols)], w_sem.at[j]) for j, w in enumerate((wq_ref, wk_ref, wv_ref))]
    place.arrive(place.everyone())
    trade = place.to_partner(wo_ref, wo_p, t_send, t_recv)

    def load_x(b):
        return pltpu.make_async_copy(x_ref.at[b], xin.at[b], in_sem.at[b])

    for b in range(nb):
        load_x(b).start()
    for c in w_copies:
        c.start()
    group = 16

    def mine(full, b):
        return full.at[b, pl.ds(pl.multiple_of(place.me * rows, 16), rows)]

    def ln_step(b, _):
        load_x(b).wait()
        shift = m_ref[0:1] + e_ref[b, 0:1]
        scale_one = 1.0 + (m_ref[1:2] + e_ref[b, 1:2])

        def ln_rows(r, _):
            sl = pl.ds(pl.multiple_of(r * group, group), group)
            x_norm, _ = norm_stats(xin[b, sl].astype(F32))
            stage[b, sl] = (x_norm * scale_one + shift).astype(BF16)
            return 0

        lax.fori_loop(0, rows // group, ln_rows, 0)
        out = pltpu.make_async_copy(stage.at[b], mine(y_full, b), st_sem)
        out.start()

        @pl.when(b == 0)
        def _():
            pl.semaphore_wait(pltpu.get_barrier_semaphore(), n - 1)

        out.wait()
        gather.start_own(b)
        return 0

    lax.fori_loop(0, nb, ln_step, 0)
    load_dy = pltpu.make_async_copy(dy_ref, xin, in_sem.at[0])
    load_dy.start()
    for j, ref in enumerate((bq_ref, bk_ref, bv_ref)):
        bias_ref[:, j * cols:(j + 1) * cols] = ref[...].reshape(1, cols)
    for j, ref in enumerate((gq_ref, gk_ref)):
        gain_ref[j:j + 1] = ref[...].reshape(1, cols)

    def tables():
        lane = lax.broadcasted_iota(jnp.int32, (128, HEAD_DIM), 1)

        def rows_of(r, _):
            sl = pl.ds(pl.multiple_of(r * 128, 128), 128)
            pos = [lanes_of(pos_ref[m:m + 1, sl].astype(F32)) for m in range(3)]
            angle = pos[0] * freq_ref[0:1] + pos[1] * freq_ref[1:2] + pos[2] * freq_ref[2:3]
            cos_ref[sl] = jnp.cos(angle)
            sin_ref[sl] = jnp.where(lane % 2 == 0, -1.0, 1.0) * jnp.sin(angle)
            return 0

        lax.fori_loop(0, pos_ref.shape[1] // 128, rows_of, 0)

    def turn_wo():
        width = wo_in.shape[2]
        n_chunks = dim // width

        def load(c):
            slot = lax.rem(c, 2)
            return pltpu.make_async_copy(wo_ref.at[:, pl.ds(pl.multiple_of(c * width, width), width)], wo_in.at[slot], wo_sem.at[slot, 0])

        def store(c):
            slot = lax.rem(c, 2)
            return pltpu.make_async_copy(wo_st.at[slot], wo_t.at[pl.ds(pl.multiple_of(c * width, width), width)], wo_sem.at[slot, 1])

        load(0).start()

        def body(c, _):
            slot = lax.rem(c, 2)

            @pl.when(c + 1 < n_chunks)
            def _():
                load(c + 1).start()

            @pl.when(c >= 2)
            def _():
                store(c).wait()

            load(c).wait()
            wo_st[slot] = wo_in[slot].T
            store(c).start()
            return 0

        lax.fori_loop(0, n_chunks, body, 0)
        for c in range(min(2, n_chunks)):
            store(c).wait()

    def gate_step(b, _):
        gate = m_ref[2:3] + e_ref[b, 2:3]

        def gate_rows(r, _):
            sl = pl.ds(pl.multiple_of(r * group, group), group)
            stage[b, sl] = (xin[b, sl].astype(F32) * gate).astype(BF16)
            return 0

        lax.fori_loop(0, rows // group, gate_rows, 0)
        out = pltpu.make_async_copy(stage.at[b], mine(d_full, b), st_sem)
        out.start()
        out.wait()
        return 0

    for c in w_copies:
        c.wait()

    def outputs(b, row0, slot):
        dst = pl.ds(row0, 2 * rows)
        return [pltpu.make_async_copy(zst.at[slot, :, pl.ds(0, cols)], q_out.at[b, dst], out_sem.at[slot, 0]),
                pltpu.make_async_copy(zst.at[slot, :, pl.ds(cols, cols)], k_out.at[b, dst], out_sem.at[slot, 1]),
                pltpu.make_async_copy(vst.at[slot], v_out.at[b, dst], out_sem.at[slot, 2])]

    def item(i, _):
        b, row0 = gather.take_item(i, nb)
        slot = lax.rem(i, 2)
        load = pltpu.make_async_copy(y_full.at[b, pl.ds(row0, 2 * rows)], xbuf, ld_sem)
        load.start()

        @pl.when(i == 3 * nb - 1)
        def _():
            for d in range(EARLY_ROWS):
                gather_d.start_own(d)

        @pl.when(i == nb)
        def _():
            load_dy.wait()
            trade.start()
            lax.fori_loop(0, nb, gate_step, 0)
            tables()
            turn_wo()

        @pl.when(i >= 2)
        def _():
            for c in outputs(0, 0, slot):
                c.wait()

        load.wait()
        for lo, hi in chunks_of(3 * cols, 512):
            zst[slot, :, lo:hi] = jnp.dot(xbuf[...], w_all[:, lo:hi], preferred_element_type=F32) + bias_ref[:, lo:hi]
        vst[slot] = zst[slot, :, 2 * cols:].astype(BF16)
        q = zst[slot, :, :cols]
        k = zst[slot, :, cols:2 * cols]
        sq[2 * b, pl.ds(row0, 2 * rows)] = head_sum(q * q)
        sq[2 * b + 1, pl.ds(row0, 2 * rows)] = head_sum(k * k)
        for c in outputs(b, row0, slot):
            c.start()
        return 0

    lax.fori_loop(0, 4 * nb, item, 0)
    ss_row[...] = jnp.zeros_like(ss_row)
    for j in range(2 * nb):
        ss_row[j:j + 1] = to_row(sq[j])
    sums = Exchange(place, ss_row, slots, e_send, e_recv)
    sums.start()
    for slot in range(2):
        for c in outputs(0, 0, slot):
            c.wait()
    for b in range(nb):
        gather.finish(b)
    for d in range(EARLY_ROWS):
        gather_d.whole_blocks_in(d)
    trade.wait()
    ss_ref[...] = sums.finish()


def gather_qkv_call(n, x_loc, dy_loc, m_block, e_loc, w_q, w_k, w_v, w_o, b_q, b_k, b_v, g_q, g_k, positions):
    nb, rows, dim = x_loc.shape
    cols = w_q.shape[1]
    tokens = rows * n
    shape = jax.ShapeDtypeStruct
    any_spec = pl.BlockSpec(memory_space=pl.ANY)
    vmem = pl.BlockSpec(memory_space=pltpu.VMEM)
    dma = pltpu.SemaphoreType.DMA
    stat_rows = -(-2 * nb // 8) * 8
    return pl.pallas_call(
        functools.partial(gather_qkv_kernel, n), name="gather_qkv",
        out_shape=[shape((nb, tokens, dim), BF16), shape((nb, tokens, dim), BF16), shape((nb, tokens, cols), F32),
                   shape((nb, tokens, cols), F32), shape((nb, tokens, cols), BF16), shape(w_o.shape, BF16), shape((dim, cols), BF16), shape((stat_rows, tokens), F32),
                   shape((tokens, HEAD_DIM), F32), shape((tokens, HEAD_DIM), F32), shape((2, cols), F32)],
        in_specs=[any_spec, any_spec, vmem, vmem] + [any_spec] * 4 + [vmem] * 7,
        out_specs=[any_spec] * 7 + [vmem] * 4,
        scratch_shapes=[
            pltpu.VMEM((1, 3 * cols), F32),
            pltpu.VMEM((dim, 3 * cols), BF16), pltpu.VMEM((nb, rows, dim), BF16), pltpu.VMEM((nb, rows, dim), BF16),
            pltpu.VMEM((2 * rows, dim), BF16), pltpu.VMEM((2, 2 * rows, 3 * cols), F32), pltpu.VMEM((2, 2 * rows, cols), BF16),
            pltpu.VMEM((2 * nb, tokens, HEAD_DIM), F32), pltpu.VMEM((stat_rows, tokens), F32), pltpu.VMEM((n, stat_rows, tokens), F32),
            pltpu.VMEM((2, cols, min(512, dim)), BF16), pltpu.VMEM((2, min(512, dim), cols), BF16), dma((2, 2)),
            dma((3,)), dma((nb,)), dma, dma, dma((2, 3)), dma((nb, GATHER_SEMS)), dma((nb, GATHER_SEMS)),
            dma((EARLY_ROWS, GATHER_SEMS)), dma((EARLY_ROWS, GATHER_SEMS)), dma((n,)), dma((n,)), dma, dma],
        compiler_params=params(collective_id=0, has_side_effects=True),
        cost_estimate=cost(6 * nb * tokens * dim * cols, 6 * dim * cols + 14 * nb * tokens * cols),
    )(x_loc, dy_loc, m_block, e_loc, w_q, w_k, w_v, w_o, b_q, b_k, b_v, g_q, g_k, positions.T, jnp.asarray(rope_freqs()))


def all_sum_kernel(n, x_ref, o_ref, pieces, total, send_a, recv_a, send_b, recv_b):
    place = Place(n)
    me = place.me
    place.barrier(place.everyone())

    def first(d, dev, src):
        return pltpu.make_async_remote_copy(src_ref=x_ref.at[src], dst_ref=pieces.at[me], send_sem=send_a.at[d], recv_sem=recv_a.at[me],
                                            device_id={'tp': dev}, device_id_type=MESH_ID)

    for d, dev in enumerate(place.everyone()):
        first(d, dev, dev).start()
    pieces[me] = x_ref[me]
    for d, dev in enumerate(place.everyone()):
        pltpu.make_async_remote_copy(src_ref=x_ref.at[me], dst_ref=pieces.at[dev], send_sem=send_a.at[d], recv_sem=recv_a.at[dev],
                                     device_id={'tp': dev}, device_id_type=MESH_ID).wait_recv()
    acc = pieces[0]
    for d in range(1, n):
        acc = acc + pieces[d]
    total[...] = acc
    o_ref[me] = acc
    for d, dev in enumerate(place.everyone()):
        first(d, dev, dev).wait_send()
    for d, dev in enumerate(place.everyone()):
        pltpu.make_async_remote_copy(src_ref=total, dst_ref=o_ref.at[me], send_sem=send_b.at[d], recv_sem=recv_b.at[me],
                                     device_id={'tp': dev}, device_id_type=MESH_ID).start()
    for d, dev in enumerate(place.everyone()):
        copy = pltpu.make_async_remote_copy(src_ref=total, dst_ref=o_ref.at[dev], send_sem=send_b.at[d], recv_sem=recv_b.at[dev],
                                            device_id={'tp': dev}, device_id_type=MESH_ID)
        copy.wait_send()
        copy.wait_recv()


def all_sum_call(n, x):
    spec = pl.BlockSpec(memory_space=pltpu.VMEM)
    dma = pltpu.SemaphoreType.DMA
    return pl.pallas_call(
        functools.partial(all_sum_kernel, n), name="all_sum",
        out_shape=jax.ShapeDtypeStruct(x.shape, x.dtype), in_specs=[spec], out_specs=spec,
        scratch_shapes=[pltpu.VMEM(x.shape, x.dtype), pltpu.VMEM(x.shape[1:], x.dtype), dma((n,)), dma((n,)), dma((n,)), dma((n,))],
        compiler_params=pltpu.CompilerParams(collective_id=4, has_side_effects=True, vmem_limit_bytes=4 * 1024 * 1024),
        cost_estimate=cost(4_000_000_000, x.size * 8),
    )(x)


def swap_pairs(x):
    lane = lax.broadcasted_iota(jnp.int32, x.shape, 1)
    return jnp.where(lane % 2 == 0, pltpu.roll(x, HEAD_DIM - 1, 1), pltpu.roll(x, 1, 1))


def rotate(x, cos, sin):
    return x * cos + swap_pairs(x) * sin


SCORE_SCALE = HEAD_DIM ** -0.5 * LOG2E


def softmax_block(s):
    top = jnp.max(s, axis=1, keepdims=True)
    p = jnp.exp2(s * SCORE_SCALE - top * SCORE_SCALE)
    total = jnp.sum(p, axis=1, keepdims=True)
    return p * (1.0 / total), top * SCORE_SCALE + jnp.log(total) * LOG2E


class Scatter:
    def __init__(self, place, part, recv_far, recv_side, send, recv, far_src=None, early=0):
        self.at, self.part, self.far, self.side, self.send, self.recv = place, part, recv_far, recv_side, send, recv
        self.far_src, self.early = part if far_src is None else far_src, early
        self.rows = part.shape[2]
        self.half = self.rows // 2

    def copy(self, j, idx, src, dst, target):
        return pltpu.make_async_remote_copy(src_ref=src, dst_ref=dst, send_sem=self.send.at[j, idx], recv_sem=self.recv.at[j, idx],
                                            device_id={'tp': target}, device_id_type=MESH_ID)

    def message(self, j, idx):
        p, part, far, side = self.at, self.part, self.far, self.side
        first, second = pl.ds(0, self.half), pl.ds(self.half, self.rows - self.half)
        src, dst, target = (
            lambda: (self.far_src.at[j, 0, first], far.at[j, 0], p.right),
            lambda: (self.far_src.at[j, 0, second], far.at[j, 1], p.left),
            lambda: (part.at[j, 1, second], side.at[j, 0, second], p.right),
            lambda: (part.at[j, 2, first], side.at[j, 1, first], p.left),
            lambda: (part.at[j, 1, first], side.at[j, 0, first], p.right),
            lambda: (part.at[j, 2, second], side.at[j, 1, second], p.left))[idx]()
        return self.copy(j, idx, src, dst, target)

    def start_far(self, j, _=0):
        for idx in (0, 1):
            self.message(j, idx).start()
        return 0

    def start_side(self, j, _):
        for idx in (2, 3):
            self.message(j, idx).start()
        return 0

    def sums(self, j):
        h = self.half

        @pl.when(j >= self.early)
        def _():
            self.message(j, 0).wait_recv()
            self.message(j, 1).wait_recv()

        self.part[j, 1, :h] = (self.part[j, 1, :h].astype(F32) + self.far[j, 0].astype(F32)).astype(BF16)
        self.part[j, 2, h:] = (self.part[j, 2, h:].astype(F32) + self.far[j, 1].astype(F32)).astype(BF16)
        self.message(j, 4).start()
        self.message(j, 5).start()

    def sums_step(self, j, _):
        self.sums(j)
        return 0

    def final(self, j):
        for idx in range(2, 6):
            self.message(j, idx).wait_recv()
        total = self.part[j, 3].astype(F32) + self.side[j, 0].astype(F32) + self.side[j, 1].astype(F32)
        self.part[j, 3] = total.astype(BF16)

    def finish(self, j):
        @pl.when(j >= self.early)
        def _():
            for idx in range(2):
                self.message(j, idx).wait_send()

        for idx in range(2, 6):
            self.message(j, idx).wait_send()

    @staticmethod
    def scratch(rows, dim):
        nc, dma = dim // CHUNK, pltpu.SemaphoreType.DMA
        return [pltpu.VMEM((nc, 4, rows, CHUNK), BF16), pltpu.VMEM((nc, 2, rows // 2, CHUNK), BF16),
                pltpu.VMEM((nc, 2, rows, CHUNK), BF16), dma((nc, 6)), dma((nc, 6))]


def scatter_outputs(part, out, sem, j):
    nb, rows, _ = out.shape
    cs = pl.ds(pl.multiple_of(j * CHUNK, CHUNK), CHUNK)
    return [pltpu.make_async_copy(part.at[j, 3, pl.ds(b * rows, rows)], out.at[b, :, cs], sem.at[b]) for b in range(nb)]


def scatter_end(scatter, out, sem, nc):
    def last(j, _):
        scatter.final(j)
        for c in scatter_outputs(scatter.part, out, sem, j):
            c.start()
        return 0

    lax.fori_loop(0, nc, last, 0)

    def drain(j, _):
        for c in scatter_outputs(scatter.part, out, sem, j):
            c.wait()
        scatter.finish(j)
        return 0

    lax.fori_loop(0, nc, drain, 0)


def pair_rows(place, nb, rows, mine, theirs, lhs, sem):
    width = mine.shape[2]
    out = []
    for d, dev in enumerate((place.far, place.right, place.left, place.me)):
        src_rows = pl.ds(pl.multiple_of(dev * rows, 16), rows)
        for b in range(nb):
            dst_rows = pl.ds((d * nb + b) * rows, rows)
            for j, src in enumerate((mine, theirs)):
                out.append(pltpu.make_async_copy(src.at[b, src_rows], lhs.at[dst_rows, pl.ds(j * width, width)], sem.at[d // 2]))
    return out


def gather_attn_kernel(n, nb, heads, dim, q_ref, k_ref, v_ref, gain_ref, cos_ref, sin_ref, ss_ref,
                       wq_ref, wo_ref, wo_p, wo_t, d_in,
                       d_full, o_out, o_p, da_out, wq_p, part_out, far_in, qr_ref, kr_ref, lse_ref, o32_ref,
                       inv_q, inv_k, o_all, wo, xbuf, ast,
                       w_sem, ld_sem, out_sem, o_sem, p_sem, l_sem, g_send, g_recv, t_send, t_recv, r_send, r_recv, s_send, s_recv):
    step = pl.program_id(0)
    tokens = q_ref.shape[1]
    rows = tokens // n
    blk = min(384, tokens)
    place = Place(n)
    gather = Gather(place, d_full, rows, g_send, g_recv, early=EARLY_ROWS)
    cols = heads * HEAD_DIM
    nc = dim // CHUNK
    early_chunks = min(EARLY_CHUNKS, nc)
    scatter = Scatter(place, part_out, far_in, None, s_send, s_recv)
    trade_o = RowTrade(place, o_out, o_p, rows, r_send, r_recv)

    def trade_w():
        return place.to_partner(wq_ref, wq_p, t_send, t_recv)


    @pl.when(step == 0)
    def _():
        pltpu.make_async_copy(wo_t, wo, w_sem).start()
        place.barrier(place.near())

        for b in range(EARLY_ROWS):
            gather.pass_left(b)
            gather.pass_right(b)

        def own(b, _):
            gather.start_own(b)
            return 0

        lax.fori_loop(EARLY_ROWS, nb, own, 0)
        trade_w().start()

    @pl.when(step < nb * heads)
    def _():
        b = step // heads
        h = lax.rem(step, heads)

        @pl.when(h == 0)
        def _():
            inv_q[...] = lanes_of(lax.rsqrt(ss_ref[pl.ds(2 * b, 1)] / dim + EPS_NORM))
            inv_k[...] = lanes_of(lax.rsqrt(ss_ref[pl.ds(2 * b + 1, 1)] / dim + EPS_NORM))

        cos, sin = cos_ref[...], sin_ref[...]
        q_rot = rotate(q_ref[0] * inv_q[...] * gain_ref[0:1], cos, sin).astype(BF16)
        k_rot = rotate(k_ref[0] * inv_k[...] * gain_ref[1:2], cos, sin).astype(BF16)
        v = v_ref[0]
        lanes = pl.ds(pl.multiple_of(h * HEAD_DIM, HEAD_DIM), HEAD_DIM)
        qr_ref[0], kr_ref[0] = q_rot, k_rot

        def scores(i):
            return lax.dot_general(q_rot[i * blk:(i + 1) * blk], k_rot, NT, preferred_element_type=F32)

        ahead = scores(0)
        for i in range(tokens // blk):
            s = ahead
            if (i + 1) * blk < tokens:
                ahead = scores(i + 1)
            p, lse = softmax_block(s)
            lse_ref[0, i * blk:(i + 1) * blk] = jnp.broadcast_to(lse, (blk, HEAD_DIM))
            o = jnp.dot(p.astype(BF16), v, preferred_element_type=F32)
            o32_ref[0, i * blk:(i + 1) * blk] = o
            o_all[b, i * blk:(i + 1) * blk, lanes] = o.astype(BF16)

    @pl.when(step == nb * heads)
    def _():
        o_copy = pltpu.make_async_copy(o_all, o_out, o_sem)
        o_copy.start()
        pltpu.make_async_copy(wo_t, wo, w_sem).wait()

        def outputs(b, row0, slot):
            return pltpu.make_async_copy(ast.at[slot], da_out.at[b, pl.ds(row0, 2 * rows)], out_sem.at[slot])

        def load(b, row0, slot):
            return pltpu.make_async_copy(d_full.at[b, pl.ds(row0, 2 * rows)], xbuf.at[slot], ld_sem.at[slot])

        def project(lhs, wbuf, stage):
            loads = pair_rows(place, nb, rows, o_out, o_p, lhs, l_sem)
            for c in loads:
                c.start()

            def chunk(j):
                cs = pl.ds(pl.multiple_of(j * CHUNK, CHUNK), CHUNK)
                slot = lax.rem(j, 2)
                return [pltpu.make_async_copy(wo_ref.at[:, cs], wbuf.at[slot, pl.ds(0, cols)], p_sem.at[slot, 0]),
                        pltpu.make_async_copy(wo_p.at[:, cs], wbuf.at[slot, pl.ds(cols, cols)], p_sem.at[slot, 1])]

            def store(j):
                slot = lax.rem(j, 2)
                return pltpu.make_async_copy(stage.at[slot], part_out.at[j], p_sem.at[slot, 2])

            def stored(j):
                store(j).wait()

                @pl.when(j < early_chunks)
                def _():
                    scatter.start_far(j)

            for c in chunk(0):
                c.start()
            for c in loads:
                c.wait()

            def body(j, _):
                slot = lax.rem(j, 2)

                @pl.when(j + 1 < nc)
                def _():
                    for c in chunk(j + 1):
                        c.start()

                for c in chunk(j):
                    c.wait()
                half = 2 * nb * rows
                for d in range(2):
                    z = jnp.dot(lhs[d * half:(d + 1) * half], wbuf[slot], preferred_element_type=F32).astype(BF16)
                    stage[slot, 2 * d] = z[:half // 2]
                    stage[slot, 2 * d + 1] = z[half // 2:]
                store(j).start()

                @pl.when(j >= 1)
                def _():
                    stored(j - 1)

                return 0

            lax.fori_loop(0, nc, body, 0)
            stored(nc - 1)

        def take(i):
            b, row0 = gather.take_item(i, nb)
            load(b, row0, lax.rem(i, 2)).start()

        take(0)

        def item(i, _):
            slot = lax.rem(i, 2)

            @pl.when((i + 1 != 3 * nb) & (i + 1 < 4 * nb - 1))
            def _():
                take(i + 1)

            @pl.when(i >= 2)
            def _():
                outputs(0, 0, slot).wait()

            load(0, 0, slot).wait()
            ast[slot] = jnp.dot(xbuf[slot], wo[...], preferred_element_type=F32).astype(BF16)
            b, row0 = gather.item_place(i, nb)
            outputs(b, row0, slot).start()

            @pl.when(i == 0)
            def _():
                o_copy.wait()
                trade_o.start()

            @pl.when(i + 1 == 3 * nb)
            def _():
                trade_o.wait_recv()
                pl.run_scoped(project, pltpu.VMEM((4 * nb * rows, 2 * cols), BF16), pltpu.VMEM((2, 2 * cols, CHUNK), BF16),
                              pltpu.VMEM((2, 4, nb * rows, CHUNK), BF16))

            @pl.when((i + 1 == 3 * nb) | (i + 1 == 4 * nb - 1))
            def _():
                take(i + 1)

            return 0

        lax.fori_loop(0, 4 * nb, item, 0)
        for slot in range(2):
            outputs(0, 0, slot).wait()
        for b in range(nb):
            gather.finish(b)
        trade_o.wait_send()
        trade_w().wait()
        for j in range(early_chunks):
            for idx in (0, 1):
                scatter.message(j, idx).wait()


def gather_attn_call(n, q, k, v, gains, cos_tab, sin_tab, ss, w_q, w_o, wo_p, wo_t, d_full):
    nb, tokens, cols = q.shape
    dim = w_o.shape[1]
    heads = cols // HEAD_DIM
    rows = tokens // n
    last = nb * heads - 1
    nc = dim // CHUNK
    early = min(EARLY_CHUNKS, nc)
    shape = jax.ShapeDtypeStruct
    dma = pltpu.SemaphoreType.DMA
    any_spec = pl.BlockSpec(memory_space=pl.ANY)

    def head_of(i):
        i = jnp.minimum(i, last)
        return i // heads, i % heads

    blk = pl.BlockSpec((1, tokens, HEAD_DIM), lambda i: (head_of(i)[0], 0, head_of(i)[1]))
    vec = pl.BlockSpec((2, HEAD_DIM), lambda i: (0, head_of(i)[1]))
    tab = pl.BlockSpec((tokens, HEAD_DIM), lambda i: (0, 0))
    head_arr = shape((nb, tokens, cols), BF16)
    return pl.pallas_call(
        functools.partial(gather_attn_kernel, n, nb, heads, dim), name="gather_attn", grid=(nb * heads + 1,),
        out_shape=[shape(d_full.shape, BF16), head_arr, head_arr, head_arr, shape(w_q.shape, BF16)]
        + [shape((nc, 4, nb * rows, CHUNK), BF16), shape((early, 2, nb * rows // 2, CHUNK), BF16), head_arr, head_arr,
           shape((nb, tokens, cols), F32), shape((nb, tokens, cols), F32)],
        in_specs=[blk, blk, blk, vec, tab, tab, pl.BlockSpec(ss.shape, lambda i: (0, 0))] + [any_spec] * 5,
        out_specs=[any_spec] * 7 + [blk] * 4,
        scratch_shapes=[
            pltpu.VMEM((tokens, HEAD_DIM), F32), pltpu.VMEM((tokens, HEAD_DIM), F32), pltpu.VMEM((nb, tokens, cols), BF16),
            pltpu.VMEM((dim, cols), BF16), pltpu.VMEM((2, 2 * rows, dim), BF16), pltpu.VMEM((2, 2 * rows, cols), BF16),
            dma, dma((2,)), dma((2,)), dma, dma((2, 3)), dma((2,)), dma((nb, GATHER_SEMS)), dma((nb, GATHER_SEMS)), dma, dma,
            dma((nb, n // 2)), dma((nb, n // 2)), dma((early, 6)), dma((early, 6))],
        input_output_aliases={11: 0},
        compiler_params=params("arbitrary", collective_id=1, has_side_effects=True),
        cost_estimate=cost(4 * nb * tokens * dim * cols + 4 * nb * tokens * tokens * cols, 8 * nb * tokens * dim),
    )(q, k, v, gains, cos_tab, sin_tab, ss, w_q, w_o, wo_p, wo_t, d_full)


class DyChunks:
    def __init__(self, lhs, wbuf, weights, w_sem):
        self.lhs, self.wbuf, self.weights, self.sem = lhs, wbuf, weights, w_sem

    def loads(self, j):
        slot = lax.rem(j, 2)
        src = pl.ds(pl.multiple_of(j * CHUNK, CHUNK), CHUNK)
        width = self.weights[0].shape[1]
        return [pltpu.make_async_copy(w.at[src], self.wbuf.at[slot, :, pl.ds(m * width, width)], self.sem.at[slot, m])
                for m, w in enumerate(self.weights)]

    def dot(self, j, d):
        half = self.lhs.shape[0] // 2
        return lax.dot_general(self.lhs[d * half:(d + 1) * half], self.wbuf[lax.rem(j, 2)], NT, preferred_element_type=F32).astype(BF16)


def attn_bwd_kernel(n, nb, heads, dim, q_ref, k_ref, qr_ref, kr_ref, v_ref, do_ref, o_ref, lse_ref, gain_ref, cos_ref, sin_ref, ss_ref,
                    q_hbm, k_hbm, o_hbm, part_in, far_in, d_full, wq_hbm, wk_hbm, wv_hbm, wq_p,
                    proj_out, g_out, g_p, dqs_out, dks_out, dwo_out, wk_p, wv_p, part_dy, far_dy, dgq_ref, dgk_ref,
                    part, recv_far, recv_side, s_send, s_recv,
                    inv_q, inv_k, acc_q, acc_k, p_all, ds_all, dq_all, qs_st, ks_st, v_st, st_row, st_sum, slots,
                    ld_sem, w_sem, fl_sem, g_sem, go_sem, out_sem, e_send, e_recv, t_send, t_recv, r_send, r_recv, c_sem, y_send, y_recv):
    step = pl.program_id(0)
    tokens = q_ref.shape[1]
    rows = tokens // n
    cols = heads * HEAD_DIM
    blk = min(256, tokens)
    nc = dim // CHUNK
    steps = nb * heads
    scale = HEAD_DIM ** -0.5
    place = Place(n)
    early = far_in.shape[0]
    scatter = Scatter(place, part, recv_far, recv_side, s_send, s_recv, far_src=part_in, early=early)

    def stored():
        return [pltpu.make_async_copy(part_in, part, ld_sem.at[0]),
                pltpu.make_async_copy(far_in, recv_far.at[pl.ds(0, early)], ld_sem.at[1])]

    def trade_w(j):
        return place.to_partner((wk_hbm, wv_hbm)[j], (wk_p, wv_p)[j], t_send.at[j], t_recv.at[j])

    @pl.when(step == 0)
    def _():
        place.barrier(place.everyone())
        lax.fori_loop(early, nc, scatter.start_far, 0)
        for c in stored():
            c.start()
        for j in range(2):
            trade_w(j).start()

    @pl.when(step == 1)
    def _():
        for c in stored():
            c.wait()

    def flush(b, h, slot):
        lanes = pl.ds(pl.multiple_of(h * HEAD_DIM, HEAD_DIM), HEAD_DIM)
        v_lanes = pl.ds(pl.multiple_of(2 * cols + h * HEAD_DIM, HEAD_DIM), HEAD_DIM)
        return [pltpu.make_async_copy(qs_st.at[slot], dqs_out.at[b, :, lanes], fl_sem.at[slot, 0]),
                pltpu.make_async_copy(ks_st.at[slot], dks_out.at[b, :, lanes], fl_sem.at[slot, 1]),
                pltpu.make_async_copy(v_st.at[slot], g_out.at[b, :, v_lanes], fl_sem.at[slot, 2])]

    mid = nc // 2
    for j in range(mid):
        at_step = 1 + j * (steps - 2) // max(mid - 1, 1)
        pl.when(step == at_step)(functools.partial(scatter.sums, j))

    @pl.when(step < steps)
    def _():
        b = step // heads
        head = lax.rem(step, heads)
        slot = lax.rem(step, 2)

        @pl.when(step == 0)
        def _():
            st_row[...] = jnp.zeros_like(st_row)

        @pl.when(head == 0)
        def _():
            inv_q[...] = lanes_of(lax.rsqrt(ss_ref[pl.ds(2 * b, 1)] / dim + EPS_NORM))
            inv_k[...] = lanes_of(lax.rsqrt(ss_ref[pl.ds(2 * b + 1, 1)] / dim + EPS_NORM))
            acc_q[...] = jnp.zeros_like(acc_q)
            acc_k[...] = jnp.zeros_like(acc_k)

        @pl.when(step >= 2)
        def _():
            for c in flush(0, 0, slot):
                c.wait()

        cos, sin = cos_ref[...], sin_ref[...]
        q_rot, k_rot, v, do = qr_ref[0], kr_ref[0], v_ref[0], do_ref[0]

        def scores(i):
            sl = slice(i * blk, (i + 1) * blk)
            return (lax.dot_general(q_rot[sl], k_rot, NT, preferred_element_type=F32),
                    lax.dot_general(do[sl], v, NT, preferred_element_type=F32))

        ahead = scores(0)
        for i in range(tokens // blk):
            sl = slice(i * blk, (i + 1) * blk)
            s, dp = ahead
            if (i + 1) * blk < tokens:
                ahead = scores(i + 1)
            lse = jnp.concatenate([lse_ref[0, sl]] * (tokens // HEAD_DIM), axis=1)
            p = jnp.exp2(s * SCORE_SCALE - lse)
            p_all[sl] = p.astype(BF16)
            delta = jnp.sum(do[sl].astype(F32) * o_ref[0, sl], axis=1, keepdims=True)
            ds = (p * (dp - delta)).astype(BF16)
            ds_all[sl] = ds
            dq_all[sl] = jnp.dot(ds, k_rot, preferred_element_type=F32) * scale
        do_t = do.astype(F32).T.astype(BF16)
        q_t = q_rot.astype(F32).T.astype(BF16)
        v_st[slot] = jnp.dot(do_t, p_all[...], preferred_element_type=F32).T.astype(BF16)
        dk_rot = (jnp.dot(q_t, ds_all[...], preferred_element_type=F32) * scale).T.astype(BF16).astype(F32)
        dq_rot = dq_all[...].astype(BF16).astype(F32)
        dq_hat = rotate(dq_rot, cos, -sin)
        dk_hat = rotate(dk_rot, cos, -sin)
        q_hat = q_ref[0] * inv_q[...]
        k_hat = k_ref[0] * inv_k[...]
        dgq_ref[0] = jnp.sum(dq_hat * q_hat, axis=0, keepdims=True)
        dgk_ref[0] = jnp.sum(dk_hat * k_hat, axis=0, keepdims=True)
        dq_s = dq_hat * gain_ref[0:1]
        dk_s = dk_hat * gain_ref[1:2]
        qs_st[slot] = dq_s
        ks_st[slot] = dk_s
        acc_q[...] += dq_s * q_hat
        acc_k[...] += dk_s * k_hat
        for c in flush(b, head, slot):
            c.start()

        @pl.when(head == heads - 1)
        def _():
            st_row[pl.ds(2 * b, 1)] = to_row(acc_q[...])
            st_row[pl.ds(2 * b + 1, 1)] = to_row(acc_k[...])

    @pl.when(step == steps)
    def _():
        for s in range(2):
            for c in flush(0, 0, s):
                c.wait()
        stats = Exchange(place, st_row, slots, e_send, e_recv)
        stats.start()
        lax.fori_loop(mid, nc, scatter.sums_step, 0)
        lax.fori_loop(0, nc, scatter.start_side, 0)
        st_sum[...] = stats.finish()
        rb = min(256, tokens)
        per = tokens // rb
        trade = RowTrade(place, g_out, g_p, rows, r_send, r_recv)

        def norm_grad(fbuf, gbuf):
            def loads(i, slot):
                b, r0 = i // per, pl.multiple_of(lax.rem(i, per) * rb, rb)
                return [pltpu.make_async_copy(src.at[b, pl.ds(r0, rb)], fbuf.at[slot, m], g_sem.at[slot, m])
                        for m, src in enumerate((dqs_out, q_hbm, dks_out, k_hbm))]

            def store(i, slot):
                b, r0 = i // per, pl.multiple_of(lax.rem(i, per) * rb, rb)
                return pltpu.make_async_copy(gbuf.at[slot], g_out.at[b, pl.ds(r0, rb), pl.ds(0, 2 * cols)], go_sem.at[slot])

            for c in loads(0, 0):
                c.start()

            def body(i, _):
                slot = lax.rem(i, 2)
                b, r0 = i // per, pl.multiple_of(lax.rem(i, per) * rb, rb)

                @pl.when(i + 1 < nb * per)
                def _():
                    for c in loads(i + 1, lax.rem(i + 1, 2)):
                        c.start()

                @pl.when(r0 == 0)
                def _():
                    inv_q[...] = lanes_of(lax.rsqrt(ss_ref[pl.ds(2 * b, 1)] / dim + EPS_NORM))
                    inv_k[...] = lanes_of(lax.rsqrt(ss_ref[pl.ds(2 * b + 1, 1)] / dim + EPS_NORM))
                    acc_q[...] = lanes_of(st_sum[pl.ds(2 * b, 1)] / dim)
                    acc_k[...] = lanes_of(st_sum[pl.ds(2 * b + 1, 1)] / dim)

                @pl.when(i >= 2)
                def _():
                    store(0, slot).wait()

                for c in loads(i, slot):
                    c.wait()
                sl = pl.ds(r0, rb)
                for m, (inv, st) in enumerate(((inv_q, acc_q), (inv_k, acc_k))):
                    inv_l, st_l = inv[sl], st[sl]
                    for h in range(heads):
                        hs = slice(h * HEAD_DIM, (h + 1) * HEAD_DIM)
                        grad = inv_l * (fbuf[slot, 2 * m, :, hs] - (fbuf[slot, 2 * m + 1, :, hs] * inv_l) * st_l)
                        gbuf[slot, :, m * cols + h * HEAD_DIM:m * cols + (h + 1) * HEAD_DIM] = grad.astype(BF16)
                store(i, slot).start()
                return 0

            lax.fori_loop(0, nb * per, body, 0)
            for s in range(min(2, nb * per)):
                store(0, s).wait()

        pl.run_scoped(norm_grad, pltpu.VMEM((2, 4, rb, cols), F32), pltpu.VMEM((2, rb, 2 * cols), BF16))
        trade.start()

        def weight_grad(turned, obuf, dbuf, wst):
            bn = min(512, dim)
            n_chunks = dim // bn

            def chunk(c):
                slot = lax.rem(c, 2)
                return pltpu.make_async_copy(d_full.at[:, :, pl.ds(pl.multiple_of(c * bn, bn), bn)], dbuf.at[slot], go_sem.at[slot])

            def store(c):
                slot = lax.rem(c, 2)
                return pltpu.make_async_copy(wst.at[slot], dwo_out.at[:, pl.ds(pl.multiple_of(c * bn, bn), bn)], w_sem.at[slot, 0])

            load_o = pltpu.make_async_copy(o_hbm, obuf, ld_sem.at[0])
            load_o.start()
            chunk(0).start()
            load_o.wait()
            for b in range(nb):
                turned[:, b * tokens:(b + 1) * tokens] = obuf[b].T

            def body(c, _):
                slot = lax.rem(c, 2)

                @pl.when(c + 1 < n_chunks)
                def _():
                    chunk(c + 1).start()

                @pl.when(c >= 2)
                def _():
                    store(c).wait()

                chunk(c).wait()
                d = dbuf[slot].reshape(nb * tokens, bn)
                wst[slot] = jnp.dot(turned[...], d, preferred_element_type=F32).astype(BF16)
                store(c).start()
                return 0

            lax.fori_loop(0, n_chunks, body, 0)
            for s in range(min(2, n_chunks)):
                store(s).wait()

        bn = min(512, dim)
        pl.run_scoped(weight_grad, pltpu.VMEM((cols, nb * tokens), BF16), pltpu.VMEM((nb, tokens, cols), BF16),
                      pltpu.VMEM((2, nb, tokens, bn), BF16), pltpu.VMEM((2, cols, bn), BF16))
        trade.wait_recv()
        for j in range(2):
            trade_w(j).wait_recv()

        n_dy = part_dy.shape[0]
        scatter_y = Scatter(place, part_dy, far_dy, None, y_send, y_recv)

        def first_dy(lhs, wbuf, pst):
            loads = pair_rows(place, nb, rows, g_out, g_p, lhs, ld_sem)
            for c in loads:
                c.start()
            dy = DyChunks(lhs, wbuf, (wq_hbm, wk_hbm, wv_hbm, wq_p, wk_p, wv_p), c_sem)
            for c in dy.loads(0):
                c.start()
            for c in loads:
                c.wait()

            def body(j, _):
                @pl.when(j + 1 < n_dy)
                def _():
                    for c in dy.loads(j + 1):
                        c.start()

                for c in dy.loads(j):
                    c.wait()
                store = pltpu.make_async_copy(pst, part_dy.at[j], go_sem.at[0])

                @pl.when(j >= 1)
                def _():
                    store.wait()
                    scatter_y.start_far(j - 1)

                for d in range(2):
                    z = dy.dot(j, d)
                    pst[2 * d] = z[:nb * rows]
                    pst[2 * d + 1] = z[nb * rows:]
                store.start()
                return 0

            lax.fori_loop(0, n_dy, body, 0)
            pltpu.make_async_copy(pst, part_dy.at[n_dy - 1], go_sem.at[0]).wait()
            scatter_y.start_far(n_dy - 1)

        pl.run_scoped(first_dy, pltpu.VMEM((4 * nb * rows, 6 * cols), BF16), pltpu.VMEM((2, CHUNK, 6 * cols), BF16),
                      pltpu.VMEM((4, nb * rows, CHUNK), BF16))
        scatter_end(scatter, proj_out, out_sem, nc)
        trade.wait_send()
        for j in range(2):
            trade_w(j).wait_send()
        for j in range(n_dy):
            for idx in (0, 1):
                scatter_y.message(j, idx).wait()


def attn_bwd_call(n, q, k, q_rot, k_rot, v, d_attn, o, o32, lse, gains, cos_tab, sin_tab, ss, part, far, d_full, w_q, w_k, w_v, wq_p):
    nb, tokens, cols = q.shape
    dim = d_full.shape[2]
    heads = cols // HEAD_DIM
    rows = tokens // n
    steps = nb * heads
    shape = jax.ShapeDtypeStruct
    dma = pltpu.SemaphoreType.DMA
    any_spec = pl.BlockSpec(memory_space=pl.ANY)

    def head_of(i):
        i = jnp.minimum(i, steps - 1)
        return i // heads, i % heads

    blk = pl.BlockSpec((1, tokens, HEAD_DIM), lambda i: (head_of(i)[0], 0, head_of(i)[1]))
    vec = pl.BlockSpec((2, HEAD_DIM), lambda i: (0, head_of(i)[1]))
    out_vec = pl.BlockSpec((1, 1, HEAD_DIM), lambda i: (head_of(i)[0], 0, head_of(i)[1]))
    tab = pl.BlockSpec((tokens, HEAD_DIM), lambda i: (0, 0))
    whole = (nb, tokens, cols)
    lane_tile = pltpu.VMEM((tokens, HEAD_DIM), F32)
    n_dy = min(EARLY_DY, dim // CHUNK)
    return pl.pallas_call(
        functools.partial(attn_bwd_kernel, n, nb, heads, dim), name="attn_bwd", grid=(steps + 1,),
        out_shape=[shape((nb, rows, dim), BF16), shape((nb, tokens, 3 * cols), BF16), shape((nb, tokens, 3 * cols), BF16),
                   shape(whole, F32), shape(whole, F32), shape((cols, dim), BF16),
                   shape(w_k.shape, BF16), shape(w_v.shape, BF16), shape((n_dy,) + part.shape[1:], BF16), shape((n_dy,) + far.shape[1:], BF16),
                   shape((nb, 1, cols), F32), shape((nb, 1, cols), F32)],
        in_specs=[blk] * 8 + [vec, tab, tab, pl.BlockSpec(ss.shape, lambda i: (0, 0))] + [any_spec] * 10,
        out_specs=[any_spec] * 10 + [out_vec, out_vec],
        scratch_shapes=Scatter.scratch(nb * rows, dim) + [lane_tile] * 4 + [pltpu.VMEM((tokens, tokens), BF16)] * 2 + [
            lane_tile, pltpu.VMEM((2, tokens, HEAD_DIM), F32), pltpu.VMEM((2, tokens, HEAD_DIM), F32),
            pltpu.VMEM((2, tokens, HEAD_DIM), BF16), pltpu.VMEM(ss.shape, F32), pltpu.VMEM(ss.shape, F32), pltpu.VMEM((n,) + ss.shape, F32),
            dma((2,)), dma((2, 2)), dma((2, 3)), dma((2, 4)), dma((2,)), dma((nb,)), dma((n,)), dma((n,)), dma((2,)), dma((2,)),
            dma((nb, n // 2)), dma((nb, n // 2)), dma((2, 6)), dma((n_dy, 6)), dma((n_dy, 6))],
        compiler_params=params("arbitrary", collective_id=2, has_side_effects=True),
        cost_estimate=cost(4 * nb * tokens * dim * cols + 36 * nb * tokens * tokens * cols, 30 * nb * tokens * cols),
    )(q, k, q_rot, k_rot, v, d_attn, o32, lse, gains, cos_tab, sin_tab, ss, q, k, o, part, far, d_full, w_q, w_k, w_v, wq_p)


def dy_dw_kernel(n, nb, dim, g_hbm, g_p, wq_hbm, wk_hbm, wv_hbm, wq_p, wk_p, wv_p, y_full, part_in, far_in,
                 dy_out, dwq_out, dwk_out, dwv_out,
                 part, recv_far, recv_side, s_send, s_recv, g, ld_sem, w_sem, y_sem, o_sem, out_sem):
    tokens = g_hbm.shape[1]
    rows = tokens // n
    cols = g_hbm.shape[2] // 3
    nc = dim // CHUNK
    early = far_in.shape[0]
    lag = 3
    place = Place(n)
    scatter = Scatter(place, part, recv_far, recv_side, s_send, s_recv, early=early)
    stored = [pltpu.make_async_copy(part_in, part.at[pl.ds(0, early)], ld_sem.at[2]),
              pltpu.make_async_copy(far_in, recv_far.at[pl.ds(0, early)], ld_sem.at[3])]
    load_g = pltpu.make_async_copy(g_hbm, g, ld_sem.at[4])

    def chain(lhs, wbuf):
        for c in stored:
            c.start()
        loads = pair_rows(place, nb, rows, g_hbm, g_p, lhs, ld_sem)
        dy = DyChunks(lhs, wbuf, (wq_hbm, wk_hbm, wv_hbm, wq_p, wk_p, wv_p), w_sem)
        if early < nc:
            for c in loads:
                c.start()
            for c in dy.loads(early):
                c.start()
        place.barrier(place.near()[:2])
        for c in stored:
            c.wait()
        lax.fori_loop(0, early, scatter.sums_step, 0)
        load_g.start()

        def body(j, _):
            @pl.when(j + 1 < nc)
            def _():
                for c in dy.loads(j + 1):
                    c.start()

            for c in dy.loads(j):
                c.wait()
            for d in range(2):
                @pl.when(j == early)
                def _(d=d):
                    for c in loads[d * len(loads) // 2:(d + 1) * len(loads) // 2]:
                        c.wait()

                z = dy.dot(j, d)
                part[j, 2 * d] = z[:nb * rows]
                part[j, 2 * d + 1] = z[nb * rows:]
                if d == 0:
                    scatter.start_far(j)

            @pl.when(j >= early + lag)
            def _():
                scatter.sums(j - lag)

            return 0

        lax.fori_loop(early, nc, body, 0)
        lax.fori_loop(0, nc, scatter.start_side, 0)

    pl.run_scoped(chain, pltpu.VMEM((4 * nb * rows, 6 * cols), BF16), pltpu.VMEM((2, CHUNK, 6 * cols), BF16))

    def weight_grad(ybuf, wst):
        bm = min(512, dim)
        n_chunks = dim // bm

        def chunk(c):
            slot = lax.rem(c, 2)
            return pltpu.make_async_copy(y_full.at[:, :, pl.ds(pl.multiple_of(c * bm, bm), bm)], ybuf.at[slot], y_sem.at[slot])

        def store(c):
            slot = lax.rem(c, 2)
            dst = pl.ds(pl.multiple_of(c * bm, bm), bm)
            return [pltpu.make_async_copy(wst.at[slot, :, pl.ds(m * cols, cols)], out.at[dst], o_sem.at[slot, m])
                    for m, out in enumerate((dwq_out, dwk_out, dwv_out))]

        chunk(0).start()
        load_g.wait()

        def body(c, _):
            slot = lax.rem(c, 2)

            @pl.when(c + 1 < n_chunks)
            def _():
                chunk(c + 1).start()

            @pl.when(c >= 2)
            def _():
                for s in store(c):
                    s.wait()

            chunk(c).wait()
            for m in range(lag):
                late = max(nc - lag, early) + m
                if late < nc:
                    pl.when(c == min(m, n_chunks - 1))(functools.partial(scatter.sums, late))
            wst[slot] = lax.dot_general(ybuf[slot].reshape(nb * tokens, bm), g[...].reshape(nb * tokens, 3 * cols), TN,
                                        preferred_element_type=F32).astype(BF16)
            for s in store(c):
                s.start()
            return 0

        lax.fori_loop(0, n_chunks, body, 0)
        for s in range(min(2, n_chunks)):
            for c in store(s):
                c.wait()

    bm = min(512, dim)
    pl.run_scoped(weight_grad, pltpu.VMEM((2, nb, tokens, bm), BF16), pltpu.VMEM((2, bm, 3 * cols), BF16))
    scatter_end(scatter, dy_out, out_sem, nc)


def dy_dw_call(n, g, g_p, w_q, w_k, w_v, wq_p, wk_p, wv_p, y_full, part, far):
    nb, tokens, wide = g.shape
    dim = y_full.shape[2]
    cols = wide // 3
    rows = tokens // n
    shape = jax.ShapeDtypeStruct
    dma = pltpu.SemaphoreType.DMA
    any_spec = pl.BlockSpec(memory_space=pl.ANY)
    return pl.pallas_call(
        functools.partial(dy_dw_kernel, n, nb, dim), name="dy_dw",
        out_shape=[shape((nb, rows, dim), BF16)] + [shape((dim, cols), BF16)] * 3,
        in_specs=[any_spec] * 11, out_specs=[any_spec] * 4,
        scratch_shapes=Scatter.scratch(nb * rows, dim) + [pltpu.VMEM((nb, tokens, 3 * cols), BF16), dma((5,)), dma((2, 6)), dma((2,)), dma((2, 3)), dma((nb,))],
        compiler_params=params(collective_id=3, has_side_effects=True),
        cost_estimate=cost(12 * nb * tokens * dim * cols, 30 * nb * tokens * cols),
    )(g, g_p, w_q, w_k, w_v, wq_p, wk_p, wv_p, y_full, part, far)


def token_kernel(n_copies, x_ref, dy_ref, pr_ref, g_ref, m_ref, e_ref, bo_ref, gq_ref, gk_ref, *refs):
    srcs, (xo_ref, dx_ref, dm_ref, dgq_ref, dgk_ref), dsts = refs[:4], refs[4:9], refs[9:13]
    bufs, (acc, in_sem, out_sem) = refs[13:17], refs[17:]
    group = 16
    step = pl.program_id(0)
    rows = x_ref.shape[1]
    groups = rows // group
    depth = bufs[0].shape[0]
    lag = depth - 1

    def move(c, out):
        copies = []
        for j, (src, dst, buf) in enumerate(zip(srcs, dsts, bufs)):
            size = buf.shape[1]
            sl = pl.ds(pl.multiple_of(c * size, 16), size)
            slot = lax.rem(c, depth)
            copies.append(pltpu.make_async_copy(buf.at[slot], dst.at[sl], out_sem.at[slot, j]) if out
                          else pltpu.make_async_copy(src.at[sl], buf.at[slot], in_sem.at[slot, j]))
        return copies

    def advance(i):
        @pl.when(i < n_copies)
        def _():
            @pl.when(i >= depth)
            def _():
                for c in move(i - depth, True):
                    c.wait()

            for c in move(i, False):
                c.start()

        @pl.when((i >= lag) & (i < n_copies + lag))
        def _():
            for c in move(i - lag, False):
                c.wait()
            for c in move(i - lag, True):
                c.start()

    mod = m_ref[...] + e_ref[0]
    for src, dst in ((gq_ref, dgq_ref), (gk_ref, dgk_ref)):
        dst[...] = jnp.sum(src[...], axis=(0, 1))
    shift_bo = bo_ref[...].reshape(1, bo_ref.shape[0])
    acc[...] = jnp.zeros_like(acc)

    def body(r, _):
        advance(step * groups + r)
        sl = pl.ds(pl.multiple_of(r * group, group), group)
        x = x_ref[0, sl].astype(F32)
        d_out = dy_ref[0, sl].astype(F32)
        proj = pr_ref[0, sl].astype(F32) + shift_bo
        xo_ref[0, sl] = (x + mod[2:3] * proj).astype(BF16)
        gate_part = d_out * proj
        x_norm, inv_std = norm_stats(x)
        d_y = g_ref[0, sl].astype(F32)
        d_norm = d_y * (1.0 + mod[1:2])
        d_x = d_out + inv_std * (
            d_norm - jnp.mean(d_norm, axis=-1, keepdims=True) - x_norm * jnp.mean(d_norm * x_norm, axis=-1, keepdims=True))
        dx_ref[0, sl] = d_x.astype(BF16)
        scale_part = d_y * x_norm
        acc[0] += d_y[:8] + d_y[8:]
        acc[1] += scale_part[:8] + scale_part[8:]
        acc[2] += gate_part[:8] + gate_part[8:]
        return 0

    lax.fori_loop(0, groups, body, 0)
    for j in range(3):
        dm_ref[0, j:j + 1] = jnp.sum(acc[j], axis=0, keepdims=True)

    @pl.when(step == pl.num_programs(0) - 1)
    def _():
        total = pl.num_programs(0) * groups

        def rest(i, _):
            advance(i)
            return 0

        lax.fori_loop(total, jnp.maximum(total, n_copies + lag), rest, 0)
        for c in range(max(n_copies - depth, 0), n_copies):
            for copy in move(c, True):
                copy.wait()


def token_call(x_loc, dy_loc, proj, d_y, m_block, e_loc, b_o, d_gq, d_gk, grads):
    nb, rows, dim = x_loc.shape
    n_copies = dim // min(512, dim)
    row = pl.BlockSpec((1, rows, dim), lambda i: (i, 0, 0))
    mod = pl.BlockSpec((1, 3, dim), lambda i: (i, 0, 0))
    any_spec = pl.BlockSpec(memory_space=pl.ANY)
    dma = pltpu.SemaphoreType.DMA
    depth = 4
    return pl.pallas_call(
        functools.partial(token_kernel, n_copies), name="tokens", grid=(nb,),
        out_shape=[jax.ShapeDtypeStruct(x_loc.shape, BF16), jax.ShapeDtypeStruct(x_loc.shape, BF16),
                   jax.ShapeDtypeStruct((nb, 3, dim), F32)] + [jax.ShapeDtypeStruct(d_gq.shape[2:], F32)] * 2 + [jax.ShapeDtypeStruct(w.shape, BF16) for w in grads],
        in_specs=[row, row, row, row, pl.BlockSpec((3, dim), lambda i: (0, 0)), mod] + [pl.BlockSpec(memory_space=pltpu.VMEM)] * 3 + [any_spec] * 4,
        out_specs=[row, row, mod] + [pl.BlockSpec(memory_space=pltpu.VMEM)] * 2 + [any_spec] * 4,
        scratch_shapes=[pltpu.VMEM((depth, w.shape[0] // n_copies, w.shape[1]), BF16) for w in grads]
        + [pltpu.VMEM((3, 8, dim), F32), dma((depth, 4)), dma((depth, 4))],
        compiler_params=params("arbitrary"),
        cost_estimate=cost(nb * rows * dim * 30, nb * rows * dim * 12),
    )(x_loc, dy_loc, proj, d_y, m_block, e_loc, b_o, d_gq, d_gk, *grads)


def solution(mesh):
    tp_size = mesh.shape['tp']

    def device_step(x_loc, e_loc, m_block, w_q, b_q, w_k, b_k, w_v, b_v, w_o, b_o, g_q, g_k, pos_part, dy_loc):
        nb, _, dim = x_loc.shape
        y_full, d_own, q, k, v, wo_p, wo_t, ss, cos_tab, sin_tab, gains = gather_qkv_call(
            tp_size, x_loc, dy_loc, m_block, e_loc, w_q, w_k, w_v, w_o, b_q, b_k, b_v, g_q, g_k, pos_part)
        d_full, o, _, d_attn, wq_p, part, far, q_rot, k_rot, lse, o32 = gather_attn_call(
            tp_size, q, k, v, gains, cos_tab, sin_tab, ss, w_q, w_o, wo_p, wo_t, d_own)
        proj, g, g_p, _, _, d_wo, wk_p, wv_p, part, far, d_gq, d_gk = attn_bwd_call(
            tp_size, q, k, q_rot, k_rot, v, d_attn, o, o32, lse, gains, cos_tab, sin_tab, ss, part, far, d_full, w_q, w_k, w_v, wq_p)
        d_y, d_wq, d_wk, d_wv = dy_dw_call(tp_size, g, g_p, w_q, w_k, w_v, wq_p, wk_p, wv_p, y_full, part, far)
        x_out, d_x, d_mod, d_gq, d_gk, d_wq, d_wk, d_wv, d_wo = token_call(
            x_loc, dy_loc, proj, d_y, m_block, e_loc, b_o, d_gq, d_gk, (d_wq, d_wk, d_wv, d_wo))
        d_e = all_sum_call(tp_size, d_mod.reshape(tp_size, -1, HEAD_DIM)).reshape(nb, 3, dim)
        return x_out, d_x, d_e, jnp.sum(d_e, axis=0), d_wq, d_wk, d_wv, d_wo, d_gq, d_gk

    in_specs = (P('dp', 'tp', None), P('dp', None, None), P(None, None), P(None, 'tp'), P('tp'), P(None, 'tp'), P('tp'),
                P(None, 'tp'), P('tp'), P('tp', None), P(None), P('tp'), P('tp'), P('dp', None), P('dp', 'tp', None))
    out_specs = (P('dp', 'tp', None), P('dp', 'tp', None), P('dp', None, None), P('dp', None), P('dp', 'tp'), P('dp', 'tp'),
                 P('dp', 'tp'), P(('dp', 'tp'), None), P(('dp', 'tp')), P(('dp', 'tp')))
    return jax.shard_map(device_step, mesh=mesh, in_specs=in_specs, out_specs=out_specs, check_vma=False)
```

```python
import functools

import jax
import jax.numpy as jnp
import numpy as np
from jax import lax
from jax.experimental import pallas as pl
from jax.experimental.pallas import tpu as pltpu
from jax.sharding import PartitionSpec as P

HEAD_DIM = 128
EPS_NORM = 1e-6
ROPE_BASE = 10000.0
LOG2E = 1.4426950408889634
CHUNK = 512
VMEM_LIMIT = 60 * 1024 * 1024
F32 = jnp.float32
BF16 = jnp.bfloat16
MESH_ID = pl.DeviceIdType.MESH
NT = (((1,), (1,)), ((), ()))
TN = (((0,), (0,)), ((), ()))


def params(*semantics, **kw):
    return pltpu.CompilerParams(dimension_semantics=semantics or None, vmem_limit_bytes=VMEM_LIMIT, **kw)


def cost(flops, nbytes):
    return pl.CostEstimate(flops=int(flops), bytes_accessed=int(nbytes), transcendentals=0)


def rope_freqs():
    half_dim = HEAD_DIM // 2
    side_len = HEAD_DIM // 6
    first_len = half_dim - 2 * side_len
    pair_idx = np.arange(HEAD_DIM) // 2
    section = (pair_idx >= first_len).astype(np.int32) + (pair_idx >= first_len + side_len).astype(np.int32)
    offset = np.where(section == 0, 0, np.where(section == 1, first_len, first_len + side_len))
    sec_width = np.where(section == 0, first_len, side_len)
    exponent = -(pair_idx - offset).astype(np.float32) / sec_width.astype(np.float32)
    freq_vals = np.power(np.float32(ROPE_BASE), exponent)
    return np.where(section[None, :] == np.arange(3)[:, None], freq_vals[None, :], np.float32(0.0)).astype(np.float32)


def norm_stats(x):
    centered = x - jnp.mean(x, axis=-1, keepdims=True)
    inv_std = lax.rsqrt(jnp.mean(centered * centered, axis=-1, keepdims=True) + EPS_NORM)
    return centered * inv_std, inv_std


def to_row(acc):
    return jnp.sum(acc.T, axis=0, keepdims=True)


def lanes_of(row):
    return jnp.broadcast_to(row, (HEAD_DIM, row.shape[1])).T


def head_sum(values):
    out = values[:, :HEAD_DIM]
    for h in range(1, values.shape[1] // HEAD_DIM):
        out = out + values[:, h * HEAD_DIM:(h + 1) * HEAD_DIM]
    return out


class Place:
    def __init__(self, n):
        self.n = n
        self.me = lax.axis_index('tp')
        self.right = lax.rem(self.me + 2, n)
        self.left = lax.rem(self.me + n - 2, n)
        self.far = lax.rem(self.me + n // 2, n)
        self.chip = self.me // 2

    def partner(self, dev):
        return dev + 1 - 2 * lax.rem(dev, 2)

    def arrive(self, devices):
        for dev in devices:
            pl.semaphore_signal(pltpu.get_barrier_semaphore(), inc=1, device_id={'tp': dev}, device_id_type=MESH_ID)

    def barrier(self, devices):
        self.arrive(devices)
        pl.semaphore_wait(pltpu.get_barrier_semaphore(), len(devices))

    def to_partner(self, src, dst, send_sem, recv_sem):
        return pltpu.make_async_remote_copy(src_ref=src, dst_ref=dst, send_sem=send_sem, recv_sem=recv_sem,
                                            device_id={'tp': self.partner(self.me)}, device_id_type=MESH_ID)

    def everyone(self):
        return [lax.rem(self.me + d, self.n) for d in range(1, self.n)]

    def near(self):
        return [self.right, self.left, self.partner(self.me)]


class Gather:
    def __init__(self, place, full, rows, send, recv, early=0):
        self.at, self.full, self.rows, self.send, self.recv, self.early = place, full, rows, send, recv, early

    def part(self, b, dev, off, count):
        return self.full.at[b, pl.ds(pl.multiple_of(dev * self.rows + off, 16), count)]

    def copy(self, b, dev, off, count, s_idx, r_idx, target):
        ref = self.part(b, dev, off, count)
        return pltpu.make_async_remote_copy(src_ref=ref, dst_ref=ref, send_sem=self.send.at[b, s_idx], recv_sem=self.recv.at[b, r_idx],
                                            device_id={'tp': target}, device_id_type=MESH_ID)

    def start_own(self, b):
        p = self.at
        self.copy(b, p.me, 0, self.rows, 0, 0, p.right).start()
        self.copy(b, p.me, 0, self.rows, 1, 1, p.left).start()
        self.copy(b, p.me, 0, self.rows, 2, 4, p.partner(p.me)).start()

    def whole_blocks_in(self, b):
        p = self.at
        self.copy(b, p.partner(p.me), 0, self.rows, 2, 4, p.me).wait_recv()
        self.copy(b, p.left, 0, self.rows, 0, 0, p.me).wait_recv()
        self.copy(b, p.right, 0, self.rows, 1, 1, p.me).wait_recv()
        for s_idx in range(3):
            self.copy(b, p.me, 0, self.rows, s_idx, s_idx, p.me).wait_send()

    def pass_left(self, b):
        p, half = self.at, self.rows // 2
        self.copy(b, p.left, 0, half, 3, 2, p.right).start()
        self.copy(b, p.left, 0, self.rows, 5, 5, p.partner(p.me)).start()

    def pass_right(self, b):
        p, half = self.at, self.rows // 2
        self.copy(b, p.right, half, half, 4, 3, p.left).start()
        self.copy(b, p.right, 0, self.rows, 6, 6, p.partner(p.me)).start()

    def finish(self, b):
        p, half = self.at, self.rows // 2
        counts = (self.rows, self.rows, self.rows, half, half, self.rows, self.rows, half, half)
        for s_idx, count in list(enumerate(counts))[3 if b < self.early else 0:]:
            self.copy(b, p.me, 0, count, s_idx, s_idx, p.me).wait_send()

    def item_place(self, i, nb):
        j = i - nb
        b = jnp.where(i < nb, i, jnp.where(i < 3 * nb, j // 2, i - 3 * nb))
        chips = self.at.n // 2
        side = jnp.where(lax.rem(j + 2 * nb, 2) == 0, chips - 1, 1)
        off = jnp.where(i < nb, 0, jnp.where(i < 3 * nb, side, chips // 2))
        return b, pl.multiple_of(lax.rem(self.at.chip + off, chips) * (2 * self.rows), 32)

    def kinds(self, i, nb):
        odd = lax.rem(i + nb, 2)
        side = (i >= nb) & (i < 3 * nb)
        return i < nb, side & (odd == 0), side & (odd == 1), i >= 3 * nb

    def arrive(self, i, nb):
        p, half = self.at, self.rows // 2
        b, _ = self.item_place(i, nb)
        _, is_left, is_right, is_far = self.kinds(i, nb)

        @pl.when(is_left & (b >= self.early))
        def _():
            self.copy(b, p.left, 0, self.rows, 0, 0, p.me).wait_recv()
            self.pass_left(b)

        @pl.when(is_right & (b >= self.early))
        def _():
            self.copy(b, p.right, 0, self.rows, 1, 1, p.me).wait_recv()
            self.pass_right(b)

        @pl.when(is_far)
        def _():
            self.copy(b, p.far, 0, half, 3, 2, p.me).wait_recv()
            self.copy(b, p.far, 0, half, 7, 7, p.partner(p.me)).start()
            self.copy(b, p.far, half, half, 4, 3, p.me).wait_recv()
            self.copy(b, p.far, half, half, 8, 8, p.partner(p.me)).start()

    def ready(self, i, nb):
        p, half = self.at, self.rows // 2
        b, row0 = self.item_place(i, nb)
        is_own, is_left, is_right, is_far = self.kinds(i, nb)

        @pl.when(is_own & (b >= self.early))
        def _():
            self.copy(b, p.partner(p.me), 0, self.rows, 2, 4, p.me).wait_recv()

        @pl.when(is_left)
        def _():
            self.copy(b, p.partner(p.left), 0, self.rows, 5, 5, p.me).wait_recv()

        @pl.when(is_right)
        def _():
            self.copy(b, p.partner(p.right), 0, self.rows, 6, 6, p.me).wait_recv()

        @pl.when(is_far)
        def _():
            self.copy(b, p.partner(p.far), 0, half, 7, 7, p.me).wait_recv()
            self.copy(b, p.partner(p.far), half, half, 8, 8, p.me).wait_recv()

        return b, row0


class RowTrade:
    def __init__(self, place, src, dst, rows, send, recv, rows_of=None):
        self.at, self.src, self.dst, self.rows, self.send, self.recv = place, src, dst, rows, send, recv
        self.batch = range(src.shape[0]) if rows_of is None else rows_of

    def copies(self, parity):
        p = self.at
        for b in self.batch:
            for k in range(p.n // 2):
                sl = pl.ds(pl.multiple_of((2 * k + parity) * self.rows, 16), self.rows)
                yield p.to_partner(self.src.at[b, sl], self.dst.at[b, sl], self.send.at[b, k], self.recv.at[b, k])

    def start(self):
        for c in self.copies(1 - lax.rem(self.at.me, 2)):
            c.start()

    def wait_recv(self):
        for c in self.copies(lax.rem(self.at.me, 2)):
            c.wait_recv()

    def wait_send(self):
        for c in self.copies(1 - lax.rem(self.at.me, 2)):
            c.wait_send()


GATHER_SEMS = 9
EARLY_ROWS = 1
EARLY_CHUNKS = 3
EARLY_DY = 4


def chunks_of(width, step):
    return [(c, min(c + step, width)) for c in range(0, width, step)]


class Exchange:
    def __init__(self, place, x_ref, slots, send_sems, recv_sems):
        self.at, self.x, self.slots, self.send, self.recv = place, x_ref, slots, send_sems, recv_sems

    def copy(self, d, dev, src):
        return pltpu.make_async_remote_copy(src_ref=self.x, dst_ref=self.slots.at[src], send_sem=self.send.at[d], recv_sem=self.recv.at[src],
                                            device_id={'tp': dev}, device_id_type=MESH_ID)

    def start(self):
        for d, dev in enumerate(self.at.everyone()):
            self.copy(d, dev, self.at.me).start()
        self.slots[self.at.me] = self.x[...]

    def finish(self):
        for d, dev in enumerate(self.at.everyone()):
            self.copy(d, dev, dev).wait()
        total = self.slots[0]
        for d in range(1, self.at.n):
            total = total + self.slots[d]
        return total


def gather_qkv_kernel(n, x_ref, dy_ref, m_ref, e_ref, wq_ref, wk_ref, wv_ref, wo_ref, bq_ref, bk_ref, bv_ref, gq_ref, gk_ref, pos_ref,
                      freq_ref, y_full, d_full, q_out, k_out, v_out, wo_p, wo_t, ss_ref, cos_ref, sin_ref, gain_ref,
                      bias_ref, w_all, xin, stage, xbuf, zst, vst, sq, ss_row, slots, wo_in, wo_st, wo_sem,
                      w_sem, in_sem, st_sem, ld_sem, out_sem, g_send, g_recv, d_send, d_recv, e_send, e_recv, t_send, t_recv):
    nb, rows, dim = x_ref.shape
    cols = wq_ref.shape[1]
    place = Place(n)
    gather = Gather(place, y_full, rows, g_send, g_recv)
    gather_d = Gather(place, d_full, rows, d_send, d_recv)
    w_copies = [pltpu.make_async_copy(w, w_all.at[:, pl.ds(j * cols, cols)], w_sem.at[j]) for j, w in enumerate((wq_ref, wk_ref, wv_ref))]
    place.arrive(place.everyone())
    trade = place.to_partner(wo_ref, wo_p, t_send, t_recv)

    def load_x(b):
        return pltpu.make_async_copy(x_ref.at[b], xin.at[b], in_sem.at[b])

    for b in range(nb):
        load_x(b).start()
    for c in w_copies:
        c.start()
    group = 16

    def mine(full, b):
        return full.at[b, pl.ds(pl.multiple_of(place.me * rows, 16), rows)]

    def ln_step(b, _):
        load_x(b).wait()
        shift = m_ref[0:1] + e_ref[b, 0:1]
        scale_one = 1.0 + (m_ref[1:2] + e_ref[b, 1:2])

        def ln_rows(r, _):
            sl = pl.ds(pl.multiple_of(r * group, group), group)
            x_norm, _ = norm_stats(xin[b, sl].astype(F32))
            stage[b, sl] = (x_norm * scale_one + shift).astype(BF16)
            return 0

        lax.fori_loop(0, rows // group, ln_rows, 0)
        out = pltpu.make_async_copy(stage.at[b], mine(y_full, b), st_sem)
        out.start()

        @pl.when(b == 0)
        def _():
            pl.semaphore_wait(pltpu.get_barrier_semaphore(), n - 1)

        out.wait()
        gather.start_own(b)
        return 0

    lax.fori_loop(0, nb, ln_step, 0)
    load_dy = pltpu.make_async_copy(dy_ref, xin, in_sem.at[0])
    load_dy.start()
    for j, ref in enumerate((bq_ref, bk_ref, bv_ref)):
        bias_ref[:, j * cols:(j + 1) * cols] = ref[...].reshape(1, cols)
    for j, ref in enumerate((gq_ref, gk_ref)):
        gain_ref[j:j + 1] = ref[...].reshape(1, cols)

    def tables():
        lane = lax.broadcasted_iota(jnp.int32, (128, HEAD_DIM), 1)

        def rows_of(r, _):
            sl = pl.ds(pl.multiple_of(r * 128, 128), 128)
            pos = [lanes_of(pos_ref[m:m + 1, sl].astype(F32)) for m in range(3)]
            angle = pos[0] * freq_ref[0:1] + pos[1] * freq_ref[1:2] + pos[2] * freq_ref[2:3]
            cos_ref[sl] = jnp.cos(angle)
            sin_ref[sl] = jnp.where(lane % 2 == 0, -1.0, 1.0) * jnp.sin(angle)
            return 0

        lax.fori_loop(0, pos_ref.shape[1] // 128, rows_of, 0)

    def turn_wo():
        width = wo_in.shape[2]
        n_chunks = dim // width

        def load(c):
            slot = lax.rem(c, 2)
            return pltpu.make_async_copy(wo_ref.at[:, pl.ds(pl.multiple_of(c * width, width), width)], wo_in.at[slot], wo_sem.at[slot, 0])

        def store(c):
            slot = lax.rem(c, 2)
            return pltpu.make_async_copy(wo_st.at[slot], wo_t.at[pl.ds(pl.multiple_of(c * width, width), width)], wo_sem.at[slot, 1])

        load(0).start()

        def body(c, _):
            slot = lax.rem(c, 2)

            @pl.when(c + 1 < n_chunks)
            def _():
                load(c + 1).start()

            @pl.when(c >= 2)
            def _():
                store(c).wait()

            load(c).wait()
            wo_st[slot] = wo_in[slot].T
            store(c).start()
            return 0

        lax.fori_loop(0, n_chunks, body, 0)
        for c in range(min(2, n_chunks)):
            store(c).wait()

    def gate_step(b, _):
        gate = m_ref[2:3] + e_ref[b, 2:3]

        def gate_rows(r, _):
            sl = pl.ds(pl.multiple_of(r * group, group), group)
            stage[b, sl] = (xin[b, sl].astype(F32) * gate).astype(BF16)
            return 0

        lax.fori_loop(0, rows // group, gate_rows, 0)
        out = pltpu.make_async_copy(stage.at[b], mine(d_full, b), st_sem)
        out.start()
        out.wait()
        return 0

    for c in w_copies:
        c.wait()

    def outputs(b, row0, slot):
        dst = pl.ds(row0, 2 * rows)
        return [pltpu.make_async_copy(zst.at[slot, :, pl.ds(0, cols)], q_out.at[b, dst], out_sem.at[slot, 0]),
                pltpu.make_async_copy(zst.at[slot, :, pl.ds(cols, cols)], k_out.at[b, dst], out_sem.at[slot, 1]),
                pltpu.make_async_copy(vst.at[slot], v_out.at[b, dst], out_sem.at[slot, 2])]

    def load(b, row0, slot):
        return pltpu.make_async_copy(y_full.at[b, pl.ds(row0, 2 * rows)], xbuf.at[slot], ld_sem.at[slot])

    load(*gather.ready(0, nb), 0).start()

    def item(i, _):
        slot = lax.rem(i, 2)
        b, row0 = gather.item_place(i, nb)

        @pl.when(i + 1 < 4 * nb)
        def _():
            gather.arrive(i + 1, nb)

        @pl.when(i + 1 == 3 * nb - 1)
        def _():
            for d in range(EARLY_ROWS):
                gather_d.start_own(d)

        @pl.when(i == nb)
        def _():
            load_dy.wait()
            trade.start()
            lax.fori_loop(0, nb, gate_step, 0)
            tables()
            turn_wo()

        @pl.when(i >= 2)
        def _():
            for c in outputs(0, 0, slot):
                c.wait()

        load(0, 0, slot).wait()
        spans = chunks_of(3 * cols, 512)
        for m, (lo, hi) in enumerate(spans):
            if m == len(spans) - 1:
                @pl.when(i + 1 < 4 * nb)
                def _():
                    load(*gather.ready(i + 1, nb), lax.rem(i + 1, 2)).start()

            zst[slot, :, lo:hi] = jnp.dot(xbuf[slot], w_all[:, lo:hi], preferred_element_type=F32) + bias_ref[:, lo:hi]
        vst[slot] = zst[slot, :, 2 * cols:].astype(BF16)
        q = zst[slot, :, :cols]
        k = zst[slot, :, cols:2 * cols]
        sq[2 * b, pl.ds(row0, 2 * rows)] = head_sum(q * q)
        sq[2 * b + 1, pl.ds(row0, 2 * rows)] = head_sum(k * k)
        for c in outputs(b, row0, slot):
            c.start()
        return 0

    lax.fori_loop(0, 4 * nb, item, 0)
    ss_row[...] = jnp.zeros_like(ss_row)
    for j in range(2 * nb):
        ss_row[j:j + 1] = to_row(sq[j])
    sums = Exchange(place, ss_row, slots, e_send, e_recv)
    sums.start()
    for slot in range(2):
        for c in outputs(0, 0, slot):
            c.wait()
    for b in range(nb):
        gather.finish(b)
    for d in range(EARLY_ROWS):
        gather_d.whole_blocks_in(d)
    trade.wait()
    ss_ref[...] = sums.finish()


def gather_qkv_call(n, x_loc, dy_loc, m_block, e_loc, w_q, w_k, w_v, w_o, b_q, b_k, b_v, g_q, g_k, positions):
    nb, rows, dim = x_loc.shape
    cols = w_q.shape[1]
    tokens = rows * n
    shape = jax.ShapeDtypeStruct
    any_spec = pl.BlockSpec(memory_space=pl.ANY)
    vmem = pl.BlockSpec(memory_space=pltpu.VMEM)
    dma = pltpu.SemaphoreType.DMA
    stat_rows = -(-2 * nb // 8) * 8
    return pl.pallas_call(
        functools.partial(gather_qkv_kernel, n), name="gather_qkv",
        out_shape=[shape((nb, tokens, dim), BF16), shape((nb, tokens, dim), BF16), shape((nb, tokens, cols), F32),
                   shape((nb, tokens, cols), F32), shape((nb, tokens, cols), BF16), shape(w_o.shape, BF16), shape((dim, cols), BF16), shape((stat_rows, tokens), F32),
                   shape((tokens, HEAD_DIM), F32), shape((tokens, HEAD_DIM), F32), shape((2, cols), F32)],
        in_specs=[any_spec, any_spec, vmem, vmem] + [any_spec] * 4 + [vmem] * 7,
        out_specs=[any_spec] * 7 + [vmem] * 4,
        scratch_shapes=[
            pltpu.VMEM((1, 3 * cols), F32),
            pltpu.VMEM((dim, 3 * cols), BF16), pltpu.VMEM((nb, rows, dim), BF16), pltpu.VMEM((nb, rows, dim), BF16),
            pltpu.VMEM((2, 2 * rows, dim), BF16), pltpu.VMEM((2, 2 * rows, 3 * cols), F32), pltpu.VMEM((2, 2 * rows, cols), BF16),
            pltpu.VMEM((2 * nb, tokens, HEAD_DIM), F32), pltpu.VMEM((stat_rows, tokens), F32), pltpu.VMEM((n, stat_rows, tokens), F32),
            pltpu.VMEM((2, cols, min(512, dim)), BF16), pltpu.VMEM((2, min(512, dim), cols), BF16), dma((2, 2)),
            dma((3,)), dma((nb,)), dma, dma((2,)), dma((2, 3)), dma((nb, GATHER_SEMS)), dma((nb, GATHER_SEMS)),
            dma((EARLY_ROWS, GATHER_SEMS)), dma((EARLY_ROWS, GATHER_SEMS)), dma((n,)), dma((n,)), dma, dma],
        compiler_params=params(collective_id=0, has_side_effects=True),
        cost_estimate=cost(6 * nb * tokens * dim * cols, 6 * dim * cols + 14 * nb * tokens * cols),
    )(x_loc, dy_loc, m_block, e_loc, w_q, w_k, w_v, w_o, b_q, b_k, b_v, g_q, g_k, positions.T, jnp.asarray(rope_freqs()))


def all_sum_kernel(n, x_ref, o_ref, pieces, total, send_a, recv_a, send_b, recv_b):
    place = Place(n)
    me = place.me
    place.barrier(place.everyone())

    def first(d, dev, src):
        return pltpu.make_async_remote_copy(src_ref=x_ref.at[src], dst_ref=pieces.at[me], send_sem=send_a.at[d], recv_sem=recv_a.at[me],
                                            device_id={'tp': dev}, device_id_type=MESH_ID)

    for d, dev in enumerate(place.everyone()):
        first(d, dev, dev).start()
    pieces[me] = x_ref[me]
    for d, dev in enumerate(place.everyone()):
        pltpu.make_async_remote_copy(src_ref=x_ref.at[me], dst_ref=pieces.at[dev], send_sem=send_a.at[d], recv_sem=recv_a.at[dev],
                                     device_id={'tp': dev}, device_id_type=MESH_ID).wait_recv()
    acc = pieces[0]
    for d in range(1, n):
        acc = acc + pieces[d]
    total[...] = acc
    o_ref[me] = acc
    for d, dev in enumerate(place.everyone()):
        first(d, dev, dev).wait_send()
    for d, dev in enumerate(place.everyone()):
        pltpu.make_async_remote_copy(src_ref=total, dst_ref=o_ref.at[me], send_sem=send_b.at[d], recv_sem=recv_b.at[me],
                                     device_id={'tp': dev}, device_id_type=MESH_ID).start()
    for d, dev in enumerate(place.everyone()):
        copy = pltpu.make_async_remote_copy(src_ref=total, dst_ref=o_ref.at[dev], send_sem=send_b.at[d], recv_sem=recv_b.at[dev],
                                            device_id={'tp': dev}, device_id_type=MESH_ID)
        copy.wait_send()
        copy.wait_recv()


def all_sum_call(n, x):
    spec = pl.BlockSpec(memory_space=pltpu.VMEM)
    dma = pltpu.SemaphoreType.DMA
    return pl.pallas_call(
        functools.partial(all_sum_kernel, n), name="all_sum",
        out_shape=jax.ShapeDtypeStruct(x.shape, x.dtype), in_specs=[spec], out_specs=spec,
        scratch_shapes=[pltpu.VMEM(x.shape, x.dtype), pltpu.VMEM(x.shape[1:], x.dtype), dma((n,)), dma((n,)), dma((n,)), dma((n,))],
        compiler_params=pltpu.CompilerParams(collective_id=4, has_side_effects=True, vmem_limit_bytes=4 * 1024 * 1024),
        cost_estimate=cost(4_000_000_000, x.size * 8),
    )(x)


def swap_pairs(x):
    lane = lax.broadcasted_iota(jnp.int32, x.shape, 1)
    return jnp.where(lane % 2 == 0, pltpu.roll(x, HEAD_DIM - 1, 1), pltpu.roll(x, 1, 1))


def rotate(x, cos, sin):
    return x * cos + swap_pairs(x) * sin


SCORE_SCALE = HEAD_DIM ** -0.5 * LOG2E


def softmax_block(s):
    top = jnp.max(s, axis=1, keepdims=True)
    p = jnp.exp2(s * SCORE_SCALE - top * SCORE_SCALE)
    total = jnp.sum(p, axis=1, keepdims=True)
    return p * (1.0 / total), top * SCORE_SCALE + jnp.log(total) * LOG2E


class Scatter:
    def __init__(self, place, part, recv_far, recv_side, send, recv, far_src=None, early=0):
        self.at, self.part, self.far, self.side, self.send, self.recv = place, part, recv_far, recv_side, send, recv
        self.far_src, self.early = part if far_src is None else far_src, early
        self.rows = part.shape[2]
        self.half = self.rows // 2

    def copy(self, j, idx, src, dst, target):
        return pltpu.make_async_remote_copy(src_ref=src, dst_ref=dst, send_sem=self.send.at[j, idx], recv_sem=self.recv.at[j, idx],
                                            device_id={'tp': target}, device_id_type=MESH_ID)

    def message(self, j, idx):
        p, part, far, side = self.at, self.part, self.far, self.side
        first, second = pl.ds(0, self.half), pl.ds(self.half, self.rows - self.half)
        src, dst, target = (
            lambda: (self.far_src.at[j, 0, first], far.at[j, 0], p.right),
            lambda: (self.far_src.at[j, 0, second], far.at[j, 1], p.left),
            lambda: (part.at[j, 1, second], side.at[j, 0, second], p.right),
            lambda: (part.at[j, 2, first], side.at[j, 1, first], p.left),
            lambda: (part.at[j, 1, first], side.at[j, 0, first], p.right),
            lambda: (part.at[j, 2, second], side.at[j, 1, second], p.left))[idx]()
        return self.copy(j, idx, src, dst, target)

    def start_far(self, j, _=0):
        for idx in (0, 1):
            self.message(j, idx).start()
        return 0

    def start_side(self, j, _):
        for idx in (2, 3):
            self.message(j, idx).start()
        return 0

    def sums(self, j):
        h = self.half

        @pl.when(j >= self.early)
        def _():
            self.message(j, 0).wait_recv()
            self.message(j, 1).wait_recv()

        self.part[j, 1, :h] = (self.part[j, 1, :h].astype(F32) + self.far[j, 0].astype(F32)).astype(BF16)
        self.part[j, 2, h:] = (self.part[j, 2, h:].astype(F32) + self.far[j, 1].astype(F32)).astype(BF16)
        self.message(j, 4).start()
        self.message(j, 5).start()

    def sums_step(self, j, _):
        self.sums(j)
        return 0

    def final(self, j):
        for idx in range(2, 6):
            self.message(j, idx).wait_recv()
        total = self.part[j, 3].astype(F32) + self.side[j, 0].astype(F32) + self.side[j, 1].astype(F32)
        self.part[j, 3] = total.astype(BF16)

    def finish(self, j):
        @pl.when(j >= self.early)
        def _():
            for idx in range(2):
                self.message(j, idx).wait_send()

        for idx in range(2, 6):
            self.message(j, idx).wait_send()

    @staticmethod
    def scratch(rows, dim):
        nc, dma = dim // CHUNK, pltpu.SemaphoreType.DMA
        return [pltpu.VMEM((nc, 4, rows, CHUNK), BF16), pltpu.VMEM((nc, 2, rows // 2, CHUNK), BF16),
                pltpu.VMEM((nc, 2, rows, CHUNK), BF16), dma((nc, 6)), dma((nc, 6))]


def scatter_outputs(part, out, sem, j):
    nb, rows, _ = out.shape
    cs = pl.ds(pl.multiple_of(j * CHUNK, CHUNK), CHUNK)
    return [pltpu.make_async_copy(part.at[j, 3, pl.ds(b * rows, rows)], out.at[b, :, cs], sem.at[b]) for b in range(nb)]


def scatter_end(scatter, out, sem, nc):
    def last(j, _):
        scatter.final(j)
        for c in scatter_outputs(scatter.part, out, sem, j):
            c.start()
        return 0

    lax.fori_loop(0, nc, last, 0)

    def drain(j, _):
        for c in scatter_outputs(scatter.part, out, sem, j):
            c.wait()
        scatter.finish(j)
        return 0

    lax.fori_loop(0, nc, drain, 0)


def pair_rows(place, nb, rows, mine, theirs, lhs, sem):
    width = mine.shape[2]
    out = []
    for d, dev in enumerate((place.far, place.right, place.left, place.me)):
        src_rows = pl.ds(pl.multiple_of(dev * rows, 16), rows)
        for b in range(nb):
            dst_rows = pl.ds((d * nb + b) * rows, rows)
            for j, src in enumerate((mine, theirs)):
                out.append(pltpu.make_async_copy(src.at[b, src_rows], lhs.at[dst_rows, pl.ds(j * width, width)], sem.at[d // 2]))
    return out


def gather_attn_kernel(n, nb, heads, dim, q_ref, k_ref, v_ref, gain_ref, cos_ref, sin_ref, ss_ref,
                       wq_ref, wo_ref, wo_p, wo_t, d_in,
                       d_full, o_out, o_p, da_out, wq_p, part_out, far_in, qr_ref, kr_ref, lse_ref, o32_ref,
                       inv_q, inv_k, o_all, wo, xbuf, ast,
                       w_sem, ld_sem, out_sem, o_sem, p_sem, l_sem, g_send, g_recv, t_send, t_recv, r_send, r_recv, s_send, s_recv):
    step = pl.program_id(0)
    tokens = q_ref.shape[1]
    rows = tokens // n
    blk = min(384, tokens)
    place = Place(n)
    gather = Gather(place, d_full, rows, g_send, g_recv, early=EARLY_ROWS)
    cols = heads * HEAD_DIM
    nc = dim // CHUNK
    early_chunks = min(EARLY_CHUNKS, nc)
    mid = nc // 2
    scatter = Scatter(place, part_out, far_in, None, s_send, s_recv)
    trade_o = RowTrade(place, o_out, o_p, rows, r_send, r_recv)

    def trade_w():
        return place.to_partner(wq_ref, wq_p, t_send, t_recv)


    @pl.when(step == 0)
    def _():
        pltpu.make_async_copy(wo_t, wo, w_sem).start()
        place.barrier(place.near())

        for b in range(EARLY_ROWS):
            gather.pass_left(b)
            gather.pass_right(b)

        def own(b, _):
            gather.start_own(b)
            return 0

        lax.fori_loop(EARLY_ROWS, nb, own, 0)
        trade_w().start()

    @pl.when(step < nb * heads)
    def _():
        b = step // heads
        h = lax.rem(step, heads)

        @pl.when(h == 0)
        def _():
            inv_q[...] = lanes_of(lax.rsqrt(ss_ref[pl.ds(2 * b, 1)] / dim + EPS_NORM))
            inv_k[...] = lanes_of(lax.rsqrt(ss_ref[pl.ds(2 * b + 1, 1)] / dim + EPS_NORM))

        cos, sin = cos_ref[...], sin_ref[...]
        q_rot = rotate(q_ref[0] * inv_q[...] * gain_ref[0:1], cos, sin).astype(BF16)
        k_rot = rotate(k_ref[0] * inv_k[...] * gain_ref[1:2], cos, sin).astype(BF16)
        v = v_ref[0]
        lanes = pl.ds(pl.multiple_of(h * HEAD_DIM, HEAD_DIM), HEAD_DIM)
        qr_ref[0], kr_ref[0] = q_rot, k_rot

        def scores(i):
            return lax.dot_general(q_rot[i * blk:(i + 1) * blk], k_rot, NT, preferred_element_type=F32)

        ahead = scores(0)
        for i in range(tokens // blk):
            s = ahead
            if (i + 1) * blk < tokens:
                ahead = scores(i + 1)
            p, lse = softmax_block(s)
            lse_ref[0, i * blk:(i + 1) * blk] = jnp.broadcast_to(lse, (blk, HEAD_DIM))
            o = jnp.dot(p.astype(BF16), v, preferred_element_type=F32)
            o32_ref[0, i * blk:(i + 1) * blk] = o
            o_all[b, i * blk:(i + 1) * blk, lanes] = o.astype(BF16)

    @pl.when(step == nb * heads)
    def _():
        o_copy = pltpu.make_async_copy(o_all, o_out, o_sem)
        o_copy.start()
        pltpu.make_async_copy(wo_t, wo, w_sem).wait()

        def outputs(b, row0, slot):
            return pltpu.make_async_copy(ast.at[slot], da_out.at[b, pl.ds(row0, 2 * rows)], out_sem.at[slot])

        def load(b, row0, slot):
            return pltpu.make_async_copy(d_full.at[b, pl.ds(row0, 2 * rows)], xbuf.at[slot], ld_sem.at[slot])

        def project(lhs, wbuf, stage):
            loads = pair_rows(place, nb, rows, o_out, o_p, lhs, l_sem)
            for c in loads:
                c.start()

            def chunk(j):
                cs = pl.ds(pl.multiple_of(j * CHUNK, CHUNK), CHUNK)
                slot = lax.rem(j, 2)
                return [pltpu.make_async_copy(wo_ref.at[:, cs], wbuf.at[slot, pl.ds(0, cols)], p_sem.at[slot, 0]),
                        pltpu.make_async_copy(wo_p.at[:, cs], wbuf.at[slot, pl.ds(cols, cols)], p_sem.at[slot, 1])]

            def store(j):
                slot = lax.rem(j, 2)
                return pltpu.make_async_copy(stage.at[slot], part_out.at[j], p_sem.at[slot, 2])

            def stored(j):
                store(j).wait()

                @pl.when((j < early_chunks) & (j >= mid))
                def _():
                    scatter.start_far(j)

            for c in chunk(0):
                c.start()
            for c in loads:
                c.wait()

            def body(j, _):
                slot = lax.rem(j, 2)

                @pl.when(j + 1 < nc)
                def _():
                    for c in chunk(j + 1):
                        c.start()

                for c in chunk(j):
                    c.wait()
                half = 2 * nb * rows
                for d in range(2):
                    z = jnp.dot(lhs[d * half:(d + 1) * half], wbuf[slot], preferred_element_type=F32).astype(BF16)
                    stage[slot, 2 * d] = z[:half // 2]
                    stage[slot, 2 * d + 1] = z[half // 2:]
                store(j).start()

                @pl.when(j >= 1)
                def _():
                    stored(j - 1)

                @pl.when(j == mid)
                def _():
                    gather.arrive(3 * nb - 2, nb)
                    gather.arrive(3 * nb - 1, nb)
                    lax.fori_loop(0, min(early_chunks, mid), scatter.start_far, 0)

                return 0

            lax.fori_loop(0, nc, body, 0)
            stored(nc - 1)

        def fetch(i):
            b, row0 = gather.ready(i, nb)
            load(b, row0, lax.rem(i, 2)).start()

        fetch(0)
        gather.arrive(jnp.int32(1), nb)

        def item(i, _):
            slot = lax.rem(i, 2)

            @pl.when((i + 2 != 3 * nb - 2) & (i + 2 != 3 * nb - 1) & (i + 2 < 4 * nb))
            def _():
                gather.arrive(i + 2, nb)

            @pl.when((i + 1 != 3 * nb - 2) & (i + 1 < 4 * nb))
            def _():
                fetch(i + 1)

            @pl.when(i >= 2)
            def _():
                outputs(0, 0, slot).wait()

            load(0, 0, slot).wait()
            ast[slot] = jnp.dot(xbuf[slot], wo[...], preferred_element_type=F32).astype(BF16)
            b, row0 = gather.item_place(i, nb)
            outputs(b, row0, slot).start()

            @pl.when(i == 0)
            def _():
                o_copy.wait()
                trade_o.start()

            @pl.when(i + 1 == 3 * nb - 2)
            def _():
                trade_o.wait_recv()
                pl.run_scoped(project, pltpu.VMEM((4 * nb * rows, 2 * cols), BF16), pltpu.VMEM((2, 2 * cols, CHUNK), BF16),
                              pltpu.VMEM((2, 4, nb * rows, CHUNK), BF16))
                fetch(i + 1)

            return 0

        lax.fori_loop(0, 4 * nb, item, 0)
        for slot in range(2):
            outputs(0, 0, slot).wait()
        for b in range(nb):
            gather.finish(b)
        trade_o.wait_send()
        trade_w().wait()
        for j in range(early_chunks):
            for idx in (0, 1):
                scatter.message(j, idx).wait()


def gather_attn_call(n, q, k, v, gains, cos_tab, sin_tab, ss, w_q, w_o, wo_p, wo_t, d_full):
    nb, tokens, cols = q.shape
    dim = w_o.shape[1]
    heads = cols // HEAD_DIM
    rows = tokens // n
    last = nb * heads - 1
    nc = dim // CHUNK
    early = min(EARLY_CHUNKS, nc)
    shape = jax.ShapeDtypeStruct
    dma = pltpu.SemaphoreType.DMA
    any_spec = pl.BlockSpec(memory_space=pl.ANY)

    def head_of(i):
        i = jnp.minimum(i, last)
        return i // heads, i % heads

    blk = pl.BlockSpec((1, tokens, HEAD_DIM), lambda i: (head_of(i)[0], 0, head_of(i)[1]))
    vec = pl.BlockSpec((2, HEAD_DIM), lambda i: (0, head_of(i)[1]))
    tab = pl.BlockSpec((tokens, HEAD_DIM), lambda i: (0, 0))
    head_arr = shape((nb, tokens, cols), BF16)
    return pl.pallas_call(
        functools.partial(gather_attn_kernel, n, nb, heads, dim), name="gather_attn", grid=(nb * heads + 1,),
        out_shape=[shape(d_full.shape, BF16), head_arr, head_arr, head_arr, shape(w_q.shape, BF16)]
        + [shape((nc, 4, nb * rows, CHUNK), BF16), shape((early, 2, nb * rows // 2, CHUNK), BF16), head_arr, head_arr,
           shape((nb, tokens, cols), F32), shape((nb, tokens, cols), F32)],
        in_specs=[blk, blk, blk, vec, tab, tab, pl.BlockSpec(ss.shape, lambda i: (0, 0))] + [any_spec] * 5,
        out_specs=[any_spec] * 7 + [blk] * 4,
        scratch_shapes=[
            pltpu.VMEM((tokens, HEAD_DIM), F32), pltpu.VMEM((tokens, HEAD_DIM), F32), pltpu.VMEM((nb, tokens, cols), BF16),
            pltpu.VMEM((dim, cols), BF16), pltpu.VMEM((2, 2 * rows, dim), BF16), pltpu.VMEM((2, 2 * rows, cols), BF16),
            dma, dma((2,)), dma((2,)), dma, dma((2, 3)), dma((2,)), dma((nb, GATHER_SEMS)), dma((nb, GATHER_SEMS)), dma, dma,
            dma((nb, n // 2)), dma((nb, n // 2)), dma((early, 6)), dma((early, 6))],
        input_output_aliases={11: 0},
        compiler_params=params("arbitrary", collective_id=1, has_side_effects=True),
        cost_estimate=cost(4 * nb * tokens * dim * cols + 4 * nb * tokens * tokens * cols, 8 * nb * tokens * dim),
    )(q, k, v, gains, cos_tab, sin_tab, ss, w_q, w_o, wo_p, wo_t, d_full)


class DyChunks:
    def __init__(self, lhs, wbuf, weights, w_sem):
        self.lhs, self.wbuf, self.weights, self.sem = lhs, wbuf, weights, w_sem

    def loads(self, j):
        slot = lax.rem(j, 2)
        src = pl.ds(pl.multiple_of(j * CHUNK, CHUNK), CHUNK)
        width = self.weights[0].shape[1]
        return [pltpu.make_async_copy(w.at[src], self.wbuf.at[slot, :, pl.ds(m * width, width)], self.sem.at[slot, m])
                for m, w in enumerate(self.weights)]

    def dot(self, j, d):
        half = self.lhs.shape[0] // 2
        return lax.dot_general(self.lhs[d * half:(d + 1) * half], self.wbuf[lax.rem(j, 2)], NT, preferred_element_type=F32).astype(BF16)


def attn_bwd_kernel(n, nb, heads, dim, q_ref, k_ref, qr_ref, kr_ref, v_ref, do_ref, o_ref, lse_ref, gain_ref, cos_ref, sin_ref, ss_ref,
                    q_hbm, k_hbm, o_hbm, part_in, far_in, d_full, wq_hbm, wk_hbm, wv_hbm, wq_p,
                    proj_out, g_out, g_p, dqs_out, dks_out, dwo_out, wk_p, wv_p, part_dy, far_dy, dgq_ref, dgk_ref,
                    part, recv_far, recv_side, s_send, s_recv,
                    inv_q, inv_k, acc_q, acc_k, p_all, ds_all, dq_all, qs_st, ks_st, v_st, st_row, st_sum, slots, fbuf, gbuf, lanes_s,
                    ld_sem, w_sem, fl_sem, g_sem, go_sem, out_sem, e_send, e_recv, t_send, t_recv, r_send, r_recv, c_sem, y_send, y_recv):
    step = pl.program_id(0)
    tokens = q_ref.shape[1]
    rows = tokens // n
    cols = heads * HEAD_DIM
    blk = min(256, tokens)
    nc = dim // CHUNK
    steps = nb * heads
    scale = HEAD_DIM ** -0.5
    place = Place(n)
    early = far_in.shape[0]
    scatter = Scatter(place, part, recv_far, recv_side, s_send, s_recv, far_src=part_in, early=early)

    def stored():
        return [pltpu.make_async_copy(part_in, part, ld_sem.at[0]),
                pltpu.make_async_copy(far_in, recv_far.at[pl.ds(0, early)], ld_sem.at[1])]

    def trade_w(j):
        return place.to_partner((wk_hbm, wv_hbm)[j], (wk_p, wv_p)[j], t_send.at[j], t_recv.at[j])

    @pl.when(step == 0)
    def _():
        place.barrier(place.everyone())
        for c in stored():
            c.start()
        for j in range(2):
            trade_w(j).start()

    @pl.when(step == 1)
    def _():
        for c in stored():
            c.wait()

    def flush(b, h, slot):
        lanes = pl.ds(pl.multiple_of(h * HEAD_DIM, HEAD_DIM), HEAD_DIM)
        v_lanes = pl.ds(pl.multiple_of(2 * cols + h * HEAD_DIM, HEAD_DIM), HEAD_DIM)
        return [pltpu.make_async_copy(qs_st.at[slot], dqs_out.at[b, :, lanes], fl_sem.at[slot, 0]),
                pltpu.make_async_copy(ks_st.at[slot], dks_out.at[b, :, lanes], fl_sem.at[slot, 1]),
                pltpu.make_async_copy(v_st.at[slot], g_out.at[b, :, v_lanes], fl_sem.at[slot, 2])]

    mid = early
    events = []
    late = list(range(mid))
    for m, j in enumerate(range(early, nc)):
        events.append(functools.partial(scatter.start_far, j))
        if m >= 2 and m % 2 == 0 and late:
            events.append(functools.partial(scatter.sums, late.pop(0)))
    events += [functools.partial(scatter.sums, j) for j in late]
    for m, event in enumerate(events):
        @pl.when(step == m * (steps - 1) // len(events))
        def _(event=event):
            event()

    rb = min(256, tokens)
    per = tokens // rb

    def stats(b):
        return Exchange(place, st_row.at[b], slots.at[b], e_send.at[b], e_recv.at[b])

    def grad_loads(b, i):
        r0 = pl.multiple_of(i * rb, rb)
        return [pltpu.make_async_copy(src.at[b, pl.ds(r0, rb)], fbuf.at[m], g_sem.at[m])
                for m, src in enumerate((dqs_out, q_hbm, dks_out, k_hbm))]

    def grad_store(b, i):
        r0 = pl.multiple_of(i * rb, rb)
        return pltpu.make_async_copy(gbuf, g_out.at[b, pl.ds(r0, rb), pl.ds(0, 2 * cols)], go_sem.at[0])

    def trade(b):
        return RowTrade(place, g_out, g_p, rows, r_send, r_recv, rows_of=(b,))

    def grad_block(b, i):
        for c in grad_loads(b, i):
            c.wait()
        sl = pl.ds(pl.multiple_of(i * rb, rb), rb)
        for m in range(2):
            inv_l = lanes_s[2 * m, sl]
            st_l = lanes_s[2 * m + 1, sl]
            for h in range(heads):
                hs = slice(h * HEAD_DIM, (h + 1) * HEAD_DIM)
                grad = inv_l * (fbuf[2 * m, :, hs] - (fbuf[2 * m + 1, :, hs] * inv_l) * st_l)
                gbuf[:, m * cols + h * HEAD_DIM:m * cols + (h + 1) * HEAD_DIM] = grad.astype(BF16)
        grad_store(b, i).start()

    def grad_begin(b):
        st_sum[...] = stats(b).finish()
        for m in range(2):
            lanes_s[2 * m] = lanes_of(lax.rsqrt(ss_ref[pl.ds(2 * b + m, 1)] / dim + EPS_NORM))
            lanes_s[2 * m + 1] = lanes_of(st_sum[m:m + 1] / dim)

    first = heads - per
    b_old = step // heads - 1
    i_old = lax.rem(step, heads) - first

    @pl.when((step >= heads) & (step < steps) & (i_old >= 0))
    def _():
        @pl.when(i_old == 0)
        def _():
            grad_begin(b_old)

        @pl.when(i_old > 0)
        def _():
            grad_store(0, 0).wait()

        for c in grad_loads(b_old, i_old):
            c.start()

    @pl.when((step >= 2 * heads) & (lax.rem(step, heads) == 0))
    def _():
        grad_store(0, 0).wait()
        for b in range(nb - 1):
            pl.when(step == (b + 2) * heads)(trade(b).start)

    @pl.when(step < steps)
    def _():
        b = step // heads
        head = lax.rem(step, heads)
        slot = lax.rem(step, 2)

        @pl.when(step == 0)
        def _():
            st_row[...] = jnp.zeros_like(st_row)

        @pl.when(head == 0)
        def _():
            inv_q[...] = lanes_of(lax.rsqrt(ss_ref[pl.ds(2 * b, 1)] / dim + EPS_NORM))
            inv_k[...] = lanes_of(lax.rsqrt(ss_ref[pl.ds(2 * b + 1, 1)] / dim + EPS_NORM))
            acc_q[...] = jnp.zeros_like(acc_q)
            acc_k[...] = jnp.zeros_like(acc_k)

        @pl.when(step >= 2)
        def _():
            for c in flush(0, 0, slot):
                c.wait()

        cos, sin = cos_ref[...], sin_ref[...]
        q_rot, k_rot, v, do = qr_ref[0], kr_ref[0], v_ref[0], do_ref[0]

        def scores(i):
            sl = slice(i * blk, (i + 1) * blk)
            return (lax.dot_general(q_rot[sl], k_rot, NT, preferred_element_type=F32),
                    lax.dot_general(do[sl], v, NT, preferred_element_type=F32))

        ahead = scores(0)
        for i in range(tokens // blk):
            sl = slice(i * blk, (i + 1) * blk)
            s, dp = ahead
            if (i + 1) * blk < tokens:
                ahead = scores(i + 1)
            lse = jnp.concatenate([lse_ref[0, sl]] * (tokens // HEAD_DIM), axis=1)
            p = jnp.exp2(s * SCORE_SCALE - lse)
            p_all[sl] = p.astype(BF16)
            delta = jnp.sum(do[sl].astype(F32) * o_ref[0, sl], axis=1, keepdims=True)
            ds = (p * (dp - delta)).astype(BF16)
            ds_all[sl] = ds
            dq_all[sl] = jnp.dot(ds, k_rot, preferred_element_type=F32) * scale
        do_t = do.astype(F32).T.astype(BF16)
        q_t = q_rot.astype(F32).T.astype(BF16)
        v_st[slot] = jnp.dot(do_t, p_all[...], preferred_element_type=F32).T.astype(BF16)
        dk_rot = (jnp.dot(q_t, ds_all[...], preferred_element_type=F32) * scale).T.astype(BF16).astype(F32)
        dq_rot = dq_all[...].astype(BF16).astype(F32)
        dq_hat = rotate(dq_rot, cos, -sin)
        dk_hat = rotate(dk_rot, cos, -sin)
        q_hat = q_ref[0] * inv_q[...]
        k_hat = k_ref[0] * inv_k[...]
        dgq_ref[0] = jnp.sum(dq_hat * q_hat, axis=0, keepdims=True)
        dgk_ref[0] = jnp.sum(dk_hat * k_hat, axis=0, keepdims=True)
        dq_s = dq_hat * gain_ref[0:1]
        dk_s = dk_hat * gain_ref[1:2]
        qs_st[slot] = dq_s
        ks_st[slot] = dk_s
        acc_q[...] += dq_s * q_hat
        acc_k[...] += dk_s * k_hat
        for c in flush(b, head, slot):
            c.start()

        @pl.when(head == heads - 1)
        def _():
            st_row[b, 0:1] = to_row(acc_q[...])
            st_row[b, 1:2] = to_row(acc_k[...])
            for m in range(nb):
                pl.when(b == m)(stats(m).start)

    @pl.when((step >= heads) & (step < steps) & (i_old >= 0))
    def _():
        grad_block(b_old, i_old)

    @pl.when(step == steps)
    def _():
        for s in range(2):
            for c in flush(0, 0, s):
                c.wait()
        lax.fori_loop(mid, nc, scatter.sums_step, 0)
        lax.fori_loop(0, nc, scatter.start_side, 0)
        for c in grad_loads(nb - 1, 0):
            c.start()
        grad_begin(nb - 1)

        def last_row(i, _):
            @pl.when(i > 0)
            def _():
                grad_store(0, 0).wait()
                for c in grad_loads(nb - 1, i):
                    c.start()

            grad_block(nb - 1, i)
            return 0

        lax.fori_loop(0, per, last_row, 0)
        grad_store(0, 0).wait()
        trade(nb - 1).start()

        def weight_grad(turned, obuf, dbuf, wst):
            bn = min(512, dim)
            n_chunks = dim // bn

            def chunk(c):
                slot = lax.rem(c, 2)
                return pltpu.make_async_copy(d_full.at[:, :, pl.ds(pl.multiple_of(c * bn, bn), bn)], dbuf.at[slot], w_sem.at[slot, 1])

            def store(c):
                slot = lax.rem(c, 2)
                return pltpu.make_async_copy(wst.at[slot], dwo_out.at[:, pl.ds(pl.multiple_of(c * bn, bn), bn)], w_sem.at[slot, 0])

            load_o = pltpu.make_async_copy(o_hbm, obuf, ld_sem.at[0])
            load_o.start()
            chunk(0).start()
            load_o.wait()
            for b in range(nb):
                turned[:, b * tokens:(b + 1) * tokens] = obuf[b].T

            def body(c, _):
                slot = lax.rem(c, 2)

                @pl.when(c + 1 < n_chunks)
                def _():
                    chunk(c + 1).start()

                @pl.when(c >= 2)
                def _():
                    store(c).wait()

                chunk(c).wait()
                d = dbuf[slot].reshape(nb * tokens, bn)
                wst[slot] = jnp.dot(turned[...], d, preferred_element_type=F32).astype(BF16)
                store(c).start()
                return 0

            lax.fori_loop(0, n_chunks, body, 0)
            for s in range(min(2, n_chunks)):
                store(s).wait()

        bn = min(512, dim)
        pl.run_scoped(weight_grad, pltpu.VMEM((cols, nb * tokens), BF16), pltpu.VMEM((nb, tokens, cols), BF16),
                      pltpu.VMEM((2, nb, tokens, bn), BF16), pltpu.VMEM((2, cols, bn), BF16))
        for b in range(nb):
            trade(b).wait_recv()
        for j in range(2):
            trade_w(j).wait_recv()

        n_dy = part_dy.shape[0]
        scatter_y = Scatter(place, part_dy, far_dy, None, y_send, y_recv)

        def first_dy(lhs, wbuf, pst):
            loads = pair_rows(place, nb, rows, g_out, g_p, lhs, ld_sem)
            for c in loads:
                c.start()
            dy = DyChunks(lhs, wbuf, (wq_hbm, wk_hbm, wv_hbm, wq_p, wk_p, wv_p), c_sem)
            for c in dy.loads(0):
                c.start()
            for c in loads:
                c.wait()

            def body(j, _):
                @pl.when(j + 1 < n_dy)
                def _():
                    for c in dy.loads(j + 1):
                        c.start()

                for c in dy.loads(j):
                    c.wait()
                store = pltpu.make_async_copy(pst, part_dy.at[j], go_sem.at[0])

                @pl.when(j >= 1)
                def _():
                    store.wait()
                    scatter_y.start_far(j - 1)

                for d in range(2):
                    z = dy.dot(j, d)
                    pst[2 * d] = z[:nb * rows]
                    pst[2 * d + 1] = z[nb * rows:]
                store.start()
                return 0

            lax.fori_loop(0, n_dy, body, 0)
            pltpu.make_async_copy(pst, part_dy.at[n_dy - 1], go_sem.at[0]).wait()
            scatter_y.start_far(n_dy - 1)

        pl.run_scoped(first_dy, pltpu.VMEM((4 * nb * rows, 6 * cols), BF16), pltpu.VMEM((2, CHUNK, 6 * cols), BF16),
                      pltpu.VMEM((4, nb * rows, CHUNK), BF16))
        scatter_end(scatter, proj_out, out_sem, nc)
        for b in range(nb):
            trade(b).wait_send()
        for j in range(2):
            trade_w(j).wait_send()
        for j in range(n_dy):
            for idx in (0, 1):
                scatter_y.message(j, idx).wait()


def attn_bwd_call(n, q, k, q_rot, k_rot, v, d_attn, o, o32, lse, gains, cos_tab, sin_tab, ss, part, far, d_full, w_q, w_k, w_v, wq_p):
    nb, tokens, cols = q.shape
    dim = d_full.shape[2]
    heads = cols // HEAD_DIM
    rows = tokens // n
    steps = nb * heads
    shape = jax.ShapeDtypeStruct
    dma = pltpu.SemaphoreType.DMA
    any_spec = pl.BlockSpec(memory_space=pl.ANY)

    def head_of(i):
        i = jnp.minimum(i, steps - 1)
        return i // heads, i % heads

    blk = pl.BlockSpec((1, tokens, HEAD_DIM), lambda i: (head_of(i)[0], 0, head_of(i)[1]))
    vec = pl.BlockSpec((2, HEAD_DIM), lambda i: (0, head_of(i)[1]))
    out_vec = pl.BlockSpec((1, 1, HEAD_DIM), lambda i: (head_of(i)[0], 0, head_of(i)[1]))
    tab = pl.BlockSpec((tokens, HEAD_DIM), lambda i: (0, 0))
    whole = (nb, tokens, cols)
    lane_tile = pltpu.VMEM((tokens, HEAD_DIM), F32)
    n_dy = min(EARLY_DY, dim // CHUNK)
    return pl.pallas_call(
        functools.partial(attn_bwd_kernel, n, nb, heads, dim), name="attn_bwd", grid=(steps + 1,),
        out_shape=[shape((nb, rows, dim), BF16), shape((nb, tokens, 3 * cols), BF16), shape((nb, tokens, 3 * cols), BF16),
                   shape(whole, F32), shape(whole, F32), shape((cols, dim), BF16),
                   shape(w_k.shape, BF16), shape(w_v.shape, BF16), shape((n_dy,) + part.shape[1:], BF16), shape((n_dy,) + far.shape[1:], BF16),
                   shape((nb, 1, cols), F32), shape((nb, 1, cols), F32)],
        in_specs=[blk] * 8 + [vec, tab, tab, pl.BlockSpec(ss.shape, lambda i: (0, 0))] + [any_spec] * 10,
        out_specs=[any_spec] * 10 + [out_vec, out_vec],
        scratch_shapes=Scatter.scratch(nb * rows, dim) + [lane_tile] * 4 + [pltpu.VMEM((tokens, tokens), BF16)] * 2 + [
            lane_tile, pltpu.VMEM((2, tokens, HEAD_DIM), F32), pltpu.VMEM((2, tokens, HEAD_DIM), F32),
            pltpu.VMEM((2, tokens, HEAD_DIM), BF16), pltpu.VMEM((nb, 8, tokens), F32), pltpu.VMEM((8, tokens), F32),
            pltpu.VMEM((nb, n, 8, tokens), F32), pltpu.VMEM((4, min(256, tokens), cols), F32), pltpu.VMEM((min(256, tokens), 2 * cols), BF16),
            pltpu.VMEM((4, tokens, HEAD_DIM), F32),
            dma((2,)), dma((2, 2)), dma((2, 3)), dma((4,)), dma((2,)), dma((nb,)), dma((nb, n)), dma((nb, n)), dma((2,)), dma((2,)),
            dma((nb, n // 2)), dma((nb, n // 2)), dma((2, 6)), dma((n_dy, 6)), dma((n_dy, 6))],
        compiler_params=params("arbitrary", collective_id=2, has_side_effects=True),
        cost_estimate=cost(4 * nb * tokens * dim * cols + 36 * nb * tokens * tokens * cols, 30 * nb * tokens * cols),
    )(q, k, q_rot, k_rot, v, d_attn, o32, lse, gains, cos_tab, sin_tab, ss, q, k, o, part, far, d_full, w_q, w_k, w_v, wq_p)


def dy_dw_kernel(n, nb, dim, g_hbm, g_p, wq_hbm, wk_hbm, wv_hbm, wq_p, wk_p, wv_p, y_full, part_in, far_in,
                 dy_out, dwq_out, dwk_out, dwv_out,
                 part, recv_far, recv_side, s_send, s_recv, g, ld_sem, w_sem, y_sem, o_sem, out_sem):
    tokens = g_hbm.shape[1]
    rows = tokens // n
    cols = g_hbm.shape[2] // 3
    nc = dim // CHUNK
    early = far_in.shape[0]
    lag = 3
    place = Place(n)
    scatter = Scatter(place, part, recv_far, recv_side, s_send, s_recv, early=early)
    stored = [pltpu.make_async_copy(part_in, part.at[pl.ds(0, early)], ld_sem.at[2]),
              pltpu.make_async_copy(far_in, recv_far.at[pl.ds(0, early)], ld_sem.at[3])]
    load_g = pltpu.make_async_copy(g_hbm, g, ld_sem.at[4])

    def chain(lhs, wbuf):
        loads = pair_rows(place, nb, rows, g_hbm, g_p, lhs, ld_sem)
        dy = DyChunks(lhs, wbuf, (wq_hbm, wk_hbm, wv_hbm, wq_p, wk_p, wv_p), w_sem)
        if early < nc:
            for c in dy.loads(early):
                c.start()
            for c in loads[:len(loads) // 2]:
                c.start()
        for c in stored:
            c.start()
        if early < nc:
            for c in loads[len(loads) // 2:]:
                c.start()
        place.barrier(place.near()[:2])
        for c in stored:
            c.wait()
        lax.fori_loop(0, early, scatter.sums_step, 0)
        load_g.start()

        def body(j, _):
            @pl.when(j + 1 < nc)
            def _():
                for c in dy.loads(j + 1):
                    c.start()

            for c in dy.loads(j):
                c.wait()
            for d in range(2):
                @pl.when(j == early)
                def _(d=d):
                    for c in loads[d * len(loads) // 2:(d + 1) * len(loads) // 2]:
                        c.wait()

                z = dy.dot(j, d)
                part[j, 2 * d] = z[:nb * rows]
                part[j, 2 * d + 1] = z[nb * rows:]
                if d == 0:
                    scatter.start_far(j)

            @pl.when(j >= early + lag)
            def _():
                scatter.sums(j - lag)

            return 0

        lax.fori_loop(early, nc, body, 0)
        lax.fori_loop(0, nc, scatter.start_side, 0)

    pl.run_scoped(chain, pltpu.VMEM((4 * nb * rows, 6 * cols), BF16), pltpu.VMEM((2, CHUNK, 6 * cols), BF16))

    def weight_grad(ybuf, wst):
        bm = min(512, dim)
        n_chunks = dim // bm

        def chunk(c):
            slot = lax.rem(c, 2)
            return pltpu.make_async_copy(y_full.at[:, :, pl.ds(pl.multiple_of(c * bm, bm), bm)], ybuf.at[slot], y_sem.at[slot])

        def store(c):
            slot = lax.rem(c, 2)
            dst = pl.ds(pl.multiple_of(c * bm, bm), bm)
            return [pltpu.make_async_copy(wst.at[slot, :, pl.ds(m * cols, cols)], out.at[dst], o_sem.at[slot, m])
                    for m, out in enumerate((dwq_out, dwk_out, dwv_out))]

        chunk(0).start()
        load_g.wait()

        def body(c, _):
            slot = lax.rem(c, 2)

            @pl.when(c + 1 < n_chunks)
            def _():
                chunk(c + 1).start()

            @pl.when(c >= 2)
            def _():
                for s in store(c):
                    s.wait()

            chunk(c).wait()
            for m in range(lag):
                late = max(nc - lag, early) + m
                if late < nc:
                    pl.when(c == min(m, n_chunks - 1))(functools.partial(scatter.sums, late))
            wst[slot] = lax.dot_general(ybuf[slot].reshape(nb * tokens, bm), g[...].reshape(nb * tokens, 3 * cols), TN,
                                        preferred_element_type=F32).astype(BF16)
            for s in store(c):
                s.start()
            return 0

        lax.fori_loop(0, n_chunks, body, 0)
        for s in range(min(2, n_chunks)):
            for c in store(s):
                c.wait()

    bm = min(512, dim)
    pl.run_scoped(weight_grad, pltpu.VMEM((2, nb, tokens, bm), BF16), pltpu.VMEM((2, bm, 3 * cols), BF16))
    scatter_end(scatter, dy_out, out_sem, nc)


def dy_dw_call(n, g, g_p, w_q, w_k, w_v, wq_p, wk_p, wv_p, y_full, part, far):
    nb, tokens, wide = g.shape
    dim = y_full.shape[2]
    cols = wide // 3
    rows = tokens // n
    shape = jax.ShapeDtypeStruct
    dma = pltpu.SemaphoreType.DMA
    any_spec = pl.BlockSpec(memory_space=pl.ANY)
    return pl.pallas_call(
        functools.partial(dy_dw_kernel, n, nb, dim), name="dy_dw",
        out_shape=[shape((nb, rows, dim), BF16)] + [shape((dim, cols), BF16)] * 3,
        in_specs=[any_spec] * 11, out_specs=[any_spec] * 4,
        scratch_shapes=Scatter.scratch(nb * rows, dim) + [pltpu.VMEM((nb, tokens, 3 * cols), BF16), dma((5,)), dma((2, 6)), dma((2,)), dma((2, 3)), dma((nb,))],
        compiler_params=params(collective_id=3, has_side_effects=True),
        cost_estimate=cost(12 * nb * tokens * dim * cols, 30 * nb * tokens * cols),
    )(g, g_p, w_q, w_k, w_v, wq_p, wk_p, wv_p, y_full, part, far)


def token_kernel(n_copies, x_ref, dy_ref, pr_ref, g_ref, m_ref, e_ref, bo_ref, gq_ref, gk_ref, *refs):
    srcs, (xo_ref, dx_ref, dm_ref, dgq_ref, dgk_ref), dsts = refs[:4], refs[4:9], refs[9:13]
    bufs, (acc, in_sem, out_sem) = refs[13:17], refs[17:]
    group = 16
    step = pl.program_id(0)
    rows = x_ref.shape[1]
    groups = rows // group
    depth = bufs[0].shape[0]
    lag = depth - 1

    def move(c, out):
        copies = []
        for j, (src, dst, buf) in enumerate(zip(srcs, dsts, bufs)):
            size = buf.shape[1]
            sl = pl.ds(pl.multiple_of(c * size, 16), size)
            slot = lax.rem(c, depth)
            copies.append(pltpu.make_async_copy(buf.at[slot], dst.at[sl], out_sem.at[slot, j]) if out
                          else pltpu.make_async_copy(src.at[sl], buf.at[slot], in_sem.at[slot, j]))
        return copies

    def advance(i):
        @pl.when(i < n_copies)
        def _():
            @pl.when(i >= depth)
            def _():
                for c in move(i - depth, True):
                    c.wait()

            for c in move(i, False):
                c.start()

        @pl.when((i >= lag) & (i < n_copies + lag))
        def _():
            for c in move(i - lag, False):
                c.wait()
            for c in move(i - lag, True):
                c.start()

    mod = m_ref[...] + e_ref[0]
    for src, dst in ((gq_ref, dgq_ref), (gk_ref, dgk_ref)):
        dst[...] = jnp.sum(src[...], axis=(0, 1))
    shift_bo = bo_ref[...].reshape(1, bo_ref.shape[0])
    acc[...] = jnp.zeros_like(acc)

    def body(r, _):
        advance(step * groups + r)
        sl = pl.ds(pl.multiple_of(r * group, group), group)
        x = x_ref[0, sl].astype(F32)
        d_out = dy_ref[0, sl].astype(F32)
        proj = pr_ref[0, sl].astype(F32) + shift_bo
        xo_ref[0, sl] = (x + mod[2:3] * proj).astype(BF16)
        gate_part = d_out * proj
        x_norm, inv_std = norm_stats(x)
        d_y = g_ref[0, sl].astype(F32)
        d_norm = d_y * (1.0 + mod[1:2])
        d_x = d_out + inv_std * (
            d_norm - jnp.mean(d_norm, axis=-1, keepdims=True) - x_norm * jnp.mean(d_norm * x_norm, axis=-1, keepdims=True))
        dx_ref[0, sl] = d_x.astype(BF16)
        scale_part = d_y * x_norm
        acc[0] += d_y[:8] + d_y[8:]
        acc[1] += scale_part[:8] + scale_part[8:]
        acc[2] += gate_part[:8] + gate_part[8:]
        return 0

    lax.fori_loop(0, groups, body, 0)
    for j in range(3):
        dm_ref[0, j:j + 1] = jnp.sum(acc[j], axis=0, keepdims=True)

    @pl.when(step == pl.num_programs(0) - 1)
    def _():
        total = pl.num_programs(0) * groups

        def rest(i, _):
            advance(i)
            return 0

        lax.fori_loop(total, jnp.maximum(total, n_copies + lag), rest, 0)
        for c in range(max(n_copies - depth, 0), n_copies):
            for copy in move(c, True):
                copy.wait()


def token_call(x_loc, dy_loc, proj, d_y, m_block, e_loc, b_o, d_gq, d_gk, grads):
    nb, rows, dim = x_loc.shape
    n_copies = dim // min(512, dim)
    row = pl.BlockSpec((1, rows, dim), lambda i: (i, 0, 0))
    mod = pl.BlockSpec((1, 3, dim), lambda i: (i, 0, 0))
    any_spec = pl.BlockSpec(memory_space=pl.ANY)
    dma = pltpu.SemaphoreType.DMA
    depth = 4
    return pl.pallas_call(
        functools.partial(token_kernel, n_copies), name="tokens", grid=(nb,),
        out_shape=[jax.ShapeDtypeStruct(x_loc.shape, BF16), jax.ShapeDtypeStruct(x_loc.shape, BF16),
                   jax.ShapeDtypeStruct((nb, 3, dim), F32)] + [jax.ShapeDtypeStruct(d_gq.shape[2:], F32)] * 2 + [jax.ShapeDtypeStruct(w.shape, BF16) for w in grads],
        in_specs=[row, row, row, row, pl.BlockSpec((3, dim), lambda i: (0, 0)), mod] + [pl.BlockSpec(memory_space=pltpu.VMEM)] * 3 + [any_spec] * 4,
        out_specs=[row, row, mod] + [pl.BlockSpec(memory_space=pltpu.VMEM)] * 2 + [any_spec] * 4,
        scratch_shapes=[pltpu.VMEM((depth, w.shape[0] // n_copies, w.shape[1]), BF16) for w in grads]
        + [pltpu.VMEM((3, 8, dim), F32), dma((depth, 4)), dma((depth, 4))],
        compiler_params=params("arbitrary"),
        cost_estimate=cost(nb * rows * dim * 30, nb * rows * dim * 12),
    )(x_loc, dy_loc, proj, d_y, m_block, e_loc, b_o, d_gq, d_gk, *grads)


def solution(mesh):
    tp_size = mesh.shape['tp']

    def device_step(x_loc, e_loc, m_block, w_q, b_q, w_k, b_k, w_v, b_v, w_o, b_o, g_q, g_k, pos_part, dy_loc):
        nb, _, dim = x_loc.shape
        y_full, d_own, q, k, v, wo_p, wo_t, ss, cos_tab, sin_tab, gains = gather_qkv_call(
            tp_size, x_loc, dy_loc, m_block, e_loc, w_q, w_k, w_v, w_o, b_q, b_k, b_v, g_q, g_k, pos_part)
        d_full, o, _, d_attn, wq_p, part, far, q_rot, k_rot, lse, o32 = gather_attn_call(
            tp_size, q, k, v, gains, cos_tab, sin_tab, ss, w_q, w_o, wo_p, wo_t, d_own)
        proj, g, g_p, _, _, d_wo, wk_p, wv_p, part, far, d_gq, d_gk = attn_bwd_call(
            tp_size, q, k, q_rot, k_rot, v, d_attn, o, o32, lse, gains, cos_tab, sin_tab, ss, part, far, d_full, w_q, w_k, w_v, wq_p)
        d_y, d_wq, d_wk, d_wv = dy_dw_call(tp_size, g, g_p, w_q, w_k, w_v, wq_p, wk_p, wv_p, y_full, part, far)
        x_out, d_x, d_mod, d_gq, d_gk, d_wq, d_wk, d_wv, d_wo = token_call(
            x_loc, dy_loc, proj, d_y, m_block, e_loc, b_o, d_gq, d_gk, (d_wq, d_wk, d_wv, d_wo))
        d_e = all_sum_call(tp_size, d_mod.reshape(tp_size, -1, HEAD_DIM)).reshape(nb, 3, dim)
        return x_out, d_x, d_e, jnp.sum(d_e, axis=0), d_wq, d_wk, d_wv, d_wo, d_gq, d_gk

    in_specs = (P('dp', 'tp', None), P('dp', None, None), P(None, None), P(None, 'tp'), P('tp'), P(None, 'tp'), P('tp'),
                P(None, 'tp'), P('tp'), P('tp', None), P(None), P('tp'), P('tp'), P('dp', None), P('dp', 'tp', None))
    out_specs = (P('dp', 'tp', None), P('dp', 'tp', None), P('dp', None, None), P('dp', None), P('dp', 'tp'), P('dp', 'tp'),
                 P('dp', 'tp'), P(('dp', 'tp'), None), P(('dp', 'tp')), P(('dp', 'tp')))
    return jax.shard_map(device_step, mesh=mesh, in_specs=in_specs, out_specs=out_specs, check_vma=False)
```

```python
import functools

import jax
import jax.numpy as jnp
import numpy as np
from jax import lax
from jax.experimental import pallas as pl
from jax.experimental.pallas import tpu as pltpu
from jax.sharding import PartitionSpec as P

HEAD_DIM = 128
EPS_NORM = 1e-6
ROPE_BASE = 10000.0
LOG2E = 1.4426950408889634
CHUNK = 512
VMEM_LIMIT = 60 * 1024 * 1024
F32 = jnp.float32
BF16 = jnp.bfloat16
MESH_ID = pl.DeviceIdType.MESH
NT = (((1,), (1,)), ((), ()))
TN = (((0,), (0,)), ((), ()))


def params(*semantics, **kw):
    return pltpu.CompilerParams(dimension_semantics=semantics or None, vmem_limit_bytes=VMEM_LIMIT, **kw)


def cost(flops, nbytes):
    return pl.CostEstimate(flops=int(flops), bytes_accessed=int(nbytes), transcendentals=0)


def rope_freqs():
    half_dim = HEAD_DIM // 2
    side_len = HEAD_DIM // 6
    first_len = half_dim - 2 * side_len
    pair_idx = np.arange(HEAD_DIM) // 2
    section = (pair_idx >= first_len).astype(np.int32) + (pair_idx >= first_len + side_len).astype(np.int32)
    offset = np.where(section == 0, 0, np.where(section == 1, first_len, first_len + side_len))
    sec_width = np.where(section == 0, first_len, side_len)
    exponent = -(pair_idx - offset).astype(np.float32) / sec_width.astype(np.float32)
    freq_vals = np.power(np.float32(ROPE_BASE), exponent)
    return np.where(section[None, :] == np.arange(3)[:, None], freq_vals[None, :], np.float32(0.0)).astype(np.float32)


def norm_stats(x):
    centered = x - jnp.mean(x, axis=-1, keepdims=True)
    inv_std = lax.rsqrt(jnp.mean(centered * centered, axis=-1, keepdims=True) + EPS_NORM)
    return centered * inv_std, inv_std


def to_row(acc):
    return jnp.sum(acc.T, axis=0, keepdims=True)


def lanes_of(row):
    return jnp.broadcast_to(row, (HEAD_DIM, row.shape[1])).T


def head_sum(values):
    out = values[:, :HEAD_DIM]
    for h in range(1, values.shape[1] // HEAD_DIM):
        out = out + values[:, h * HEAD_DIM:(h + 1) * HEAD_DIM]
    return out


class Place:
    def __init__(self, n):
        self.n = n
        self.me = lax.axis_index('tp')
        self.right = lax.rem(self.me + 2, n)
        self.left = lax.rem(self.me + n - 2, n)
        self.far = lax.rem(self.me + n // 2, n)
        self.chip = self.me // 2

    def partner(self, dev):
        return dev + 1 - 2 * lax.rem(dev, 2)

    def arrive(self, devices):
        for dev in devices:
            pl.semaphore_signal(pltpu.get_barrier_semaphore(), inc=1, device_id={'tp': dev}, device_id_type=MESH_ID)

    def barrier(self, devices):
        self.arrive(devices)
        pl.semaphore_wait(pltpu.get_barrier_semaphore(), len(devices))

    def to_partner(self, src, dst, send_sem, recv_sem):
        return pltpu.make_async_remote_copy(src_ref=src, dst_ref=dst, send_sem=send_sem, recv_sem=recv_sem,
                                            device_id={'tp': self.partner(self.me)}, device_id_type=MESH_ID)

    def everyone(self):
        return [lax.rem(self.me + d, self.n) for d in range(1, self.n)]

    def near(self):
        return [self.right, self.left, self.partner(self.me)]


class Gather:
    def __init__(self, place, full, rows, send, recv, early=0):
        self.at, self.full, self.rows, self.send, self.recv, self.early = place, full, rows, send, recv, early

    def part(self, b, dev, off, count):
        return self.full.at[b, pl.ds(pl.multiple_of(dev * self.rows + off, 16), count)]

    def copy(self, b, dev, off, count, s_idx, r_idx, target):
        ref = self.part(b, dev, off, count)
        return pltpu.make_async_remote_copy(src_ref=ref, dst_ref=ref, send_sem=self.send.at[b, s_idx], recv_sem=self.recv.at[b, r_idx],
                                            device_id={'tp': target}, device_id_type=MESH_ID)

    def start_own(self, b):
        p = self.at
        self.copy(b, p.me, 0, self.rows, 0, 0, p.right).start()
        self.copy(b, p.me, 0, self.rows, 1, 1, p.left).start()
        self.copy(b, p.me, 0, self.rows, 2, 4, p.partner(p.me)).start()

    def whole_blocks_in(self, b):
        p = self.at
        self.copy(b, p.partner(p.me), 0, self.rows, 2, 4, p.me).wait_recv()
        self.copy(b, p.left, 0, self.rows, 0, 0, p.me).wait_recv()
        self.copy(b, p.right, 0, self.rows, 1, 1, p.me).wait_recv()
        for s_idx in range(3):
            self.copy(b, p.me, 0, self.rows, s_idx, s_idx, p.me).wait_send()

    def pass_left(self, b):
        p, half = self.at, self.rows // 2
        self.copy(b, p.left, 0, half, 3, 2, p.right).start()
        self.copy(b, p.left, 0, self.rows, 5, 5, p.partner(p.me)).start()

    def pass_right(self, b):
        p, half = self.at, self.rows // 2
        self.copy(b, p.right, half, half, 4, 3, p.left).start()
        self.copy(b, p.right, 0, self.rows, 6, 6, p.partner(p.me)).start()

    def finish(self, b):
        p, half = self.at, self.rows // 2
        counts = (self.rows, self.rows, self.rows, half, half, self.rows, self.rows, half, half)
        for s_idx, count in list(enumerate(counts))[3 if b < self.early else 0:]:
            self.copy(b, p.me, 0, count, s_idx, s_idx, p.me).wait_send()

    def item_place(self, i, nb):
        j = i - nb
        b = jnp.where(i < nb, i, jnp.where(i < 3 * nb, j // 2, i - 3 * nb))
        chips = self.at.n // 2
        side = jnp.where(lax.rem(j + 2 * nb, 2) == 0, chips - 1, 1)
        off = jnp.where(i < nb, 0, jnp.where(i < 3 * nb, side, chips // 2))
        return b, pl.multiple_of(lax.rem(self.at.chip + off, chips) * (2 * self.rows), 32)

    def kinds(self, i, nb):
        odd = lax.rem(i + nb, 2)
        side = (i >= nb) & (i < 3 * nb)
        return i < nb, side & (odd == 0), side & (odd == 1), i >= 3 * nb

    def arrive(self, i, nb):
        p, half = self.at, self.rows // 2
        b, _ = self.item_place(i, nb)
        _, is_left, is_right, is_far = self.kinds(i, nb)

        @pl.when(is_left & (b >= self.early))
        def _():
            self.copy(b, p.left, 0, self.rows, 0, 0, p.me).wait_recv()
            self.pass_left(b)

        @pl.when(is_right & (b >= self.early))
        def _():
            self.copy(b, p.right, 0, self.rows, 1, 1, p.me).wait_recv()
            self.pass_right(b)

        @pl.when(is_far)
        def _():
            self.copy(b, p.far, 0, half, 3, 2, p.me).wait_recv()
            self.copy(b, p.far, 0, half, 7, 7, p.partner(p.me)).start()
            self.copy(b, p.far, half, half, 4, 3, p.me).wait_recv()
            self.copy(b, p.far, half, half, 8, 8, p.partner(p.me)).start()

    def ready(self, i, nb):
        p, half = self.at, self.rows // 2
        b, row0 = self.item_place(i, nb)
        is_own, is_left, is_right, is_far = self.kinds(i, nb)

        @pl.when(is_own & (b >= self.early))
        def _():
            self.copy(b, p.partner(p.me), 0, self.rows, 2, 4, p.me).wait_recv()

        @pl.when(is_left)
        def _():
            self.copy(b, p.partner(p.left), 0, self.rows, 5, 5, p.me).wait_recv()

        @pl.when(is_right)
        def _():
            self.copy(b, p.partner(p.right), 0, self.rows, 6, 6, p.me).wait_recv()

        @pl.when(is_far)
        def _():
            self.copy(b, p.partner(p.far), 0, half, 7, 7, p.me).wait_recv()
            self.copy(b, p.partner(p.far), half, half, 8, 8, p.me).wait_recv()

        return b, row0


class RowTrade:
    def __init__(self, place, src, dst, rows, send, recv, rows_of=None):
        self.at, self.src, self.dst, self.rows, self.send, self.recv = place, src, dst, rows, send, recv
        self.batch = range(src.shape[0]) if rows_of is None else rows_of

    def copies(self, parity):
        p = self.at
        for b in self.batch:
            for k in range(p.n // 2):
                sl = pl.ds(pl.multiple_of((2 * k + parity) * self.rows, 16), self.rows)
                yield p.to_partner(self.src.at[b, sl], self.dst.at[b, sl], self.send.at[b, k], self.recv.at[b, k])

    def start(self):
        for c in self.copies(1 - lax.rem(self.at.me, 2)):
            c.start()

    def wait_recv(self):
        for c in self.copies(lax.rem(self.at.me, 2)):
            c.wait_recv()

    def wait_send(self):
        for c in self.copies(1 - lax.rem(self.at.me, 2)):
            c.wait_send()


GATHER_SEMS = 9
EARLY_ROWS = 1
EARLY_CHUNKS = 3
EARLY_DY = 4


def chunks_of(width, step):
    return [(c, min(c + step, width)) for c in range(0, width, step)]


class Exchange:
    def __init__(self, place, x_ref, slots, send_sems, recv_sems):
        self.at, self.x, self.slots, self.send, self.recv = place, x_ref, slots, send_sems, recv_sems

    def copy(self, d, dev, src):
        return pltpu.make_async_remote_copy(src_ref=self.x, dst_ref=self.slots.at[src], send_sem=self.send.at[d], recv_sem=self.recv.at[src],
                                            device_id={'tp': dev}, device_id_type=MESH_ID)

    def start(self):
        for d, dev in enumerate(self.at.everyone()):
            self.copy(d, dev, self.at.me).start()
        self.slots[self.at.me] = self.x[...]

    def finish(self):
        for d, dev in enumerate(self.at.everyone()):
            self.copy(d, dev, dev).wait()
        total = self.slots[0]
        for d in range(1, self.at.n):
            total = total + self.slots[d]
        return total


def gather_qkv_kernel(n, x_ref, dy_ref, m_ref, e_ref, wq_ref, wk_ref, wv_ref, wo_ref, bq_ref, bk_ref, bv_ref, gq_ref, gk_ref, pos_ref,
                      freq_ref, y_full, d_full, q_out, k_out, v_out, wo_p, wo_t, ss_ref, cos_ref, sin_ref, gain_ref,
                      bias_ref, w_all, xin, stage, xbuf, zst, vst, sq, ss_row, slots, wo_in, wo_st, wo_sem,
                      w_sem, in_sem, st_sem, ld_sem, out_sem, g_send, g_recv, d_send, d_recv, e_send, e_recv, t_send, t_recv):
    nb, rows, dim = x_ref.shape
    cols = wq_ref.shape[1]
    place = Place(n)
    gather = Gather(place, y_full, rows, g_send, g_recv)
    gather_d = Gather(place, d_full, rows, d_send, d_recv)
    w_copies = [pltpu.make_async_copy(w, w_all.at[:, pl.ds(j * cols, cols)], w_sem.at[j]) for j, w in enumerate((wq_ref, wk_ref, wv_ref))]
    place.arrive(place.everyone())
    trade = place.to_partner(wo_ref, wo_p, t_send, t_recv)

    def load_x(b):
        return pltpu.make_async_copy(x_ref.at[b], xin.at[b], in_sem.at[b])

    for b in range(nb):
        load_x(b).start()
    for c in w_copies:
        c.start()
    group = 16

    def mine(full, b):
        return full.at[b, pl.ds(pl.multiple_of(place.me * rows, 16), rows)]

    def ln_step(b, _):
        load_x(b).wait()
        shift = m_ref[0:1] + e_ref[b, 0:1]
        scale_one = 1.0 + (m_ref[1:2] + e_ref[b, 1:2])

        def ln_rows(r, _):
            sl = pl.ds(pl.multiple_of(r * group, group), group)
            x_norm, _ = norm_stats(xin[b, sl].astype(F32))
            stage[b, sl] = (x_norm * scale_one + shift).astype(BF16)
            return 0

        lax.fori_loop(0, rows // group, ln_rows, 0)
        out = pltpu.make_async_copy(stage.at[b], mine(y_full, b), st_sem)
        out.start()

        @pl.when(b == 0)
        def _():
            pl.semaphore_wait(pltpu.get_barrier_semaphore(), n - 1)

        out.wait()
        gather.start_own(b)
        return 0

    lax.fori_loop(0, nb, ln_step, 0)
    load_dy = pltpu.make_async_copy(dy_ref, xin, in_sem.at[0])
    load_dy.start()
    for j, ref in enumerate((bq_ref, bk_ref, bv_ref)):
        bias_ref[:, j * cols:(j + 1) * cols] = ref[...].reshape(1, cols)
    for j, ref in enumerate((gq_ref, gk_ref)):
        gain_ref[j:j + 1] = ref[...].reshape(1, cols)

    def tables():
        lane = lax.broadcasted_iota(jnp.int32, (128, HEAD_DIM), 1)

        def rows_of(r, _):
            sl = pl.ds(pl.multiple_of(r * 128, 128), 128)
            pos = [lanes_of(pos_ref[m:m + 1, sl].astype(F32)) for m in range(3)]
            angle = pos[0] * freq_ref[0:1] + pos[1] * freq_ref[1:2] + pos[2] * freq_ref[2:3]
            cos_ref[sl] = jnp.cos(angle)
            sin_ref[sl] = jnp.where(lane % 2 == 0, -1.0, 1.0) * jnp.sin(angle)
            return 0

        lax.fori_loop(0, pos_ref.shape[1] // 128, rows_of, 0)

    def turn_wo():
        width = wo_in.shape[2]
        n_chunks = dim // width

        def load(c):
            slot = lax.rem(c, 2)
            return pltpu.make_async_copy(wo_ref.at[:, pl.ds(pl.multiple_of(c * width, width), width)], wo_in.at[slot], wo_sem.at[slot, 0])

        def store(c):
            slot = lax.rem(c, 2)
            return pltpu.make_async_copy(wo_st.at[slot], wo_t.at[pl.ds(pl.multiple_of(c * width, width), width)], wo_sem.at[slot, 1])

        load(0).start()

        def body(c, _):
            slot = lax.rem(c, 2)

            @pl.when(c + 1 < n_chunks)
            def _():
                load(c + 1).start()

            @pl.when(c >= 2)
            def _():
                store(c).wait()

            load(c).wait()
            wo_st[slot] = wo_in[slot].T
            store(c).start()
            return 0

        lax.fori_loop(0, n_chunks, body, 0)
        for c in range(min(2, n_chunks)):
            store(c).wait()

    def gate_step(b, _):
        gate = m_ref[2:3] + e_ref[b, 2:3]

        def gate_rows(r, _):
            sl = pl.ds(pl.multiple_of(r * group, group), group)
            stage[b, sl] = (xin[b, sl].astype(F32) * gate).astype(BF16)
            return 0

        lax.fori_loop(0, rows // group, gate_rows, 0)
        out = pltpu.make_async_copy(stage.at[b], mine(d_full, b), st_sem)
        out.start()
        out.wait()
        return 0

    for c in w_copies:
        c.wait()

    def outputs(b, row0, slot):
        dst = pl.ds(row0, 2 * rows)
        return [pltpu.make_async_copy(zst.at[slot, :, pl.ds(0, cols)], q_out.at[b, dst], out_sem.at[slot, 0]),
                pltpu.make_async_copy(zst.at[slot, :, pl.ds(cols, cols)], k_out.at[b, dst], out_sem.at[slot, 1]),
                pltpu.make_async_copy(vst.at[slot], v_out.at[b, dst], out_sem.at[slot, 2])]

    def load(b, row0, slot):
        return pltpu.make_async_copy(y_full.at[b, pl.ds(row0, 2 * rows)], xbuf.at[slot], ld_sem.at[slot])

    load(*gather.ready(0, nb), 0).start()

    def item(i, _):
        slot = lax.rem(i, 2)
        b, row0 = gather.item_place(i, nb)

        @pl.when(i + 1 < 4 * nb)
        def _():
            gather.arrive(i + 1, nb)

        @pl.when(i + 1 == 3 * nb - 1)
        def _():
            for d in range(EARLY_ROWS):
                gather_d.start_own(d)

        @pl.when(i == nb)
        def _():
            load_dy.wait()
            trade.start()
            lax.fori_loop(0, nb, gate_step, 0)
            tables()
            turn_wo()

        @pl.when(i >= 2)
        def _():
            for c in outputs(0, 0, slot):
                c.wait()

        load(0, 0, slot).wait()
        spans = chunks_of(3 * cols, 512)
        for m, (lo, hi) in enumerate(spans):
            if m == len(spans) - 1:
                @pl.when(i + 1 < 4 * nb)
                def _():
                    load(*gather.ready(i + 1, nb), lax.rem(i + 1, 2)).start()

            zst[slot, :, lo:hi] = jnp.dot(xbuf[slot], w_all[:, lo:hi], preferred_element_type=F32) + bias_ref[:, lo:hi]
        vst[slot] = zst[slot, :, 2 * cols:].astype(BF16)
        q = zst[slot, :, :cols]
        k = zst[slot, :, cols:2 * cols]
        sq[2 * b, pl.ds(row0, 2 * rows)] = head_sum(q * q)
        sq[2 * b + 1, pl.ds(row0, 2 * rows)] = head_sum(k * k)
        for c in outputs(b, row0, slot):
            c.start()
        return 0

    lax.fori_loop(0, 4 * nb, item, 0)
    ss_row[...] = jnp.zeros_like(ss_row)
    for j in range(2 * nb):
        ss_row[j:j + 1] = to_row(sq[j])
    sums = Exchange(place, ss_row, slots, e_send, e_recv)
    sums.start()
    for slot in range(2):
        for c in outputs(0, 0, slot):
            c.wait()
    for b in range(nb):
        gather.finish(b)
    for d in range(EARLY_ROWS):
        gather_d.whole_blocks_in(d)
    trade.wait()
    ss_ref[...] = sums.finish()


def gather_qkv_call(n, x_loc, dy_loc, m_block, e_loc, w_q, w_k, w_v, w_o, b_q, b_k, b_v, g_q, g_k, positions):
    nb, rows, dim = x_loc.shape
    cols = w_q.shape[1]
    tokens = rows * n
    shape = jax.ShapeDtypeStruct
    any_spec = pl.BlockSpec(memory_space=pl.ANY)
    vmem = pl.BlockSpec(memory_space=pltpu.VMEM)
    dma = pltpu.SemaphoreType.DMA
    stat_rows = -(-2 * nb // 8) * 8
    return pl.pallas_call(
        functools.partial(gather_qkv_kernel, n), name="gather_qkv",
        out_shape=[shape((nb, tokens, dim), BF16), shape((nb, tokens, dim), BF16), shape((nb, tokens, cols), F32),
                   shape((nb, tokens, cols), F32), shape((nb, tokens, cols), BF16), shape(w_o.shape, BF16), shape((dim, cols), BF16), shape((stat_rows, tokens), F32),
                   shape((tokens, HEAD_DIM), F32), shape((tokens, HEAD_DIM), F32), shape((2, cols), F32)],
        in_specs=[any_spec, any_spec, vmem, vmem] + [any_spec] * 4 + [vmem] * 7,
        out_specs=[any_spec] * 7 + [vmem] * 4,
        scratch_shapes=[
            pltpu.VMEM((1, 3 * cols), F32),
            pltpu.VMEM((dim, 3 * cols), BF16), pltpu.VMEM((nb, rows, dim), BF16), pltpu.VMEM((nb, rows, dim), BF16),
            pltpu.VMEM((2, 2 * rows, dim), BF16), pltpu.VMEM((2, 2 * rows, 3 * cols), F32), pltpu.VMEM((2, 2 * rows, cols), BF16),
            pltpu.VMEM((2 * nb, tokens, HEAD_DIM), F32), pltpu.VMEM((stat_rows, tokens), F32), pltpu.VMEM((n, stat_rows, tokens), F32),
            pltpu.VMEM((2, cols, min(512, dim)), BF16), pltpu.VMEM((2, min(512, dim), cols), BF16), dma((2, 2)),
            dma((3,)), dma((nb,)), dma, dma((2,)), dma((2, 3)), dma((nb, GATHER_SEMS)), dma((nb, GATHER_SEMS)),
            dma((EARLY_ROWS, GATHER_SEMS)), dma((EARLY_ROWS, GATHER_SEMS)), dma((n,)), dma((n,)), dma, dma],
        compiler_params=params(collective_id=0, has_side_effects=True),
        cost_estimate=cost(6 * nb * tokens * dim * cols, 6 * dim * cols + 14 * nb * tokens * cols),
    )(x_loc, dy_loc, m_block, e_loc, w_q, w_k, w_v, w_o, b_q, b_k, b_v, g_q, g_k, positions.T, jnp.asarray(rope_freqs()))


def all_sum_kernel(n, x_ref, o_ref, pieces, total, send_a, recv_a, send_b, recv_b):
    place = Place(n)
    me = place.me
    place.barrier(place.everyone())

    def first(d, dev, src):
        return pltpu.make_async_remote_copy(src_ref=x_ref.at[src], dst_ref=pieces.at[me], send_sem=send_a.at[d], recv_sem=recv_a.at[me],
                                            device_id={'tp': dev}, device_id_type=MESH_ID)

    for d, dev in enumerate(place.everyone()):
        first(d, dev, dev).start()
    pieces[me] = x_ref[me]
    for d, dev in enumerate(place.everyone()):
        pltpu.make_async_remote_copy(src_ref=x_ref.at[me], dst_ref=pieces.at[dev], send_sem=send_a.at[d], recv_sem=recv_a.at[dev],
                                     device_id={'tp': dev}, device_id_type=MESH_ID).wait_recv()
    acc = pieces[0]
    for d in range(1, n):
        acc = acc + pieces[d]
    total[...] = acc
    o_ref[me] = acc
    for d, dev in enumerate(place.everyone()):
        first(d, dev, dev).wait_send()
    for d, dev in enumerate(place.everyone()):
        pltpu.make_async_remote_copy(src_ref=total, dst_ref=o_ref.at[me], send_sem=send_b.at[d], recv_sem=recv_b.at[me],
                                     device_id={'tp': dev}, device_id_type=MESH_ID).start()
    for d, dev in enumerate(place.everyone()):
        copy = pltpu.make_async_remote_copy(src_ref=total, dst_ref=o_ref.at[dev], send_sem=send_b.at[d], recv_sem=recv_b.at[dev],
                                            device_id={'tp': dev}, device_id_type=MESH_ID)
        copy.wait_send()
        copy.wait_recv()


def all_sum_call(n, x):
    spec = pl.BlockSpec(memory_space=pltpu.VMEM)
    dma = pltpu.SemaphoreType.DMA
    return pl.pallas_call(
        functools.partial(all_sum_kernel, n), name="all_sum",
        out_shape=jax.ShapeDtypeStruct(x.shape, x.dtype), in_specs=[spec], out_specs=spec,
        scratch_shapes=[pltpu.VMEM(x.shape, x.dtype), pltpu.VMEM(x.shape[1:], x.dtype), dma((n,)), dma((n,)), dma((n,)), dma((n,))],
        compiler_params=pltpu.CompilerParams(collective_id=4, has_side_effects=True, vmem_limit_bytes=4 * 1024 * 1024),
        cost_estimate=cost(4_000_000_000, x.size * 8),
    )(x)


def swap_pairs(x):
    lane = lax.broadcasted_iota(jnp.int32, x.shape, 1)
    return jnp.where(lane % 2 == 0, pltpu.roll(x, HEAD_DIM - 1, 1), pltpu.roll(x, 1, 1))


def rotate(x, cos, sin):
    return x * cos + swap_pairs(x) * sin


SCORE_SCALE = HEAD_DIM ** -0.5 * LOG2E


def softmax_block(s):
    top = jnp.max(s, axis=1, keepdims=True)
    p = jnp.exp2(s * SCORE_SCALE - top * SCORE_SCALE)
    total = jnp.sum(p, axis=1, keepdims=True)
    return p * (1.0 / total), top * SCORE_SCALE + jnp.log(total) * LOG2E


class Scatter:
    def __init__(self, place, part, recv_far, recv_side, send, recv, far_src=None, early=0):
        self.at, self.part, self.far, self.side, self.send, self.recv = place, part, recv_far, recv_side, send, recv
        self.far_src, self.early = part if far_src is None else far_src, early
        self.rows = part.shape[2]
        self.half = self.rows // 2

    def copy(self, j, idx, src, dst, target):
        return pltpu.make_async_remote_copy(src_ref=src, dst_ref=dst, send_sem=self.send.at[j, idx], recv_sem=self.recv.at[j, idx],
                                            device_id={'tp': target}, device_id_type=MESH_ID)

    def message(self, j, idx):
        p, part, far, side = self.at, self.part, self.far, self.side
        first, second = pl.ds(0, self.half), pl.ds(self.half, self.rows - self.half)
        src, dst, target = (
            lambda: (self.far_src.at[j, 0, first], far.at[j, 0], p.right),
            lambda: (self.far_src.at[j, 0, second], far.at[j, 1], p.left),
            lambda: (part.at[j, 1, second], side.at[j, 0, second], p.right),
            lambda: (part.at[j, 2, first], side.at[j, 1, first], p.left),
            lambda: (part.at[j, 1, first], side.at[j, 0, first], p.right),
            lambda: (part.at[j, 2, second], side.at[j, 1, second], p.left))[idx]()
        return self.copy(j, idx, src, dst, target)

    def start_far(self, j, _=0):
        for idx in (0, 1):
            self.message(j, idx).start()
        return 0

    def start_side(self, j, _):
        for idx in (2, 3):
            self.message(j, idx).start()
        return 0

    def sums(self, j):
        h = self.half

        @pl.when(j >= self.early)
        def _():
            self.message(j, 0).wait_recv()
            self.message(j, 1).wait_recv()

        self.part[j, 1, :h] = (self.part[j, 1, :h].astype(F32) + self.far[j, 0].astype(F32)).astype(BF16)
        self.part[j, 2, h:] = (self.part[j, 2, h:].astype(F32) + self.far[j, 1].astype(F32)).astype(BF16)
        self.message(j, 4).start()
        self.message(j, 5).start()

    def sums_step(self, j, _):
        self.sums(j)
        return 0

    def final(self, j):
        for idx in range(2, 6):
            self.message(j, idx).wait_recv()
        total = self.part[j, 3].astype(F32) + self.side[j, 0].astype(F32) + self.side[j, 1].astype(F32)
        self.part[j, 3] = total.astype(BF16)

    def finish(self, j):
        @pl.when(j >= self.early)
        def _():
            for idx in range(2):
                self.message(j, idx).wait_send()

        for idx in range(2, 6):
            self.message(j, idx).wait_send()

    @staticmethod
    def scratch(rows, dim):
        nc, dma = dim // CHUNK, pltpu.SemaphoreType.DMA
        return [pltpu.VMEM((nc, 4, rows, CHUNK), BF16), pltpu.VMEM((nc, 2, rows // 2, CHUNK), BF16),
                pltpu.VMEM((nc, 2, rows, CHUNK), BF16), dma((nc, 6)), dma((nc, 6))]


def scatter_outputs(part, out, sem, j):
    nb, rows, _ = out.shape
    cs = pl.ds(pl.multiple_of(j * CHUNK, CHUNK), CHUNK)
    return [pltpu.make_async_copy(part.at[j, 3, pl.ds(b * rows, rows)], out.at[b, :, cs], sem.at[b]) for b in range(nb)]


def scatter_end(scatter, out, sem, nc):
    def last(j, _):
        scatter.final(j)
        for c in scatter_outputs(scatter.part, out, sem, j):
            c.start()
        return 0

    lax.fori_loop(0, nc, last, 0)

    def drain(j, _):
        for c in scatter_outputs(scatter.part, out, sem, j):
            c.wait()
        scatter.finish(j)
        return 0

    lax.fori_loop(0, nc, drain, 0)


def pair_rows(place, nb, rows, mine, theirs, lhs, sem):
    width = mine.shape[2]
    out = []
    for d, dev in enumerate((place.far, place.right, place.left, place.me)):
        src_rows = pl.ds(pl.multiple_of(dev * rows, 16), rows)
        for b in range(nb):
            dst_rows = pl.ds((d * nb + b) * rows, rows)
            for j, src in enumerate((mine, theirs)):
                out.append(pltpu.make_async_copy(src.at[b, src_rows], lhs.at[dst_rows, pl.ds(j * width, width)], sem.at[d // 2]))
    return out


def gather_attn_kernel(n, nb, heads, dim, q_ref, k_ref, v_ref, gain_ref, cos_ref, sin_ref, ss_ref,
                       wq_ref, wo_ref, wo_p, wo_t, d_in,
                       d_full, o_out, o_p, da_out, wq_p, part_out, far_in, dwo_part, qr_ref, kr_ref, lse_ref, o32_ref,
                       inv_q, inv_k, o_all, wo, xbuf, ast,
                       w_sem, ld_sem, out_sem, o_sem, p_sem, l_sem, g_send, g_recv, t_send, t_recv, r_send, r_recv, s_send, s_recv):
    step = pl.program_id(0)
    tokens = q_ref.shape[1]
    rows = tokens // n
    blk = min(384, tokens)
    place = Place(n)
    gather = Gather(place, d_full, rows, g_send, g_recv, early=EARLY_ROWS)
    cols = heads * HEAD_DIM
    nc = dim // CHUNK
    early_chunks = min(EARLY_CHUNKS, nc)
    mid = nc // 2
    scatter = Scatter(place, part_out, far_in, None, s_send, s_recv)
    trade_o = RowTrade(place, o_out, o_p, rows, r_send, r_recv)

    def trade_w():
        return place.to_partner(wq_ref, wq_p, t_send, t_recv)


    @pl.when(step == 0)
    def _():
        pltpu.make_async_copy(wo_t, wo, w_sem).start()
        place.barrier(place.near())

        for b in range(EARLY_ROWS):
            gather.pass_left(b)
            gather.pass_right(b)

        def own(b, _):
            gather.start_own(b)
            return 0

        lax.fori_loop(EARLY_ROWS, nb, own, 0)
        trade_w().start()

    @pl.when(step < nb * heads)
    def _():
        b = step // heads
        h = lax.rem(step, heads)

        @pl.when(h == 0)
        def _():
            inv_q[...] = lanes_of(lax.rsqrt(ss_ref[pl.ds(2 * b, 1)] / dim + EPS_NORM))
            inv_k[...] = lanes_of(lax.rsqrt(ss_ref[pl.ds(2 * b + 1, 1)] / dim + EPS_NORM))

        cos, sin = cos_ref[...], sin_ref[...]
        q_rot = rotate(q_ref[0] * inv_q[...] * gain_ref[0:1], cos, sin).astype(BF16)
        k_rot = rotate(k_ref[0] * inv_k[...] * gain_ref[1:2], cos, sin).astype(BF16)
        v = v_ref[0]
        lanes = pl.ds(pl.multiple_of(h * HEAD_DIM, HEAD_DIM), HEAD_DIM)
        qr_ref[0], kr_ref[0] = q_rot, k_rot

        def scores(i):
            return lax.dot_general(q_rot[i * blk:(i + 1) * blk], k_rot, NT, preferred_element_type=F32)

        ahead = scores(0)
        for i in range(tokens // blk):
            s = ahead
            if (i + 1) * blk < tokens:
                ahead = scores(i + 1)
            p, lse = softmax_block(s)
            lse_ref[0, i * blk:(i + 1) * blk] = jnp.broadcast_to(lse, (blk, HEAD_DIM))
            o = jnp.dot(p.astype(BF16), v, preferred_element_type=F32)
            o32_ref[0, i * blk:(i + 1) * blk] = o
            o_all[b, i * blk:(i + 1) * blk, lanes] = o.astype(BF16)

    @pl.when(step == nb * heads)
    def _():
        o_copy = pltpu.make_async_copy(o_all, o_out, o_sem)
        o_copy.start()
        pltpu.make_async_copy(wo_t, wo, w_sem).wait()

        def outputs(b, row0, slot):
            return pltpu.make_async_copy(ast.at[slot], da_out.at[b, pl.ds(row0, 2 * rows)], out_sem.at[slot])

        def load(b, row0, slot):
            return pltpu.make_async_copy(d_full.at[b, pl.ds(row0, 2 * rows)], xbuf.at[slot], ld_sem.at[slot])

        def project(lhs, wbuf, stage):
            loads = pair_rows(place, nb, rows, o_out, o_p, lhs, l_sem)
            for c in loads:
                c.start()

            def chunk(j):
                cs = pl.ds(pl.multiple_of(j * CHUNK, CHUNK), CHUNK)
                slot = lax.rem(j, 2)
                return [pltpu.make_async_copy(wo_ref.at[:, cs], wbuf.at[slot, pl.ds(0, cols)], p_sem.at[slot, 0]),
                        pltpu.make_async_copy(wo_p.at[:, cs], wbuf.at[slot, pl.ds(cols, cols)], p_sem.at[slot, 1])]

            def store(j):
                slot = lax.rem(j, 2)
                return pltpu.make_async_copy(stage.at[slot], part_out.at[j], p_sem.at[slot, 2])

            def stored(j):
                store(j).wait()

                @pl.when((j < early_chunks) & (j >= mid))
                def _():
                    scatter.start_far(j)

            for c in chunk(0):
                c.start()
            for c in loads:
                c.wait()

            def body(j, _):
                slot = lax.rem(j, 2)

                @pl.when(j + 1 < nc)
                def _():
                    for c in chunk(j + 1):
                        c.start()

                for c in chunk(j):
                    c.wait()
                half = 2 * nb * rows
                for d in range(2):
                    z = jnp.dot(lhs[d * half:(d + 1) * half], wbuf[slot], preferred_element_type=F32).astype(BF16)
                    stage[slot, 2 * d] = z[:half // 2]
                    stage[slot, 2 * d + 1] = z[half // 2:]
                store(j).start()

                @pl.when(j >= 1)
                def _():
                    stored(j - 1)

                @pl.when(j == mid)
                def _():
                    gather.arrive(3 * nb - 2, nb)
                    gather.arrive(3 * nb - 1, nb)
                    lax.fori_loop(0, min(early_chunks, mid), scatter.start_far, 0)

                return 0

            lax.fori_loop(0, nc, body, 0)
            stored(nc - 1)

        def first_dwo(turned, dbuf, fst):
            bn = min(512, dim)
            n_chunks = dim // bn

            def chunk(c):
                slot = lax.rem(c, 2)
                cs = pl.ds(pl.multiple_of(c * bn, bn), bn)
                return pltpu.make_async_copy(d_full.at[pl.ds(0, nb - 1), :, cs], dbuf.at[slot], p_sem.at[slot, 0])

            def store(c):
                slot = lax.rem(c, 2)
                return pltpu.make_async_copy(fst.at[slot], dwo_part.at[:, pl.ds(pl.multiple_of(c * bn, bn), bn)], p_sem.at[slot, 1])

            chunk(0).start()
            for b in range(nb - 1):
                turned[:, b * tokens:(b + 1) * tokens] = o_all[b].T

            def body(c, _):
                slot = lax.rem(c, 2)

                @pl.when(c + 1 < n_chunks)
                def _():
                    chunk(c + 1).start()

                @pl.when(c == n_chunks // 2)
                def _():
                    gather.arrive(4 * nb - 1, nb)

                @pl.when(c >= 2)
                def _():
                    store(c).wait()

                chunk(c).wait()
                fst[slot] = jnp.dot(turned[...], dbuf[slot].reshape((nb - 1) * tokens, bn), preferred_element_type=F32)
                store(c).start()
                return 0

            lax.fori_loop(0, n_chunks, body, 0)
            for c in range(min(2, n_chunks)):
                store(c).wait()

        def fetch(i):
            b, row0 = gather.ready(i, nb)
            load(b, row0, lax.rem(i, 2)).start()

        fetch(0)
        gather.arrive(jnp.int32(1), nb)

        def item(i, _):
            slot = lax.rem(i, 2)

            @pl.when((i + 2 != 3 * nb - 2) & (i + 2 != 3 * nb - 1) & (i + 2 < 4 * nb - 1))
            def _():
                gather.arrive(i + 2, nb)

            @pl.when((i + 1 != 3 * nb - 2) & (i + 1 < 4 * nb - 1))
            def _():
                fetch(i + 1)

            @pl.when(i >= 2)
            def _():
                outputs(0, 0, slot).wait()

            load(0, 0, slot).wait()
            ast[slot] = jnp.dot(xbuf[slot], wo[...], preferred_element_type=F32).astype(BF16)
            b, row0 = gather.item_place(i, nb)
            outputs(b, row0, slot).start()

            @pl.when(i == 0)
            def _():
                o_copy.wait()
                trade_o.start()

            @pl.when(i + 1 == 3 * nb - 2)
            def _():
                trade_o.wait_recv()
                pl.run_scoped(project, pltpu.VMEM((4 * nb * rows, 2 * cols), BF16), pltpu.VMEM((2, 2 * cols, CHUNK), BF16),
                              pltpu.VMEM((2, 4, nb * rows, CHUNK), BF16))
                fetch(i + 1)

            @pl.when(i + 1 == 4 * nb - 1)
            def _():
                bn = min(512, dim)
                pl.run_scoped(first_dwo, pltpu.VMEM((cols, (nb - 1) * tokens), BF16), pltpu.VMEM((2, nb - 1, tokens, bn), BF16),
                              pltpu.VMEM((2, cols, bn), F32))
                fetch(i + 1)

            return 0

        lax.fori_loop(0, 4 * nb, item, 0)
        for slot in range(2):
            outputs(0, 0, slot).wait()
        for b in range(nb):
            gather.finish(b)
        trade_o.wait_send()
        trade_w().wait()
        for j in range(early_chunks):
            for idx in (0, 1):
                scatter.message(j, idx).wait()


def gather_attn_call(n, q, k, v, gains, cos_tab, sin_tab, ss, w_q, w_o, wo_p, wo_t, d_full):
    nb, tokens, cols = q.shape
    dim = w_o.shape[1]
    heads = cols // HEAD_DIM
    rows = tokens // n
    last = nb * heads - 1
    nc = dim // CHUNK
    early = min(EARLY_CHUNKS, nc)
    shape = jax.ShapeDtypeStruct
    dma = pltpu.SemaphoreType.DMA
    any_spec = pl.BlockSpec(memory_space=pl.ANY)

    def head_of(i):
        i = jnp.minimum(i, last)
        return i // heads, i % heads

    blk = pl.BlockSpec((1, tokens, HEAD_DIM), lambda i: (head_of(i)[0], 0, head_of(i)[1]))
    vec = pl.BlockSpec((2, HEAD_DIM), lambda i: (0, head_of(i)[1]))
    tab = pl.BlockSpec((tokens, HEAD_DIM), lambda i: (0, 0))
    head_arr = shape((nb, tokens, cols), BF16)
    return pl.pallas_call(
        functools.partial(gather_attn_kernel, n, nb, heads, dim), name="gather_attn", grid=(nb * heads + 1,),
        out_shape=[shape(d_full.shape, BF16), head_arr, head_arr, head_arr, shape(w_q.shape, BF16)]
        + [shape((nc, 4, nb * rows, CHUNK), BF16), shape((early, 2, nb * rows // 2, CHUNK), BF16), shape((cols, dim), F32), head_arr, head_arr,
           shape((nb, tokens, cols), F32), shape((nb, tokens, cols), F32)],
        in_specs=[blk, blk, blk, vec, tab, tab, pl.BlockSpec(ss.shape, lambda i: (0, 0))] + [any_spec] * 5,
        out_specs=[any_spec] * 8 + [blk] * 4,
        scratch_shapes=[
            pltpu.VMEM((tokens, HEAD_DIM), F32), pltpu.VMEM((tokens, HEAD_DIM), F32), pltpu.VMEM((nb, tokens, cols), BF16),
            pltpu.VMEM((dim, cols), BF16), pltpu.VMEM((2, 2 * rows, dim), BF16), pltpu.VMEM((2, 2 * rows, cols), BF16),
            dma, dma((2,)), dma((2,)), dma, dma((2, 3)), dma((2,)), dma((nb, GATHER_SEMS)), dma((nb, GATHER_SEMS)), dma, dma,
            dma((nb, n // 2)), dma((nb, n // 2)), dma((early, 6)), dma((early, 6))],
        input_output_aliases={11: 0},
        compiler_params=params("arbitrary", collective_id=1, has_side_effects=True),
        cost_estimate=cost(4 * nb * tokens * dim * cols + 4 * nb * tokens * tokens * cols, 8 * nb * tokens * dim),
    )(q, k, v, gains, cos_tab, sin_tab, ss, w_q, w_o, wo_p, wo_t, d_full)


class DyChunks:
    def __init__(self, lhs, wbuf, weights, w_sem):
        self.lhs, self.wbuf, self.weights, self.sem = lhs, wbuf, weights, w_sem

    def loads(self, j):
        slot = lax.rem(j, 2)
        src = pl.ds(pl.multiple_of(j * CHUNK, CHUNK), CHUNK)
        width = self.weights[0].shape[1]
        return [pltpu.make_async_copy(w.at[src], self.wbuf.at[slot, :, pl.ds(m * width, width)], self.sem.at[slot, m])
                for m, w in enumerate(self.weights)]

    def dot(self, j, d):
        half = self.lhs.shape[0] // 2
        return lax.dot_general(self.lhs[d * half:(d + 1) * half], self.wbuf[lax.rem(j, 2)], NT, preferred_element_type=F32).astype(BF16)


def attn_bwd_kernel(n, nb, heads, dim, q_ref, k_ref, qr_ref, kr_ref, v_ref, do_ref, o_ref, lse_ref, gain_ref, cos_ref, sin_ref, ss_ref,
                    q_hbm, k_hbm, o_hbm, part_in, far_in, d_full, dwo_part, wq_hbm, wk_hbm, wv_hbm, wq_p,
                    proj_out, g_out, g_p, dqs_out, dks_out, dwo_out, wk_p, wv_p, part_dy, far_dy, dgq_ref, dgk_ref,
                    part, recv_far, recv_side, s_send, s_recv,
                    inv_q, inv_k, acc_q, acc_k, p_all, ds_all, dq_all, qs_st, ks_st, v_st, st_row, st_sum, slots, fbuf, gbuf, lanes_s,
                    ld_sem, w_sem, fl_sem, g_sem, go_sem, out_sem, e_send, e_recv, t_send, t_recv, r_send, r_recv, c_sem, y_send, y_recv):
    step = pl.program_id(0)
    tokens = q_ref.shape[1]
    rows = tokens // n
    cols = heads * HEAD_DIM
    blk = min(256, tokens)
    nc = dim // CHUNK
    steps = nb * heads
    scale = HEAD_DIM ** -0.5
    place = Place(n)
    early = far_in.shape[0]
    scatter = Scatter(place, part, recv_far, recv_side, s_send, s_recv, far_src=part_in, early=early)

    def stored():
        return [pltpu.make_async_copy(part_in, part, ld_sem.at[0]),
                pltpu.make_async_copy(far_in, recv_far.at[pl.ds(0, early)], ld_sem.at[1])]

    n_pieces = 8

    def trade_w(j):
        m = j % (n_pieces // 2)
        size = dim // (n_pieces // 2)
        src, dst = ((wk_hbm, wk_p), (wv_hbm, wv_p))[j // (n_pieces // 2)]
        return place.to_partner(src.at[pl.ds(m * size, size)], dst.at[pl.ds(m * size, size)], t_send.at[j], t_recv.at[j])


    @pl.when(step == 0)
    def _():
        place.barrier(place.everyone())
        for c in stored():
            c.start()

    @pl.when(step == 1)
    def _():
        for c in stored():
            c.wait()

    def flush(b, h, slot):
        lanes = pl.ds(pl.multiple_of(h * HEAD_DIM, HEAD_DIM), HEAD_DIM)
        v_lanes = pl.ds(pl.multiple_of(2 * cols + h * HEAD_DIM, HEAD_DIM), HEAD_DIM)
        return [pltpu.make_async_copy(qs_st.at[slot], dqs_out.at[b, :, lanes], fl_sem.at[slot, 0]),
                pltpu.make_async_copy(ks_st.at[slot], dks_out.at[b, :, lanes], fl_sem.at[slot, 1]),
                pltpu.make_async_copy(v_st.at[slot], g_out.at[b, :, v_lanes], fl_sem.at[slot, 2])]

    for j in range(n_pieces):
        pl.when(step == j * (steps - 1) // n_pieces + 1)(lambda j=j: trade_w(j).start())

    mid = early
    events = []
    late = list(range(mid))
    for m, j in enumerate(range(early, nc)):
        events.append(functools.partial(scatter.start_far, j))
        if m >= 2 and m % 2 == 0 and late:
            events.append(functools.partial(scatter.sums, late.pop(0)))
    events += [functools.partial(scatter.sums, j) for j in late]
    for m, event in enumerate(events):
        @pl.when(step == m * (steps - 1) // len(events))
        def _(event=event):
            event()

    rb = min(256, tokens)
    per = tokens // rb

    def stats(b):
        return Exchange(place, st_row.at[b], slots.at[b], e_send.at[b], e_recv.at[b])

    def grad_loads(b, i):
        r0 = pl.multiple_of(i * rb, rb)
        return [pltpu.make_async_copy(src.at[b, pl.ds(r0, rb)], fbuf.at[m], g_sem.at[m])
                for m, src in enumerate((dqs_out, q_hbm, dks_out, k_hbm))]

    def grad_store(b, i):
        r0 = pl.multiple_of(i * rb, rb)
        return pltpu.make_async_copy(gbuf, g_out.at[b, pl.ds(r0, rb), pl.ds(0, 2 * cols)], go_sem.at[0])

    def trade(b):
        return RowTrade(place, g_out, g_p, rows, r_send, r_recv, rows_of=(b,))

    def grad_block(b, i):
        for c in grad_loads(b, i):
            c.wait()
        sl = pl.ds(pl.multiple_of(i * rb, rb), rb)
        for m in range(2):
            inv_l = lanes_s[2 * m, sl]
            st_l = lanes_s[2 * m + 1, sl]
            for h in range(heads):
                hs = slice(h * HEAD_DIM, (h + 1) * HEAD_DIM)
                grad = inv_l * (fbuf[2 * m, :, hs] - (fbuf[2 * m + 1, :, hs] * inv_l) * st_l)
                gbuf[:, m * cols + h * HEAD_DIM:m * cols + (h + 1) * HEAD_DIM] = grad.astype(BF16)
        grad_store(b, i).start()

    def grad_begin(b):
        st_sum[...] = stats(b).finish()
        for m in range(2):
            lanes_s[2 * m] = lanes_of(lax.rsqrt(ss_ref[pl.ds(2 * b + m, 1)] / dim + EPS_NORM))
            lanes_s[2 * m + 1] = lanes_of(st_sum[m:m + 1] / dim)

    first = heads - per
    assert first >= 2
    b_old = step // heads - 1
    i_old = lax.rem(step, heads) - first

    @pl.when((step >= heads) & (step < steps) & (i_old >= 0))
    def _():
        @pl.when(i_old == 0)
        def _():
            grad_begin(b_old)

        @pl.when(i_old > 0)
        def _():
            grad_store(0, 0).wait()

        for c in grad_loads(b_old, i_old):
            c.start()

    @pl.when((step >= 2 * heads) & (lax.rem(step, heads) == 0))
    def _():
        grad_store(0, 0).wait()
        for b in range(nb - 1):
            pl.when(step == (b + 2) * heads)(trade(b).start)

    @pl.when(step < steps)
    def _():
        b = step // heads
        head = lax.rem(step, heads)
        slot = lax.rem(step, 2)

        @pl.when(step == 0)
        def _():
            st_row[...] = jnp.zeros_like(st_row)

        @pl.when(head == 0)
        def _():
            inv_q[...] = lanes_of(lax.rsqrt(ss_ref[pl.ds(2 * b, 1)] / dim + EPS_NORM))
            inv_k[...] = lanes_of(lax.rsqrt(ss_ref[pl.ds(2 * b + 1, 1)] / dim + EPS_NORM))
            acc_q[...] = jnp.zeros_like(acc_q)
            acc_k[...] = jnp.zeros_like(acc_k)

        @pl.when(step >= 2)
        def _():
            for c in flush(0, 0, slot):
                c.wait()

        cos, sin = cos_ref[...], sin_ref[...]
        q_rot, k_rot, v, do = qr_ref[0], kr_ref[0], v_ref[0], do_ref[0]

        def scores(i):
            sl = slice(i * blk, (i + 1) * blk)
            return (lax.dot_general(q_rot[sl], k_rot, NT, preferred_element_type=F32),
                    lax.dot_general(do[sl], v, NT, preferred_element_type=F32))

        ahead = scores(0)
        for i in range(tokens // blk):
            sl = slice(i * blk, (i + 1) * blk)
            s, dp = ahead
            if (i + 1) * blk < tokens:
                ahead = scores(i + 1)
            lse = jnp.concatenate([lse_ref[0, sl]] * (tokens // HEAD_DIM), axis=1)
            p = jnp.exp2(s * SCORE_SCALE - lse)
            p_all[sl] = p.astype(BF16)
            delta = jnp.sum(do[sl].astype(F32) * o_ref[0, sl], axis=1, keepdims=True)
            ds = (p * (dp - delta)).astype(BF16)
            ds_all[sl] = ds
            dq_all[sl] = jnp.dot(ds, k_rot, preferred_element_type=F32) * scale
        do_t = do.astype(F32).T.astype(BF16)
        q_t = q_rot.astype(F32).T.astype(BF16)
        v_st[slot] = jnp.dot(do_t, p_all[...], preferred_element_type=F32).T.astype(BF16)
        dk_rot = (jnp.dot(q_t, ds_all[...], preferred_element_type=F32) * scale).T.astype(BF16).astype(F32)
        dq_rot = dq_all[...].astype(BF16).astype(F32)
        dq_hat = rotate(dq_rot, cos, -sin)
        dk_hat = rotate(dk_rot, cos, -sin)
        q_hat = q_ref[0] * inv_q[...]
        k_hat = k_ref[0] * inv_k[...]
        dgq_ref[0] = jnp.sum(dq_hat * q_hat, axis=0, keepdims=True)
        dgk_ref[0] = jnp.sum(dk_hat * k_hat, axis=0, keepdims=True)
        dq_s = dq_hat * gain_ref[0:1]
        dk_s = dk_hat * gain_ref[1:2]
        qs_st[slot] = dq_s
        ks_st[slot] = dk_s
        acc_q[...] += dq_s * q_hat
        acc_k[...] += dk_s * k_hat
        for c in flush(b, head, slot):
            c.start()

        @pl.when(head == heads - 1)
        def _():
            st_row[b, 0:1] = to_row(acc_q[...])
            st_row[b, 1:2] = to_row(acc_k[...])
            for m in range(nb):
                pl.when(b == m)(stats(m).start)

    @pl.when((step >= heads) & (step < steps) & (i_old >= 0))
    def _():
        grad_block(b_old, i_old)

    @pl.when(step == steps)
    def _():
        for s in range(2):
            for c in flush(0, 0, s):
                c.wait()
        lax.fori_loop(mid, nc, scatter.sums_step, 0)
        lax.fori_loop(0, nc, scatter.start_side, 0)
        for c in grad_loads(nb - 1, 0):
            c.start()
        grad_begin(nb - 1)

        def last_row(i, _):
            @pl.when(i > 0)
            def _():
                grad_store(0, 0).wait()
                for c in grad_loads(nb - 1, i):
                    c.start()

            grad_block(nb - 1, i)
            return 0

        lax.fori_loop(0, per, last_row, 0)
        grad_store(0, 0).wait()
        trade(nb - 1).start()

        def weight_grad(turned, obuf, dbuf, fst, wst):
            bn = min(512, dim)
            n_chunks = dim // bn

            def chunk(c):
                slot = lax.rem(c, 2)
                cs = pl.ds(pl.multiple_of(c * bn, bn), bn)
                return [pltpu.make_async_copy(d_full.at[nb - 1, :, cs], dbuf.at[slot], w_sem.at[slot, 1]),
                        pltpu.make_async_copy(dwo_part.at[:, cs], fst.at[slot], w_sem.at[slot, 2])]

            def store(c):
                slot = lax.rem(c, 2)
                return pltpu.make_async_copy(wst.at[slot], dwo_out.at[:, pl.ds(pl.multiple_of(c * bn, bn), bn)], w_sem.at[slot, 0])

            load_o = pltpu.make_async_copy(o_hbm.at[nb - 1], obuf, ld_sem.at[0])
            load_o.start()
            for c in chunk(0):
                c.start()
            load_o.wait()
            turned[...] = obuf[...].T

            def body(c, _):
                slot = lax.rem(c, 2)

                @pl.when(c + 1 < n_chunks)
                def _():
                    for m in chunk(c + 1):
                        m.start()

                @pl.when(c >= 2)
                def _():
                    store(c).wait()

                for m in chunk(c):
                    m.wait()
                wst[slot] = (fst[slot] + jnp.dot(turned[...], dbuf[slot], preferred_element_type=F32)).astype(BF16)
                store(c).start()
                return 0

            lax.fori_loop(0, n_chunks, body, 0)
            for s in range(min(2, n_chunks)):
                store(s).wait()

        bn = min(512, dim)
        pl.run_scoped(weight_grad, pltpu.VMEM((cols, tokens), BF16), pltpu.VMEM((tokens, cols), BF16),
                      pltpu.VMEM((2, tokens, bn), BF16), pltpu.VMEM((2, cols, bn), F32), pltpu.VMEM((2, cols, bn), BF16))
        for b in range(nb):
            trade(b).wait_recv()
        for j in range(n_pieces):
            trade_w(j).wait_recv()

        n_dy = part_dy.shape[0]
        scatter_y = Scatter(place, part_dy, far_dy, None, y_send, y_recv)

        def first_dy(lhs, wbuf, pst):
            loads = pair_rows(place, nb, rows, g_out, g_p, lhs, ld_sem)
            for c in loads:
                c.start()
            dy = DyChunks(lhs, wbuf, (wq_hbm, wk_hbm, wv_hbm, wq_p, wk_p, wv_p), c_sem)
            for c in dy.loads(0):
                c.start()
            for c in loads:
                c.wait()

            def body(j, _):
                @pl.when(j + 1 < n_dy)
                def _():
                    for c in dy.loads(j + 1):
                        c.start()

                for c in dy.loads(j):
                    c.wait()
                store = pltpu.make_async_copy(pst, part_dy.at[j], go_sem.at[0])

                @pl.when(j >= 1)
                def _():
                    store.wait()
                    scatter_y.start_far(j - 1)

                for d in range(2):
                    z = dy.dot(j, d)
                    pst[2 * d] = z[:nb * rows]
                    pst[2 * d + 1] = z[nb * rows:]
                store.start()
                return 0

            lax.fori_loop(0, n_dy, body, 0)
            pltpu.make_async_copy(pst, part_dy.at[n_dy - 1], go_sem.at[0]).wait()
            scatter_y.start_far(n_dy - 1)

        pl.run_scoped(first_dy, pltpu.VMEM((4 * nb * rows, 6 * cols), BF16), pltpu.VMEM((2, CHUNK, 6 * cols), BF16),
                      pltpu.VMEM((4, nb * rows, CHUNK), BF16))
        scatter_end(scatter, proj_out, out_sem, nc)
        for b in range(nb):
            trade(b).wait_send()
        for j in range(n_pieces):
            trade_w(j).wait_send()
        for j in range(n_dy):
            for idx in (0, 1):
                scatter_y.message(j, idx).wait()


def attn_bwd_call(n, q, k, q_rot, k_rot, v, d_attn, o, o32, lse, gains, cos_tab, sin_tab, ss, part, far, d_full, dwo_part, w_q, w_k, w_v, wq_p):
    nb, tokens, cols = q.shape
    dim = d_full.shape[2]
    heads = cols // HEAD_DIM
    rows = tokens // n
    steps = nb * heads
    shape = jax.ShapeDtypeStruct
    dma = pltpu.SemaphoreType.DMA
    any_spec = pl.BlockSpec(memory_space=pl.ANY)

    def head_of(i):
        i = jnp.minimum(i, steps - 1)
        return i // heads, i % heads

    blk = pl.BlockSpec((1, tokens, HEAD_DIM), lambda i: (head_of(i)[0], 0, head_of(i)[1]))
    vec = pl.BlockSpec((2, HEAD_DIM), lambda i: (0, head_of(i)[1]))
    out_vec = pl.BlockSpec((1, 1, HEAD_DIM), lambda i: (head_of(i)[0], 0, head_of(i)[1]))
    tab = pl.BlockSpec((tokens, HEAD_DIM), lambda i: (0, 0))
    whole = (nb, tokens, cols)
    lane_tile = pltpu.VMEM((tokens, HEAD_DIM), F32)
    n_dy = min(EARLY_DY, dim // CHUNK)
    return pl.pallas_call(
        functools.partial(attn_bwd_kernel, n, nb, heads, dim), name="attn_bwd", grid=(steps + 1,),
        out_shape=[shape((nb, rows, dim), BF16), shape((nb, tokens, 3 * cols), BF16), shape((nb, tokens, 3 * cols), BF16),
                   shape(whole, F32), shape(whole, F32), shape((cols, dim), BF16),
                   shape(w_k.shape, BF16), shape(w_v.shape, BF16), shape((n_dy,) + part.shape[1:], BF16), shape((n_dy,) + far.shape[1:], BF16),
                   shape((nb, 1, cols), F32), shape((nb, 1, cols), F32)],
        in_specs=[blk] * 8 + [vec, tab, tab, pl.BlockSpec(ss.shape, lambda i: (0, 0))] + [any_spec] * 11,
        out_specs=[any_spec] * 10 + [out_vec, out_vec],
        scratch_shapes=Scatter.scratch(nb * rows, dim) + [lane_tile] * 4 + [pltpu.VMEM((tokens, tokens), BF16)] * 2 + [
            lane_tile, pltpu.VMEM((2, tokens, HEAD_DIM), F32), pltpu.VMEM((2, tokens, HEAD_DIM), F32),
            pltpu.VMEM((2, tokens, HEAD_DIM), BF16), pltpu.VMEM((nb, 8, tokens), F32), pltpu.VMEM((8, tokens), F32),
            pltpu.VMEM((nb, n, 8, tokens), F32), pltpu.VMEM((4, min(256, tokens), cols), F32), pltpu.VMEM((min(256, tokens), 2 * cols), BF16),
            pltpu.VMEM((4, tokens, HEAD_DIM), F32),
            dma((2,)), dma((2, 3)), dma((2, 3)), dma((4,)), dma((2,)), dma((nb,)), dma((nb, n)), dma((nb, n)), dma((8,)), dma((8,)),
            dma((nb, n // 2)), dma((nb, n // 2)), dma((2, 6)), dma((n_dy, 6)), dma((n_dy, 6))],
        compiler_params=params("arbitrary", collective_id=2, has_side_effects=True),
        cost_estimate=cost(4 * nb * tokens * dim * cols + 36 * nb * tokens * tokens * cols, 30 * nb * tokens * cols),
    )(q, k, q_rot, k_rot, v, d_attn, o32, lse, gains, cos_tab, sin_tab, ss, q, k, o, part, far, d_full, dwo_part, w_q, w_k, w_v, wq_p)


def dy_dw_kernel(n, nb, dim, g_hbm, g_p, wq_hbm, wk_hbm, wv_hbm, wq_p, wk_p, wv_p, y_full, part_in, far_in,
                 dy_out, dwq_out, dwk_out, dwv_out,
                 part, recv_far, recv_side, s_send, s_recv, g, ld_sem, w_sem, y_sem, o_sem, out_sem):
    tokens = g_hbm.shape[1]
    rows = tokens // n
    cols = g_hbm.shape[2] // 3
    nc = dim // CHUNK
    early = far_in.shape[0]
    lag = 3
    place = Place(n)
    scatter = Scatter(place, part, recv_far, recv_side, s_send, s_recv, early=early)
    stored = [pltpu.make_async_copy(part_in, part.at[pl.ds(0, early)], ld_sem.at[2]),
              pltpu.make_async_copy(far_in, recv_far.at[pl.ds(0, early)], ld_sem.at[3])]
    load_g = pltpu.make_async_copy(g_hbm, g, ld_sem.at[4])

    def chain(lhs, wbuf):
        loads = pair_rows(place, nb, rows, g_hbm, g_p, lhs, ld_sem)
        dy = DyChunks(lhs, wbuf, (wq_hbm, wk_hbm, wv_hbm, wq_p, wk_p, wv_p), w_sem)
        if early < nc:
            for c in dy.loads(early):
                c.start()
            for c in loads[:len(loads) // 2]:
                c.start()
        for c in stored:
            c.start()
        if early < nc:
            for c in loads[len(loads) // 2:]:
                c.start()
        place.barrier(place.near()[:2])
        for c in stored:
            c.wait()
        lax.fori_loop(0, early, scatter.sums_step, 0)
        load_g.start()

        def body(j, _):
            @pl.when(j + 1 < nc)
            def _():
                for c in dy.loads(j + 1):
                    c.start()

            for c in dy.loads(j):
                c.wait()
            for d in range(2):
                @pl.when(j == early)
                def _(d=d):
                    for c in loads[d * len(loads) // 2:(d + 1) * len(loads) // 2]:
                        c.wait()

                z = dy.dot(j, d)
                part[j, 2 * d] = z[:nb * rows]
                part[j, 2 * d + 1] = z[nb * rows:]
                if d == 0:
                    scatter.start_far(j)

            @pl.when(j >= early + lag)
            def _():
                scatter.sums(j - lag)

            return 0

        lax.fori_loop(early, nc, body, 0)
        lax.fori_loop(0, nc, scatter.start_side, 0)

    pl.run_scoped(chain, pltpu.VMEM((4 * nb * rows, 6 * cols), BF16), pltpu.VMEM((2, CHUNK, 6 * cols), BF16))

    def weight_grad(ybuf, wst):
        bm = min(512, dim)
        n_chunks = dim // bm

        def chunk(c):
            slot = lax.rem(c, 2)
            return pltpu.make_async_copy(y_full.at[:, :, pl.ds(pl.multiple_of(c * bm, bm), bm)], ybuf.at[slot], y_sem.at[slot])

        def store(c):
            slot = lax.rem(c, 2)
            dst = pl.ds(pl.multiple_of(c * bm, bm), bm)
            return [pltpu.make_async_copy(wst.at[slot, :, pl.ds(m * cols, cols)], out.at[dst], o_sem.at[slot, m])
                    for m, out in enumerate((dwq_out, dwk_out, dwv_out))]

        chunk(0).start()
        load_g.wait()

        def body(c, _):
            slot = lax.rem(c, 2)

            @pl.when(c + 1 < n_chunks)
            def _():
                chunk(c + 1).start()

            @pl.when(c >= 2)
            def _():
                for s in store(c):
                    s.wait()

            chunk(c).wait()
            for m in range(lag):
                late = max(nc - lag, early) + m
                if late < nc:
                    pl.when(c == min(m, n_chunks - 1))(functools.partial(scatter.sums, late))
            wst[slot] = lax.dot_general(ybuf[slot].reshape(nb * tokens, bm), g[...].reshape(nb * tokens, 3 * cols), TN,
                                        preferred_element_type=F32).astype(BF16)
            for s in store(c):
                s.start()
            return 0

        lax.fori_loop(0, n_chunks, body, 0)
        for s in range(min(2, n_chunks)):
            for c in store(s):
                c.wait()

    bm = min(512, dim)
    pl.run_scoped(weight_grad, pltpu.VMEM((2, nb, tokens, bm), BF16), pltpu.VMEM((2, bm, 3 * cols), BF16))
    scatter_end(scatter, dy_out, out_sem, nc)


def dy_dw_call(n, g, g_p, w_q, w_k, w_v, wq_p, wk_p, wv_p, y_full, part, far):
    nb, tokens, wide = g.shape
    dim = y_full.shape[2]
    cols = wide // 3
    rows = tokens // n
    shape = jax.ShapeDtypeStruct
    dma = pltpu.SemaphoreType.DMA
    any_spec = pl.BlockSpec(memory_space=pl.ANY)
    return pl.pallas_call(
        functools.partial(dy_dw_kernel, n, nb, dim), name="dy_dw",
        out_shape=[shape((nb, rows, dim), BF16)] + [shape((dim, cols), BF16)] * 3,
        in_specs=[any_spec] * 11, out_specs=[any_spec] * 4,
        scratch_shapes=Scatter.scratch(nb * rows, dim) + [pltpu.VMEM((nb, tokens, 3 * cols), BF16), dma((5,)), dma((2, 6)), dma((2,)), dma((2, 3)), dma((nb,))],
        compiler_params=params(collective_id=3, has_side_effects=True),
        cost_estimate=cost(12 * nb * tokens * dim * cols, 30 * nb * tokens * cols),
    )(g, g_p, w_q, w_k, w_v, wq_p, wk_p, wv_p, y_full, part, far)


def token_kernel(n_copies, x_ref, dy_ref, pr_ref, g_ref, m_ref, e_ref, bo_ref, gq_ref, gk_ref, *refs):
    srcs, (xo_ref, dx_ref, dm_ref, dgq_ref, dgk_ref), dsts = refs[:4], refs[4:9], refs[9:13]
    bufs, (acc, in_sem, out_sem) = refs[13:17], refs[17:]
    group = 16
    step = pl.program_id(0)
    rows = x_ref.shape[1]
    groups = rows // group
    depth = bufs[0].shape[0]
    lag = depth - 1

    def move(c, out):
        copies = []
        for j, (src, dst, buf) in enumerate(zip(srcs, dsts, bufs)):
            size = buf.shape[1]
            sl = pl.ds(pl.multiple_of(c * size, 16), size)
            slot = lax.rem(c, depth)
            copies.append(pltpu.make_async_copy(buf.at[slot], dst.at[sl], out_sem.at[slot, j]) if out
                          else pltpu.make_async_copy(src.at[sl], buf.at[slot], in_sem.at[slot, j]))
        return copies

    def advance(i):
        @pl.when(i < n_copies)
        def _():
            @pl.when(i >= depth)
            def _():
                for c in move(i - depth, True):
                    c.wait()

            for c in move(i, False):
                c.start()

        @pl.when((i >= lag) & (i < n_copies + lag))
        def _():
            for c in move(i - lag, False):
                c.wait()
            for c in move(i - lag, True):
                c.start()

    mod = m_ref[...] + e_ref[0]
    for src, dst in ((gq_ref, dgq_ref), (gk_ref, dgk_ref)):
        dst[...] = jnp.sum(src[...], axis=(0, 1))
    shift_bo = bo_ref[...].reshape(1, bo_ref.shape[0])
    acc[...] = jnp.zeros_like(acc)

    def body(r, _):
        advance(step * groups + r)
        sl = pl.ds(pl.multiple_of(r * group, group), group)
        x = x_ref[0, sl].astype(F32)
        d_out = dy_ref[0, sl].astype(F32)
        proj = pr_ref[0, sl].astype(F32) + shift_bo
        xo_ref[0, sl] = (x + mod[2:3] * proj).astype(BF16)
        gate_part = d_out * proj
        x_norm, inv_std = norm_stats(x)
        d_y = g_ref[0, sl].astype(F32)
        d_norm = d_y * (1.0 + mod[1:2])
        d_x = d_out + inv_std * (
            d_norm - jnp.mean(d_norm, axis=-1, keepdims=True) - x_norm * jnp.mean(d_norm * x_norm, axis=-1, keepdims=True))
        dx_ref[0, sl] = d_x.astype(BF16)
        scale_part = d_y * x_norm
        acc[0] += d_y[:8] + d_y[8:]
        acc[1] += scale_part[:8] + scale_part[8:]
        acc[2] += gate_part[:8] + gate_part[8:]
        return 0

    lax.fori_loop(0, groups, body, 0)
    for j in range(3):
        dm_ref[0, j:j + 1] = jnp.sum(acc[j], axis=0, keepdims=True)

    @pl.when(step == pl.num_programs(0) - 1)
    def _():
        total = pl.num_programs(0) * groups

        def rest(i, _):
            advance(i)
            return 0

        lax.fori_loop(total, jnp.maximum(total, n_copies + lag), rest, 0)
        for c in range(max(n_copies - depth, 0), n_copies):
            for copy in move(c, True):
                copy.wait()


def token_call(x_loc, dy_loc, proj, d_y, m_block, e_loc, b_o, d_gq, d_gk, grads):
    nb, rows, dim = x_loc.shape
    n_copies = dim // min(512, dim)
    row = pl.BlockSpec((1, rows, dim), lambda i: (i, 0, 0))
    mod = pl.BlockSpec((1, 3, dim), lambda i: (i, 0, 0))
    any_spec = pl.BlockSpec(memory_space=pl.ANY)
    dma = pltpu.SemaphoreType.DMA
    depth = 4
    return pl.pallas_call(
        functools.partial(token_kernel, n_copies), name="tokens", grid=(nb,),
        out_shape=[jax.ShapeDtypeStruct(x_loc.shape, BF16), jax.ShapeDtypeStruct(x_loc.shape, BF16),
                   jax.ShapeDtypeStruct((nb, 3, dim), F32)] + [jax.ShapeDtypeStruct(d_gq.shape[2:], F32)] * 2 + [jax.ShapeDtypeStruct(w.shape, BF16) for w in grads],
        in_specs=[row, row, row, row, pl.BlockSpec((3, dim), lambda i: (0, 0)), mod] + [pl.BlockSpec(memory_space=pltpu.VMEM)] * 3 + [any_spec] * 4,
        out_specs=[row, row, mod] + [pl.BlockSpec(memory_space=pltpu.VMEM)] * 2 + [any_spec] * 4,
        scratch_shapes=[pltpu.VMEM((depth, w.shape[0] // n_copies, w.shape[1]), BF16) for w in grads]
        + [pltpu.VMEM((3, 8, dim), F32), dma((depth, 4)), dma((depth, 4))],
        compiler_params=params("arbitrary"),
        cost_estimate=cost(nb * rows * dim * 30, nb * rows * dim * 12),
    )(x_loc, dy_loc, proj, d_y, m_block, e_loc, b_o, d_gq, d_gk, *grads)


def solution(mesh):
    tp_size = mesh.shape['tp']

    def device_step(x_loc, e_loc, m_block, w_q, b_q, w_k, b_k, w_v, b_v, w_o, b_o, g_q, g_k, pos_part, dy_loc):
        nb, _, dim = x_loc.shape
        y_full, d_own, q, k, v, wo_p, wo_t, ss, cos_tab, sin_tab, gains = gather_qkv_call(
            tp_size, x_loc, dy_loc, m_block, e_loc, w_q, w_k, w_v, w_o, b_q, b_k, b_v, g_q, g_k, pos_part)
        d_full, o, _, d_attn, wq_p, part, far, dwo_part, q_rot, k_rot, lse, o32 = gather_attn_call(
            tp_size, q, k, v, gains, cos_tab, sin_tab, ss, w_q, w_o, wo_p, wo_t, d_own)
        proj, g, g_p, _, _, d_wo, wk_p, wv_p, part, far, d_gq, d_gk = attn_bwd_call(
            tp_size, q, k, q_rot, k_rot, v, d_attn, o, o32, lse, gains, cos_tab, sin_tab, ss, part, far, d_full, dwo_part, w_q, w_k, w_v, wq_p)
        d_y, d_wq, d_wk, d_wv = dy_dw_call(tp_size, g, g_p, w_q, w_k, w_v, wq_p, wk_p, wv_p, y_full, part, far)
        x_out, d_x, d_mod, d_gq, d_gk, d_wq, d_wk, d_wv, d_wo = token_call(
            x_loc, dy_loc, proj, d_y, m_block, e_loc, b_o, d_gq, d_gk, (d_wq, d_wk, d_wv, d_wo))
        d_e = all_sum_call(tp_size, d_mod.reshape(tp_size, -1, HEAD_DIM)).reshape(nb, 3, dim)
        return x_out, d_x, d_e, jnp.sum(d_e, axis=0), d_wq, d_wk, d_wv, d_wo, d_gq, d_gk

    in_specs = (P('dp', 'tp', None), P('dp', None, None), P(None, None), P(None, 'tp'), P('tp'), P(None, 'tp'), P('tp'),
                P(None, 'tp'), P('tp'), P('tp', None), P(None), P('tp'), P('tp'), P('dp', None), P('dp', 'tp', None))
    out_specs = (P('dp', 'tp', None), P('dp', 'tp', None), P('dp', None, None), P('dp', None), P('dp', 'tp'), P('dp', 'tp'),
                 P('dp', 'tp'), P(('dp', 'tp'), None), P(('dp', 'tp')), P(('dp', 'tp')))
    return jax.shard_map(device_step, mesh=mesh, in_specs=in_specs, out_specs=out_specs, check_vma=False)
```

```python
import functools

import jax
import jax.numpy as jnp
import numpy as np
from jax import lax
from jax.experimental import pallas as pl
from jax.experimental.pallas import tpu as pltpu
from jax.sharding import PartitionSpec as P

HEAD_DIM = 128
EPS_NORM = 1e-6
ROPE_BASE = 10000.0
LOG2E = 1.4426950408889634
CHUNK = 512
VMEM_LIMIT = 60 * 1024 * 1024
F32 = jnp.float32
BF16 = jnp.bfloat16
MESH_ID = pl.DeviceIdType.MESH
NT = (((1,), (1,)), ((), ()))
TN = (((0,), (0,)), ((), ()))


def params(*semantics, **kw):
    return pltpu.CompilerParams(dimension_semantics=semantics or None, vmem_limit_bytes=VMEM_LIMIT, **kw)


def cost(flops, nbytes):
    return pl.CostEstimate(flops=int(flops), bytes_accessed=int(nbytes), transcendentals=0)


def rope_freqs():
    half_dim = HEAD_DIM // 2
    side_len = HEAD_DIM // 6
    first_len = half_dim - 2 * side_len
    pair_idx = np.arange(HEAD_DIM) // 2
    section = (pair_idx >= first_len).astype(np.int32) + (pair_idx >= first_len + side_len).astype(np.int32)
    offset = np.where(section == 0, 0, np.where(section == 1, first_len, first_len + side_len))
    sec_width = np.where(section == 0, first_len, side_len)
    exponent = -(pair_idx - offset).astype(np.float32) / sec_width.astype(np.float32)
    freq_vals = np.power(np.float32(ROPE_BASE), exponent)
    return np.where(section[None, :] == np.arange(3)[:, None], freq_vals[None, :], np.float32(0.0)).astype(np.float32)


def norm_stats(x):
    centered = x - jnp.mean(x, axis=-1, keepdims=True)
    inv_std = lax.rsqrt(jnp.mean(centered * centered, axis=-1, keepdims=True) + EPS_NORM)
    return centered * inv_std, inv_std


def to_row(acc):
    return jnp.sum(acc.T, axis=0, keepdims=True)


def lanes_of(row):
    return jnp.broadcast_to(row, (HEAD_DIM, row.shape[1])).T


def head_sum(values):
    out = values[:, :HEAD_DIM]
    for h in range(1, values.shape[1] // HEAD_DIM):
        out = out + values[:, h * HEAD_DIM:(h + 1) * HEAD_DIM]
    return out


class Place:
    def __init__(self, n):
        self.n = n
        self.me = lax.axis_index('tp')
        self.right = lax.rem(self.me + 2, n)
        self.left = lax.rem(self.me + n - 2, n)
        self.far = lax.rem(self.me + n // 2, n)
        self.chip = self.me // 2

    def partner(self, dev):
        return dev + 1 - 2 * lax.rem(dev, 2)

    def arrive(self, devices):
        for dev in devices:
            pl.semaphore_signal(pltpu.get_barrier_semaphore(), inc=1, device_id={'tp': dev}, device_id_type=MESH_ID)

    def barrier(self, devices):
        self.arrive(devices)
        pl.semaphore_wait(pltpu.get_barrier_semaphore(), len(devices))

    def to_partner(self, src, dst, send_sem, recv_sem):
        return pltpu.make_async_remote_copy(src_ref=src, dst_ref=dst, send_sem=send_sem, recv_sem=recv_sem,
                                            device_id={'tp': self.partner(self.me)}, device_id_type=MESH_ID)

    def everyone(self):
        return [lax.rem(self.me + d, self.n) for d in range(1, self.n)]

    def near(self):
        return [self.right, self.left, self.partner(self.me)]


class Gather:
    def __init__(self, place, full, rows, send, recv, early=0):
        self.at, self.full, self.rows, self.send, self.recv, self.early = place, full, rows, send, recv, early

    def part(self, b, dev, off, count):
        return self.full.at[b, pl.ds(pl.multiple_of(dev * self.rows + off, 16), count)]

    def copy(self, b, dev, off, count, s_idx, r_idx, target):
        ref = self.part(b, dev, off, count)
        return pltpu.make_async_remote_copy(src_ref=ref, dst_ref=ref, send_sem=self.send.at[b, s_idx], recv_sem=self.recv.at[b, r_idx],
                                            device_id={'tp': target}, device_id_type=MESH_ID)

    def start_own(self, b):
        p = self.at
        self.copy(b, p.me, 0, self.rows, 0, 0, p.right).start()
        self.copy(b, p.me, 0, self.rows, 1, 1, p.left).start()
        self.copy(b, p.me, 0, self.rows, 2, 4, p.partner(p.me)).start()

    def whole_blocks_in(self, b):
        p = self.at
        self.copy(b, p.partner(p.me), 0, self.rows, 2, 4, p.me).wait_recv()
        self.copy(b, p.left, 0, self.rows, 0, 0, p.me).wait_recv()
        self.copy(b, p.right, 0, self.rows, 1, 1, p.me).wait_recv()
        for s_idx in range(3):
            self.copy(b, p.me, 0, self.rows, s_idx, s_idx, p.me).wait_send()

    def pass_left(self, b):
        p, half = self.at, self.rows // 2
        self.copy(b, p.left, 0, half, 3, 2, p.right).start()
        self.copy(b, p.left, 0, self.rows, 5, 5, p.partner(p.me)).start()

    def pass_right(self, b):
        p, half = self.at, self.rows // 2
        self.copy(b, p.right, half, half, 4, 3, p.left).start()
        self.copy(b, p.right, 0, self.rows, 6, 6, p.partner(p.me)).start()

    def finish(self, b):
        p, half = self.at, self.rows // 2
        counts = (self.rows, self.rows, self.rows, half, half, self.rows, self.rows, half, half)
        for s_idx, count in list(enumerate(counts))[3 if b < self.early else 0:]:
            self.copy(b, p.me, 0, count, s_idx, s_idx, p.me).wait_send()

    def item_place(self, i, nb):
        j = i - nb
        b = jnp.where(i < nb, i, jnp.where(i < 3 * nb, j // 2, i - 3 * nb))
        chips = self.at.n // 2
        side = jnp.where(lax.rem(j + 2 * nb, 2) == 0, chips - 1, 1)
        off = jnp.where(i < nb, 0, jnp.where(i < 3 * nb, side, chips // 2))
        return b, pl.multiple_of(lax.rem(self.at.chip + off, chips) * (2 * self.rows), 32)

    def kinds(self, i, nb):
        odd = lax.rem(i + nb, 2)
        side = (i >= nb) & (i < 3 * nb)
        return i < nb, side & (odd == 0), side & (odd == 1), i >= 3 * nb

    def arrive(self, i, nb):
        p, half = self.at, self.rows // 2
        b, _ = self.item_place(i, nb)
        _, is_left, is_right, is_far = self.kinds(i, nb)

        @pl.when(is_left & (b >= self.early))
        def _():
            self.copy(b, p.left, 0, self.rows, 0, 0, p.me).wait_recv()
            self.pass_left(b)

        @pl.when(is_right & (b >= self.early))
        def _():
            self.copy(b, p.right, 0, self.rows, 1, 1, p.me).wait_recv()
            self.pass_right(b)

        @pl.when(is_far)
        def _():
            self.copy(b, p.far, 0, half, 3, 2, p.me).wait_recv()
            self.copy(b, p.far, 0, half, 7, 7, p.partner(p.me)).start()
            self.copy(b, p.far, half, half, 4, 3, p.me).wait_recv()
            self.copy(b, p.far, half, half, 8, 8, p.partner(p.me)).start()

    def ready(self, i, nb):
        p, half = self.at, self.rows // 2
        b, row0 = self.item_place(i, nb)
        is_own, is_left, is_right, is_far = self.kinds(i, nb)

        @pl.when(is_own & (b >= self.early))
        def _():
            self.copy(b, p.partner(p.me), 0, self.rows, 2, 4, p.me).wait_recv()

        @pl.when(is_left)
        def _():
            self.copy(b, p.partner(p.left), 0, self.rows, 5, 5, p.me).wait_recv()

        @pl.when(is_right)
        def _():
            self.copy(b, p.partner(p.right), 0, self.rows, 6, 6, p.me).wait_recv()

        @pl.when(is_far)
        def _():
            self.copy(b, p.partner(p.far), 0, half, 7, 7, p.me).wait_recv()
            self.copy(b, p.partner(p.far), half, half, 8, 8, p.me).wait_recv()

        return b, row0


class RowTrade:
    def __init__(self, place, src, dst, rows, send, recv, rows_of=None):
        self.at, self.src, self.dst, self.rows, self.send, self.recv = place, src, dst, rows, send, recv
        self.batch = range(src.shape[0]) if rows_of is None else rows_of

    def copies(self, parity):
        p = self.at
        for b in self.batch:
            for k in range(p.n // 2):
                sl = pl.ds(pl.multiple_of((2 * k + parity) * self.rows, 16), self.rows)
                yield p.to_partner(self.src.at[b, sl], self.dst.at[b, sl], self.send.at[b, k], self.recv.at[b, k])

    def start(self):
        for c in self.copies(1 - lax.rem(self.at.me, 2)):
            c.start()

    def wait_recv(self):
        for c in self.copies(lax.rem(self.at.me, 2)):
            c.wait_recv()

    def wait_send(self):
        for c in self.copies(1 - lax.rem(self.at.me, 2)):
            c.wait_send()


GATHER_SEMS = 9
EARLY_ROWS = 1
EARLY_CHUNKS = 3
EARLY_DY = 4


def chunks_of(width, step):
    return [(c, min(c + step, width)) for c in range(0, width, step)]


class Exchange:
    def __init__(self, place, x_ref, slots, send_sems, recv_sems):
        self.at, self.x, self.slots, self.send, self.recv = place, x_ref, slots, send_sems, recv_sems

    def copy(self, d, dev, src):
        return pltpu.make_async_remote_copy(src_ref=self.x, dst_ref=self.slots.at[src], send_sem=self.send.at[d], recv_sem=self.recv.at[src],
                                            device_id={'tp': dev}, device_id_type=MESH_ID)

    def start(self):
        for d, dev in enumerate(self.at.everyone()):
            self.copy(d, dev, self.at.me).start()
        self.slots[self.at.me] = self.x[...]

    def finish(self):
        for d, dev in enumerate(self.at.everyone()):
            self.copy(d, dev, dev).wait()
        total = self.slots[0]
        for d in range(1, self.at.n):
            total = total + self.slots[d]
        return total


def gather_qkv_kernel(n, x_ref, dy_ref, m_ref, e_ref, wq_ref, wk_ref, wv_ref, wo_ref, bq_ref, bk_ref, bv_ref, gq_ref, gk_ref, pos_ref,
                      freq_ref, y_full, d_full, q_out, k_out, v_out, wo_p, wo_t, ss_ref, cos_ref, sin_ref, gain_ref,
                      bias_ref, w_all, xin, stage, xbuf, zst, vst, sq, ss_row, slots, wo_in, wo_st, wo_sem,
                      w_sem, in_sem, st_sem, ld_sem, out_sem, g_send, g_recv, d_send, d_recv, e_send, e_recv, t_send, t_recv):
    nb, rows, dim = x_ref.shape
    cols = wq_ref.shape[1]
    place = Place(n)
    gather = Gather(place, y_full, rows, g_send, g_recv)
    gather_d = Gather(place, d_full, rows, d_send, d_recv)
    w_copies = [pltpu.make_async_copy(w, w_all.at[:, pl.ds(j * cols, cols)], w_sem.at[j]) for j, w in enumerate((wq_ref, wk_ref, wv_ref))]
    place.arrive(place.everyone())
    trade = place.to_partner(wo_ref, wo_p, t_send, t_recv)

    def load_x(b):
        return pltpu.make_async_copy(x_ref.at[b], xin.at[b], in_sem.at[b])

    for b in range(nb):
        load_x(b).start()
    for c in w_copies:
        c.start()
    group = 16

    def mine(full, b):
        return full.at[b, pl.ds(pl.multiple_of(place.me * rows, 16), rows)]

    def ln_step(b, _):
        load_x(b).wait()
        shift = m_ref[0:1] + e_ref[b, 0:1]
        scale_one = 1.0 + (m_ref[1:2] + e_ref[b, 1:2])

        def ln_rows(r, _):
            sl = pl.ds(pl.multiple_of(r * group, group), group)
            x_norm, _ = norm_stats(xin[b, sl].astype(F32))
            stage[b, sl] = (x_norm * scale_one + shift).astype(BF16)
            return 0

        lax.fori_loop(0, rows // group, ln_rows, 0)
        out = pltpu.make_async_copy(stage.at[b], mine(y_full, b), st_sem)
        out.start()

        @pl.when(b == 0)
        def _():
            pl.semaphore_wait(pltpu.get_barrier_semaphore(), n - 1)

        out.wait()
        gather.start_own(b)
        return 0

    lax.fori_loop(0, nb, ln_step, 0)
    load_dy = pltpu.make_async_copy(dy_ref, xin, in_sem.at[0])
    load_dy.start()
    for j, ref in enumerate((bq_ref, bk_ref, bv_ref)):
        bias_ref[:, j * cols:(j + 1) * cols] = ref[...].reshape(1, cols)
    for j, ref in enumerate((gq_ref, gk_ref)):
        gain_ref[j:j + 1] = ref[...].reshape(1, cols)

    def tables():
        lane = lax.broadcasted_iota(jnp.int32, (128, HEAD_DIM), 1)

        def rows_of(r, _):
            sl = pl.ds(pl.multiple_of(r * 128, 128), 128)
            pos = [lanes_of(pos_ref[m:m + 1, sl].astype(F32)) for m in range(3)]
            angle = pos[0] * freq_ref[0:1] + pos[1] * freq_ref[1:2] + pos[2] * freq_ref[2:3]
            cos_ref[sl] = jnp.cos(angle)
            sin_ref[sl] = jnp.where(lane % 2 == 0, -1.0, 1.0) * jnp.sin(angle)
            return 0

        lax.fori_loop(0, pos_ref.shape[1] // 128, rows_of, 0)

    def turn_wo():
        width = wo_in.shape[2]
        n_chunks = dim // width

        def load(c):
            slot = lax.rem(c, 2)
            return pltpu.make_async_copy(wo_ref.at[:, pl.ds(pl.multiple_of(c * width, width), width)], wo_in.at[slot], wo_sem.at[slot, 0])

        def store(c):
            slot = lax.rem(c, 2)
            return pltpu.make_async_copy(wo_st.at[slot], wo_t.at[pl.ds(pl.multiple_of(c * width, width), width)], wo_sem.at[slot, 1])

        load(0).start()

        def body(c, _):
            slot = lax.rem(c, 2)

            @pl.when(c + 1 < n_chunks)
            def _():
                load(c + 1).start()

            @pl.when(c >= 2)
            def _():
                store(c).wait()

            load(c).wait()
            wo_st[slot] = wo_in[slot].T
            store(c).start()
            return 0

        lax.fori_loop(0, n_chunks, body, 0)
        for c in range(min(2, n_chunks)):
            store(c).wait()

    def gate_step(b, _):
        gate = m_ref[2:3] + e_ref[b, 2:3]

        def gate_rows(r, _):
            sl = pl.ds(pl.multiple_of(r * group, group), group)
            stage[b, sl] = (xin[b, sl].astype(F32) * gate).astype(BF16)
            return 0

        lax.fori_loop(0, rows // group, gate_rows, 0)
        out = pltpu.make_async_copy(stage.at[b], mine(d_full, b), st_sem)
        out.start()
        out.wait()
        return 0

    for c in w_copies:
        c.wait()

    def outputs(b, row0, slot):
        dst = pl.ds(row0, 2 * rows)
        return [pltpu.make_async_copy(zst.at[slot, :, pl.ds(0, cols)], q_out.at[b, dst], out_sem.at[slot, 0]),
                pltpu.make_async_copy(zst.at[slot, :, pl.ds(cols, cols)], k_out.at[b, dst], out_sem.at[slot, 1]),
                pltpu.make_async_copy(vst.at[slot], v_out.at[b, dst], out_sem.at[slot, 2])]

    def load(b, row0, slot):
        return pltpu.make_async_copy(y_full.at[b, pl.ds(row0, 2 * rows)], xbuf.at[slot], ld_sem.at[slot])

    load(*gather.ready(0, nb), 0).start()

    def item(i, _):
        slot = lax.rem(i, 2)
        b, row0 = gather.item_place(i, nb)

        @pl.when(i + 1 < 4 * nb)
        def _():
            gather.arrive(i + 1, nb)

        @pl.when(i + 1 == 3 * nb - 1)
        def _():
            for d in range(EARLY_ROWS):
                gather_d.start_own(d)

        @pl.when(i == nb)
        def _():
            load_dy.wait()
            trade.start()
            lax.fori_loop(0, nb, gate_step, 0)
            tables()
            turn_wo()

        @pl.when(i >= 2)
        def _():
            for c in outputs(0, 0, slot):
                c.wait()

        load(0, 0, slot).wait()
        spans = chunks_of(3 * cols, 512)
        for m, (lo, hi) in enumerate(spans):
            if m == len(spans) - 1:
                @pl.when(i + 1 < 4 * nb)
                def _():
                    load(*gather.ready(i + 1, nb), lax.rem(i + 1, 2)).start()

            zst[slot, :, lo:hi] = jnp.dot(xbuf[slot], w_all[:, lo:hi], preferred_element_type=F32) + bias_ref[:, lo:hi]
        vst[slot] = zst[slot, :, 2 * cols:].astype(BF16)
        q = zst[slot, :, :cols]
        k = zst[slot, :, cols:2 * cols]
        sq[2 * b, pl.ds(row0, 2 * rows)] = head_sum(q * q)
        sq[2 * b + 1, pl.ds(row0, 2 * rows)] = head_sum(k * k)
        for c in outputs(b, row0, slot):
            c.start()
        return 0

    lax.fori_loop(0, 4 * nb, item, 0)
    ss_row[...] = jnp.zeros_like(ss_row)
    for j in range(2 * nb):
        ss_row[j:j + 1] = to_row(sq[j])
    sums = Exchange(place, ss_row, slots, e_send, e_recv)
    sums.start()
    for slot in range(2):
        for c in outputs(0, 0, slot):
            c.wait()
    for b in range(nb):
        gather.finish(b)
    for d in range(EARLY_ROWS):
        gather_d.whole_blocks_in(d)
    trade.wait()
    ss_ref[...] = sums.finish()


def gather_qkv_call(n, x_loc, dy_loc, m_block, e_loc, w_q, w_k, w_v, w_o, b_q, b_k, b_v, g_q, g_k, positions):
    nb, rows, dim = x_loc.shape
    cols = w_q.shape[1]
    tokens = rows * n
    shape = jax.ShapeDtypeStruct
    any_spec = pl.BlockSpec(memory_space=pl.ANY)
    vmem = pl.BlockSpec(memory_space=pltpu.VMEM)
    dma = pltpu.SemaphoreType.DMA
    stat_rows = -(-2 * nb // 8) * 8
    return pl.pallas_call(
        functools.partial(gather_qkv_kernel, n), name="gather_qkv",
        out_shape=[shape((nb, tokens, dim), BF16), shape((nb, tokens, dim), BF16), shape((nb, tokens, cols), F32),
                   shape((nb, tokens, cols), F32), shape((nb, tokens, cols), BF16), shape(w_o.shape, BF16), shape((dim, cols), BF16), shape((stat_rows, tokens), F32),
                   shape((tokens, HEAD_DIM), F32), shape((tokens, HEAD_DIM), F32), shape((2, cols), F32)],
        in_specs=[any_spec, any_spec, vmem, vmem] + [any_spec] * 4 + [vmem] * 7,
        out_specs=[any_spec] * 7 + [vmem] * 4,
        scratch_shapes=[
            pltpu.VMEM((1, 3 * cols), F32),
            pltpu.VMEM((dim, 3 * cols), BF16), pltpu.VMEM((nb, rows, dim), BF16), pltpu.VMEM((nb, rows, dim), BF16),
            pltpu.VMEM((2, 2 * rows, dim), BF16), pltpu.VMEM((2, 2 * rows, 3 * cols), F32), pltpu.VMEM((2, 2 * rows, cols), BF16),
            pltpu.VMEM((2 * nb, tokens, HEAD_DIM), F32), pltpu.VMEM((stat_rows, tokens), F32), pltpu.VMEM((n, stat_rows, tokens), F32),
            pltpu.VMEM((2, cols, min(512, dim)), BF16), pltpu.VMEM((2, min(512, dim), cols), BF16), dma((2, 2)),
            dma((3,)), dma((nb,)), dma, dma((2,)), dma((2, 3)), dma((nb, GATHER_SEMS)), dma((nb, GATHER_SEMS)),
            dma((EARLY_ROWS, GATHER_SEMS)), dma((EARLY_ROWS, GATHER_SEMS)), dma((n,)), dma((n,)), dma, dma],
        compiler_params=params(collective_id=0, has_side_effects=True),
        cost_estimate=cost(6 * nb * tokens * dim * cols, 6 * dim * cols + 14 * nb * tokens * cols),
    )(x_loc, dy_loc, m_block, e_loc, w_q, w_k, w_v, w_o, b_q, b_k, b_v, g_q, g_k, positions.T, jnp.asarray(rope_freqs()))


def all_sum_kernel(n, x_ref, o_ref, pieces, total, send_a, recv_a, send_b, recv_b):
    place = Place(n)
    me = place.me
    place.barrier(place.everyone())

    def first(d, dev, src):
        return pltpu.make_async_remote_copy(src_ref=x_ref.at[src], dst_ref=pieces.at[me], send_sem=send_a.at[d], recv_sem=recv_a.at[me],
                                            device_id={'tp': dev}, device_id_type=MESH_ID)

    for d, dev in enumerate(place.everyone()):
        first(d, dev, dev).start()
    pieces[me] = x_ref[me]
    for d, dev in enumerate(place.everyone()):
        pltpu.make_async_remote_copy(src_ref=x_ref.at[me], dst_ref=pieces.at[dev], send_sem=send_a.at[d], recv_sem=recv_a.at[dev],
                                     device_id={'tp': dev}, device_id_type=MESH_ID).wait_recv()
    acc = pieces[0]
    for d in range(1, n):
        acc = acc + pieces[d]
    total[...] = acc
    o_ref[me] = acc
    for d, dev in enumerate(place.everyone()):
        first(d, dev, dev).wait_send()
    for d, dev in enumerate(place.everyone()):
        pltpu.make_async_remote_copy(src_ref=total, dst_ref=o_ref.at[me], send_sem=send_b.at[d], recv_sem=recv_b.at[me],
                                     device_id={'tp': dev}, device_id_type=MESH_ID).start()
    for d, dev in enumerate(place.everyone()):
        copy = pltpu.make_async_remote_copy(src_ref=total, dst_ref=o_ref.at[dev], send_sem=send_b.at[d], recv_sem=recv_b.at[dev],
                                            device_id={'tp': dev}, device_id_type=MESH_ID)
        copy.wait_send()
        copy.wait_recv()


def all_sum_call(n, x):
    spec = pl.BlockSpec(memory_space=pltpu.VMEM)
    dma = pltpu.SemaphoreType.DMA
    return pl.pallas_call(
        functools.partial(all_sum_kernel, n), name="all_sum",
        out_shape=jax.ShapeDtypeStruct(x.shape, x.dtype), in_specs=[spec], out_specs=spec,
        scratch_shapes=[pltpu.VMEM(x.shape, x.dtype), pltpu.VMEM(x.shape[1:], x.dtype), dma((n,)), dma((n,)), dma((n,)), dma((n,))],
        compiler_params=pltpu.CompilerParams(collective_id=4, has_side_effects=True, vmem_limit_bytes=4 * 1024 * 1024),
        cost_estimate=cost(4_000_000_000, x.size * 8),
    )(x)


def swap_pairs(x):
    lane = lax.broadcasted_iota(jnp.int32, x.shape, 1)
    return jnp.where(lane % 2 == 0, pltpu.roll(x, HEAD_DIM - 1, 1), pltpu.roll(x, 1, 1))


def rotate(x, cos, sin):
    return x * cos + swap_pairs(x) * sin


SCORE_SCALE = HEAD_DIM ** -0.5 * LOG2E


def softmax_block(s):
    top = jnp.max(s, axis=1, keepdims=True)
    p = jnp.exp2(s * SCORE_SCALE - top * SCORE_SCALE)
    total = jnp.sum(p, axis=1, keepdims=True)
    return p * (1.0 / total), top * SCORE_SCALE + jnp.log(total) * LOG2E


class Scatter:
    def __init__(self, place, part, recv_far, recv_side, send, recv, far_src=None):
        self.at, self.part, self.far, self.side, self.send, self.recv = place, part, recv_far, recv_side, send, recv
        self.far_src = part if far_src is None else far_src
        self.rows = part.shape[2]
        self.half = self.rows // 2

    def message(self, idx, j, count=1):
        js, p = pl.ds(j, count), self.at
        rows = pl.ds(0, self.half) if idx in (0, 3, 4) else pl.ds(self.half, self.rows - self.half)
        src = (self.far_src if idx < 2 else self.part).at[js, (0, 0, 1, 2, 1, 2)[idx], rows]
        dst = self.far.at[js, idx] if idx < 2 else self.side.at[js, idx % 2, rows]
        return pltpu.make_async_remote_copy(src_ref=src, dst_ref=dst, send_sem=self.send.at[j, idx], recv_sem=self.recv.at[j, idx],
                                            device_id={'tp': p.left if idx % 2 else p.right}, device_id_type=MESH_ID)

    def start(self, kind, j, count=1):
        for idx in (2 * kind, 2 * kind + 1):
            self.message(idx, j, count).start()

    def wait_recv(self, kind, j, count=1):
        for idx in (2 * kind, 2 * kind + 1):
            self.message(idx, j, count).wait_recv()

    def wait_send(self, kind, j, count=1):
        for idx in (2 * kind, 2 * kind + 1):
            self.message(idx, j, count).wait_send()

    def add(self, j):
        h = self.half
        self.part[j, 1, :h] = (self.part[j, 1, :h].astype(F32) + self.far[j, 0].astype(F32)).astype(BF16)
        self.part[j, 2, h:] = (self.part[j, 2, h:].astype(F32) + self.far[j, 1].astype(F32)).astype(BF16)

    def sums(self, j, count=1):
        def step(m, _):
            self.add(j + m)
            return 0

        lax.fori_loop(0, count, step, 0)
        self.start(SUMS, j, count)

    def final(self, j):
        total = self.part[j, 3].astype(F32) + self.side[j, 0].astype(F32) + self.side[j, 1].astype(F32)
        self.part[j, 3] = total.astype(BF16)

    @staticmethod
    def scratch(rows, dim):
        nc, dma = dim // CHUNK, pltpu.SemaphoreType.DMA
        return [pltpu.VMEM((nc, 4, rows, CHUNK), BF16), pltpu.VMEM((nc, 2, rows // 2, CHUNK), BF16),
                pltpu.VMEM((nc, 2, rows, CHUNK), BF16), dma((nc, 6)), dma((nc, 6))]


def scatter_outputs(part, out, sem, j):
    nb, rows, _ = out.shape
    cs = pl.ds(pl.multiple_of(j * CHUNK, CHUNK), CHUNK)
    return [pltpu.make_async_copy(part.at[j, 3, pl.ds(b * rows, rows)], out.at[b, :, cs], sem.at[b]) for b in range(nb)]


FAR, SIDES, SUMS = range(3)


def halves_of(nc):
    return [(0, nc // 2), (nc // 2, nc - nc // 2)] if nc > 1 else [(0, nc)]


def scatter_end(scatter, out, sem, nc, far_groups, sum_groups):
    waiting = list(sum_groups)
    for lo, count in halves_of(nc):
        scatter.wait_recv(SIDES, lo, count)
        while waiting and waiting[0][0] < lo + count:
            scatter.wait_recv(SUMS, *waiting.pop(0))

        def last(j, _):
            scatter.final(j)
            for c in scatter_outputs(scatter.part, out, sem, j):
                c.start()
            return 0

        lax.fori_loop(lo, lo + count, last, 0)

    def drain(j, _):
        for c in scatter_outputs(scatter.part, out, sem, j):
            c.wait()
        return 0

    lax.fori_loop(0, nc, drain, 0)
    for kind, groups in ((FAR, far_groups), (SIDES, halves_of(nc)), (SUMS, sum_groups)):
        for group in groups:
            scatter.wait_send(kind, *group)


def pairs_of(lo, hi, size=2):
    return [(j, min(size, hi - j)) for j in range(lo, hi, size)]


def pair_rows(place, nb, rows, mine, theirs, lhs, sem):
    width = mine.shape[2]
    out = []
    for d, dev in enumerate((place.far, place.right, place.left, place.me)):
        src_rows = pl.ds(pl.multiple_of(dev * rows, 16), rows)
        for b in range(nb):
            dst_rows = pl.ds((d * nb + b) * rows, rows)
            for j, src in enumerate((mine, theirs)):
                out.append(pltpu.make_async_copy(src.at[b, src_rows], lhs.at[dst_rows, pl.ds(j * width, width)], sem.at[d // 2]))
    return out


def gather_attn_kernel(n, nb, heads, dim, q_ref, k_ref, v_ref, gain_ref, cos_ref, sin_ref, ss_ref,
                       wq_ref, wo_ref, wo_p, wo_t, d_in,
                       d_full, o_out, o_p, da_out, wq_p, part_out, far_in, qr_ref, kr_ref, lse_ref, o32_ref,
                       inv_q, inv_k, o_all, wo, xbuf, ast,
                       w_sem, ld_sem, out_sem, o_sem, p_sem, l_sem, g_send, g_recv, t_send, t_recv, r_send, r_recv, s_send, s_recv):
    step = pl.program_id(0)
    tokens = q_ref.shape[1]
    rows = tokens // n
    blk = min(384, tokens)
    place = Place(n)
    gather = Gather(place, d_full, rows, g_send, g_recv, early=EARLY_ROWS)
    cols = heads * HEAD_DIM
    nc = dim // CHUNK
    mid = nc // 2
    early_chunks = min(EARLY_CHUNKS, mid)
    scatter = Scatter(place, part_out, far_in, None, s_send, s_recv)
    trade_o = RowTrade(place, o_out, o_p, rows, r_send, r_recv)

    def trade_w():
        return place.to_partner(wq_ref, wq_p, t_send, t_recv)


    @pl.when(step == 0)
    def _():
        pltpu.make_async_copy(wo_t, wo, w_sem).start()
        place.barrier(place.near())

        for b in range(EARLY_ROWS):
            gather.pass_left(b)
            gather.pass_right(b)

        def own(b, _):
            gather.start_own(b)
            return 0

        lax.fori_loop(EARLY_ROWS, nb, own, 0)
        trade_w().start()

    @pl.when(step < nb * heads)
    def _():
        b = step // heads
        h = lax.rem(step, heads)

        @pl.when(h == 0)
        def _():
            inv_q[...] = lanes_of(lax.rsqrt(ss_ref[pl.ds(2 * b, 1)] / dim + EPS_NORM))
            inv_k[...] = lanes_of(lax.rsqrt(ss_ref[pl.ds(2 * b + 1, 1)] / dim + EPS_NORM))

        cos, sin = cos_ref[...], sin_ref[...]
        q_rot = rotate(q_ref[0] * inv_q[...] * gain_ref[0:1], cos, sin).astype(BF16)
        k_rot = rotate(k_ref[0] * inv_k[...] * gain_ref[1:2], cos, sin).astype(BF16)
        v = v_ref[0]
        lanes = pl.ds(pl.multiple_of(h * HEAD_DIM, HEAD_DIM), HEAD_DIM)
        qr_ref[0], kr_ref[0] = q_rot, k_rot

        def scores(i):
            return lax.dot_general(q_rot[i * blk:(i + 1) * blk], k_rot, NT, preferred_element_type=F32)

        ahead = scores(0)
        for i in range(tokens // blk):
            s = ahead
            if (i + 1) * blk < tokens:
                ahead = scores(i + 1)
            p, lse = softmax_block(s)
            lse_ref[0, i * blk:(i + 1) * blk] = jnp.broadcast_to(lse, (blk, HEAD_DIM))
            o = jnp.dot(p.astype(BF16), v, preferred_element_type=F32)
            o32_ref[0, i * blk:(i + 1) * blk] = o
            o_all[b, i * blk:(i + 1) * blk, lanes] = o.astype(BF16)

    @pl.when(step == nb * heads)
    def _():
        o_copy = pltpu.make_async_copy(o_all, o_out, o_sem)
        o_copy.start()
        pltpu.make_async_copy(wo_t, wo, w_sem).wait()

        def outputs(b, row0, slot):
            return pltpu.make_async_copy(ast.at[slot], da_out.at[b, pl.ds(row0, 2 * rows)], out_sem.at[slot])

        def load(b, row0, slot):
            return pltpu.make_async_copy(d_full.at[b, pl.ds(row0, 2 * rows)], xbuf.at[slot], ld_sem.at[slot])

        def project(lhs, wbuf, stage):
            loads = pair_rows(place, nb, rows, o_out, o_p, lhs, l_sem)
            for c in loads:
                c.start()

            def chunk(j):
                cs = pl.ds(pl.multiple_of(j * CHUNK, CHUNK), CHUNK)
                slot = lax.rem(j, 2)
                return [pltpu.make_async_copy(wo_ref.at[:, cs], wbuf.at[slot, pl.ds(0, cols)], p_sem.at[slot, 0]),
                        pltpu.make_async_copy(wo_p.at[:, cs], wbuf.at[slot, pl.ds(cols, cols)], p_sem.at[slot, 1])]

            def store(j):
                slot = lax.rem(j, 2)
                return pltpu.make_async_copy(stage.at[slot], part_out.at[j], p_sem.at[slot, 2])

            def stored(j):
                store(j).wait()

            for c in chunk(0):
                c.start()
            for c in loads:
                c.wait()

            def body(j, _):
                slot = lax.rem(j, 2)

                @pl.when(j + 1 < nc)
                def _():
                    for c in chunk(j + 1):
                        c.start()

                for c in chunk(j):
                    c.wait()
                half = 2 * nb * rows
                for d in range(2):
                    z = jnp.dot(lhs[d * half:(d + 1) * half], wbuf[slot], preferred_element_type=F32).astype(BF16)
                    stage[slot, 2 * d] = z[:half // 2]
                    stage[slot, 2 * d + 1] = z[half // 2:]
                store(j).start()

                @pl.when(j >= 1)
                def _():
                    stored(j - 1)

                @pl.when(j == mid)
                def _():
                    gather.arrive(3 * nb - 2, nb)
                    gather.arrive(3 * nb - 1, nb)
                    scatter.start(FAR, 0, early_chunks)

                return 0

            lax.fori_loop(0, nc, body, 0)
            stored(nc - 1)

        def fetch(i):
            b, row0 = gather.ready(i, nb)
            load(b, row0, lax.rem(i, 2)).start()

        fetch(0)
        gather.arrive(jnp.int32(1), nb)

        def item(i, _):
            slot = lax.rem(i, 2)

            @pl.when((i + 2 != 3 * nb - 2) & (i + 2 != 3 * nb - 1) & (i + 2 < 4 * nb))
            def _():
                gather.arrive(i + 2, nb)

            @pl.when((i + 1 != 3 * nb - 2) & (i + 1 < 4 * nb))
            def _():
                fetch(i + 1)

            @pl.when(i >= 2)
            def _():
                outputs(0, 0, slot).wait()

            load(0, 0, slot).wait()
            ast[slot] = jnp.dot(xbuf[slot], wo[...], preferred_element_type=F32).astype(BF16)
            b, row0 = gather.item_place(i, nb)
            outputs(b, row0, slot).start()

            @pl.when(i == 0)
            def _():
                o_copy.wait()
                trade_o.start()

            @pl.when(i + 1 == 3 * nb - 2)
            def _():
                trade_o.wait_recv()
                pl.run_scoped(project, pltpu.VMEM((4 * nb * rows, 2 * cols), BF16), pltpu.VMEM((2, 2 * cols, CHUNK), BF16),
                              pltpu.VMEM((2, 4, nb * rows, CHUNK), BF16))
                fetch(i + 1)

            return 0

        lax.fori_loop(0, 4 * nb, item, 0)
        for slot in range(2):
            outputs(0, 0, slot).wait()
        for b in range(nb):
            gather.finish(b)
        trade_o.wait_send()
        trade_w().wait()
        scatter.wait_recv(FAR, 0, early_chunks)
        scatter.wait_send(FAR, 0, early_chunks)


def gather_attn_call(n, q, k, v, gains, cos_tab, sin_tab, ss, w_q, w_o, wo_p, wo_t, d_full):
    nb, tokens, cols = q.shape
    dim = w_o.shape[1]
    heads = cols // HEAD_DIM
    rows = tokens // n
    last = nb * heads - 1
    nc = dim // CHUNK
    early = min(EARLY_CHUNKS, nc // 2)
    shape = jax.ShapeDtypeStruct
    dma = pltpu.SemaphoreType.DMA
    any_spec = pl.BlockSpec(memory_space=pl.ANY)

    def head_of(i):
        i = jnp.minimum(i, last)
        return i // heads, i % heads

    blk = pl.BlockSpec((1, tokens, HEAD_DIM), lambda i: (head_of(i)[0], 0, head_of(i)[1]))
    vec = pl.BlockSpec((2, HEAD_DIM), lambda i: (0, head_of(i)[1]))
    tab = pl.BlockSpec((tokens, HEAD_DIM), lambda i: (0, 0))
    head_arr = shape((nb, tokens, cols), BF16)
    return pl.pallas_call(
        functools.partial(gather_attn_kernel, n, nb, heads, dim), name="gather_attn", grid=(nb * heads + 1,),
        out_shape=[shape(d_full.shape, BF16), head_arr, head_arr, head_arr, shape(w_q.shape, BF16)]
        + [shape((nc, 4, nb * rows, CHUNK), BF16), shape((early, 2, nb * rows // 2, CHUNK), BF16), head_arr, head_arr,
           shape((nb, tokens, cols), F32), shape((nb, tokens, cols), F32)],
        in_specs=[blk, blk, blk, vec, tab, tab, pl.BlockSpec(ss.shape, lambda i: (0, 0))] + [any_spec] * 5,
        out_specs=[any_spec] * 7 + [blk] * 4,
        scratch_shapes=[
            pltpu.VMEM((tokens, HEAD_DIM), F32), pltpu.VMEM((tokens, HEAD_DIM), F32), pltpu.VMEM((nb, tokens, cols), BF16),
            pltpu.VMEM((dim, cols), BF16), pltpu.VMEM((2, 2 * rows, dim), BF16), pltpu.VMEM((2, 2 * rows, cols), BF16),
            dma, dma((2,)), dma((2,)), dma, dma((2, 3)), dma((2,)), dma((nb, GATHER_SEMS)), dma((nb, GATHER_SEMS)), dma, dma,
            dma((nb, n // 2)), dma((nb, n // 2)), dma((early, 6)), dma((early, 6))],
        input_output_aliases={11: 0},
        compiler_params=params("arbitrary", collective_id=1, has_side_effects=True),
        cost_estimate=cost(4 * nb * tokens * dim * cols + 4 * nb * tokens * tokens * cols, 8 * nb * tokens * dim),
    )(q, k, v, gains, cos_tab, sin_tab, ss, w_q, w_o, wo_p, wo_t, d_full)


class DyChunks:
    def __init__(self, lhs, wbuf, weights, w_sem):
        self.lhs, self.wbuf, self.weights, self.sem = lhs, wbuf, weights, w_sem

    def loads(self, j):
        slot = lax.rem(j, 2)
        src = pl.ds(pl.multiple_of(j * CHUNK, CHUNK), CHUNK)
        width = self.weights[0].shape[1]
        return [pltpu.make_async_copy(w.at[src], self.wbuf.at[slot, :, pl.ds(m * width, width)], self.sem.at[slot, m])
                for m, w in enumerate(self.weights)]

    def dot(self, j, d):
        half = self.lhs.shape[0] // 2
        return lax.dot_general(self.lhs[d * half:(d + 1) * half], self.wbuf[lax.rem(j, 2)], NT, preferred_element_type=F32).astype(BF16)


def attn_bwd_kernel(n, nb, heads, dim, q_ref, k_ref, qr_ref, kr_ref, v_ref, do_ref, o_ref, lse_ref, gain_ref, cos_ref, sin_ref, ss_ref,
                    q_hbm, k_hbm, o_hbm, part_in, far_in, d_full, wq_hbm, wk_hbm, wv_hbm, wq_p,
                    proj_out, g_out, g_p, dqs_out, dks_out, dwo_out, wk_p, wv_p, part_dy, far_dy, dgq_ref, dgk_ref,
                    part, recv_far, recv_side, s_send, s_recv,
                    inv_q, inv_k, acc_q, acc_k, p_all, ds_all, dq_all, qs_st, ks_st, v_st, st_row, st_sum, slots, fbuf, gbuf, lanes_s,
                    ld_sem, w_sem, fl_sem, g_sem, go_sem, out_sem, e_send, e_recv, t_send, t_recv, r_send, r_recv, c_sem, y_send, y_recv):
    step = pl.program_id(0)
    tokens = q_ref.shape[1]
    rows = tokens // n
    cols = heads * HEAD_DIM
    blk = min(256, tokens)
    nc = dim // CHUNK
    steps = nb * heads
    scale = HEAD_DIM ** -0.5
    place = Place(n)
    early = far_in.shape[0]
    scatter = Scatter(place, part, recv_far, recv_side, s_send, s_recv, far_src=part_in)

    def stored():
        return [pltpu.make_async_copy(part_in, part, ld_sem.at[0]),
                pltpu.make_async_copy(far_in, recv_far.at[pl.ds(0, early)], ld_sem.at[1])]

    n_pieces = 8

    def trade_w(j):
        m = j % (n_pieces // 2)
        size = dim // (n_pieces // 2)
        src, dst = ((wk_hbm, wk_p), (wv_hbm, wv_p))[j // (n_pieces // 2)]
        return place.to_partner(src.at[pl.ds(m * size, size)], dst.at[pl.ds(m * size, size)], t_send.at[j], t_recv.at[j])

    @pl.when(step == 0)
    def _():
        place.barrier(place.everyone())
        for c in stored():
            c.start()

    @pl.when(step == 1)
    def _():
        for c in stored():
            c.wait()

    def flush(b, h, slot):
        lanes = pl.ds(pl.multiple_of(h * HEAD_DIM, HEAD_DIM), HEAD_DIM)
        v_lanes = pl.ds(pl.multiple_of(2 * cols + h * HEAD_DIM, HEAD_DIM), HEAD_DIM)
        return [pltpu.make_async_copy(qs_st.at[slot], dqs_out.at[b, :, lanes], fl_sem.at[slot, 0]),
                pltpu.make_async_copy(ks_st.at[slot], dks_out.at[b, :, lanes], fl_sem.at[slot, 1]),
                pltpu.make_async_copy(v_st.at[slot], g_out.at[b, :, v_lanes], fl_sem.at[slot, 2])]

    for j in range(n_pieces):
        pl.when(step == j * (steps - 1) // n_pieces + 1)(lambda j=j: trade_w(j).start())

    far_groups = pairs_of(early, nc)
    early_sums = [(0, early - early // 2)] + ([(early - early // 2, early // 2)] if early > 1 else [])
    late_sums = pairs_of(early, nc, 4)
    events = []
    for m, group in enumerate(far_groups):
        events.append((group[1], functools.partial(scatter.start, FAR, *group)))
        if m >= 1 and m - 1 < len(early_sums):
            events.append((early_sums[m - 1][1], functools.partial(scatter.sums, *early_sums[m - 1])))
    for group in early_sums[max(len(far_groups) - 1, 0):]:
        events.append((group[1], functools.partial(scatter.sums, *group)))
    total, done = sum(size for size, _ in events), 0
    for size, event in events:
        @pl.when(step == max(done * (steps - 1) // total, 0 if done == 0 else 2))
        def _(event=event):
            event()

        done += size

    rb = min(256, tokens)
    per = tokens // rb

    def stats(b):
        return Exchange(place, st_row.at[b], slots.at[b], e_send.at[b], e_recv.at[b])

    def grad_loads(b, i):
        r0 = pl.multiple_of(i * rb, rb)
        return [pltpu.make_async_copy(src.at[b, pl.ds(r0, rb)], fbuf.at[m], g_sem.at[m])
                for m, src in enumerate((dqs_out, q_hbm, dks_out, k_hbm))]

    def grad_store(b, i):
        r0 = pl.multiple_of(i * rb, rb)
        return pltpu.make_async_copy(gbuf, g_out.at[b, pl.ds(r0, rb), pl.ds(0, 2 * cols)], go_sem.at[0])

    def trade(b):
        return RowTrade(place, g_out, g_p, rows, r_send, r_recv, rows_of=(b,))

    def grad_block(b, i):
        for c in grad_loads(b, i):
            c.wait()
        sl = pl.ds(pl.multiple_of(i * rb, rb), rb)
        for m in range(2):
            inv_l = lanes_s[2 * m, sl]
            st_l = lanes_s[2 * m + 1, sl]
            for h in range(heads):
                hs = slice(h * HEAD_DIM, (h + 1) * HEAD_DIM)
                grad = inv_l * (fbuf[2 * m, :, hs] - (fbuf[2 * m + 1, :, hs] * inv_l) * st_l)
                gbuf[:, m * cols + h * HEAD_DIM:m * cols + (h + 1) * HEAD_DIM] = grad.astype(BF16)
        grad_store(b, i).start()

    def grad_begin(b):
        st_sum[...] = stats(b).finish()
        for m in range(2):
            lanes_s[2 * m] = lanes_of(lax.rsqrt(ss_ref[pl.ds(2 * b + m, 1)] / dim + EPS_NORM))
            lanes_s[2 * m + 1] = lanes_of(st_sum[m:m + 1] / dim)

    first = heads - per
    assert first >= 2
    b_old = step // heads - 1
    i_old = lax.rem(step, heads) - first

    @pl.when((step >= heads) & (step < steps) & (i_old >= 0))
    def _():
        @pl.when(i_old == 0)
        def _():
            grad_begin(b_old)

        @pl.when(i_old > 0)
        def _():
            grad_store(0, 0).wait()

        for c in grad_loads(b_old, i_old):
            c.start()

    @pl.when((step >= 2 * heads) & (lax.rem(step, heads) == 0))
    def _():
        grad_store(0, 0).wait()
        for b in range(nb - 1):
            pl.when(step == (b + 2) * heads)(trade(b).start)

    @pl.when(step < steps)
    def _():
        b = step // heads
        head = lax.rem(step, heads)
        slot = lax.rem(step, 2)

        @pl.when(step == 0)
        def _():
            st_row[...] = jnp.zeros_like(st_row)

        @pl.when(head == 0)
        def _():
            inv_q[...] = lanes_of(lax.rsqrt(ss_ref[pl.ds(2 * b, 1)] / dim + EPS_NORM))
            inv_k[...] = lanes_of(lax.rsqrt(ss_ref[pl.ds(2 * b + 1, 1)] / dim + EPS_NORM))
            acc_q[...] = jnp.zeros_like(acc_q)
            acc_k[...] = jnp.zeros_like(acc_k)

        @pl.when(step >= 2)
        def _():
            for c in flush(0, 0, slot):
                c.wait()

        cos, sin = cos_ref[...], sin_ref[...]
        q_rot, k_rot, v, do = qr_ref[0], kr_ref[0], v_ref[0], do_ref[0]

        def scores(i):
            sl = slice(i * blk, (i + 1) * blk)
            return (lax.dot_general(q_rot[sl], k_rot, NT, preferred_element_type=F32),
                    lax.dot_general(do[sl], v, NT, preferred_element_type=F32))

        ahead = scores(0)
        for i in range(tokens // blk):
            sl = slice(i * blk, (i + 1) * blk)
            s, dp = ahead
            if (i + 1) * blk < tokens:
                ahead = scores(i + 1)
            lse = jnp.concatenate([lse_ref[0, sl]] * (tokens // HEAD_DIM), axis=1)
            p = jnp.exp2(s * SCORE_SCALE - lse)
            p_all[sl] = p.astype(BF16)
            delta = jnp.sum(do[sl].astype(F32) * o_ref[0, sl], axis=1, keepdims=True)
            ds = (p * (dp - delta)).astype(BF16)
            ds_all[sl] = ds
            dq_all[sl] = jnp.dot(ds, k_rot, preferred_element_type=F32) * scale
        do_t = do.astype(F32).T.astype(BF16)
        q_t = q_rot.astype(F32).T.astype(BF16)
        v_st[slot] = jnp.dot(do_t, p_all[...], preferred_element_type=F32).T.astype(BF16)
        dk_rot = (jnp.dot(q_t, ds_all[...], preferred_element_type=F32) * scale).T.astype(BF16).astype(F32)
        dq_rot = dq_all[...].astype(BF16).astype(F32)
        dq_hat = rotate(dq_rot, cos, -sin)
        dk_hat = rotate(dk_rot, cos, -sin)
        q_hat = q_ref[0] * inv_q[...]
        k_hat = k_ref[0] * inv_k[...]
        dgq_ref[0] = jnp.sum(dq_hat * q_hat, axis=0, keepdims=True)
        dgk_ref[0] = jnp.sum(dk_hat * k_hat, axis=0, keepdims=True)
        dq_s = dq_hat * gain_ref[0:1]
        dk_s = dk_hat * gain_ref[1:2]
        qs_st[slot] = dq_s
        ks_st[slot] = dk_s
        acc_q[...] += dq_s * q_hat
        acc_k[...] += dk_s * k_hat
        for c in flush(b, head, slot):
            c.start()

        @pl.when(head == heads - 1)
        def _():
            st_row[b, 0:1] = to_row(acc_q[...])
            st_row[b, 1:2] = to_row(acc_k[...])
            for m in range(nb):
                pl.when(b == m)(stats(m).start)

    @pl.when((step >= heads) & (step < steps) & (i_old >= 0))
    def _():
        grad_block(b_old, i_old)

    @pl.when(step == steps)
    def _():
        for s in range(2):
            for c in flush(0, 0, s):
                c.wait()
        for group in far_groups:
            scatter.wait_recv(FAR, *group)
        for group in late_sums:
            scatter.sums(*group)
        for group in halves_of(nc):
            scatter.start(SIDES, *group)
        for c in grad_loads(nb - 1, 0):
            c.start()
        grad_begin(nb - 1)

        def last_row(i, _):
            @pl.when(i > 0)
            def _():
                grad_store(0, 0).wait()
                for c in grad_loads(nb - 1, i):
                    c.start()

            grad_block(nb - 1, i)
            return 0

        lax.fori_loop(0, per, last_row, 0)
        grad_store(0, 0).wait()
        trade(nb - 1).start()

        def weight_grad(turned, obuf, dbuf, wst):
            bn = min(512, dim)
            n_chunks = dim // bn

            def chunk(c):
                slot = lax.rem(c, 2)
                return pltpu.make_async_copy(d_full.at[:, :, pl.ds(pl.multiple_of(c * bn, bn), bn)], dbuf.at[slot], w_sem.at[slot, 1])

            def store(c):
                slot = lax.rem(c, 2)
                return pltpu.make_async_copy(wst.at[slot], dwo_out.at[:, pl.ds(pl.multiple_of(c * bn, bn), bn)], w_sem.at[slot, 0])

            load_o = pltpu.make_async_copy(o_hbm, obuf, ld_sem.at[0])
            load_o.start()
            chunk(0).start()
            load_o.wait()
            for b in range(nb):
                turned[:, b * tokens:(b + 1) * tokens] = obuf[b].T

            def body(c, _):
                slot = lax.rem(c, 2)

                @pl.when(c + 1 < n_chunks)
                def _():
                    chunk(c + 1).start()

                @pl.when(c >= 2)
                def _():
                    store(c).wait()

                chunk(c).wait()
                d = dbuf[slot].reshape(nb * tokens, bn)
                wst[slot] = jnp.dot(turned[...], d, preferred_element_type=F32).astype(BF16)
                store(c).start()
                return 0

            lax.fori_loop(0, n_chunks, body, 0)
            for s in range(min(2, n_chunks)):
                store(s).wait()

        bn = min(512, dim)
        pl.run_scoped(weight_grad, pltpu.VMEM((cols, nb * tokens), BF16), pltpu.VMEM((nb, tokens, cols), BF16),
                      pltpu.VMEM((2, nb, tokens, bn), BF16), pltpu.VMEM((2, cols, bn), BF16))
        for b in range(nb):
            trade(b).wait_recv()
        for j in range(n_pieces):
            trade_w(j).wait_recv()

        n_dy = part_dy.shape[0]
        dy_groups = pairs_of(0, n_dy)
        scatter_y = Scatter(place, part_dy, far_dy, None, y_send, y_recv)

        def first_dy(lhs, wbuf, pst):
            loads = pair_rows(place, nb, rows, g_out, g_p, lhs, ld_sem)
            for c in loads:
                c.start()
            dy = DyChunks(lhs, wbuf, (wq_hbm, wk_hbm, wv_hbm, wq_p, wk_p, wv_p), c_sem)
            for c in dy.loads(0):
                c.start()
            for c in loads:
                c.wait()

            def body(j, _):
                @pl.when(j + 1 < n_dy)
                def _():
                    for c in dy.loads(j + 1):
                        c.start()

                for c in dy.loads(j):
                    c.wait()
                store = pltpu.make_async_copy(pst, part_dy.at[j], go_sem.at[0])

                @pl.when(j >= 1)
                def _():
                    store.wait()

                for lo, count in dy_groups:
                    pl.when(j == lo + count)(functools.partial(scatter_y.start, FAR, lo, count))

                for d in range(2):
                    z = dy.dot(j, d)
                    pst[2 * d] = z[:nb * rows]
                    pst[2 * d + 1] = z[nb * rows:]
                store.start()
                return 0

            lax.fori_loop(0, n_dy, body, 0)
            pltpu.make_async_copy(pst, part_dy.at[n_dy - 1], go_sem.at[0]).wait()
            scatter_y.start(FAR, *dy_groups[-1])

        pl.run_scoped(first_dy, pltpu.VMEM((4 * nb * rows, 6 * cols), BF16), pltpu.VMEM((2, CHUNK, 6 * cols), BF16),
                      pltpu.VMEM((4, nb * rows, CHUNK), BF16))
        scatter_end(scatter, proj_out, out_sem, nc, far_groups, early_sums + late_sums)
        for b in range(nb):
            trade(b).wait_send()
        for j in range(n_pieces):
            trade_w(j).wait_send()
        for group in dy_groups:
            scatter_y.wait_recv(FAR, *group)
            scatter_y.wait_send(FAR, *group)


def attn_bwd_call(n, q, k, q_rot, k_rot, v, d_attn, o, o32, lse, gains, cos_tab, sin_tab, ss, part, far, d_full, w_q, w_k, w_v, wq_p):
    nb, tokens, cols = q.shape
    dim = d_full.shape[2]
    heads = cols // HEAD_DIM
    rows = tokens // n
    steps = nb * heads
    shape = jax.ShapeDtypeStruct
    dma = pltpu.SemaphoreType.DMA
    any_spec = pl.BlockSpec(memory_space=pl.ANY)

    def head_of(i):
        i = jnp.minimum(i, steps - 1)
        return i // heads, i % heads

    blk = pl.BlockSpec((1, tokens, HEAD_DIM), lambda i: (head_of(i)[0], 0, head_of(i)[1]))
    vec = pl.BlockSpec((2, HEAD_DIM), lambda i: (0, head_of(i)[1]))
    out_vec = pl.BlockSpec((1, 1, HEAD_DIM), lambda i: (head_of(i)[0], 0, head_of(i)[1]))
    tab = pl.BlockSpec((tokens, HEAD_DIM), lambda i: (0, 0))
    whole = (nb, tokens, cols)
    lane_tile = pltpu.VMEM((tokens, HEAD_DIM), F32)
    n_dy = min(EARLY_DY, dim // CHUNK)
    return pl.pallas_call(
        functools.partial(attn_bwd_kernel, n, nb, heads, dim), name="attn_bwd", grid=(steps + 1,),
        out_shape=[shape((nb, rows, dim), BF16), shape((nb, tokens, 3 * cols), BF16), shape((nb, tokens, 3 * cols), BF16),
                   shape(whole, F32), shape(whole, F32), shape((cols, dim), BF16),
                   shape(w_k.shape, BF16), shape(w_v.shape, BF16), shape((n_dy,) + part.shape[1:], BF16), shape((n_dy,) + far.shape[1:], BF16),
                   shape((nb, 1, cols), F32), shape((nb, 1, cols), F32)],
        in_specs=[blk] * 8 + [vec, tab, tab, pl.BlockSpec(ss.shape, lambda i: (0, 0))] + [any_spec] * 10,
        out_specs=[any_spec] * 10 + [out_vec, out_vec],
        scratch_shapes=Scatter.scratch(nb * rows, dim) + [lane_tile] * 4 + [pltpu.VMEM((tokens, tokens), BF16)] * 2 + [
            lane_tile, pltpu.VMEM((2, tokens, HEAD_DIM), F32), pltpu.VMEM((2, tokens, HEAD_DIM), F32),
            pltpu.VMEM((2, tokens, HEAD_DIM), BF16), pltpu.VMEM((nb, 8, tokens), F32), pltpu.VMEM((8, tokens), F32),
            pltpu.VMEM((nb, n, 8, tokens), F32), pltpu.VMEM((4, min(256, tokens), cols), F32), pltpu.VMEM((min(256, tokens), 2 * cols), BF16),
            pltpu.VMEM((4, tokens, HEAD_DIM), F32),
            dma((2,)), dma((2, 2)), dma((2, 3)), dma((4,)), dma((2,)), dma((nb,)), dma((nb, n)), dma((nb, n)), dma((8,)), dma((8,)),
            dma((nb, n // 2)), dma((nb, n // 2)), dma((2, 6)), dma((n_dy, 6)), dma((n_dy, 6))],
        compiler_params=params("arbitrary", collective_id=2, has_side_effects=True),
        cost_estimate=cost(4 * nb * tokens * dim * cols + 36 * nb * tokens * tokens * cols, 30 * nb * tokens * cols),
    )(q, k, q_rot, k_rot, v, d_attn, o32, lse, gains, cos_tab, sin_tab, ss, q, k, o, part, far, d_full, w_q, w_k, w_v, wq_p)


def dy_dw_kernel(n, nb, dim, g_hbm, g_p, wq_hbm, wk_hbm, wv_hbm, wq_p, wk_p, wv_p, y_full, part_in, far_in,
                 dy_out, dwq_out, dwk_out, dwv_out,
                 part, recv_far, recv_side, s_send, s_recv, g, ld_sem, w_sem, y_sem, o_sem, out_sem):
    tokens = g_hbm.shape[1]
    rows = tokens // n
    cols = g_hbm.shape[2] // 3
    nc = dim // CHUNK
    early = far_in.shape[0]
    lag = 3
    place = Place(n)
    scatter = Scatter(place, part, recv_far, recv_side, s_send, s_recv)
    far_groups = pairs_of(early, nc, 1)
    in_loop = max(nc - lag - early, 0)
    sum_groups = [(0, early)] + pairs_of(early, early + in_loop, 1) + [(early + in_loop, nc - early - in_loop)]
    stored = [pltpu.make_async_copy(part_in, part.at[pl.ds(0, early)], ld_sem.at[2]),
              pltpu.make_async_copy(far_in, recv_far.at[pl.ds(0, early)], ld_sem.at[3])]
    load_g = pltpu.make_async_copy(g_hbm, g, ld_sem.at[4])

    def chain(lhs, wbuf):
        loads = pair_rows(place, nb, rows, g_hbm, g_p, lhs, ld_sem)
        dy = DyChunks(lhs, wbuf, (wq_hbm, wk_hbm, wv_hbm, wq_p, wk_p, wv_p), w_sem)
        if early < nc:
            for c in dy.loads(early):
                c.start()
            for c in loads[:len(loads) // 2]:
                c.start()
        for c in stored:
            c.start()
        if early < nc:
            for c in loads[len(loads) // 2:]:
                c.start()
        place.barrier(place.near()[:2])
        for c in stored:
            c.wait()
        scatter.sums(0, early)
        load_g.start()

        def body(j, _):
            @pl.when(j + 1 < nc)
            def _():
                for c in dy.loads(j + 1):
                    c.start()

            for c in dy.loads(j):
                c.wait()
            for d in range(2):
                @pl.when(j == early)
                def _(d=d):
                    for c in loads[d * len(loads) // 2:(d + 1) * len(loads) // 2]:
                        c.wait()

                z = dy.dot(j, d)
                part[j, 2 * d] = z[:nb * rows]
                part[j, 2 * d + 1] = z[nb * rows:]
                if d == 0:
                    scatter.start(FAR, j)

            @pl.when(j >= early + lag)
            def _():
                scatter.wait_recv(FAR, j - lag)
                scatter.sums(j - lag)

            return 0

        lax.fori_loop(early, nc, body, 0)
        for group in halves_of(nc):
            scatter.start(SIDES, *group)

    pl.run_scoped(chain, pltpu.VMEM((4 * nb * rows, 6 * cols), BF16), pltpu.VMEM((2, CHUNK, 6 * cols), BF16))

    def weight_grad(ybuf, wst):
        bm = min(512, dim)
        n_chunks = dim // bm

        def chunk(c):
            slot = lax.rem(c, 2)
            return pltpu.make_async_copy(y_full.at[:, :, pl.ds(pl.multiple_of(c * bm, bm), bm)], ybuf.at[slot], y_sem.at[slot])

        def store(c):
            slot = lax.rem(c, 2)
            dst = pl.ds(pl.multiple_of(c * bm, bm), bm)
            return [pltpu.make_async_copy(wst.at[slot, :, pl.ds(m * cols, cols)], out.at[dst], o_sem.at[slot, m])
                    for m, out in enumerate((dwq_out, dwk_out, dwv_out))]

        chunk(0).start()
        load_g.wait()

        def body(c, _):
            slot = lax.rem(c, 2)

            @pl.when(c + 1 < n_chunks)
            def _():
                chunk(c + 1).start()

            @pl.when(c >= 2)
            def _():
                for s in store(c):
                    s.wait()

            chunk(c).wait()
            @pl.when(c == min(1, n_chunks - 1))
            def _():
                for group in far_groups[in_loop:]:
                    scatter.wait_recv(FAR, *group)
                scatter.sums(*sum_groups[-1])

            wst[slot] = lax.dot_general(ybuf[slot].reshape(nb * tokens, bm), g[...].reshape(nb * tokens, 3 * cols), TN,
                                        preferred_element_type=F32).astype(BF16)
            for s in store(c):
                s.start()
            return 0

        lax.fori_loop(0, n_chunks, body, 0)
        for s in range(min(2, n_chunks)):
            for c in store(s):
                c.wait()

    bm = min(512, dim)
    pl.run_scoped(weight_grad, pltpu.VMEM((2, nb, tokens, bm), BF16), pltpu.VMEM((2, bm, 3 * cols), BF16))
    scatter_end(scatter, dy_out, out_sem, nc, far_groups, sum_groups)


def dy_dw_call(n, g, g_p, w_q, w_k, w_v, wq_p, wk_p, wv_p, y_full, part, far):
    nb, tokens, wide = g.shape
    dim = y_full.shape[2]
    cols = wide // 3
    rows = tokens // n
    shape = jax.ShapeDtypeStruct
    dma = pltpu.SemaphoreType.DMA
    any_spec = pl.BlockSpec(memory_space=pl.ANY)
    return pl.pallas_call(
        functools.partial(dy_dw_kernel, n, nb, dim), name="dy_dw",
        out_shape=[shape((nb, rows, dim), BF16)] + [shape((dim, cols), BF16)] * 3,
        in_specs=[any_spec] * 11, out_specs=[any_spec] * 4,
        scratch_shapes=Scatter.scratch(nb * rows, dim) + [pltpu.VMEM((nb, tokens, 3 * cols), BF16), dma((5,)), dma((2, 6)), dma((2,)), dma((2, 3)), dma((nb,))],
        compiler_params=params(collective_id=3, has_side_effects=True),
        cost_estimate=cost(12 * nb * tokens * dim * cols, 30 * nb * tokens * cols),
    )(g, g_p, w_q, w_k, w_v, wq_p, wk_p, wv_p, y_full, part, far)


def token_kernel(n_copies, x_ref, dy_ref, pr_ref, g_ref, m_ref, e_ref, bo_ref, gq_ref, gk_ref, *refs):
    srcs, (xo_ref, dx_ref, dm_ref, dgq_ref, dgk_ref), dsts = refs[:4], refs[4:9], refs[9:13]
    bufs, (acc, in_sem, out_sem) = refs[13:17], refs[17:]
    group = 16
    step = pl.program_id(0)
    rows = x_ref.shape[1]
    groups = rows // group
    depth = bufs[0].shape[0]
    lag = depth - 1

    def move(c, out):
        copies = []
        for j, (src, dst, buf) in enumerate(zip(srcs, dsts, bufs)):
            size = buf.shape[1]
            sl = pl.ds(pl.multiple_of(c * size, 16), size)
            slot = lax.rem(c, depth)
            copies.append(pltpu.make_async_copy(buf.at[slot], dst.at[sl], out_sem.at[slot, j]) if out
                          else pltpu.make_async_copy(src.at[sl], buf.at[slot], in_sem.at[slot, j]))
        return copies

    def advance(i):
        @pl.when(i < n_copies)
        def _():
            @pl.when(i >= depth)
            def _():
                for c in move(i - depth, True):
                    c.wait()

            for c in move(i, False):
                c.start()

        @pl.when((i >= lag) & (i < n_copies + lag))
        def _():
            for c in move(i - lag, False):
                c.wait()
            for c in move(i - lag, True):
                c.start()

    mod = m_ref[...] + e_ref[0]
    for src, dst in ((gq_ref, dgq_ref), (gk_ref, dgk_ref)):
        dst[...] = jnp.sum(src[...], axis=(0, 1))
    shift_bo = bo_ref[...].reshape(1, bo_ref.shape[0])
    acc[...] = jnp.zeros_like(acc)

    def body(r, _):
        advance(step * groups + r)
        sl = pl.ds(pl.multiple_of(r * group, group), group)
        x = x_ref[0, sl].astype(F32)
        d_out = dy_ref[0, sl].astype(F32)
        proj = pr_ref[0, sl].astype(F32) + shift_bo
        xo_ref[0, sl] = (x + mod[2:3] * proj).astype(BF16)
        gate_part = d_out * proj
        x_norm, inv_std = norm_stats(x)
        d_y = g_ref[0, sl].astype(F32)
        d_norm = d_y * (1.0 + mod[1:2])
        d_x = d_out + inv_std * (
            d_norm - jnp.mean(d_norm, axis=-1, keepdims=True) - x_norm * jnp.mean(d_norm * x_norm, axis=-1, keepdims=True))
        dx_ref[0, sl] = d_x.astype(BF16)
        scale_part = d_y * x_norm
        acc[0] += d_y[:8] + d_y[8:]
        acc[1] += scale_part[:8] + scale_part[8:]
        acc[2] += gate_part[:8] + gate_part[8:]
        return 0

    lax.fori_loop(0, groups, body, 0)
    for j in range(3):
        dm_ref[0, j:j + 1] = jnp.sum(acc[j], axis=0, keepdims=True)

    @pl.when(step == pl.num_programs(0) - 1)
    def _():
        total = pl.num_programs(0) * groups

        def rest(i, _):
            advance(i)
            return 0

        lax.fori_loop(total, jnp.maximum(total, n_copies + lag), rest, 0)
        for c in range(max(n_copies - depth, 0), n_copies):
            for copy in move(c, True):
                copy.wait()


def token_call(x_loc, dy_loc, proj, d_y, m_block, e_loc, b_o, d_gq, d_gk, grads):
    nb, rows, dim = x_loc.shape
    n_copies = dim // min(512, dim)
    row = pl.BlockSpec((1, rows, dim), lambda i: (i, 0, 0))
    mod = pl.BlockSpec((1, 3, dim), lambda i: (i, 0, 0))
    any_spec = pl.BlockSpec(memory_space=pl.ANY)
    dma = pltpu.SemaphoreType.DMA
    depth = 4
    return pl.pallas_call(
        functools.partial(token_kernel, n_copies), name="tokens", grid=(nb,),
        out_shape=[jax.ShapeDtypeStruct(x_loc.shape, BF16), jax.ShapeDtypeStruct(x_loc.shape, BF16),
                   jax.ShapeDtypeStruct((nb, 3, dim), F32)] + [jax.ShapeDtypeStruct(d_gq.shape[2:], F32)] * 2 + [jax.ShapeDtypeStruct(w.shape, BF16) for w in grads],
        in_specs=[row, row, row, row, pl.BlockSpec((3, dim), lambda i: (0, 0)), mod] + [pl.BlockSpec(memory_space=pltpu.VMEM)] * 3 + [any_spec] * 4,
        out_specs=[row, row, mod] + [pl.BlockSpec(memory_space=pltpu.VMEM)] * 2 + [any_spec] * 4,
        scratch_shapes=[pltpu.VMEM((depth, w.shape[0] // n_copies, w.shape[1]), BF16) for w in grads]
        + [pltpu.VMEM((3, 8, dim), F32), dma((depth, 4)), dma((depth, 4))],
        compiler_params=params("arbitrary"),
        cost_estimate=cost(nb * rows * dim * 30, nb * rows * dim * 12),
    )(x_loc, dy_loc, proj, d_y, m_block, e_loc, b_o, d_gq, d_gk, *grads)


def solution(mesh):
    tp_size = mesh.shape['tp']

    def device_step(x_loc, e_loc, m_block, w_q, b_q, w_k, b_k, w_v, b_v, w_o, b_o, g_q, g_k, pos_part, dy_loc):
        nb, _, dim = x_loc.shape
        y_full, d_own, q, k, v, wo_p, wo_t, ss, cos_tab, sin_tab, gains = gather_qkv_call(
            tp_size, x_loc, dy_loc, m_block, e_loc, w_q, w_k, w_v, w_o, b_q, b_k, b_v, g_q, g_k, pos_part)
        d_full, o, _, d_attn, wq_p, part, far, q_rot, k_rot, lse, o32 = gather_attn_call(
            tp_size, q, k, v, gains, cos_tab, sin_tab, ss, w_q, w_o, wo_p, wo_t, d_own)
        proj, g, g_p, _, _, d_wo, wk_p, wv_p, part, far, d_gq, d_gk = attn_bwd_call(
            tp_size, q, k, q_rot, k_rot, v, d_attn, o, o32, lse, gains, cos_tab, sin_tab, ss, part, far, d_full, w_q, w_k, w_v, wq_p)
        d_y, d_wq, d_wk, d_wv = dy_dw_call(tp_size, g, g_p, w_q, w_k, w_v, wq_p, wk_p, wv_p, y_full, part, far)
        x_out, d_x, d_mod, d_gq, d_gk, d_wq, d_wk, d_wv, d_wo = token_call(
            x_loc, dy_loc, proj, d_y, m_block, e_loc, b_o, d_gq, d_gk, (d_wq, d_wk, d_wv, d_wo))
        d_e = all_sum_call(tp_size, d_mod.reshape(tp_size, -1, HEAD_DIM)).reshape(nb, 3, dim)
        return x_out, d_x, d_e, jnp.sum(d_e, axis=0), d_wq, d_wk, d_wv, d_wo, d_gq, d_gk

    in_specs = (P('dp', 'tp', None), P('dp', None, None), P(None, None), P(None, 'tp'), P('tp'), P(None, 'tp'), P('tp'),
                P(None, 'tp'), P('tp'), P('tp', None), P(None), P('tp'), P('tp'), P('dp', None), P('dp', 'tp', None))
    out_specs = (P('dp', 'tp', None), P('dp', 'tp', None), P('dp', None, None), P('dp', None), P('dp', 'tp'), P('dp', 'tp'),
                 P('dp', 'tp'), P(('dp', 'tp'), None), P(('dp', 'tp')), P(('dp', 'tp')))
    return jax.shard_map(device_step, mesh=mesh, in_specs=in_specs, out_specs=out_specs, check_vma=False)
```

```python
import functools

import jax
import jax.numpy as jnp
import numpy as np
from jax import lax
from jax.experimental import pallas as pl
from jax.experimental.pallas import tpu as pltpu
from jax.sharding import PartitionSpec as P

HEAD_DIM = 128
EPS_NORM = 1e-6
ROPE_BASE = 10000.0
LOG2E = 1.4426950408889634
CHUNK = 512
VMEM_LIMIT = 60 * 1024 * 1024
F32 = jnp.float32
BF16 = jnp.bfloat16
MESH_ID = pl.DeviceIdType.MESH
NT = (((1,), (1,)), ((), ()))
TN = (((0,), (0,)), ((), ()))


def params(*semantics, **kw):
    return pltpu.CompilerParams(dimension_semantics=semantics or None, vmem_limit_bytes=VMEM_LIMIT, **kw)


def cost(flops, nbytes):
    return pl.CostEstimate(flops=int(flops), bytes_accessed=int(nbytes), transcendentals=0)


def rope_freqs():
    half_dim = HEAD_DIM // 2
    side_len = HEAD_DIM // 6
    first_len = half_dim - 2 * side_len
    pair_idx = np.arange(HEAD_DIM) // 2
    section = (pair_idx >= first_len).astype(np.int32) + (pair_idx >= first_len + side_len).astype(np.int32)
    offset = np.where(section == 0, 0, np.where(section == 1, first_len, first_len + side_len))
    sec_width = np.where(section == 0, first_len, side_len)
    exponent = -(pair_idx - offset).astype(np.float32) / sec_width.astype(np.float32)
    freq_vals = np.power(np.float32(ROPE_BASE), exponent)
    return np.where(section[None, :] == np.arange(3)[:, None], freq_vals[None, :], np.float32(0.0)).astype(np.float32)


def norm_stats(x):
    centered = x - jnp.mean(x, axis=-1, keepdims=True)
    inv_std = lax.rsqrt(jnp.mean(centered * centered, axis=-1, keepdims=True) + EPS_NORM)
    return centered * inv_std, inv_std


def to_row(acc):
    return jnp.sum(acc.T, axis=0, keepdims=True)


def lanes_of(row):
    return jnp.broadcast_to(row, (HEAD_DIM, row.shape[1])).T


def head_sum(values):
    out = values[:, :HEAD_DIM]
    for h in range(1, values.shape[1] // HEAD_DIM):
        out = out + values[:, h * HEAD_DIM:(h + 1) * HEAD_DIM]
    return out


class Place:
    def __init__(self, n):
        self.n = n
        self.me = lax.axis_index('tp')
        self.right = lax.rem(self.me + 2, n)
        self.left = lax.rem(self.me + n - 2, n)
        self.far = lax.rem(self.me + n // 2, n)
        self.chip = self.me // 2

    def partner(self, dev):
        return dev + 1 - 2 * lax.rem(dev, 2)

    def arrive(self, devices):
        for dev in devices:
            pl.semaphore_signal(pltpu.get_barrier_semaphore(), inc=1, device_id={'tp': dev}, device_id_type=MESH_ID)

    def barrier(self, devices):
        self.arrive(devices)
        pl.semaphore_wait(pltpu.get_barrier_semaphore(), len(devices))

    def to_partner(self, src, dst, send_sem, recv_sem):
        return pltpu.make_async_remote_copy(src_ref=src, dst_ref=dst, send_sem=send_sem, recv_sem=recv_sem,
                                            device_id={'tp': self.partner(self.me)}, device_id_type=MESH_ID)

    def everyone(self):
        return [lax.rem(self.me + d, self.n) for d in range(1, self.n)]

    def near(self):
        return [self.right, self.left, self.partner(self.me)]


class Gather:
    def __init__(self, place, full, rows, send, recv, early=0):
        self.at, self.full, self.rows, self.send, self.recv, self.early = place, full, rows, send, recv, early

    def part(self, b, dev, off, count):
        return self.full.at[b, pl.ds(pl.multiple_of(dev * self.rows + off, 16), count)]

    def copy(self, b, dev, off, count, s_idx, r_idx, target):
        ref = self.part(b, dev, off, count)
        return pltpu.make_async_remote_copy(src_ref=ref, dst_ref=ref, send_sem=self.send.at[b, s_idx], recv_sem=self.recv.at[b, r_idx],
                                            device_id={'tp': target}, device_id_type=MESH_ID)

    def start_own(self, b):
        p = self.at
        self.copy(b, p.me, 0, self.rows, 0, 0, p.right).start()
        self.copy(b, p.me, 0, self.rows, 1, 1, p.left).start()
        self.copy(b, p.me, 0, self.rows, 2, 4, p.partner(p.me)).start()

    def whole_blocks_in(self, b):
        p = self.at
        self.copy(b, p.partner(p.me), 0, self.rows, 2, 4, p.me).wait_recv()
        self.copy(b, p.left, 0, self.rows, 0, 0, p.me).wait_recv()
        self.copy(b, p.right, 0, self.rows, 1, 1, p.me).wait_recv()
        for s_idx in range(3):
            self.copy(b, p.me, 0, self.rows, s_idx, s_idx, p.me).wait_send()

    def pass_left(self, b):
        p, half = self.at, self.rows // 2
        self.copy(b, p.left, 0, half, 3, 2, p.right).start()
        self.copy(b, p.left, 0, self.rows, 5, 5, p.partner(p.me)).start()

    def pass_right(self, b):
        p, half = self.at, self.rows // 2
        self.copy(b, p.right, half, half, 4, 3, p.left).start()
        self.copy(b, p.right, 0, self.rows, 6, 6, p.partner(p.me)).start()

    def finish(self, b):
        p, half = self.at, self.rows // 2
        counts = (self.rows, self.rows, self.rows, half, half, self.rows, self.rows, half, half)
        for s_idx, count in list(enumerate(counts))[3 if b < self.early else 0:]:
            self.copy(b, p.me, 0, count, s_idx, s_idx, p.me).wait_send()

    def item_place(self, i, nb):
        j = i - nb
        b = jnp.where(i < nb, i, jnp.where(i < 3 * nb, j // 2, i - 3 * nb))
        chips = self.at.n // 2
        side = jnp.where(lax.rem(j + 2 * nb, 2) == 0, chips - 1, 1)
        off = jnp.where(i < nb, 0, jnp.where(i < 3 * nb, side, chips // 2))
        return b, pl.multiple_of(lax.rem(self.at.chip + off, chips) * (2 * self.rows), 32)

    def kinds(self, i, nb):
        odd = lax.rem(i + nb, 2)
        side = (i >= nb) & (i < 3 * nb)
        return i < nb, side & (odd == 0), side & (odd == 1), i >= 3 * nb

    def arrive(self, i, nb):
        p, half = self.at, self.rows // 2
        b, _ = self.item_place(i, nb)
        _, is_left, is_right, is_far = self.kinds(i, nb)

        @pl.when(is_left & (b >= self.early))
        def _():
            self.copy(b, p.left, 0, self.rows, 0, 0, p.me).wait_recv()
            self.pass_left(b)

        @pl.when(is_right & (b >= self.early))
        def _():
            self.copy(b, p.right, 0, self.rows, 1, 1, p.me).wait_recv()
            self.pass_right(b)

        @pl.when(is_far)
        def _():
            self.copy(b, p.far, 0, half, 3, 2, p.me).wait_recv()
            self.copy(b, p.far, 0, half, 7, 7, p.partner(p.me)).start()
            self.copy(b, p.far, half, half, 4, 3, p.me).wait_recv()
            self.copy(b, p.far, half, half, 8, 8, p.partner(p.me)).start()

    def ready(self, i, nb):
        p, half = self.at, self.rows // 2
        b, row0 = self.item_place(i, nb)
        is_own, is_left, is_right, is_far = self.kinds(i, nb)

        @pl.when(is_own & (b >= self.early))
        def _():
            self.copy(b, p.partner(p.me), 0, self.rows, 2, 4, p.me).wait_recv()

        @pl.when(is_left)
        def _():
            self.copy(b, p.partner(p.left), 0, self.rows, 5, 5, p.me).wait_recv()

        @pl.when(is_right)
        def _():
            self.copy(b, p.partner(p.right), 0, self.rows, 6, 6, p.me).wait_recv()

        @pl.when(is_far)
        def _():
            self.copy(b, p.partner(p.far), 0, half, 7, 7, p.me).wait_recv()
            self.copy(b, p.partner(p.far), half, half, 8, 8, p.me).wait_recv()

        return b, row0


class RowTrade:
    def __init__(self, place, src, dst, rows, send, recv, rows_of=None):
        self.at, self.src, self.dst, self.rows, self.send, self.recv = place, src, dst, rows, send, recv
        self.batch = range(src.shape[0]) if rows_of is None else rows_of

    def copies(self, parity):
        p = self.at
        for b in self.batch:
            for k in range(p.n // 2):
                sl = pl.ds(pl.multiple_of((2 * k + parity) * self.rows, 16), self.rows)
                yield p.to_partner(self.src.at[b, sl], self.dst.at[b, sl], self.send.at[b, k], self.recv.at[b, k])

    def start(self):
        for c in self.copies(1 - lax.rem(self.at.me, 2)):
            c.start()

    def wait_recv(self):
        for c in self.copies(lax.rem(self.at.me, 2)):
            c.wait_recv()

    def wait_send(self):
        for c in self.copies(1 - lax.rem(self.at.me, 2)):
            c.wait_send()


GATHER_SEMS = 9
EARLY_ROWS = 1
EARLY_CHUNKS = 1
EARLY_DY = 4


def chunks_of(width, step):
    return [(c, min(c + step, width)) for c in range(0, width, step)]


class Exchange:
    def __init__(self, place, x_ref, slots, send_sems, recv_sems):
        self.at, self.x, self.slots, self.send, self.recv = place, x_ref, slots, send_sems, recv_sems

    def copy(self, d, dev, src):
        return pltpu.make_async_remote_copy(src_ref=self.x, dst_ref=self.slots.at[src], send_sem=self.send.at[d], recv_sem=self.recv.at[src],
                                            device_id={'tp': dev}, device_id_type=MESH_ID)

    def start(self):
        for d, dev in enumerate(self.at.everyone()):
            self.copy(d, dev, self.at.me).start()
        self.slots[self.at.me] = self.x[...]

    def finish(self):
        for d, dev in enumerate(self.at.everyone()):
            self.copy(d, dev, dev).wait()
        total = self.slots[0]
        for d in range(1, self.at.n):
            total = total + self.slots[d]
        return total


def gather_qkv_kernel(n, x_ref, dy_ref, m_ref, e_ref, wq_ref, wk_ref, wv_ref, wo_ref, bq_ref, bk_ref, bv_ref, gq_ref, gk_ref, pos_ref,
                      freq_ref, y_full, d_full, q_out, k_out, v_out, wo_p, wo_t, ss_ref, cos_ref, sin_ref, gain_ref,
                      bias_ref, w_all, xin, stage, xbuf, zst, vst, sq, ss_row, slots, wo_in, wo_st, wo_sem,
                      w_sem, in_sem, st_sem, ld_sem, out_sem, g_send, g_recv, d_send, d_recv, e_send, e_recv, t_send, t_recv):
    nb, rows, dim = x_ref.shape
    cols = wq_ref.shape[1]
    place = Place(n)
    gather = Gather(place, y_full, rows, g_send, g_recv)
    gather_d = Gather(place, d_full, rows, d_send, d_recv)
    w_copies = [pltpu.make_async_copy(w, w_all.at[:, pl.ds(j * cols, cols)], w_sem.at[j]) for j, w in enumerate((wq_ref, wk_ref, wv_ref))]
    place.arrive(place.everyone())
    trade = place.to_partner(wo_ref, wo_p, t_send, t_recv)

    def load_x(b):
        return pltpu.make_async_copy(x_ref.at[b], xin.at[b], in_sem.at[b])

    for b in range(nb):
        load_x(b).start()
    for c in w_copies:
        c.start()
    group = 16

    def mine(full, b):
        return full.at[b, pl.ds(pl.multiple_of(place.me * rows, 16), rows)]

    def ln_step(b, _):
        load_x(b).wait()
        shift = m_ref[0:1] + e_ref[b, 0:1]
        scale_one = 1.0 + (m_ref[1:2] + e_ref[b, 1:2])

        def ln_rows(r, _):
            sl = pl.ds(pl.multiple_of(r * group, group), group)
            x_norm, _ = norm_stats(xin[b, sl].astype(F32))
            stage[b, sl] = (x_norm * scale_one + shift).astype(BF16)
            return 0

        lax.fori_loop(0, rows // group, ln_rows, 0)
        out = pltpu.make_async_copy(stage.at[b], mine(y_full, b), st_sem)
        out.start()

        @pl.when(b == 0)
        def _():
            pl.semaphore_wait(pltpu.get_barrier_semaphore(), n - 1)

        out.wait()
        gather.start_own(b)
        return 0

    lax.fori_loop(0, nb, ln_step, 0)
    load_dy = pltpu.make_async_copy(dy_ref, xin, in_sem.at[0])
    load_dy.start()
    for j, ref in enumerate((bq_ref, bk_ref, bv_ref)):
        bias_ref[:, j * cols:(j + 1) * cols] = ref[...].reshape(1, cols)
    for j, ref in enumerate((gq_ref, gk_ref)):
        gain_ref[j:j + 1] = ref[...].reshape(1, cols)

    def tables():
        lane = lax.broadcasted_iota(jnp.int32, (128, HEAD_DIM), 1)

        def rows_of(r, _):
            sl = pl.ds(pl.multiple_of(r * 128, 128), 128)
            pos = [lanes_of(pos_ref[m:m + 1, sl].astype(F32)) for m in range(3)]
            angle = pos[0] * freq_ref[0:1] + pos[1] * freq_ref[1:2] + pos[2] * freq_ref[2:3]
            cos_ref[sl] = jnp.cos(angle)
            sin_ref[sl] = jnp.where(lane % 2 == 0, -1.0, 1.0) * jnp.sin(angle)
            return 0

        lax.fori_loop(0, pos_ref.shape[1] // 128, rows_of, 0)

    def turn_wo():
        width = wo_in.shape[2]
        n_chunks = dim // width

        def load(c):
            slot = lax.rem(c, 2)
            return pltpu.make_async_copy(wo_ref.at[:, pl.ds(pl.multiple_of(c * width, width), width)], wo_in.at[slot], wo_sem.at[slot, 0])

        def store(c):
            slot = lax.rem(c, 2)
            return pltpu.make_async_copy(wo_st.at[slot], wo_t.at[pl.ds(pl.multiple_of(c * width, width), width)], wo_sem.at[slot, 1])

        load(0).start()

        def body(c, _):
            slot = lax.rem(c, 2)

            @pl.when(c + 1 < n_chunks)
            def _():
                load(c + 1).start()

            @pl.when(c >= 2)
            def _():
                store(c).wait()

            load(c).wait()
            wo_st[slot] = wo_in[slot].T
            store(c).start()
            return 0

        lax.fori_loop(0, n_chunks, body, 0)
        for c in range(min(2, n_chunks)):
            store(c).wait()

    def gate_step(b, _):
        gate = m_ref[2:3] + e_ref[b, 2:3]

        def gate_rows(r, _):
            sl = pl.ds(pl.multiple_of(r * group, group), group)
            stage[b, sl] = (xin[b, sl].astype(F32) * gate).astype(BF16)
            return 0

        lax.fori_loop(0, rows // group, gate_rows, 0)
        out = pltpu.make_async_copy(stage.at[b], mine(d_full, b), st_sem)
        out.start()
        out.wait()
        return 0

    for c in w_copies:
        c.wait()

    def outputs(b, row0, slot):
        dst = pl.ds(row0, 2 * rows)
        return [pltpu.make_async_copy(zst.at[slot, :, pl.ds(0, cols)], q_out.at[b, dst], out_sem.at[slot, 0]),
                pltpu.make_async_copy(zst.at[slot, :, pl.ds(cols, cols)], k_out.at[b, dst], out_sem.at[slot, 1]),
                pltpu.make_async_copy(vst.at[slot], v_out.at[b, dst], out_sem.at[slot, 2])]

    def load(b, row0, slot):
        return pltpu.make_async_copy(y_full.at[b, pl.ds(row0, 2 * rows)], xbuf.at[slot], ld_sem.at[slot])

    load(*gather.ready(0, nb), 0).start()

    def item(i, _):
        slot = lax.rem(i, 2)
        b, row0 = gather.item_place(i, nb)

        @pl.when(i + 1 < 4 * nb)
        def _():
            gather.arrive(i + 1, nb)

        @pl.when(i + 1 == 3 * nb - 1)
        def _():
            for d in range(EARLY_ROWS):
                gather_d.start_own(d)

        @pl.when(i == nb)
        def _():
            load_dy.wait()
            trade.start()
            lax.fori_loop(0, nb, gate_step, 0)
            tables()
            turn_wo()

        @pl.when(i >= 2)
        def _():
            for c in outputs(0, 0, slot):
                c.wait()

        load(0, 0, slot).wait()
        spans = chunks_of(3 * cols, 512)
        for m, (lo, hi) in enumerate(spans):
            if m == len(spans) - 1:
                @pl.when(i + 1 < 4 * nb)
                def _():
                    load(*gather.ready(i + 1, nb), lax.rem(i + 1, 2)).start()

            zst[slot, :, lo:hi] = jnp.dot(xbuf[slot], w_all[:, lo:hi], preferred_element_type=F32) + bias_ref[:, lo:hi]
        vst[slot] = zst[slot, :, 2 * cols:].astype(BF16)
        q = zst[slot, :, :cols]
        k = zst[slot, :, cols:2 * cols]
        sq[2 * b, pl.ds(row0, 2 * rows)] = head_sum(q * q)
        sq[2 * b + 1, pl.ds(row0, 2 * rows)] = head_sum(k * k)
        for c in outputs(b, row0, slot):
            c.start()
        return 0

    lax.fori_loop(0, 4 * nb, item, 0)
    ss_row[...] = jnp.zeros_like(ss_row)
    for j in range(2 * nb):
        ss_row[j:j + 1] = to_row(sq[j])
    sums = Exchange(place, ss_row, slots, e_send, e_recv)
    sums.start()
    for slot in range(2):
        for c in outputs(0, 0, slot):
            c.wait()
    for b in range(nb):
        gather.finish(b)
    for d in range(EARLY_ROWS):
        gather_d.whole_blocks_in(d)
    trade.wait()
    ss_ref[...] = sums.finish()


def gather_qkv_call(n, x_loc, dy_loc, m_block, e_loc, w_q, w_k, w_v, w_o, b_q, b_k, b_v, g_q, g_k, positions):
    nb, rows, dim = x_loc.shape
    cols = w_q.shape[1]
    tokens = rows * n
    shape = jax.ShapeDtypeStruct
    any_spec = pl.BlockSpec(memory_space=pl.ANY)
    vmem = pl.BlockSpec(memory_space=pltpu.VMEM)
    dma = pltpu.SemaphoreType.DMA
    stat_rows = -(-2 * nb // 8) * 8
    return pl.pallas_call(
        functools.partial(gather_qkv_kernel, n), name="gather_qkv",
        out_shape=[shape((nb, tokens, dim), BF16), shape((nb, tokens, dim), BF16), shape((nb, tokens, cols), F32),
                   shape((nb, tokens, cols), F32), shape((nb, tokens, cols), BF16), shape(w_o.shape, BF16), shape((dim, cols), BF16), shape((stat_rows, tokens), F32),
                   shape((tokens, HEAD_DIM), F32), shape((tokens, HEAD_DIM), F32), shape((2, cols), F32)],
        in_specs=[any_spec, any_spec, vmem, vmem] + [any_spec] * 4 + [vmem] * 7,
        out_specs=[any_spec] * 7 + [vmem] * 4,
        scratch_shapes=[
            pltpu.VMEM((1, 3 * cols), F32),
            pltpu.VMEM((dim, 3 * cols), BF16), pltpu.VMEM((nb, rows, dim), BF16), pltpu.VMEM((nb, rows, dim), BF16),
            pltpu.VMEM((2, 2 * rows, dim), BF16), pltpu.VMEM((2, 2 * rows, 3 * cols), F32), pltpu.VMEM((2, 2 * rows, cols), BF16),
            pltpu.VMEM((2 * nb, tokens, HEAD_DIM), F32), pltpu.VMEM((stat_rows, tokens), F32), pltpu.VMEM((n, stat_rows, tokens), F32),
            pltpu.VMEM((2, cols, min(512, dim)), BF16), pltpu.VMEM((2, min(512, dim), cols), BF16), dma((2, 2)),
            dma((3,)), dma((nb,)), dma, dma((2,)), dma((2, 3)), dma((nb, GATHER_SEMS)), dma((nb, GATHER_SEMS)),
            dma((EARLY_ROWS, GATHER_SEMS)), dma((EARLY_ROWS, GATHER_SEMS)), dma((n,)), dma((n,)), dma, dma],
        compiler_params=params(collective_id=0, has_side_effects=True),
        cost_estimate=cost(6 * nb * tokens * dim * cols, 6 * dim * cols + 14 * nb * tokens * cols),
    )(x_loc, dy_loc, m_block, e_loc, w_q, w_k, w_v, w_o, b_q, b_k, b_v, g_q, g_k, positions.T, jnp.asarray(rope_freqs()))


def all_sum_kernel(n, x_ref, o_ref, pieces, total, send_a, recv_a, send_b, recv_b):
    place = Place(n)
    me = place.me
    place.barrier(place.everyone())

    def first(d, dev, src):
        return pltpu.make_async_remote_copy(src_ref=x_ref.at[src], dst_ref=pieces.at[me], send_sem=send_a.at[d], recv_sem=recv_a.at[me],
                                            device_id={'tp': dev}, device_id_type=MESH_ID)

    for d, dev in enumerate(place.everyone()):
        first(d, dev, dev).start()
    pieces[me] = x_ref[me]
    for d, dev in enumerate(place.everyone()):
        pltpu.make_async_remote_copy(src_ref=x_ref.at[me], dst_ref=pieces.at[dev], send_sem=send_a.at[d], recv_sem=recv_a.at[dev],
                                     device_id={'tp': dev}, device_id_type=MESH_ID).wait_recv()
    acc = pieces[0]
    for d in range(1, n):
        acc = acc + pieces[d]
    total[...] = acc
    o_ref[me] = acc
    for d, dev in enumerate(place.everyone()):
        first(d, dev, dev).wait_send()
    for d, dev in enumerate(place.everyone()):
        pltpu.make_async_remote_copy(src_ref=total, dst_ref=o_ref.at[me], send_sem=send_b.at[d], recv_sem=recv_b.at[me],
                                     device_id={'tp': dev}, device_id_type=MESH_ID).start()
    for d, dev in enumerate(place.everyone()):
        copy = pltpu.make_async_remote_copy(src_ref=total, dst_ref=o_ref.at[dev], send_sem=send_b.at[d], recv_sem=recv_b.at[dev],
                                            device_id={'tp': dev}, device_id_type=MESH_ID)
        copy.wait_send()
        copy.wait_recv()


def all_sum_call(n, x):
    spec = pl.BlockSpec(memory_space=pltpu.VMEM)
    dma = pltpu.SemaphoreType.DMA
    return pl.pallas_call(
        functools.partial(all_sum_kernel, n), name="all_sum",
        out_shape=jax.ShapeDtypeStruct(x.shape, x.dtype), in_specs=[spec], out_specs=spec,
        scratch_shapes=[pltpu.VMEM(x.shape, x.dtype), pltpu.VMEM(x.shape[1:], x.dtype), dma((n,)), dma((n,)), dma((n,)), dma((n,))],
        compiler_params=pltpu.CompilerParams(collective_id=4, has_side_effects=True, vmem_limit_bytes=4 * 1024 * 1024),
        cost_estimate=cost(4_000_000_000, x.size * 8),
    )(x)


def swap_pairs(x):
    lane = lax.broadcasted_iota(jnp.int32, x.shape, 1)
    return jnp.where(lane % 2 == 0, pltpu.roll(x, HEAD_DIM - 1, 1), pltpu.roll(x, 1, 1))


def rotate(x, cos, sin):
    return x * cos + swap_pairs(x) * sin


SCORE_SCALE = HEAD_DIM ** -0.5 * LOG2E


def softmax_block(s):
    top = jnp.max(s, axis=1, keepdims=True)
    p = jnp.exp2(s * SCORE_SCALE - top * SCORE_SCALE)
    total = jnp.sum(p, axis=1, keepdims=True)
    return p * (1.0 / total), top * SCORE_SCALE + jnp.log(total) * LOG2E


class Scatter:
    def __init__(self, place, part, recv_far, recv_side, send, recv, far_src=None, early=0):
        self.at, self.part, self.far, self.side, self.send, self.recv = place, part, recv_far, recv_side, send, recv
        self.far_src, self.early = part if far_src is None else far_src, early
        self.rows = part.shape[2]
        self.half = self.rows // 2

    def copy(self, j, idx, src, dst, target):
        return pltpu.make_async_remote_copy(src_ref=src, dst_ref=dst, send_sem=self.send.at[j, idx], recv_sem=self.recv.at[j, idx],
                                            device_id={'tp': target}, device_id_type=MESH_ID)

    def message(self, j, idx):
        p, part, far, side = self.at, self.part, self.far, self.side
        first, second = pl.ds(0, self.half), pl.ds(self.half, self.rows - self.half)
        src, dst, target = (
            lambda: (self.far_src.at[j, 0, first], far.at[j, 0], p.right),
            lambda: (self.far_src.at[j, 0, second], far.at[j, 1], p.left),
            lambda: (part.at[j, 1, second], side.at[j, 0, second], p.right),
            lambda: (part.at[j, 2, first], side.at[j, 1, first], p.left),
            lambda: (part.at[j, 1, first], side.at[j, 0, first], p.right),
            lambda: (part.at[j, 2, second], side.at[j, 1, second], p.left))[idx]()
        return self.copy(j, idx, src, dst, target)

    def start_far(self, j, _=0):
        for idx in (0, 1):
            self.message(j, idx).start()
        return 0

    def start_side(self, j, _):
        for idx in (2, 3):
            self.message(j, idx).start()
        return 0

    def sums(self, j):
        h = self.half

        @pl.when(j >= self.early)
        def _():
            self.message(j, 0).wait_recv()
            self.message(j, 1).wait_recv()

        self.part[j, 1, :h] = (self.part[j, 1, :h].astype(F32) + self.far[j, 0].astype(F32)).astype(BF16)
        self.part[j, 2, h:] = (self.part[j, 2, h:].astype(F32) + self.far[j, 1].astype(F32)).astype(BF16)
        self.message(j, 4).start()
        self.message(j, 5).start()

    def sums_step(self, j, _):
        self.sums(j)
        return 0

    def final(self, j):
        for idx in range(2, 6):
            self.message(j, idx).wait_recv()
        total = self.part[j, 3].astype(F32) + self.side[j, 0].astype(F32) + self.side[j, 1].astype(F32)
        self.part[j, 3] = total.astype(BF16)

    def finish(self, j):
        @pl.when(j >= self.early)
        def _():
            for idx in range(2):
                self.message(j, idx).wait_send()

        for idx in range(2, 6):
            self.message(j, idx).wait_send()

    @staticmethod
    def scratch(rows, dim):
        nc, dma = dim // CHUNK, pltpu.SemaphoreType.DMA
        return [pltpu.VMEM((nc, 4, rows, CHUNK), BF16), pltpu.VMEM((nc, 2, rows // 2, CHUNK), BF16),
                pltpu.VMEM((nc, 2, rows, CHUNK), BF16), dma((nc, 6)), dma((nc, 6))]


def scatter_outputs(part, out, sem, j):
    nb, rows, _ = out.shape
    cs = pl.ds(pl.multiple_of(j * CHUNK, CHUNK), CHUNK)
    return [pltpu.make_async_copy(part.at[j, 3, pl.ds(b * rows, rows)], out.at[b, :, cs], sem.at[b]) for b in range(nb)]


def scatter_end(scatter, out, sem, nc):
    def last(j, _):
        scatter.final(j)
        for c in scatter_outputs(scatter.part, out, sem, j):
            c.start()
        return 0

    lax.fori_loop(0, nc, last, 0)

    def drain(j, _):
        for c in scatter_outputs(scatter.part, out, sem, j):
            c.wait()
        scatter.finish(j)
        return 0

    lax.fori_loop(0, nc, drain, 0)


def pair_rows(place, nb, rows, mine, theirs, lhs, sem):
    width = mine.shape[2]
    out = []
    for d, dev in enumerate((place.far, place.right, place.left, place.me)):
        src_rows = pl.ds(pl.multiple_of(dev * rows, 16), rows)
        for b in range(nb):
            dst_rows = pl.ds((d * nb + b) * rows, rows)
            for j, src in enumerate((mine, theirs)):
                out.append(pltpu.make_async_copy(src.at[b, src_rows], lhs.at[dst_rows, pl.ds(j * width, width)], sem.at[d // 2]))
    return out


def gather_attn_kernel(n, nb, heads, dim, q_ref, k_ref, v_ref, gain_ref, cos_ref, sin_ref, ss_ref,
                       wq_ref, wo_ref, wo_p, wo_t, d_in,
                       d_full, o_out, o_p, da_out, wq_p, part_out, far_in, o_t, qr_ref, kr_ref, lse_ref, o32_ref,
                       inv_q, inv_k, o_all, wo, xbuf, ast,
                       w_sem, ld_sem, out_sem, o_sem, p_sem, l_sem, g_send, g_recv, t_send, t_recv, r_send, r_recv, s_send, s_recv):
    step = pl.program_id(0)
    tokens = q_ref.shape[1]
    rows = tokens // n
    blk = min(384, tokens)
    place = Place(n)
    gather = Gather(place, d_full, rows, g_send, g_recv, early=EARLY_ROWS)
    cols = heads * HEAD_DIM
    nc = dim // CHUNK
    early_chunks = min(EARLY_CHUNKS, nc)
    mid = nc // 2
    scatter = Scatter(place, part_out, far_in, None, s_send, s_recv)
    trade_o = RowTrade(place, o_out, o_p, rows, r_send, r_recv)

    def trade_w():
        return place.to_partner(wq_ref, wq_p, t_send, t_recv)


    @pl.when(step == 0)
    def _():
        pltpu.make_async_copy(wo_t, wo, w_sem).start()
        place.barrier(place.near())

        for b in range(EARLY_ROWS):
            gather.pass_left(b)
            gather.pass_right(b)

        def own(b, _):
            gather.start_own(b)
            return 0

        lax.fori_loop(EARLY_ROWS, nb, own, 0)
        trade_w().start()

    @pl.when(step < nb * heads)
    def _():
        b = step // heads
        h = lax.rem(step, heads)

        @pl.when(h == 0)
        def _():
            inv_q[...] = lanes_of(lax.rsqrt(ss_ref[pl.ds(2 * b, 1)] / dim + EPS_NORM))
            inv_k[...] = lanes_of(lax.rsqrt(ss_ref[pl.ds(2 * b + 1, 1)] / dim + EPS_NORM))

        cos, sin = cos_ref[...], sin_ref[...]
        q_rot = rotate(q_ref[0] * inv_q[...] * gain_ref[0:1], cos, sin).astype(BF16)
        k_rot = rotate(k_ref[0] * inv_k[...] * gain_ref[1:2], cos, sin).astype(BF16)
        v = v_ref[0]
        lanes = pl.ds(pl.multiple_of(h * HEAD_DIM, HEAD_DIM), HEAD_DIM)
        qr_ref[0], kr_ref[0] = q_rot, k_rot

        def scores(i):
            return lax.dot_general(q_rot[i * blk:(i + 1) * blk], k_rot, NT, preferred_element_type=F32)

        ahead = scores(0)
        for i in range(tokens // blk):
            s = ahead
            if (i + 1) * blk < tokens:
                ahead = scores(i + 1)
            p, lse = softmax_block(s)
            lse_ref[0, i * blk:(i + 1) * blk] = jnp.broadcast_to(lse, (blk, HEAD_DIM))
            o = jnp.dot(p.astype(BF16), v, preferred_element_type=F32)
            o32_ref[0, i * blk:(i + 1) * blk] = o
            o_all[b, i * blk:(i + 1) * blk, lanes] = o.astype(BF16)

    @pl.when(step == nb * heads)
    def _():
        o_copy = pltpu.make_async_copy(o_all, o_out, o_sem)
        o_copy.start()
        pltpu.make_async_copy(wo_t, wo, w_sem).wait()

        def outputs(b, row0, slot):
            return pltpu.make_async_copy(ast.at[slot], da_out.at[b, pl.ds(row0, 2 * rows)], out_sem.at[slot])

        def load(b, row0, slot):
            return pltpu.make_async_copy(d_full.at[b, pl.ds(row0, 2 * rows)], xbuf.at[slot], ld_sem.at[slot])

        def project(lhs, wbuf, stage):
            loads = pair_rows(place, nb, rows, o_out, o_p, lhs, l_sem)
            for c in loads:
                c.start()

            def chunk(j):
                cs = pl.ds(pl.multiple_of(j * CHUNK, CHUNK), CHUNK)
                slot = lax.rem(j, 2)
                return [pltpu.make_async_copy(wo_ref.at[:, cs], wbuf.at[slot, pl.ds(0, cols)], p_sem.at[slot, 0]),
                        pltpu.make_async_copy(wo_p.at[:, cs], wbuf.at[slot, pl.ds(cols, cols)], p_sem.at[slot, 1])]

            def store(j):
                slot = lax.rem(j, 2)
                return pltpu.make_async_copy(stage.at[slot], part_out.at[j], p_sem.at[slot, 2])

            def stored(j):
                store(j).wait()

                @pl.when((j < early_chunks) & (j >= mid))
                def _():
                    scatter.start_far(j)

            for c in chunk(0):
                c.start()
            for c in loads:
                c.wait()

            def body(j, _):
                slot = lax.rem(j, 2)

                @pl.when(j + 1 < nc)
                def _():
                    for c in chunk(j + 1):
                        c.start()

                for c in chunk(j):
                    c.wait()
                half = 2 * nb * rows
                for d in range(2):
                    z = jnp.dot(lhs[d * half:(d + 1) * half], wbuf[slot], preferred_element_type=F32).astype(BF16)
                    stage[slot, 2 * d] = z[:half // 2]
                    stage[slot, 2 * d + 1] = z[half // 2:]
                store(j).start()

                @pl.when(j >= 1)
                def _():
                    stored(j - 1)

                @pl.when(j == mid)
                def _():
                    gather.arrive(3 * nb - 2, nb)
                    gather.arrive(3 * nb - 1, nb)
                    lax.fori_loop(0, min(early_chunks, mid), scatter.start_far, 0)

                return 0

            lax.fori_loop(0, nc, body, 0)
            stored(nc - 1)

        def fetch(i):
            b, row0 = gather.ready(i, nb)
            load(b, row0, lax.rem(i, 2)).start()

        fetch(0)
        gather.arrive(jnp.int32(1), nb)

        def item(i, _):
            slot = lax.rem(i, 2)

            @pl.when((i + 2 != 3 * nb - 2) & (i + 2 != 3 * nb - 1) & (i + 2 < 4 * nb))
            def _():
                gather.arrive(i + 2, nb)

            @pl.when((i + 1 != 3 * nb - 2) & (i + 1 < 4 * nb))
            def _():
                fetch(i + 1)

            @pl.when(i >= 2)
            def _():
                outputs(0, 0, slot).wait()

            load(0, 0, slot).wait()
            ast[slot] = jnp.dot(xbuf[slot], wo[...], preferred_element_type=F32).astype(BF16)
            b, row0 = gather.item_place(i, nb)
            outputs(b, row0, slot).start()

            @pl.when(i == 0)
            def _():
                o_copy.wait()
                trade_o.start()

            @pl.when(i + 1 == 3 * nb - 2)
            def _():
                trade_o.wait_recv()
                pl.run_scoped(project, pltpu.VMEM((4 * nb * rows, 2 * cols), BF16), pltpu.VMEM((2, 2 * cols, CHUNK), BF16),
                              pltpu.VMEM((2, 4, nb * rows, CHUNK), BF16))
                fetch(i + 1)

                def turn(turned):
                    for b in range(nb):
                        turned[:, b * tokens:(b + 1) * tokens] = o_all[b].T
                    pltpu.sync_copy(turned, o_t)

                pl.run_scoped(turn, pltpu.VMEM((cols, nb * tokens), BF16))

            return 0

        lax.fori_loop(0, 4 * nb, item, 0)
        for slot in range(2):
            outputs(0, 0, slot).wait()
        for b in range(nb):
            gather.finish(b)
        trade_o.wait_send()
        trade_w().wait()
        for j in range(early_chunks):
            for idx in (0, 1):
                scatter.message(j, idx).wait()


def gather_attn_call(n, q, k, v, gains, cos_tab, sin_tab, ss, w_q, w_o, wo_p, wo_t, d_full):
    nb, tokens, cols = q.shape
    dim = w_o.shape[1]
    heads = cols // HEAD_DIM
    rows = tokens // n
    last = nb * heads - 1
    nc = dim // CHUNK
    early = min(EARLY_CHUNKS, nc)
    shape = jax.ShapeDtypeStruct
    dma = pltpu.SemaphoreType.DMA
    any_spec = pl.BlockSpec(memory_space=pl.ANY)

    def head_of(i):
        i = jnp.minimum(i, last)
        return i // heads, i % heads

    blk = pl.BlockSpec((1, tokens, HEAD_DIM), lambda i: (head_of(i)[0], 0, head_of(i)[1]))
    vec = pl.BlockSpec((2, HEAD_DIM), lambda i: (0, head_of(i)[1]))
    tab = pl.BlockSpec((tokens, HEAD_DIM), lambda i: (0, 0))
    head_arr = shape((nb, tokens, cols), BF16)
    return pl.pallas_call(
        functools.partial(gather_attn_kernel, n, nb, heads, dim), name="gather_attn", grid=(nb * heads + 1,),
        out_shape=[shape(d_full.shape, BF16), head_arr, head_arr, head_arr, shape(w_q.shape, BF16)]
        + [shape((nc, 4, nb * rows, CHUNK), BF16), shape((early, 2, nb * rows // 2, CHUNK), BF16), shape((cols, nb * tokens), BF16), head_arr, head_arr,
           shape((nb, tokens, cols), F32), shape((nb, tokens, cols), F32)],
        in_specs=[blk, blk, blk, vec, tab, tab, pl.BlockSpec(ss.shape, lambda i: (0, 0))] + [any_spec] * 5,
        out_specs=[any_spec] * 8 + [blk] * 4,
        scratch_shapes=[
            pltpu.VMEM((tokens, HEAD_DIM), F32), pltpu.VMEM((tokens, HEAD_DIM), F32), pltpu.VMEM((nb, tokens, cols), BF16),
            pltpu.VMEM((dim, cols), BF16), pltpu.VMEM((2, 2 * rows, dim), BF16), pltpu.VMEM((2, 2 * rows, cols), BF16),
            dma, dma((2,)), dma((2,)), dma, dma((2, 3)), dma((2,)), dma((nb, GATHER_SEMS)), dma((nb, GATHER_SEMS)), dma, dma,
            dma((nb, n // 2)), dma((nb, n // 2)), dma((early, 6)), dma((early, 6))],
        input_output_aliases={11: 0},
        compiler_params=params("arbitrary", collective_id=1, has_side_effects=True),
        cost_estimate=cost(4 * nb * tokens * dim * cols + 4 * nb * tokens * tokens * cols, 8 * nb * tokens * dim),
    )(q, k, v, gains, cos_tab, sin_tab, ss, w_q, w_o, wo_p, wo_t, d_full)


class DyChunks:
    def __init__(self, lhs, wbuf, weights, w_sem):
        self.lhs, self.wbuf, self.weights, self.sem = lhs, wbuf, weights, w_sem

    def loads(self, j):
        slot = lax.rem(j, 2)
        src = pl.ds(pl.multiple_of(j * CHUNK, CHUNK), CHUNK)
        width = self.weights[0].shape[1]
        return [pltpu.make_async_copy(w.at[src], self.wbuf.at[slot, :, pl.ds(m * width, width)], self.sem.at[slot, m])
                for m, w in enumerate(self.weights)]

    def dot(self, j, d):
        half = self.lhs.shape[0] // 2
        return lax.dot_general(self.lhs[d * half:(d + 1) * half], self.wbuf[lax.rem(j, 2)], NT, preferred_element_type=F32).astype(BF16)


def attn_bwd_kernel(n, nb, heads, dim, q_ref, k_ref, qr_ref, kr_ref, v_ref, do_ref, o_ref, lse_ref, gain_ref, cos_ref, sin_ref, ss_ref,
                    q_hbm, k_hbm, o_t, part_in, far_in, d_full, wq_hbm, wk_hbm, wv_hbm, wq_p,
                    proj_out, g_out, g_p, dqs_out, dks_out, dwo_out, wk_p, wv_p, part_dy, far_dy, dgq_ref, dgk_ref,
                    part, recv_far, recv_side, s_send, s_recv,
                    inv_q, inv_k, acc_q, acc_k, p_all, ds_all, dq_all, qs_st, ks_st, v_st, st_row, st_sum, slots, fbuf, gbuf, lanes_s,
                    ld_sem, w_sem, fl_sem, g_sem, go_sem, out_sem, e_send, e_recv, t_send, t_recv, r_send, r_recv, c_sem, y_send, y_recv):
    step = pl.program_id(0)
    tokens = q_ref.shape[1]
    rows = tokens // n
    cols = heads * HEAD_DIM
    blk = min(256, tokens)
    nc = dim // CHUNK
    steps = nb * heads
    scale = HEAD_DIM ** -0.5
    place = Place(n)
    early = far_in.shape[0]
    scatter = Scatter(place, part, recv_far, recv_side, s_send, s_recv, far_src=part_in, early=early)

    def stored():
        return [pltpu.make_async_copy(part_in, part, ld_sem.at[0]),
                pltpu.make_async_copy(far_in, recv_far.at[pl.ds(0, early)], ld_sem.at[1])]

    n_pieces = 8

    def trade_w(j):
        m = j % (n_pieces // 2)
        size = dim // (n_pieces // 2)
        src, dst = ((wk_hbm, wk_p), (wv_hbm, wv_p))[j // (n_pieces // 2)]
        return place.to_partner(src.at[pl.ds(m * size, size)], dst.at[pl.ds(m * size, size)], t_send.at[j], t_recv.at[j])

    @pl.when(step == 0)
    def _():
        place.barrier(place.everyone())
        for c in stored():
            c.start()

    @pl.when(step == 1)
    def _():
        for c in stored():
            c.wait()

    def flush(b, h, slot):
        lanes = pl.ds(pl.multiple_of(h * HEAD_DIM, HEAD_DIM), HEAD_DIM)
        v_lanes = pl.ds(pl.multiple_of(2 * cols + h * HEAD_DIM, HEAD_DIM), HEAD_DIM)
        return [pltpu.make_async_copy(qs_st.at[slot], dqs_out.at[b, :, lanes], fl_sem.at[slot, 0]),
                pltpu.make_async_copy(ks_st.at[slot], dks_out.at[b, :, lanes], fl_sem.at[slot, 1]),
                pltpu.make_async_copy(v_st.at[slot], g_out.at[b, :, v_lanes], fl_sem.at[slot, 2])]

    for j in range(n_pieces):
        pl.when(step == j * (steps - 1) // n_pieces + 1)(lambda j=j: trade_w(j).start())

    mid = early
    events = []
    late = list(range(mid))
    for m, j in enumerate(range(early, nc)):
        events.append(functools.partial(scatter.start_far, j))
        if m >= 2 and m % 2 == 0 and late:
            events.append(functools.partial(scatter.sums, late.pop(0)))
    events += [functools.partial(scatter.sums, j) for j in late]
    for m, event in enumerate(events):
        @pl.when(step == m * (steps - 1) // len(events))
        def _(event=event):
            event()

    rb = min(256, tokens)
    per = tokens // rb

    def stats(b):
        return Exchange(place, st_row.at[b], slots.at[b], e_send.at[b], e_recv.at[b])

    def grad_loads(b, i):
        r0 = pl.multiple_of(i * rb, rb)
        return [pltpu.make_async_copy(src.at[b, pl.ds(r0, rb)], fbuf.at[m], g_sem.at[m])
                for m, src in enumerate((dqs_out, q_hbm, dks_out, k_hbm))]

    def grad_store(b, i):
        r0 = pl.multiple_of(i * rb, rb)
        return pltpu.make_async_copy(gbuf, g_out.at[b, pl.ds(r0, rb), pl.ds(0, 2 * cols)], go_sem.at[0])

    def trade(b):
        return RowTrade(place, g_out, g_p, rows, r_send, r_recv, rows_of=(b,))

    def grad_block(b, i):
        for c in grad_loads(b, i):
            c.wait()
        sl = pl.ds(pl.multiple_of(i * rb, rb), rb)
        for m in range(2):
            inv_l = lanes_s[2 * m, sl]
            st_l = lanes_s[2 * m + 1, sl]
            for h in range(heads):
                hs = slice(h * HEAD_DIM, (h + 1) * HEAD_DIM)
                grad = inv_l * (fbuf[2 * m, :, hs] - (fbuf[2 * m + 1, :, hs] * inv_l) * st_l)
                gbuf[:, m * cols + h * HEAD_DIM:m * cols + (h + 1) * HEAD_DIM] = grad.astype(BF16)
        grad_store(b, i).start()

    def grad_begin(b):
        st_sum[...] = stats(b).finish()
        for m in range(2):
            lanes_s[2 * m] = lanes_of(lax.rsqrt(ss_ref[pl.ds(2 * b + m, 1)] / dim + EPS_NORM))
            lanes_s[2 * m + 1] = lanes_of(st_sum[m:m + 1] / dim)

    first = heads - per
    assert first >= 2
    b_old = step // heads - 1
    i_old = lax.rem(step, heads) - first

    @pl.when((step >= heads) & (step < steps) & (i_old >= 0))
    def _():
        @pl.when(i_old == 0)
        def _():
            grad_begin(b_old)

        @pl.when(i_old > 0)
        def _():
            grad_store(0, 0).wait()

        for c in grad_loads(b_old, i_old):
            c.start()

    @pl.when((step >= 2 * heads) & (lax.rem(step, heads) == 0))
    def _():
        grad_store(0, 0).wait()
        for b in range(nb - 1):
            pl.when(step == (b + 2) * heads)(trade(b).start)

    @pl.when(step < steps)
    def _():
        b = step // heads
        head = lax.rem(step, heads)
        slot = lax.rem(step, 2)

        @pl.when(step == 0)
        def _():
            st_row[...] = jnp.zeros_like(st_row)

        @pl.when(head == 0)
        def _():
            inv_q[...] = lanes_of(lax.rsqrt(ss_ref[pl.ds(2 * b, 1)] / dim + EPS_NORM))
            inv_k[...] = lanes_of(lax.rsqrt(ss_ref[pl.ds(2 * b + 1, 1)] / dim + EPS_NORM))
            acc_q[...] = jnp.zeros_like(acc_q)
            acc_k[...] = jnp.zeros_like(acc_k)

        @pl.when(step >= 2)
        def _():
            for c in flush(0, 0, slot):
                c.wait()

        cos, sin = cos_ref[...], sin_ref[...]
        q_rot, k_rot, v, do = qr_ref[0], kr_ref[0], v_ref[0], do_ref[0]

        def scores(i):
            sl = slice(i * blk, (i + 1) * blk)
            return (lax.dot_general(q_rot[sl], k_rot, NT, preferred_element_type=F32),
                    lax.dot_general(do[sl], v, NT, preferred_element_type=F32))

        ahead = scores(0)
        for i in range(tokens // blk):
            sl = slice(i * blk, (i + 1) * blk)
            s, dp = ahead
            if (i + 1) * blk < tokens:
                ahead = scores(i + 1)
            lse = jnp.concatenate([lse_ref[0, sl]] * (tokens // HEAD_DIM), axis=1)
            p = jnp.exp2(s * SCORE_SCALE - lse)
            p_all[sl] = p.astype(BF16)
            delta = jnp.sum(do[sl].astype(F32) * o_ref[0, sl], axis=1, keepdims=True)
            ds = (p * (dp - delta)).astype(BF16)
            ds_all[sl] = ds
            dq_all[sl] = jnp.dot(ds, k_rot, preferred_element_type=F32) * scale
        do_t = do.astype(F32).T.astype(BF16)
        q_t = q_rot.astype(F32).T.astype(BF16)
        v_st[slot] = jnp.dot(do_t, p_all[...], preferred_element_type=F32).T.astype(BF16)
        dk_rot = (jnp.dot(q_t, ds_all[...], preferred_element_type=F32) * scale).T.astype(BF16).astype(F32)
        dq_rot = dq_all[...].astype(BF16).astype(F32)
        dq_hat = rotate(dq_rot, cos, -sin)
        dk_hat = rotate(dk_rot, cos, -sin)
        q_hat = q_ref[0] * inv_q[...]
        k_hat = k_ref[0] * inv_k[...]
        dgq_ref[0] = jnp.sum(dq_hat * q_hat, axis=0, keepdims=True)
        dgk_ref[0] = jnp.sum(dk_hat * k_hat, axis=0, keepdims=True)
        dq_s = dq_hat * gain_ref[0:1]
        dk_s = dk_hat * gain_ref[1:2]
        qs_st[slot] = dq_s
        ks_st[slot] = dk_s
        acc_q[...] += dq_s * q_hat
        acc_k[...] += dk_s * k_hat
        for c in flush(b, head, slot):
            c.start()

        @pl.when(head == heads - 1)
        def _():
            st_row[b, 0:1] = to_row(acc_q[...])
            st_row[b, 1:2] = to_row(acc_k[...])
            for m in range(nb):
                pl.when(b == m)(stats(m).start)

    @pl.when((step >= heads) & (step < steps) & (i_old >= 0))
    def _():
        grad_block(b_old, i_old)

    @pl.when(step == steps)
    def _():
        for s in range(2):
            for c in flush(0, 0, s):
                c.wait()
        lax.fori_loop(mid, nc, scatter.sums_step, 0)
        lax.fori_loop(0, nc, scatter.start_side, 0)
        for c in grad_loads(nb - 1, 0):
            c.start()

        def last_grad():
            grad_begin(nb - 1)

            def last_row(i, _):
                @pl.when(i > 0)
                def _():
                    grad_store(0, 0).wait()
                    for c in grad_loads(nb - 1, i):
                        c.start()

                grad_block(nb - 1, i)
                return 0

            lax.fori_loop(0, per, last_row, 0)
            grad_store(0, 0).wait()
            trade(nb - 1).start()

        def weight_grad(turned, dbuf, wst):
            bn = min(512, dim)
            n_chunks = dim // bn

            def chunk(c):
                slot = lax.rem(c, 2)
                return pltpu.make_async_copy(d_full.at[:, :, pl.ds(pl.multiple_of(c * bn, bn), bn)], dbuf.at[slot], w_sem.at[slot, 1])

            def store(c):
                slot = lax.rem(c, 2)
                return pltpu.make_async_copy(wst.at[slot], dwo_out.at[:, pl.ds(pl.multiple_of(c * bn, bn), bn)], w_sem.at[slot, 0])

            load_o = pltpu.make_async_copy(o_t, turned, ld_sem.at[0])
            load_o.start()
            chunk(0).start()
            load_o.wait()

            def body(c, _):
                slot = lax.rem(c, 2)

                @pl.when(c + 1 < n_chunks)
                def _():
                    chunk(c + 1).start()

                @pl.when(c >= 2)
                def _():
                    store(c).wait()

                chunk(c).wait()
                d = dbuf[slot].reshape(nb * tokens, bn)
                wst[slot] = jnp.dot(turned[...], d, preferred_element_type=F32).astype(BF16)
                store(c).start()
                pl.when(c == max(n_chunks // 2 - 2, 0))(last_grad)
                return 0

            lax.fori_loop(0, n_chunks, body, 0)
            for s in range(min(2, n_chunks)):
                store(s).wait()

        bn = min(512, dim)
        pl.run_scoped(weight_grad, pltpu.VMEM((cols, nb * tokens), BF16), pltpu.VMEM((2, nb, tokens, bn), BF16),
                      pltpu.VMEM((2, cols, bn), BF16))
        for b in range(nb):
            trade(b).wait_recv()
        for j in range(n_pieces):
            trade_w(j).wait_recv()

        n_dy = part_dy.shape[0]
        scatter_y = Scatter(place, part_dy, far_dy, None, y_send, y_recv)

        def first_dy(lhs, wbuf, pst):
            loads = pair_rows(place, nb, rows, g_out, g_p, lhs, ld_sem)
            for c in loads:
                c.start()
            dy = DyChunks(lhs, wbuf, (wq_hbm, wk_hbm, wv_hbm, wq_p, wk_p, wv_p), c_sem)
            for c in dy.loads(0):
                c.start()
            for c in loads:
                c.wait()

            def body(j, _):
                @pl.when(j + 1 < n_dy)
                def _():
                    for c in dy.loads(j + 1):
                        c.start()

                for c in dy.loads(j):
                    c.wait()
                store = pltpu.make_async_copy(pst, part_dy.at[j], go_sem.at[0])

                @pl.when(j >= 1)
                def _():
                    store.wait()
                    scatter_y.start_far(j - 1)

                for d in range(2):
                    z = dy.dot(j, d)
                    pst[2 * d] = z[:nb * rows]
                    pst[2 * d + 1] = z[nb * rows:]
                store.start()
                return 0

            lax.fori_loop(0, n_dy, body, 0)
            pltpu.make_async_copy(pst, part_dy.at[n_dy - 1], go_sem.at[0]).wait()
            scatter_y.start_far(n_dy - 1)

        pl.run_scoped(first_dy, pltpu.VMEM((4 * nb * rows, 6 * cols), BF16), pltpu.VMEM((2, CHUNK, 6 * cols), BF16),
                      pltpu.VMEM((4, nb * rows, CHUNK), BF16))
        scatter_end(scatter, proj_out, out_sem, nc)
        for b in range(nb):
            trade(b).wait_send()
        for j in range(n_pieces):
            trade_w(j).wait_send()
        for j in range(n_dy):
            for idx in (0, 1):
                scatter_y.message(j, idx).wait()


def attn_bwd_call(n, q, k, q_rot, k_rot, v, d_attn, o_t, o32, lse, gains, cos_tab, sin_tab, ss, part, far, d_full, w_q, w_k, w_v, wq_p):
    nb, tokens, cols = q.shape
    dim = d_full.shape[2]
    heads = cols // HEAD_DIM
    rows = tokens // n
    steps = nb * heads
    shape = jax.ShapeDtypeStruct
    dma = pltpu.SemaphoreType.DMA
    any_spec = pl.BlockSpec(memory_space=pl.ANY)

    def head_of(i):
        i = jnp.minimum(i, steps - 1)
        return i // heads, i % heads

    blk = pl.BlockSpec((1, tokens, HEAD_DIM), lambda i: (head_of(i)[0], 0, head_of(i)[1]))
    vec = pl.BlockSpec((2, HEAD_DIM), lambda i: (0, head_of(i)[1]))
    out_vec = pl.BlockSpec((1, 1, HEAD_DIM), lambda i: (head_of(i)[0], 0, head_of(i)[1]))
    tab = pl.BlockSpec((tokens, HEAD_DIM), lambda i: (0, 0))
    whole = (nb, tokens, cols)
    lane_tile = pltpu.VMEM((tokens, HEAD_DIM), F32)
    n_dy = min(EARLY_DY, dim // CHUNK)
    return pl.pallas_call(
        functools.partial(attn_bwd_kernel, n, nb, heads, dim), name="attn_bwd", grid=(steps + 1,),
        out_shape=[shape((nb, rows, dim), BF16), shape((nb, tokens, 3 * cols), BF16), shape((nb, tokens, 3 * cols), BF16),
                   shape(whole, F32), shape(whole, F32), shape((cols, dim), BF16),
                   shape(w_k.shape, BF16), shape(w_v.shape, BF16), shape((n_dy,) + part.shape[1:], BF16), shape((n_dy,) + far.shape[1:], BF16),
                   shape((nb, 1, cols), F32), shape((nb, 1, cols), F32)],
        in_specs=[blk] * 8 + [vec, tab, tab, pl.BlockSpec(ss.shape, lambda i: (0, 0))] + [any_spec] * 10,
        out_specs=[any_spec] * 10 + [out_vec, out_vec],
        scratch_shapes=Scatter.scratch(nb * rows, dim) + [lane_tile] * 4 + [pltpu.VMEM((tokens, tokens), BF16)] * 2 + [
            lane_tile, pltpu.VMEM((2, tokens, HEAD_DIM), F32), pltpu.VMEM((2, tokens, HEAD_DIM), F32),
            pltpu.VMEM((2, tokens, HEAD_DIM), BF16), pltpu.VMEM((nb, 8, tokens), F32), pltpu.VMEM((8, tokens), F32),
            pltpu.VMEM((nb, n, 8, tokens), F32), pltpu.VMEM((4, min(256, tokens), cols), F32), pltpu.VMEM((min(256, tokens), 2 * cols), BF16),
            pltpu.VMEM((4, tokens, HEAD_DIM), F32),
            dma((2,)), dma((2, 2)), dma((2, 3)), dma((4,)), dma((2,)), dma((nb,)), dma((nb, n)), dma((nb, n)), dma((8,)), dma((8,)),
            dma((nb, n // 2)), dma((nb, n // 2)), dma((2, 6)), dma((n_dy, 6)), dma((n_dy, 6))],
        compiler_params=params("arbitrary", collective_id=2, has_side_effects=True),
        cost_estimate=cost(4 * nb * tokens * dim * cols + 36 * nb * tokens * tokens * cols, 30 * nb * tokens * cols),
    )(q, k, q_rot, k_rot, v, d_attn, o32, lse, gains, cos_tab, sin_tab, ss, q, k, o_t, part, far, d_full, w_q, w_k, w_v, wq_p)


def dy_dw_kernel(n, nb, dim, g_hbm, g_p, wq_hbm, wk_hbm, wv_hbm, wq_p, wk_p, wv_p, y_full, part_in, far_in,
                 dy_out, dwq_out, dwk_out, dwv_out,
                 part, recv_far, recv_side, s_send, s_recv, g, ld_sem, w_sem, y_sem, o_sem, out_sem):
    tokens = g_hbm.shape[1]
    rows = tokens // n
    cols = g_hbm.shape[2] // 3
    nc = dim // CHUNK
    early = far_in.shape[0]
    lag = 3
    place = Place(n)
    scatter = Scatter(place, part, recv_far, recv_side, s_send, s_recv, early=early)
    stored = [pltpu.make_async_copy(part_in, part.at[pl.ds(0, early)], ld_sem.at[2]),
              pltpu.make_async_copy(far_in, recv_far.at[pl.ds(0, early)], ld_sem.at[3])]
    load_g = pltpu.make_async_copy(g_hbm, g, ld_sem.at[4])

    def chain(lhs, wbuf):
        loads = pair_rows(place, nb, rows, g_hbm, g_p, lhs, ld_sem)
        dy = DyChunks(lhs, wbuf, (wq_hbm, wk_hbm, wv_hbm, wq_p, wk_p, wv_p), w_sem)
        if early < nc:
            for c in dy.loads(early):
                c.start()
            for c in loads[:len(loads) // 2]:
                c.start()
        for c in stored:
            c.start()
        if early < nc:
            for c in loads[len(loads) // 2:]:
                c.start()
        place.barrier(place.near()[:2])
        for c in stored:
            c.wait()
        lax.fori_loop(0, early, scatter.sums_step, 0)
        load_g.start()

        def body(j, _):
            @pl.when(j + 1 < nc)
            def _():
                for c in dy.loads(j + 1):
                    c.start()

            for c in dy.loads(j):
                c.wait()
            for d in range(2):
                @pl.when(j == early)
                def _(d=d):
                    for c in loads[d * len(loads) // 2:(d + 1) * len(loads) // 2]:
                        c.wait()

                z = dy.dot(j, d)
                part[j, 2 * d] = z[:nb * rows]
                part[j, 2 * d + 1] = z[nb * rows:]
                if d == 0:
                    scatter.start_far(j)

            @pl.when(j >= early + lag)
            def _():
                scatter.sums(j - lag)

            return 0

        lax.fori_loop(early, nc, body, 0)
        lax.fori_loop(0, nc, scatter.start_side, 0)

    pl.run_scoped(chain, pltpu.VMEM((4 * nb * rows, 6 * cols), BF16), pltpu.VMEM((2, CHUNK, 6 * cols), BF16))

    def weight_grad(ybuf, wst):
        bm = min(512, dim)
        n_chunks = dim // bm

        def chunk(c):
            slot = lax.rem(c, 2)
            return pltpu.make_async_copy(y_full.at[:, :, pl.ds(pl.multiple_of(c * bm, bm), bm)], ybuf.at[slot], y_sem.at[slot])

        def store(c):
            slot = lax.rem(c, 2)
            dst = pl.ds(pl.multiple_of(c * bm, bm), bm)
            return [pltpu.make_async_copy(wst.at[slot, :, pl.ds(m * cols, cols)], out.at[dst], o_sem.at[slot, m])
                    for m, out in enumerate((dwq_out, dwk_out, dwv_out))]

        chunk(0).start()
        load_g.wait()

        def body(c, _):
            slot = lax.rem(c, 2)

            @pl.when(c + 1 < n_chunks)
            def _():
                chunk(c + 1).start()

            @pl.when(c >= 2)
            def _():
                for s in store(c):
                    s.wait()

            chunk(c).wait()
            for m in range(lag):
                late = max(nc - lag, early) + m
                if late < nc:
                    pl.when(c == min(m, n_chunks - 1))(functools.partial(scatter.sums, late))
            wst[slot] = lax.dot_general(ybuf[slot].reshape(nb * tokens, bm), g[...].reshape(nb * tokens, 3 * cols), TN,
                                        preferred_element_type=F32).astype(BF16)
            for s in store(c):
                s.start()
            return 0

        lax.fori_loop(0, n_chunks, body, 0)
        for s in range(min(2, n_chunks)):
            for c in store(s):
                c.wait()

    bm = min(512, dim)
    pl.run_scoped(weight_grad, pltpu.VMEM((2, nb, tokens, bm), BF16), pltpu.VMEM((2, bm, 3 * cols), BF16))
    scatter_end(scatter, dy_out, out_sem, nc)


def dy_dw_call(n, g, g_p, w_q, w_k, w_v, wq_p, wk_p, wv_p, y_full, part, far):
    nb, tokens, wide = g.shape
    dim = y_full.shape[2]
    cols = wide // 3
    rows = tokens // n
    shape = jax.ShapeDtypeStruct
    dma = pltpu.SemaphoreType.DMA
    any_spec = pl.BlockSpec(memory_space=pl.ANY)
    return pl.pallas_call(
        functools.partial(dy_dw_kernel, n, nb, dim), name="dy_dw",
        out_shape=[shape((nb, rows, dim), BF16)] + [shape((dim, cols), BF16)] * 3,
        in_specs=[any_spec] * 11, out_specs=[any_spec] * 4,
        scratch_shapes=Scatter.scratch(nb * rows, dim) + [pltpu.VMEM((nb, tokens, 3 * cols), BF16), dma((5,)), dma((2, 6)), dma((2,)), dma((2, 3)), dma((nb,))],
        compiler_params=params(collective_id=3, has_side_effects=True),
        cost_estimate=cost(12 * nb * tokens * dim * cols, 30 * nb * tokens * cols),
    )(g, g_p, w_q, w_k, w_v, wq_p, wk_p, wv_p, y_full, part, far)


def token_kernel(n_copies, x_ref, dy_ref, pr_ref, g_ref, m_ref, e_ref, bo_ref, gq_ref, gk_ref, *refs):
    srcs, (xo_ref, dx_ref, dm_ref, dgq_ref, dgk_ref), dsts = refs[:4], refs[4:9], refs[9:13]
    bufs, (acc, in_sem, out_sem) = refs[13:17], refs[17:]
    group = 16
    step = pl.program_id(0)
    rows = x_ref.shape[1]
    groups = rows // group
    depth = bufs[0].shape[0]
    lag = depth - 1

    def move(c, out):
        copies = []
        for j, (src, dst, buf) in enumerate(zip(srcs, dsts, bufs)):
            size = buf.shape[1]
            sl = pl.ds(pl.multiple_of(c * size, 16), size)
            slot = lax.rem(c, depth)
            copies.append(pltpu.make_async_copy(buf.at[slot], dst.at[sl], out_sem.at[slot, j]) if out
                          else pltpu.make_async_copy(src.at[sl], buf.at[slot], in_sem.at[slot, j]))
        return copies

    def advance(i):
        @pl.when(i < n_copies)
        def _():
            @pl.when(i >= depth)
            def _():
                for c in move(i - depth, True):
                    c.wait()

            for c in move(i, False):
                c.start()

        @pl.when((i >= lag) & (i < n_copies + lag))
        def _():
            for c in move(i - lag, False):
                c.wait()
            for c in move(i - lag, True):
                c.start()

    mod = m_ref[...] + e_ref[0]
    for src, dst in ((gq_ref, dgq_ref), (gk_ref, dgk_ref)):
        dst[...] = jnp.sum(src[...], axis=(0, 1))
    shift_bo = bo_ref[...].reshape(1, bo_ref.shape[0])
    acc[...] = jnp.zeros_like(acc)

    def body(r, _):
        advance(step * groups + r)
        sl = pl.ds(pl.multiple_of(r * group, group), group)
        x = x_ref[0, sl].astype(F32)
        d_out = dy_ref[0, sl].astype(F32)
        proj = pr_ref[0, sl].astype(F32) + shift_bo
        xo_ref[0, sl] = (x + mod[2:3] * proj).astype(BF16)
        gate_part = d_out * proj
        x_norm, inv_std = norm_stats(x)
        d_y = g_ref[0, sl].astype(F32)
        d_norm = d_y * (1.0 + mod[1:2])
        d_x = d_out + inv_std * (
            d_norm - jnp.mean(d_norm, axis=-1, keepdims=True) - x_norm * jnp.mean(d_norm * x_norm, axis=-1, keepdims=True))
        dx_ref[0, sl] = d_x.astype(BF16)
        scale_part = d_y * x_norm
        acc[0] += d_y[:8] + d_y[8:]
        acc[1] += scale_part[:8] + scale_part[8:]
        acc[2] += gate_part[:8] + gate_part[8:]
        return 0

    lax.fori_loop(0, groups, body, 0)
    for j in range(3):
        dm_ref[0, j:j + 1] = jnp.sum(acc[j], axis=0, keepdims=True)

    @pl.when(step == pl.num_programs(0) - 1)
    def _():
        total = pl.num_programs(0) * groups

        def rest(i, _):
            advance(i)
            return 0

        lax.fori_loop(total, jnp.maximum(total, n_copies + lag), rest, 0)
        for c in range(max(n_copies - depth, 0), n_copies):
            for copy in move(c, True):
                copy.wait()


def token_call(x_loc, dy_loc, proj, d_y, m_block, e_loc, b_o, d_gq, d_gk, grads):
    nb, rows, dim = x_loc.shape
    n_copies = dim // min(512, dim)
    row = pl.BlockSpec((1, rows, dim), lambda i: (i, 0, 0))
    mod = pl.BlockSpec((1, 3, dim), lambda i: (i, 0, 0))
    any_spec = pl.BlockSpec(memory_space=pl.ANY)
    dma = pltpu.SemaphoreType.DMA
    depth = 4
    return pl.pallas_call(
        functools.partial(token_kernel, n_copies), name="tokens", grid=(nb,),
        out_shape=[jax.ShapeDtypeStruct(x_loc.shape, BF16), jax.ShapeDtypeStruct(x_loc.shape, BF16),
                   jax.ShapeDtypeStruct((nb, 3, dim), F32)] + [jax.ShapeDtypeStruct(d_gq.shape[2:], F32)] * 2 + [jax.ShapeDtypeStruct(w.shape, BF16) for w in grads],
        in_specs=[row, row, row, row, pl.BlockSpec((3, dim), lambda i: (0, 0)), mod] + [pl.BlockSpec(memory_space=pltpu.VMEM)] * 3 + [any_spec] * 4,
        out_specs=[row, row, mod] + [pl.BlockSpec(memory_space=pltpu.VMEM)] * 2 + [any_spec] * 4,
        scratch_shapes=[pltpu.VMEM((depth, w.shape[0] // n_copies, w.shape[1]), BF16) for w in grads]
        + [pltpu.VMEM((3, 8, dim), F32), dma((depth, 4)), dma((depth, 4))],
        compiler_params=params("arbitrary"),
        cost_estimate=cost(nb * rows * dim * 30, nb * rows * dim * 12),
    )(x_loc, dy_loc, proj, d_y, m_block, e_loc, b_o, d_gq, d_gk, *grads)


def solution(mesh):
    tp_size = mesh.shape['tp']

    def device_step(x_loc, e_loc, m_block, w_q, b_q, w_k, b_k, w_v, b_v, w_o, b_o, g_q, g_k, pos_part, dy_loc):
        nb, _, dim = x_loc.shape
        y_full, d_own, q, k, v, wo_p, wo_t, ss, cos_tab, sin_tab, gains = gather_qkv_call(
            tp_size, x_loc, dy_loc, m_block, e_loc, w_q, w_k, w_v, w_o, b_q, b_k, b_v, g_q, g_k, pos_part)
        d_full, _, _, d_attn, wq_p, part, far, o_t, q_rot, k_rot, lse, o32 = gather_attn_call(
            tp_size, q, k, v, gains, cos_tab, sin_tab, ss, w_q, w_o, wo_p, wo_t, d_own)
        proj, g, g_p, _, _, d_wo, wk_p, wv_p, part, far, d_gq, d_gk = attn_bwd_call(
            tp_size, q, k, q_rot, k_rot, v, d_attn, o_t, o32, lse, gains, cos_tab, sin_tab, ss, part, far, d_full, w_q, w_k, w_v, wq_p)
        d_y, d_wq, d_wk, d_wv = dy_dw_call(tp_size, g, g_p, w_q, w_k, w_v, wq_p, wk_p, wv_p, y_full, part, far)
        x_out, d_x, d_mod, d_gq, d_gk, d_wq, d_wk, d_wv, d_wo = token_call(
            x_loc, dy_loc, proj, d_y, m_block, e_loc, b_o, d_gq, d_gk, (d_wq, d_wk, d_wv, d_wo))
        d_e = all_sum_call(tp_size, d_mod.reshape(tp_size, -1, HEAD_DIM)).reshape(nb, 3, dim)
        return x_out, d_x, d_e, jnp.sum(d_e, axis=0), d_wq, d_wk, d_wv, d_wo, d_gq, d_gk

    in_specs = (P('dp', 'tp', None), P('dp', None, None), P(None, None), P(None, 'tp'), P('tp'), P(None, 'tp'), P('tp'),
                P(None, 'tp'), P('tp'), P('tp', None), P(None), P('tp'), P('tp'), P('dp', None), P('dp', 'tp', None))
    out_specs = (P('dp', 'tp', None), P('dp', 'tp', None), P('dp', None, None), P('dp', None), P('dp', 'tp'), P('dp', 'tp'),
                 P('dp', 'tp'), P(('dp', 'tp'), None), P(('dp', 'tp')), P(('dp', 'tp')))
    return jax.shard_map(device_step, mesh=mesh, in_specs=in_specs, out_specs=out_specs, check_vma=False)
```

```python
import functools

import jax
import jax.numpy as jnp
import numpy as np
from jax import lax
from jax.experimental import pallas as pl
from jax.experimental.pallas import tpu as pltpu
from jax.sharding import PartitionSpec as P

HEAD_DIM = 128
EPS_NORM = 1e-6
ROPE_BASE = 10000.0
LOG2E = 1.4426950408889634
CHUNK = 512
VMEM_LIMIT = 60 * 1024 * 1024
F32 = jnp.float32
BF16 = jnp.bfloat16
MESH_ID = pl.DeviceIdType.MESH
NT = (((1,), (1,)), ((), ()))
TN = (((0,), (0,)), ((), ()))


def params(*semantics, **kw):
    return pltpu.CompilerParams(dimension_semantics=semantics or None, vmem_limit_bytes=VMEM_LIMIT, **kw)


def cost(flops, nbytes):
    return pl.CostEstimate(flops=int(flops), bytes_accessed=int(nbytes), transcendentals=0)


def rope_freqs():
    half_dim = HEAD_DIM // 2
    side_len = HEAD_DIM // 6
    first_len = half_dim - 2 * side_len
    pair_idx = np.arange(HEAD_DIM) // 2
    section = (pair_idx >= first_len).astype(np.int32) + (pair_idx >= first_len + side_len).astype(np.int32)
    offset = np.where(section == 0, 0, np.where(section == 1, first_len, first_len + side_len))
    sec_width = np.where(section == 0, first_len, side_len)
    exponent = -(pair_idx - offset).astype(np.float32) / sec_width.astype(np.float32)
    freq_vals = np.power(np.float32(ROPE_BASE), exponent)
    return np.where(section[None, :] == np.arange(3)[:, None], freq_vals[None, :], np.float32(0.0)).astype(np.float32)


def norm_stats(x):
    centered = x - jnp.mean(x, axis=-1, keepdims=True)
    inv_std = lax.rsqrt(jnp.mean(centered * centered, axis=-1, keepdims=True) + EPS_NORM)
    return centered * inv_std, inv_std


def to_row(acc):
    return jnp.sum(acc.T, axis=0, keepdims=True)


def lanes_of(row):
    return jnp.broadcast_to(row, (HEAD_DIM, row.shape[1])).T


def head_sum(values):
    out = values[:, :HEAD_DIM]
    for h in range(1, values.shape[1] // HEAD_DIM):
        out = out + values[:, h * HEAD_DIM:(h + 1) * HEAD_DIM]
    return out


class Place:
    def __init__(self, n):
        self.n = n
        self.me = lax.axis_index('tp')
        self.right = lax.rem(self.me + 2, n)
        self.left = lax.rem(self.me + n - 2, n)
        self.far = lax.rem(self.me + n // 2, n)
        self.chip = self.me // 2

    def partner(self, dev):
        return dev + 1 - 2 * lax.rem(dev, 2)

    def arrive(self, devices):
        for dev in devices:
            pl.semaphore_signal(pltpu.get_barrier_semaphore(), inc=1, device_id={'tp': dev}, device_id_type=MESH_ID)

    def barrier(self, devices):
        self.arrive(devices)
        pl.semaphore_wait(pltpu.get_barrier_semaphore(), len(devices))

    def to_partner(self, src, dst, send_sem, recv_sem):
        return pltpu.make_async_remote_copy(src_ref=src, dst_ref=dst, send_sem=send_sem, recv_sem=recv_sem,
                                            device_id={'tp': self.partner(self.me)}, device_id_type=MESH_ID)

    def everyone(self):
        return [lax.rem(self.me + d, self.n) for d in range(1, self.n)]

    def near(self):
        return [self.right, self.left, self.partner(self.me)]


class Gather:
    def __init__(self, place, full, rows, send, recv, early=0):
        self.at, self.full, self.rows, self.send, self.recv, self.early = place, full, rows, send, recv, early

    def part(self, b, dev, off, count):
        return self.full.at[b, pl.ds(pl.multiple_of(dev * self.rows + off, 16), count)]

    def copy(self, b, dev, off, count, s_idx, r_idx, target):
        ref = self.part(b, dev, off, count)
        return pltpu.make_async_remote_copy(src_ref=ref, dst_ref=ref, send_sem=self.send.at[b, s_idx], recv_sem=self.recv.at[b, r_idx],
                                            device_id={'tp': target}, device_id_type=MESH_ID)

    def start_own(self, b):
        p = self.at
        self.copy(b, p.me, 0, self.rows, 0, 0, p.right).start()
        self.copy(b, p.me, 0, self.rows, 1, 1, p.left).start()
        self.copy(b, p.me, 0, self.rows, 2, 4, p.partner(p.me)).start()

    def whole_blocks_in(self, b):
        p = self.at
        self.copy(b, p.partner(p.me), 0, self.rows, 2, 4, p.me).wait_recv()
        self.copy(b, p.left, 0, self.rows, 0, 0, p.me).wait_recv()
        self.copy(b, p.right, 0, self.rows, 1, 1, p.me).wait_recv()
        for s_idx in range(3):
            self.copy(b, p.me, 0, self.rows, s_idx, s_idx, p.me).wait_send()

    def pass_left(self, b):
        p, half = self.at, self.rows // 2
        self.copy(b, p.left, 0, half, 3, 2, p.right).start()
        self.copy(b, p.left, 0, self.rows, 5, 5, p.partner(p.me)).start()

    def pass_right(self, b):
        p, half = self.at, self.rows // 2
        self.copy(b, p.right, half, half, 4, 3, p.left).start()
        self.copy(b, p.right, 0, self.rows, 6, 6, p.partner(p.me)).start()

    def finish(self, b):
        p, half = self.at, self.rows // 2
        counts = (self.rows, self.rows, self.rows, half, half, self.rows, self.rows, half, half)
        for s_idx, count in list(enumerate(counts))[3 if b < self.early else 0:]:
            self.copy(b, p.me, 0, count, s_idx, s_idx, p.me).wait_send()

    def item_place(self, i, nb):
        j = i - nb
        b = jnp.where(i < nb, i, jnp.where(i < 3 * nb, j // 2, i - 3 * nb))
        chips = self.at.n // 2
        side = jnp.where(lax.rem(j + 2 * nb, 2) == 0, chips - 1, 1)
        off = jnp.where(i < nb, 0, jnp.where(i < 3 * nb, side, chips // 2))
        return b, pl.multiple_of(lax.rem(self.at.chip + off, chips) * (2 * self.rows), 32)

    def kinds(self, i, nb):
        odd = lax.rem(i + nb, 2)
        side = (i >= nb) & (i < 3 * nb)
        return i < nb, side & (odd == 0), side & (odd == 1), i >= 3 * nb

    def arrive(self, i, nb):
        p, half = self.at, self.rows // 2
        b, _ = self.item_place(i, nb)
        _, is_left, is_right, is_far = self.kinds(i, nb)

        @pl.when(is_left & (b >= self.early))
        def _():
            self.copy(b, p.left, 0, self.rows, 0, 0, p.me).wait_recv()
            self.pass_left(b)

        @pl.when(is_right & (b >= self.early))
        def _():
            self.copy(b, p.right, 0, self.rows, 1, 1, p.me).wait_recv()
            self.pass_right(b)

        @pl.when(is_far)
        def _():
            self.copy(b, p.far, 0, half, 3, 2, p.me).wait_recv()
            self.copy(b, p.far, 0, half, 7, 7, p.partner(p.me)).start()
            self.copy(b, p.far, half, half, 4, 3, p.me).wait_recv()
            self.copy(b, p.far, half, half, 8, 8, p.partner(p.me)).start()

    def ready(self, i, nb):
        p, half = self.at, self.rows // 2
        b, row0 = self.item_place(i, nb)
        is_own, is_left, is_right, is_far = self.kinds(i, nb)

        @pl.when(is_own & (b >= self.early))
        def _():
            self.copy(b, p.partner(p.me), 0, self.rows, 2, 4, p.me).wait_recv()

        @pl.when(is_left)
        def _():
            self.copy(b, p.partner(p.left), 0, self.rows, 5, 5, p.me).wait_recv()

        @pl.when(is_right)
        def _():
            self.copy(b, p.partner(p.right), 0, self.rows, 6, 6, p.me).wait_recv()

        @pl.when(is_far)
        def _():
            self.copy(b, p.partner(p.far), 0, half, 7, 7, p.me).wait_recv()
            self.copy(b, p.partner(p.far), half, half, 8, 8, p.me).wait_recv()

        return b, row0


class RowTrade:
    def __init__(self, place, src, dst, rows, send, recv, rows_of=None):
        self.at, self.src, self.dst, self.rows, self.send, self.recv = place, src, dst, rows, send, recv
        self.batch = range(src.shape[0]) if rows_of is None else rows_of

    def copies(self, parity):
        p = self.at
        for b in self.batch:
            for k in range(p.n // 2):
                sl = pl.ds(pl.multiple_of((2 * k + parity) * self.rows, 16), self.rows)
                yield p.to_partner(self.src.at[b, sl], self.dst.at[b, sl], self.send.at[b, k], self.recv.at[b, k])

    def start(self):
        for c in self.copies(1 - lax.rem(self.at.me, 2)):
            c.start()

    def wait_recv(self):
        for c in self.copies(lax.rem(self.at.me, 2)):
            c.wait_recv()

    def wait_send(self):
        for c in self.copies(1 - lax.rem(self.at.me, 2)):
            c.wait_send()


GATHER_SEMS = 9
EARLY_ROWS = 1
EARLY_CHUNKS = 3
EARLY_DY = 5


def chunks_of(width, step):
    return [(c, min(c + step, width)) for c in range(0, width, step)]


class Exchange:
    def __init__(self, place, x_ref, slots, send_sems, recv_sems):
        self.at, self.x, self.slots, self.send, self.recv = place, x_ref, slots, send_sems, recv_sems

    def copy(self, d, dev, src):
        return pltpu.make_async_remote_copy(src_ref=self.x, dst_ref=self.slots.at[src], send_sem=self.send.at[d], recv_sem=self.recv.at[src],
                                            device_id={'tp': dev}, device_id_type=MESH_ID)

    def start(self):
        for d, dev in enumerate(self.at.everyone()):
            self.copy(d, dev, self.at.me).start()
        self.slots[self.at.me] = self.x[...]

    def finish(self):
        for d, dev in enumerate(self.at.everyone()):
            self.copy(d, dev, dev).wait()
        total = self.slots[0]
        for d in range(1, self.at.n):
            total = total + self.slots[d]
        return total


def gather_qkv_kernel(n, x_ref, dy_ref, m_ref, e_ref, wq_ref, wk_ref, wv_ref, wo_ref, bq_ref, bk_ref, bv_ref, gq_ref, gk_ref, pos_ref,
                      freq_ref, y_full, d_full, q_out, k_out, v_out, wo_p, wo_t, ss_ref, cos_ref, sin_ref, gain_ref,
                      bias_ref, w_all, xin, stage, xbuf, zst, vst, sq, ss_row, slots, wo_in, wo_st, wo_sem,
                      w_sem, in_sem, st_sem, ld_sem, out_sem, g_send, g_recv, d_send, d_recv, e_send, e_recv, t_send, t_recv):
    nb, rows, dim = x_ref.shape
    cols = wq_ref.shape[1]
    place = Place(n)
    gather = Gather(place, y_full, rows, g_send, g_recv)
    gather_d = Gather(place, d_full, rows, d_send, d_recv)
    w_copies = [pltpu.make_async_copy(w, w_all.at[:, pl.ds(j * cols, cols)], w_sem.at[j]) for j, w in enumerate((wq_ref, wk_ref, wv_ref))]
    place.arrive(place.everyone())
    trade = place.to_partner(wo_ref, wo_p, t_send, t_recv)

    def load_x(b):
        return pltpu.make_async_copy(x_ref.at[b], xin.at[b], in_sem.at[b])

    for b in range(nb):
        load_x(b).start()
    for c in w_copies:
        c.start()
    group = 16

    def mine(full, b):
        return full.at[b, pl.ds(pl.multiple_of(place.me * rows, 16), rows)]

    def ln_step(b, _):
        load_x(b).wait()
        shift = m_ref[0:1] + e_ref[b, 0:1]
        scale_one = 1.0 + (m_ref[1:2] + e_ref[b, 1:2])

        def ln_rows(r, _):
            sl = pl.ds(pl.multiple_of(r * group, group), group)
            x_norm, _ = norm_stats(xin[b, sl].astype(F32))
            stage[b, sl] = (x_norm * scale_one + shift).astype(BF16)
            return 0

        lax.fori_loop(0, rows // group, ln_rows, 0)
        out = pltpu.make_async_copy(stage.at[b], mine(y_full, b), st_sem)
        out.start()

        @pl.when(b == 0)
        def _():
            pl.semaphore_wait(pltpu.get_barrier_semaphore(), n - 1)

        out.wait()
        gather.start_own(b)
        return 0

    lax.fori_loop(0, nb, ln_step, 0)
    load_dy = pltpu.make_async_copy(dy_ref, xin, in_sem.at[0])
    load_dy.start()
    for j, ref in enumerate((bq_ref, bk_ref, bv_ref)):
        bias_ref[:, j * cols:(j + 1) * cols] = ref[...].reshape(1, cols)
    for j, ref in enumerate((gq_ref, gk_ref)):
        gain_ref[j:j + 1] = ref[...].reshape(1, cols)

    def tables():
        lane = lax.broadcasted_iota(jnp.int32, (128, HEAD_DIM), 1)

        def rows_of(r, _):
            sl = pl.ds(pl.multiple_of(r * 128, 128), 128)
            pos = [lanes_of(pos_ref[m:m + 1, sl].astype(F32)) for m in range(3)]
            angle = pos[0] * freq_ref[0:1] + pos[1] * freq_ref[1:2] + pos[2] * freq_ref[2:3]
            cos_ref[sl] = jnp.cos(angle)
            sin_ref[sl] = jnp.where(lane % 2 == 0, -1.0, 1.0) * jnp.sin(angle)
            return 0

        lax.fori_loop(0, pos_ref.shape[1] // 128, rows_of, 0)

    def turn_wo():
        width = wo_in.shape[2]
        n_chunks = dim // width

        def load(c):
            slot = lax.rem(c, 2)
            return pltpu.make_async_copy(wo_ref.at[:, pl.ds(pl.multiple_of(c * width, width), width)], wo_in.at[slot], wo_sem.at[slot, 0])

        def store(c):
            slot = lax.rem(c, 2)
            return pltpu.make_async_copy(wo_st.at[slot], wo_t.at[pl.ds(pl.multiple_of(c * width, width), width)], wo_sem.at[slot, 1])

        load(0).start()

        def body(c, _):
            slot = lax.rem(c, 2)

            @pl.when(c + 1 < n_chunks)
            def _():
                load(c + 1).start()

            @pl.when(c >= 2)
            def _():
                store(c).wait()

            load(c).wait()
            wo_st[slot] = wo_in[slot].T
            store(c).start()
            return 0

        lax.fori_loop(0, n_chunks, body, 0)
        for c in range(min(2, n_chunks)):
            store(c).wait()

    def gate_step(b, _):
        gate = m_ref[2:3] + e_ref[b, 2:3]

        def gate_rows(r, _):
            sl = pl.ds(pl.multiple_of(r * group, group), group)
            stage[b, sl] = (xin[b, sl].astype(F32) * gate).astype(BF16)
            return 0

        lax.fori_loop(0, rows // group, gate_rows, 0)
        out = pltpu.make_async_copy(stage.at[b], mine(d_full, b), st_sem)
        out.start()
        out.wait()
        return 0

    for c in w_copies:
        c.wait()

    def outputs(b, row0, slot):
        dst = pl.ds(row0, 2 * rows)
        return [pltpu.make_async_copy(zst.at[slot, :, pl.ds(0, cols)], q_out.at[b, dst], out_sem.at[slot, 0]),
                pltpu.make_async_copy(zst.at[slot, :, pl.ds(cols, cols)], k_out.at[b, dst], out_sem.at[slot, 1]),
                pltpu.make_async_copy(vst.at[slot], v_out.at[b, dst], out_sem.at[slot, 2])]

    def load(b, row0, slot):
        return pltpu.make_async_copy(y_full.at[b, pl.ds(row0, 2 * rows)], xbuf.at[slot], ld_sem.at[slot])

    load(*gather.ready(0, nb), 0).start()

    def item(i, _):
        slot = lax.rem(i, 2)
        b, row0 = gather.item_place(i, nb)

        @pl.when(i + 1 < 4 * nb)
        def _():
            gather.arrive(i + 1, nb)

        @pl.when(i + 1 == 3 * nb - 1)
        def _():
            for d in range(EARLY_ROWS):
                gather_d.start_own(d)

        @pl.when(i == nb)
        def _():
            load_dy.wait()
            trade.start()
            lax.fori_loop(0, nb, gate_step, 0)
            tables()
            turn_wo()

        @pl.when(i >= 2)
        def _():
            for c in outputs(0, 0, slot):
                c.wait()

        load(0, 0, slot).wait()
        spans = chunks_of(3 * cols, 512)
        for m, (lo, hi) in enumerate(spans):
            if m == len(spans) - 1:
                @pl.when(i + 1 < 4 * nb)
                def _():
                    load(*gather.ready(i + 1, nb), lax.rem(i + 1, 2)).start()

            zst[slot, :, lo:hi] = jnp.dot(xbuf[slot], w_all[:, lo:hi], preferred_element_type=F32) + bias_ref[:, lo:hi]
        vst[slot] = zst[slot, :, 2 * cols:].astype(BF16)
        q = zst[slot, :, :cols]
        k = zst[slot, :, cols:2 * cols]
        sq[2 * b, pl.ds(row0, 2 * rows)] = head_sum(q * q)
        sq[2 * b + 1, pl.ds(row0, 2 * rows)] = head_sum(k * k)
        for c in outputs(b, row0, slot):
            c.start()
        return 0

    lax.fori_loop(0, 4 * nb, item, 0)
    ss_row[...] = jnp.zeros_like(ss_row)
    for j in range(2 * nb):
        ss_row[j:j + 1] = to_row(sq[j])
    sums = Exchange(place, ss_row, slots, e_send, e_recv)
    sums.start()
    for slot in range(2):
        for c in outputs(0, 0, slot):
            c.wait()
    for b in range(nb):
        gather.finish(b)
    for d in range(EARLY_ROWS):
        gather_d.whole_blocks_in(d)
    trade.wait()
    ss_ref[...] = sums.finish()


def gather_qkv_call(n, x_loc, dy_loc, m_block, e_loc, w_q, w_k, w_v, w_o, b_q, b_k, b_v, g_q, g_k, positions):
    nb, rows, dim = x_loc.shape
    cols = w_q.shape[1]
    tokens = rows * n
    shape = jax.ShapeDtypeStruct
    any_spec = pl.BlockSpec(memory_space=pl.ANY)
    vmem = pl.BlockSpec(memory_space=pltpu.VMEM)
    dma = pltpu.SemaphoreType.DMA
    stat_rows = -(-2 * nb // 8) * 8
    return pl.pallas_call(
        functools.partial(gather_qkv_kernel, n), name="gather_qkv",
        out_shape=[shape((nb, tokens, dim), BF16), shape((nb, tokens, dim), BF16), shape((nb, tokens, cols), F32),
                   shape((nb, tokens, cols), F32), shape((nb, tokens, cols), BF16), shape(w_o.shape, BF16), shape((dim, cols), BF16), shape((stat_rows, tokens), F32),
                   shape((tokens, HEAD_DIM), F32), shape((tokens, HEAD_DIM), F32), shape((2, cols), F32)],
        in_specs=[any_spec, any_spec, vmem, vmem] + [any_spec] * 4 + [vmem] * 7,
        out_specs=[any_spec] * 7 + [vmem] * 4,
        scratch_shapes=[
            pltpu.VMEM((1, 3 * cols), F32),
            pltpu.VMEM((dim, 3 * cols), BF16), pltpu.VMEM((nb, rows, dim), BF16), pltpu.VMEM((nb, rows, dim), BF16),
            pltpu.VMEM((2, 2 * rows, dim), BF16), pltpu.VMEM((2, 2 * rows, 3 * cols), F32), pltpu.VMEM((2, 2 * rows, cols), BF16),
            pltpu.VMEM((2 * nb, tokens, HEAD_DIM), F32), pltpu.VMEM((stat_rows, tokens), F32), pltpu.VMEM((n, stat_rows, tokens), F32),
            pltpu.VMEM((2, cols, min(512, dim)), BF16), pltpu.VMEM((2, min(512, dim), cols), BF16), dma((2, 2)),
            dma((3,)), dma((nb,)), dma, dma((2,)), dma((2, 3)), dma((nb, GATHER_SEMS)), dma((nb, GATHER_SEMS)),
            dma((EARLY_ROWS, GATHER_SEMS)), dma((EARLY_ROWS, GATHER_SEMS)), dma((n,)), dma((n,)), dma, dma],
        compiler_params=params(collective_id=0, has_side_effects=True),
        cost_estimate=cost(6 * nb * tokens * dim * cols, 6 * dim * cols + 14 * nb * tokens * cols),
    )(x_loc, dy_loc, m_block, e_loc, w_q, w_k, w_v, w_o, b_q, b_k, b_v, g_q, g_k, positions.T, jnp.asarray(rope_freqs()))


def all_sum_kernel(n, x_ref, o_ref, pieces, total, send_a, recv_a, send_b, recv_b):
    place = Place(n)
    me = place.me
    place.barrier(place.everyone())

    def first(d, dev, src):
        return pltpu.make_async_remote_copy(src_ref=x_ref.at[src], dst_ref=pieces.at[me], send_sem=send_a.at[d], recv_sem=recv_a.at[me],
                                            device_id={'tp': dev}, device_id_type=MESH_ID)

    for d, dev in enumerate(place.everyone()):
        first(d, dev, dev).start()
    pieces[me] = x_ref[me]
    for d, dev in enumerate(place.everyone()):
        pltpu.make_async_remote_copy(src_ref=x_ref.at[me], dst_ref=pieces.at[dev], send_sem=send_a.at[d], recv_sem=recv_a.at[dev],
                                     device_id={'tp': dev}, device_id_type=MESH_ID).wait_recv()
    acc = pieces[0]
    for d in range(1, n):
        acc = acc + pieces[d]
    total[...] = acc
    o_ref[me] = acc
    for d, dev in enumerate(place.everyone()):
        first(d, dev, dev).wait_send()
    for d, dev in enumerate(place.everyone()):
        pltpu.make_async_remote_copy(src_ref=total, dst_ref=o_ref.at[me], send_sem=send_b.at[d], recv_sem=recv_b.at[me],
                                     device_id={'tp': dev}, device_id_type=MESH_ID).start()
    for d, dev in enumerate(place.everyone()):
        copy = pltpu.make_async_remote_copy(src_ref=total, dst_ref=o_ref.at[dev], send_sem=send_b.at[d], recv_sem=recv_b.at[dev],
                                            device_id={'tp': dev}, device_id_type=MESH_ID)
        copy.wait_send()
        copy.wait_recv()


def all_sum_call(n, x):
    spec = pl.BlockSpec(memory_space=pltpu.VMEM)
    dma = pltpu.SemaphoreType.DMA
    return pl.pallas_call(
        functools.partial(all_sum_kernel, n), name="all_sum",
        out_shape=jax.ShapeDtypeStruct(x.shape, x.dtype), in_specs=[spec], out_specs=spec,
        scratch_shapes=[pltpu.VMEM(x.shape, x.dtype), pltpu.VMEM(x.shape[1:], x.dtype), dma((n,)), dma((n,)), dma((n,)), dma((n,))],
        compiler_params=pltpu.CompilerParams(collective_id=4, has_side_effects=True, vmem_limit_bytes=4 * 1024 * 1024),
        cost_estimate=cost(4_000_000_000, x.size * 8),
    )(x)


def swap_pairs(x):
    lane = lax.broadcasted_iota(jnp.int32, x.shape, 1)
    return jnp.where(lane % 2 == 0, pltpu.roll(x, HEAD_DIM - 1, 1), pltpu.roll(x, 1, 1))


def rotate(x, cos, sin):
    return x * cos + swap_pairs(x) * sin


SCORE_SCALE = HEAD_DIM ** -0.5 * LOG2E


def softmax_block(s):
    top = jnp.max(s, axis=1, keepdims=True)
    p = jnp.exp2(s * SCORE_SCALE - top * SCORE_SCALE)
    total = jnp.sum(p, axis=1, keepdims=True)
    return p * (1.0 / total), top * SCORE_SCALE + jnp.log(total) * LOG2E


class Scatter:
    def __init__(self, place, part, recv_far, recv_side, send, recv, far_src=None, early=0):
        self.at, self.part, self.far, self.side, self.send, self.recv = place, part, recv_far, recv_side, send, recv
        self.far_src, self.early = part if far_src is None else far_src, early
        self.rows = part.shape[2]
        self.half = self.rows // 2

    def copy(self, j, idx, src, dst, target):
        return pltpu.make_async_remote_copy(src_ref=src, dst_ref=dst, send_sem=self.send.at[j, idx], recv_sem=self.recv.at[j, idx],
                                            device_id={'tp': target}, device_id_type=MESH_ID)

    def message(self, j, idx):
        p, part, far, side = self.at, self.part, self.far, self.side
        first, second = pl.ds(0, self.half), pl.ds(self.half, self.rows - self.half)
        src, dst, target = (
            lambda: (self.far_src.at[j, 0, first], far.at[j, 0], p.right),
            lambda: (self.far_src.at[j, 0, second], far.at[j, 1], p.left),
            lambda: (part.at[j, 1, second], side.at[j, 0, second], p.right),
            lambda: (part.at[j, 2, first], side.at[j, 1, first], p.left),
            lambda: (part.at[j, 1, first], side.at[j, 0, first], p.right),
            lambda: (part.at[j, 2, second], side.at[j, 1, second], p.left))[idx]()
        return self.copy(j, idx, src, dst, target)

    def start_far(self, j, _=0):
        for idx in (0, 1):
            self.message(j, idx).start()
        return 0

    def start_side(self, j, _):
        for idx in (2, 3):
            self.message(j, idx).start()
        return 0

    def sums(self, j):
        h = self.half

        @pl.when(j >= self.early)
        def _():
            self.message(j, 0).wait_recv()
            self.message(j, 1).wait_recv()

        self.part[j, 1, :h] = (self.part[j, 1, :h].astype(F32) + self.far[j, 0].astype(F32)).astype(BF16)
        self.part[j, 2, h:] = (self.part[j, 2, h:].astype(F32) + self.far[j, 1].astype(F32)).astype(BF16)
        self.message(j, 4).start()
        self.message(j, 5).start()

    def sums_step(self, j, _):
        self.sums(j)
        return 0

    def final(self, j):
        for idx in range(2, 6):
            self.message(j, idx).wait_recv()
        total = self.part[j, 3].astype(F32) + self.side[j, 0].astype(F32) + self.side[j, 1].astype(F32)
        self.part[j, 3] = total.astype(BF16)

    def finish(self, j):
        @pl.when(j >= self.early)
        def _():
            for idx in range(2):
                self.message(j, idx).wait_send()

        for idx in range(2, 6):
            self.message(j, idx).wait_send()

    @staticmethod
    def scratch(rows, dim):
        nc, dma = dim // CHUNK, pltpu.SemaphoreType.DMA
        return [pltpu.VMEM((nc, 4, rows, CHUNK), BF16), pltpu.VMEM((nc, 2, rows // 2, CHUNK), BF16),
                pltpu.VMEM((nc, 2, rows, CHUNK), BF16), dma((nc, 6)), dma((nc, 6))]


def scatter_outputs(part, out, sem, j):
    nb, rows, _ = out.shape
    cs = pl.ds(pl.multiple_of(j * CHUNK, CHUNK), CHUNK)
    return [pltpu.make_async_copy(part.at[j, 3, pl.ds(b * rows, rows)], out.at[b, :, cs], sem.at[b]) for b in range(nb)]


def scatter_end(scatter, out, sem, nc):
    def last(j, _):
        scatter.final(j)
        for c in scatter_outputs(scatter.part, out, sem, j):
            c.start()
        return 0

    lax.fori_loop(0, nc, last, 0)

    def drain(j, _):
        for c in scatter_outputs(scatter.part, out, sem, j):
            c.wait()
        scatter.finish(j)
        return 0

    lax.fori_loop(0, nc, drain, 0)


def pair_rows(place, nb, rows, mine, theirs, lhs, sem):
    width = mine.shape[2]
    out = []
    for d, dev in enumerate((place.far, place.right, place.left, place.me)):
        src_rows = pl.ds(pl.multiple_of(dev * rows, 16), rows)
        for b in range(nb):
            dst_rows = pl.ds((d * nb + b) * rows, rows)
            for j, src in enumerate((mine, theirs)):
                out.append(pltpu.make_async_copy(src.at[b, src_rows], lhs.at[dst_rows, pl.ds(j * width, width)], sem.at[d // 2]))
    return out


def gather_attn_kernel(n, nb, heads, dim, q_ref, k_ref, v_ref, gain_ref, cos_ref, sin_ref, ss_ref,
                       wq_ref, wo_ref, wo_p, wo_t, d_in,
                       d_full, o_out, o_p, da_out, wq_p, part_out, far_in, o_t, qr_ref, kr_ref, lse_ref, o32_ref,
                       inv_q, inv_k, o_all, wo, xbuf, ast,
                       w_sem, ld_sem, out_sem, o_sem, p_sem, l_sem, g_send, g_recv, t_send, t_recv, r_send, r_recv, s_send, s_recv):
    step = pl.program_id(0)
    tokens = q_ref.shape[1]
    rows = tokens // n
    blk = min(384, tokens)
    place = Place(n)
    gather = Gather(place, d_full, rows, g_send, g_recv, early=EARLY_ROWS)
    cols = heads * HEAD_DIM
    nc = dim // CHUNK
    early_chunks = min(EARLY_CHUNKS, nc)
    mid = nc // 2
    scatter = Scatter(place, part_out, far_in, None, s_send, s_recv)
    trade_o = RowTrade(place, o_out, o_p, rows, r_send, r_recv)

    def trade_w():
        return place.to_partner(wq_ref, wq_p, t_send, t_recv)


    @pl.when(step == 0)
    def _():
        pltpu.make_async_copy(wo_t, wo, w_sem).start()
        place.barrier(place.near())

        for b in range(EARLY_ROWS):
            gather.pass_left(b)
            gather.pass_right(b)

        def own(b, _):
            gather.start_own(b)
            return 0

        lax.fori_loop(EARLY_ROWS, nb, own, 0)
        trade_w().start()

    @pl.when(step < nb * heads)
    def _():
        b = step // heads
        h = lax.rem(step, heads)

        @pl.when(h == 0)
        def _():
            inv_q[...] = lanes_of(lax.rsqrt(ss_ref[pl.ds(2 * b, 1)] / dim + EPS_NORM))
            inv_k[...] = lanes_of(lax.rsqrt(ss_ref[pl.ds(2 * b + 1, 1)] / dim + EPS_NORM))

        cos, sin = cos_ref[...], sin_ref[...]
        q_rot = rotate(q_ref[0] * inv_q[...] * gain_ref[0:1], cos, sin).astype(BF16)
        k_rot = rotate(k_ref[0] * inv_k[...] * gain_ref[1:2], cos, sin).astype(BF16)
        v = v_ref[0]
        lanes = pl.ds(pl.multiple_of(h * HEAD_DIM, HEAD_DIM), HEAD_DIM)
        qr_ref[0], kr_ref[0] = q_rot, k_rot

        def scores(i):
            return lax.dot_general(q_rot[i * blk:(i + 1) * blk], k_rot, NT, preferred_element_type=F32)

        ahead = scores(0)
        for i in range(tokens // blk):
            s = ahead
            if (i + 1) * blk < tokens:
                ahead = scores(i + 1)
            p, lse = softmax_block(s)
            lse_ref[0, i * blk:(i + 1) * blk] = jnp.broadcast_to(lse, (blk, HEAD_DIM))
            o = jnp.dot(p.astype(BF16), v, preferred_element_type=F32)
            o32_ref[0, i * blk:(i + 1) * blk] = o
            o_all[b, i * blk:(i + 1) * blk, lanes] = o.astype(BF16)

    @pl.when(step == nb * heads)
    def _():
        o_copy = pltpu.make_async_copy(o_all, o_out, o_sem)
        o_copy.start()
        pltpu.make_async_copy(wo_t, wo, w_sem).wait()

        def outputs(b, row0, slot):
            return pltpu.make_async_copy(ast.at[slot], da_out.at[b, pl.ds(row0, 2 * rows)], out_sem.at[slot])

        def load(b, row0, slot):
            return pltpu.make_async_copy(d_full.at[b, pl.ds(row0, 2 * rows)], xbuf.at[slot], ld_sem.at[slot])

        def project(lhs, wbuf, stage):
            loads = pair_rows(place, nb, rows, o_out, o_p, lhs, l_sem)
            for c in loads:
                c.start()

            def chunk(j):
                cs = pl.ds(pl.multiple_of(j * CHUNK, CHUNK), CHUNK)
                slot = lax.rem(j, 2)
                return [pltpu.make_async_copy(wo_ref.at[:, cs], wbuf.at[slot, pl.ds(0, cols)], p_sem.at[slot, 0]),
                        pltpu.make_async_copy(wo_p.at[:, cs], wbuf.at[slot, pl.ds(cols, cols)], p_sem.at[slot, 1])]

            def store(j):
                slot = lax.rem(j, 2)
                return pltpu.make_async_copy(stage.at[slot], part_out.at[j], p_sem.at[slot, 2])

            def stored(j):
                store(j).wait()

                @pl.when((j < early_chunks) & (j >= mid))
                def _():
                    scatter.start_far(j)

            for c in chunk(0):
                c.start()
            for c in loads:
                c.wait()

            def body(j, _):
                slot = lax.rem(j, 2)

                @pl.when(j + 1 < nc)
                def _():
                    for c in chunk(j + 1):
                        c.start()

                for c in chunk(j):
                    c.wait()
                half = 2 * nb * rows
                for d in range(2):
                    z = jnp.dot(lhs[d * half:(d + 1) * half], wbuf[slot], preferred_element_type=F32).astype(BF16)
                    stage[slot, 2 * d] = z[:half // 2]
                    stage[slot, 2 * d + 1] = z[half // 2:]
                store(j).start()

                @pl.when(j >= 1)
                def _():
                    stored(j - 1)

                @pl.when(j == mid)
                def _():
                    gather.arrive(3 * nb - 2, nb)
                    gather.arrive(3 * nb - 1, nb)
                    lax.fori_loop(0, min(early_chunks, mid), scatter.start_far, 0)

                return 0

            lax.fori_loop(0, nc, body, 0)
            stored(nc - 1)

        def fetch(i):
            b, row0 = gather.ready(i, nb)
            load(b, row0, lax.rem(i, 2)).start()

        fetch(0)
        gather.arrive(jnp.int32(1), nb)

        def item(i, _):
            slot = lax.rem(i, 2)

            @pl.when((i + 2 != 3 * nb - 2) & (i + 2 != 3 * nb - 1) & (i + 2 < 4 * nb))
            def _():
                gather.arrive(i + 2, nb)

            @pl.when((i + 1 != 3 * nb - 2) & (i + 1 < 4 * nb))
            def _():
                fetch(i + 1)

            @pl.when(i >= 2)
            def _():
                outputs(0, 0, slot).wait()

            load(0, 0, slot).wait()
            ast[slot] = jnp.dot(xbuf[slot], wo[...], preferred_element_type=F32).astype(BF16)
            b, row0 = gather.item_place(i, nb)
            outputs(b, row0, slot).start()

            @pl.when(i == 0)
            def _():
                o_copy.wait()
                trade_o.start()

            @pl.when(i + 1 == 3 * nb - 2)
            def _():
                trade_o.wait_recv()
                pl.run_scoped(project, pltpu.VMEM((4 * nb * rows, 2 * cols), BF16), pltpu.VMEM((2, 2 * cols, CHUNK), BF16),
                              pltpu.VMEM((2, 4, nb * rows, CHUNK), BF16))
                fetch(i + 1)

                def turn(turned):
                    for b in range(nb):
                        turned[:, b * tokens:(b + 1) * tokens] = o_all[b].T
                    pltpu.sync_copy(turned, o_t)

                pl.run_scoped(turn, pltpu.VMEM((cols, nb * tokens), BF16))

            return 0

        lax.fori_loop(0, 4 * nb, item, 0)
        for slot in range(2):
            outputs(0, 0, slot).wait()
        for b in range(nb):
            gather.finish(b)
        trade_o.wait_send()
        trade_w().wait()
        for j in range(early_chunks):
            for idx in (0, 1):
                scatter.message(j, idx).wait()


def gather_attn_call(n, q, k, v, gains, cos_tab, sin_tab, ss, w_q, w_o, wo_p, wo_t, d_full):
    nb, tokens, cols = q.shape
    dim = w_o.shape[1]
    heads = cols // HEAD_DIM
    rows = tokens // n
    last = nb * heads - 1
    nc = dim // CHUNK
    early = min(EARLY_CHUNKS, nc)
    shape = jax.ShapeDtypeStruct
    dma = pltpu.SemaphoreType.DMA
    any_spec = pl.BlockSpec(memory_space=pl.ANY)

    def head_of(i):
        i = jnp.minimum(i, last)
        return i // heads, i % heads

    blk = pl.BlockSpec((1, tokens, HEAD_DIM), lambda i: (head_of(i)[0], 0, head_of(i)[1]))
    vec = pl.BlockSpec((2, HEAD_DIM), lambda i: (0, head_of(i)[1]))
    tab = pl.BlockSpec((tokens, HEAD_DIM), lambda i: (0, 0))
    head_arr = shape((nb, tokens, cols), BF16)
    return pl.pallas_call(
        functools.partial(gather_attn_kernel, n, nb, heads, dim), name="gather_attn", grid=(nb * heads + 1,),
        out_shape=[shape(d_full.shape, BF16), head_arr, head_arr, head_arr, shape(w_q.shape, BF16)]
        + [shape((nc, 4, nb * rows, CHUNK), BF16), shape((early, 2, nb * rows // 2, CHUNK), BF16), shape((cols, nb * tokens), BF16), head_arr, head_arr,
           shape((nb, tokens, cols), F32), shape((nb, tokens, cols), F32)],
        in_specs=[blk, blk, blk, vec, tab, tab, pl.BlockSpec(ss.shape, lambda i: (0, 0))] + [any_spec] * 5,
        out_specs=[any_spec] * 8 + [blk] * 4,
        scratch_shapes=[
            pltpu.VMEM((tokens, HEAD_DIM), F32), pltpu.VMEM((tokens, HEAD_DIM), F32), pltpu.VMEM((nb, tokens, cols), BF16),
            pltpu.VMEM((dim, cols), BF16), pltpu.VMEM((2, 2 * rows, dim), BF16), pltpu.VMEM((2, 2 * rows, cols), BF16),
            dma, dma((2,)), dma((2,)), dma, dma((2, 3)), dma((2,)), dma((nb, GATHER_SEMS)), dma((nb, GATHER_SEMS)), dma, dma,
            dma((nb, n // 2)), dma((nb, n // 2)), dma((early, 6)), dma((early, 6))],
        input_output_aliases={11: 0},
        compiler_params=params("arbitrary", collective_id=1, has_side_effects=True),
        cost_estimate=cost(4 * nb * tokens * dim * cols + 4 * nb * tokens * tokens * cols, 8 * nb * tokens * dim),
    )(q, k, v, gains, cos_tab, sin_tab, ss, w_q, w_o, wo_p, wo_t, d_full)


class DyChunks:
    def __init__(self, lhs, wbuf, weights, w_sem):
        self.lhs, self.wbuf, self.weights, self.sem = lhs, wbuf, weights, w_sem

    def loads(self, j):
        slot = lax.rem(j, 2)
        src = pl.ds(pl.multiple_of(j * CHUNK, CHUNK), CHUNK)
        width = self.weights[0].shape[1]
        return [pltpu.make_async_copy(w.at[src], self.wbuf.at[slot, :, pl.ds(m * width, width)], self.sem.at[slot, m])
                for m, w in enumerate(self.weights)]

    def dot(self, j, d):
        half = self.lhs.shape[0] // 2
        return lax.dot_general(self.lhs[d * half:(d + 1) * half], self.wbuf[lax.rem(j, 2)], NT, preferred_element_type=F32).astype(BF16)


def attn_bwd_kernel(n, nb, heads, dim, q_ref, k_ref, qr_ref, kr_ref, v_ref, do_ref, o_ref, lse_ref, gain_ref, cos_ref, sin_ref, ss_ref,
                    q_hbm, k_hbm, o_t, part_in, far_in, d_full, wq_hbm, wk_hbm, wv_hbm, wq_p,
                    proj_out, g_out, g_p, dqs_out, dks_out, dwo_out, wk_p, wv_p, part_dy, far_dy, dgq_ref, dgk_ref,
                    part, recv_far, recv_side, s_send, s_recv,
                    inv_q, inv_k, acc_q, acc_k, p_all, ds_all, dq_all, qs_st, ks_st, v_st, st_row, st_sum, slots, fbuf, gbuf, lanes_s,
                    ld_sem, w_sem, fl_sem, g_sem, go_sem, out_sem, e_send, e_recv, t_send, t_recv, r_send, r_recv, c_sem, y_send, y_recv):
    step = pl.program_id(0)
    tokens = q_ref.shape[1]
    rows = tokens // n
    cols = heads * HEAD_DIM
    blk = min(256, tokens)
    nc = dim // CHUNK
    steps = nb * heads
    scale = HEAD_DIM ** -0.5
    place = Place(n)
    early = far_in.shape[0]
    scatter = Scatter(place, part, recv_far, recv_side, s_send, s_recv, far_src=part_in, early=early)

    def stored():
        return [pltpu.make_async_copy(part_in, part, ld_sem.at[0]),
                pltpu.make_async_copy(far_in, recv_far.at[pl.ds(0, early)], ld_sem.at[1])]

    n_pieces = 8

    def trade_w(j):
        m = j % (n_pieces // 2)
        size = dim // (n_pieces // 2)
        src, dst = ((wk_hbm, wk_p), (wv_hbm, wv_p))[j // (n_pieces // 2)]
        return place.to_partner(src.at[pl.ds(m * size, size)], dst.at[pl.ds(m * size, size)], t_send.at[j], t_recv.at[j])

    @pl.when(step == 0)
    def _():
        place.barrier(place.everyone())
        for c in stored():
            c.start()

    @pl.when(step == 1)
    def _():
        for c in stored():
            c.wait()

    def flush(b, h, slot):
        lanes = pl.ds(pl.multiple_of(h * HEAD_DIM, HEAD_DIM), HEAD_DIM)
        v_lanes = pl.ds(pl.multiple_of(2 * cols + h * HEAD_DIM, HEAD_DIM), HEAD_DIM)
        return [pltpu.make_async_copy(qs_st.at[slot], dqs_out.at[b, :, lanes], fl_sem.at[slot, 0]),
                pltpu.make_async_copy(ks_st.at[slot], dks_out.at[b, :, lanes], fl_sem.at[slot, 1]),
                pltpu.make_async_copy(v_st.at[slot], g_out.at[b, :, v_lanes], fl_sem.at[slot, 2])]

    for j in range(n_pieces):
        pl.when(step == j * (steps - 1) // n_pieces + 1)(lambda j=j: trade_w(j).start())

    mid = min(early + 2, nc)
    events = []
    late = list(range(mid))
    for m, j in enumerate(range(early, nc)):
        events.append(functools.partial(scatter.start_far, j))
        if m >= 2 and late:
            events.append(functools.partial(scatter.sums, late.pop(0)))
    events += [functools.partial(scatter.sums, j) for j in late]
    for m, event in enumerate(events):
        @pl.when(step == m * (steps - 1) // len(events))
        def _(event=event):
            event()

    rb = min(256, tokens)
    per = tokens // rb

    def stats(b):
        return Exchange(place, st_row.at[b], slots.at[b], e_send.at[b], e_recv.at[b])

    def grad_loads(b, i):
        r0 = pl.multiple_of(i * rb, rb)
        return [pltpu.make_async_copy(src.at[b, pl.ds(r0, rb)], fbuf.at[m], g_sem.at[m])
                for m, src in enumerate((dqs_out, q_hbm, dks_out, k_hbm))]

    def grad_store(b, i):
        r0 = pl.multiple_of(i * rb, rb)
        return pltpu.make_async_copy(gbuf, g_out.at[b, pl.ds(r0, rb), pl.ds(0, 2 * cols)], go_sem.at[0])

    def trade(b):
        return RowTrade(place, g_out, g_p, rows, r_send, r_recv, rows_of=(b,))

    def grad_block(b, i):
        for c in grad_loads(b, i):
            c.wait()
        sl = pl.ds(pl.multiple_of(i * rb, rb), rb)
        for m in range(2):
            inv_l = lanes_s[2 * m, sl]
            st_l = lanes_s[2 * m + 1, sl]
            for h in range(heads):
                hs = slice(h * HEAD_DIM, (h + 1) * HEAD_DIM)
                grad = inv_l * (fbuf[2 * m, :, hs] - (fbuf[2 * m + 1, :, hs] * inv_l) * st_l)
                gbuf[:, m * cols + h * HEAD_DIM:m * cols + (h + 1) * HEAD_DIM] = grad.astype(BF16)
        grad_store(b, i).start()

    def grad_begin(b):
        st_sum[...] = stats(b).finish()
        for m in range(2):
            lanes_s[2 * m] = lanes_of(lax.rsqrt(ss_ref[pl.ds(2 * b + m, 1)] / dim + EPS_NORM))
            lanes_s[2 * m + 1] = lanes_of(st_sum[m:m + 1] / dim)

    first = heads - per
    assert first >= 2
    b_old = step // heads - 1
    i_old = lax.rem(step, heads) - first

    @pl.when((step >= heads) & (step < steps) & (i_old >= 0))
    def _():
        @pl.when(i_old == 0)
        def _():
            grad_begin(b_old)

        @pl.when(i_old > 0)
        def _():
            grad_store(0, 0).wait()

        for c in grad_loads(b_old, i_old):
            c.start()

    @pl.when((step >= 2 * heads) & (lax.rem(step, heads) == 0))
    def _():
        grad_store(0, 0).wait()
        for b in range(nb - 1):
            pl.when(step == (b + 2) * heads)(trade(b).start)

    @pl.when(step < steps)
    def _():
        b = step // heads
        head = lax.rem(step, heads)
        slot = lax.rem(step, 2)

        @pl.when(step == 0)
        def _():
            st_row[...] = jnp.zeros_like(st_row)

        @pl.when(head == 0)
        def _():
            inv_q[...] = lanes_of(lax.rsqrt(ss_ref[pl.ds(2 * b, 1)] / dim + EPS_NORM))
            inv_k[...] = lanes_of(lax.rsqrt(ss_ref[pl.ds(2 * b + 1, 1)] / dim + EPS_NORM))
            acc_q[...] = jnp.zeros_like(acc_q)
            acc_k[...] = jnp.zeros_like(acc_k)

        @pl.when(step >= 2)
        def _():
            for c in flush(0, 0, slot):
                c.wait()

        cos, sin = cos_ref[...], sin_ref[...]
        q_rot, k_rot, v, do = qr_ref[0], kr_ref[0], v_ref[0], do_ref[0]

        def scores(i):
            sl = slice(i * blk, (i + 1) * blk)
            return (lax.dot_general(q_rot[sl], k_rot, NT, preferred_element_type=F32),
                    lax.dot_general(do[sl], v, NT, preferred_element_type=F32))

        ahead = scores(0)
        for i in range(tokens // blk):
            sl = slice(i * blk, (i + 1) * blk)
            s, dp = ahead
            if (i + 1) * blk < tokens:
                ahead = scores(i + 1)
            lse = jnp.concatenate([lse_ref[0, sl]] * (tokens // HEAD_DIM), axis=1)
            p = jnp.exp2(s * SCORE_SCALE - lse)
            p_all[sl] = p.astype(BF16)
            delta = jnp.sum(do[sl].astype(F32) * o_ref[0, sl], axis=1, keepdims=True)
            ds = (p * (dp - delta)).astype(BF16)
            ds_all[sl] = ds
            dq_all[sl] = jnp.dot(ds, k_rot, preferred_element_type=F32) * scale
        do_t = do.astype(F32).T.astype(BF16)
        q_t = q_rot.astype(F32).T.astype(BF16)
        v_st[slot] = jnp.dot(do_t, p_all[...], preferred_element_type=F32).T.astype(BF16)
        dk_rot = (jnp.dot(q_t, ds_all[...], preferred_element_type=F32) * scale).T.astype(BF16).astype(F32)
        dq_rot = dq_all[...].astype(BF16).astype(F32)
        dq_hat = rotate(dq_rot, cos, -sin)
        dk_hat = rotate(dk_rot, cos, -sin)
        q_hat = q_ref[0] * inv_q[...]
        k_hat = k_ref[0] * inv_k[...]
        dgq_ref[0] = jnp.sum(dq_hat * q_hat, axis=0, keepdims=True)
        dgk_ref[0] = jnp.sum(dk_hat * k_hat, axis=0, keepdims=True)
        dq_s = dq_hat * gain_ref[0:1]
        dk_s = dk_hat * gain_ref[1:2]
        qs_st[slot] = dq_s
        ks_st[slot] = dk_s
        acc_q[...] += dq_s * q_hat
        acc_k[...] += dk_s * k_hat
        for c in flush(b, head, slot):
            c.start()

        @pl.when(head == heads - 1)
        def _():
            st_row[b, 0:1] = to_row(acc_q[...])
            st_row[b, 1:2] = to_row(acc_k[...])
            for m in range(nb):
                pl.when(b == m)(stats(m).start)

    @pl.when((step >= heads) & (step < steps) & (i_old >= 0))
    def _():
        grad_block(b_old, i_old)

    @pl.when(step == steps)
    def _():
        for s in range(2):
            for c in flush(0, 0, s):
                c.wait()
        lax.fori_loop(mid, nc, scatter.sums_step, 0)
        lax.fori_loop(0, nc, scatter.start_side, 0)
        for c in grad_loads(nb - 1, 0):
            c.start()

        def last_grad():
            grad_begin(nb - 1)

            def last_row(i, _):
                @pl.when(i > 0)
                def _():
                    grad_store(0, 0).wait()
                    for c in grad_loads(nb - 1, i):
                        c.start()

                grad_block(nb - 1, i)
                return 0

            lax.fori_loop(0, per, last_row, 0)
            grad_store(0, 0).wait()
            trade(nb - 1).start()

        def weight_grad(turned, dbuf, wst):
            bn = min(512, dim)
            n_chunks = dim // bn

            def chunk(c):
                slot = lax.rem(c, 2)
                return pltpu.make_async_copy(d_full.at[:, :, pl.ds(pl.multiple_of(c * bn, bn), bn)], dbuf.at[slot], w_sem.at[slot, 1])

            def store(c):
                slot = lax.rem(c, 2)
                return pltpu.make_async_copy(wst.at[slot], dwo_out.at[:, pl.ds(pl.multiple_of(c * bn, bn), bn)], w_sem.at[slot, 0])

            load_o = pltpu.make_async_copy(o_t, turned, ld_sem.at[0])
            load_o.start()
            chunk(0).start()
            load_o.wait()

            def body(c, _):
                slot = lax.rem(c, 2)

                @pl.when(c + 1 < n_chunks)
                def _():
                    chunk(c + 1).start()

                @pl.when(c >= 2)
                def _():
                    store(c).wait()

                chunk(c).wait()
                d = dbuf[slot].reshape(nb * tokens, bn)
                wst[slot] = jnp.dot(turned[...], d, preferred_element_type=F32).astype(BF16)
                store(c).start()
                pl.when(c == max(n_chunks // 2 - 2, 0))(last_grad)
                return 0

            lax.fori_loop(0, n_chunks, body, 0)
            for s in range(min(2, n_chunks)):
                store(s).wait()

        bn = min(512, dim)
        pl.run_scoped(weight_grad, pltpu.VMEM((cols, nb * tokens), BF16), pltpu.VMEM((2, nb, tokens, bn), BF16),
                      pltpu.VMEM((2, cols, bn), BF16))
        for b in range(nb):
            trade(b).wait_recv()
        for j in range(n_pieces):
            trade_w(j).wait_recv()

        n_dy = part_dy.shape[0]
        scatter_y = Scatter(place, part_dy, far_dy, None, y_send, y_recv)

        def first_dy(lhs, wbuf, pst):
            loads = pair_rows(place, nb, rows, g_out, g_p, lhs, ld_sem)
            for c in loads:
                c.start()
            dy = DyChunks(lhs, wbuf, (wq_hbm, wk_hbm, wv_hbm, wq_p, wk_p, wv_p), c_sem)
            for c in dy.loads(0):
                c.start()
            for c in loads:
                c.wait()

            def body(j, _):
                @pl.when(j + 1 < n_dy)
                def _():
                    for c in dy.loads(j + 1):
                        c.start()

                for c in dy.loads(j):
                    c.wait()
                store = pltpu.make_async_copy(pst, part_dy.at[j], go_sem.at[0])

                @pl.when(j >= 1)
                def _():
                    store.wait()
                    scatter_y.start_far(j - 1)

                for d in range(2):
                    z = dy.dot(j, d)
                    pst[2 * d] = z[:nb * rows]
                    pst[2 * d + 1] = z[nb * rows:]
                store.start()
                return 0

            lax.fori_loop(0, n_dy, body, 0)
            pltpu.make_async_copy(pst, part_dy.at[n_dy - 1], go_sem.at[0]).wait()
            scatter_y.start_far(n_dy - 1)

        pl.run_scoped(first_dy, pltpu.VMEM((4 * nb * rows, 6 * cols), BF16), pltpu.VMEM((2, CHUNK, 6 * cols), BF16),
                      pltpu.VMEM((4, nb * rows, CHUNK), BF16))
        scatter_end(scatter, proj_out, out_sem, nc)
        for b in range(nb):
            trade(b).wait_send()
        for j in range(n_pieces):
            trade_w(j).wait_send()
        for j in range(n_dy):
            for idx in (0, 1):
                scatter_y.message(j, idx).wait()


def attn_bwd_call(n, q, k, q_rot, k_rot, v, d_attn, o_t, o32, lse, gains, cos_tab, sin_tab, ss, part, far, d_full, w_q, w_k, w_v, wq_p):
    nb, tokens, cols = q.shape
    dim = d_full.shape[2]
    heads = cols // HEAD_DIM
    rows = tokens // n
    steps = nb * heads
    shape = jax.ShapeDtypeStruct
    dma = pltpu.SemaphoreType.DMA
    any_spec = pl.BlockSpec(memory_space=pl.ANY)

    def head_of(i):
        i = jnp.minimum(i, steps - 1)
        return i // heads, i % heads

    blk = pl.BlockSpec((1, tokens, HEAD_DIM), lambda i: (head_of(i)[0], 0, head_of(i)[1]))
    vec = pl.BlockSpec((2, HEAD_DIM), lambda i: (0, head_of(i)[1]))
    out_vec = pl.BlockSpec((1, 1, HEAD_DIM), lambda i: (head_of(i)[0], 0, head_of(i)[1]))
    tab = pl.BlockSpec((tokens, HEAD_DIM), lambda i: (0, 0))
    whole = (nb, tokens, cols)
    lane_tile = pltpu.VMEM((tokens, HEAD_DIM), F32)
    n_dy = min(EARLY_DY, dim // CHUNK)
    return pl.pallas_call(
        functools.partial(attn_bwd_kernel, n, nb, heads, dim), name="attn_bwd", grid=(steps + 1,),
        out_shape=[shape((nb, rows, dim), BF16), shape((nb, tokens, 3 * cols), BF16), shape((nb, tokens, 3 * cols), BF16),
                   shape(whole, F32), shape(whole, F32), shape((cols, dim), BF16),
                   shape(w_k.shape, BF16), shape(w_v.shape, BF16), shape((n_dy,) + part.shape[1:], BF16), shape((n_dy,) + far.shape[1:], BF16),
                   shape((nb, 1, cols), F32), shape((nb, 1, cols), F32)],
        in_specs=[blk] * 8 + [vec, tab, tab, pl.BlockSpec(ss.shape, lambda i: (0, 0))] + [any_spec] * 10,
        out_specs=[any_spec] * 10 + [out_vec, out_vec],
        scratch_shapes=Scatter.scratch(nb * rows, dim) + [lane_tile] * 4 + [pltpu.VMEM((tokens, tokens), BF16)] * 2 + [
            lane_tile, pltpu.VMEM((2, tokens, HEAD_DIM), F32), pltpu.VMEM((2, tokens, HEAD_DIM), F32),
            pltpu.VMEM((2, tokens, HEAD_DIM), BF16), pltpu.VMEM((nb, 8, tokens), F32), pltpu.VMEM((8, tokens), F32),
            pltpu.VMEM((nb, n, 8, tokens), F32), pltpu.VMEM((4, min(256, tokens), cols), F32), pltpu.VMEM((min(256, tokens), 2 * cols), BF16),
            pltpu.VMEM((4, tokens, HEAD_DIM), F32),
            dma((2,)), dma((2, 2)), dma((2, 3)), dma((4,)), dma((2,)), dma((nb,)), dma((nb, n)), dma((nb, n)), dma((8,)), dma((8,)),
            dma((nb, n // 2)), dma((nb, n // 2)), dma((2, 6)), dma((n_dy, 6)), dma((n_dy, 6))],
        compiler_params=params("arbitrary", collective_id=2, has_side_effects=True),
        cost_estimate=cost(4 * nb * tokens * dim * cols + 36 * nb * tokens * tokens * cols, 30 * nb * tokens * cols),
    )(q, k, q_rot, k_rot, v, d_attn, o32, lse, gains, cos_tab, sin_tab, ss, q, k, o_t, part, far, d_full, w_q, w_k, w_v, wq_p)


def dy_dw_kernel(n, nb, dim, g_hbm, g_p, wq_hbm, wk_hbm, wv_hbm, wq_p, wk_p, wv_p, y_full, part_in, far_in,
                 dy_out, dwq_out, dwk_out, dwv_out,
                 part, recv_far, recv_side, s_send, s_recv, g, ld_sem, w_sem, y_sem, o_sem, out_sem):
    tokens = g_hbm.shape[1]
    rows = tokens // n
    cols = g_hbm.shape[2] // 3
    nc = dim // CHUNK
    early = far_in.shape[0]
    lag = 3
    place = Place(n)
    scatter = Scatter(place, part, recv_far, recv_side, s_send, s_recv, early=early)
    stored = [pltpu.make_async_copy(part_in, part.at[pl.ds(0, early)], ld_sem.at[2]),
              pltpu.make_async_copy(far_in, recv_far.at[pl.ds(0, early)], ld_sem.at[3])]
    load_g = pltpu.make_async_copy(g_hbm, g, ld_sem.at[4])

    def chain(lhs, wbuf):
        loads = pair_rows(place, nb, rows, g_hbm, g_p, lhs, ld_sem)
        dy = DyChunks(lhs, wbuf, (wq_hbm, wk_hbm, wv_hbm, wq_p, wk_p, wv_p), w_sem)
        if early < nc:
            for c in dy.loads(early):
                c.start()
            for c in loads[:len(loads) // 2]:
                c.start()
        for c in stored:
            c.start()
        if early < nc:
            for c in loads[len(loads) // 2:]:
                c.start()
        place.barrier(place.near()[:2])
        for c in stored:
            c.wait()
        lax.fori_loop(0, early, scatter.sums_step, 0)
        load_g.start()

        def body(j, _):
            @pl.when(j + 1 < nc)
            def _():
                for c in dy.loads(j + 1):
                    c.start()

            for c in dy.loads(j):
                c.wait()
            for d in range(2):
                @pl.when(j == early)
                def _(d=d):
                    for c in loads[d * len(loads) // 2:(d + 1) * len(loads) // 2]:
                        c.wait()

                z = dy.dot(j, d)
                part[j, 2 * d] = z[:nb * rows]
                part[j, 2 * d + 1] = z[nb * rows:]
                if d == 0:
                    scatter.start_far(j)

            @pl.when(j >= early + lag)
            def _():
                scatter.sums(j - lag)

            return 0

        lax.fori_loop(early, nc, body, 0)
        lax.fori_loop(0, nc, scatter.start_side, 0)

    pl.run_scoped(chain, pltpu.VMEM((4 * nb * rows, 6 * cols), BF16), pltpu.VMEM((2, CHUNK, 6 * cols), BF16))

    def weight_grad(ybuf, wst):
        bm = min(512, dim)
        n_chunks = dim // bm

        def chunk(c):
            slot = lax.rem(c, 2)
            return pltpu.make_async_copy(y_full.at[:, :, pl.ds(pl.multiple_of(c * bm, bm), bm)], ybuf.at[slot], y_sem.at[slot])

        def store(c):
            slot = lax.rem(c, 2)
            dst = pl.ds(pl.multiple_of(c * bm, bm), bm)
            return [pltpu.make_async_copy(wst.at[slot, :, pl.ds(m * cols, cols)], out.at[dst], o_sem.at[slot, m])
                    for m, out in enumerate((dwq_out, dwk_out, dwv_out))]

        chunk(0).start()
        load_g.wait()

        def body(c, _):
            slot = lax.rem(c, 2)

            @pl.when(c + 1 < n_chunks)
            def _():
                chunk(c + 1).start()

            @pl.when(c >= 2)
            def _():
                for s in store(c):
                    s.wait()

            chunk(c).wait()
            for m in range(lag):
                late = max(nc - lag, early) + m
                if late < nc:
                    pl.when(c == min(m, n_chunks - 1))(functools.partial(scatter.sums, late))
            wst[slot] = lax.dot_general(ybuf[slot].reshape(nb * tokens, bm), g[...].reshape(nb * tokens, 3 * cols), TN,
                                        preferred_element_type=F32).astype(BF16)
            for s in store(c):
                s.start()
            return 0

        lax.fori_loop(0, n_chunks, body, 0)
        for s in range(min(2, n_chunks)):
            for c in store(s):
                c.wait()

    bm = min(512, dim)
    pl.run_scoped(weight_grad, pltpu.VMEM((2, nb, tokens, bm), BF16), pltpu.VMEM((2, bm, 3 * cols), BF16))
    scatter_end(scatter, dy_out, out_sem, nc)


def dy_dw_call(n, g, g_p, w_q, w_k, w_v, wq_p, wk_p, wv_p, y_full, part, far):
    nb, tokens, wide = g.shape
    dim = y_full.shape[2]
    cols = wide // 3
    rows = tokens // n
    shape = jax.ShapeDtypeStruct
    dma = pltpu.SemaphoreType.DMA
    any_spec = pl.BlockSpec(memory_space=pl.ANY)
    return pl.pallas_call(
        functools.partial(dy_dw_kernel, n, nb, dim), name="dy_dw",
        out_shape=[shape((nb, rows, dim), BF16)] + [shape((dim, cols), BF16)] * 3,
        in_specs=[any_spec] * 11, out_specs=[any_spec] * 4,
        scratch_shapes=Scatter.scratch(nb * rows, dim) + [pltpu.VMEM((nb, tokens, 3 * cols), BF16), dma((5,)), dma((2, 6)), dma((2,)), dma((2, 3)), dma((nb,))],
        compiler_params=params(collective_id=3, has_side_effects=True),
        cost_estimate=cost(12 * nb * tokens * dim * cols, 30 * nb * tokens * cols),
    )(g, g_p, w_q, w_k, w_v, wq_p, wk_p, wv_p, y_full, part, far)


def token_kernel(n_copies, x_ref, dy_ref, pr_ref, g_ref, m_ref, e_ref, bo_ref, gq_ref, gk_ref, *refs):
    srcs, (xo_ref, dx_ref, dm_ref, dgq_ref, dgk_ref), dsts = refs[:4], refs[4:9], refs[9:13]
    bufs, (acc, in_sem, out_sem) = refs[13:17], refs[17:]
    group = 16
    step = pl.program_id(0)
    rows = x_ref.shape[1]
    groups = rows // group
    depth = bufs[0].shape[0]
    lag = depth - 1

    def move(c, out):
        copies = []
        for j, (src, dst, buf) in enumerate(zip(srcs, dsts, bufs)):
            size = buf.shape[1]
            sl = pl.ds(pl.multiple_of(c * size, 16), size)
            slot = lax.rem(c, depth)
            copies.append(pltpu.make_async_copy(buf.at[slot], dst.at[sl], out_sem.at[slot, j]) if out
                          else pltpu.make_async_copy(src.at[sl], buf.at[slot], in_sem.at[slot, j]))
        return copies

    def advance(i):
        @pl.when(i < n_copies)
        def _():
            @pl.when(i >= depth)
            def _():
                for c in move(i - depth, True):
                    c.wait()

            for c in move(i, False):
                c.start()

        @pl.when((i >= lag) & (i < n_copies + lag))
        def _():
            for c in move(i - lag, False):
                c.wait()
            for c in move(i - lag, True):
                c.start()

    mod = m_ref[...] + e_ref[0]
    for src, dst in ((gq_ref, dgq_ref), (gk_ref, dgk_ref)):
        dst[...] = jnp.sum(src[...], axis=(0, 1))
    shift_bo = bo_ref[...].reshape(1, bo_ref.shape[0])
    acc[...] = jnp.zeros_like(acc)

    def body(r, _):
        advance(step * groups + r)
        sl = pl.ds(pl.multiple_of(r * group, group), group)
        x = x_ref[0, sl].astype(F32)
        d_out = dy_ref[0, sl].astype(F32)
        proj = pr_ref[0, sl].astype(F32) + shift_bo
        xo_ref[0, sl] = (x + mod[2:3] * proj).astype(BF16)
        gate_part = d_out * proj
        x_norm, inv_std = norm_stats(x)
        d_y = g_ref[0, sl].astype(F32)
        d_norm = d_y * (1.0 + mod[1:2])
        d_x = d_out + inv_std * (
            d_norm - jnp.mean(d_norm, axis=-1, keepdims=True) - x_norm * jnp.mean(d_norm * x_norm, axis=-1, keepdims=True))
        dx_ref[0, sl] = d_x.astype(BF16)
        scale_part = d_y * x_norm
        acc[0] += d_y[:8] + d_y[8:]
        acc[1] += scale_part[:8] + scale_part[8:]
        acc[2] += gate_part[:8] + gate_part[8:]
        return 0

    lax.fori_loop(0, groups, body, 0)
    for j in range(3):
        dm_ref[0, j:j + 1] = jnp.sum(acc[j], axis=0, keepdims=True)

    @pl.when(step == pl.num_programs(0) - 1)
    def _():
        total = pl.num_programs(0) * groups

        def rest(i, _):
            advance(i)
            return 0

        lax.fori_loop(total, jnp.maximum(total, n_copies + lag), rest, 0)
        for c in range(max(n_copies - depth, 0), n_copies):
            for copy in move(c, True):
                copy.wait()


def token_call(x_loc, dy_loc, proj, d_y, m_block, e_loc, b_o, d_gq, d_gk, grads):
    nb, rows, dim = x_loc.shape
    n_copies = dim // min(512, dim)
    row = pl.BlockSpec((1, rows, dim), lambda i: (i, 0, 0))
    mod = pl.BlockSpec((1, 3, dim), lambda i: (i, 0, 0))
    any_spec = pl.BlockSpec(memory_space=pl.ANY)
    dma = pltpu.SemaphoreType.DMA
    depth = 4
    return pl.pallas_call(
        functools.partial(token_kernel, n_copies), name="tokens", grid=(nb,),
        out_shape=[jax.ShapeDtypeStruct(x_loc.shape, BF16), jax.ShapeDtypeStruct(x_loc.shape, BF16),
                   jax.ShapeDtypeStruct((nb, 3, dim), F32)] + [jax.ShapeDtypeStruct(d_gq.shape[2:], F32)] * 2 + [jax.ShapeDtypeStruct(w.shape, BF16) for w in grads],
        in_specs=[row, row, row, row, pl.BlockSpec((3, dim), lambda i: (0, 0)), mod] + [pl.BlockSpec(memory_space=pltpu.VMEM)] * 3 + [any_spec] * 4,
        out_specs=[row, row, mod] + [pl.BlockSpec(memory_space=pltpu.VMEM)] * 2 + [any_spec] * 4,
        scratch_shapes=[pltpu.VMEM((depth, w.shape[0] // n_copies, w.shape[1]), BF16) for w in grads]
        + [pltpu.VMEM((3, 8, dim), F32), dma((depth, 4)), dma((depth, 4))],
        compiler_params=params("arbitrary"),
        cost_estimate=cost(nb * rows * dim * 30, nb * rows * dim * 12),
    )(x_loc, dy_loc, proj, d_y, m_block, e_loc, b_o, d_gq, d_gk, *grads)


def solution(mesh):
    tp_size = mesh.shape['tp']

    def device_step(x_loc, e_loc, m_block, w_q, b_q, w_k, b_k, w_v, b_v, w_o, b_o, g_q, g_k, pos_part, dy_loc):
        nb, _, dim = x_loc.shape
        y_full, d_own, q, k, v, wo_p, wo_t, ss, cos_tab, sin_tab, gains = gather_qkv_call(
            tp_size, x_loc, dy_loc, m_block, e_loc, w_q, w_k, w_v, w_o, b_q, b_k, b_v, g_q, g_k, pos_part)
        d_full, _, _, d_attn, wq_p, part, far, o_t, q_rot, k_rot, lse, o32 = gather_attn_call(
            tp_size, q, k, v, gains, cos_tab, sin_tab, ss, w_q, w_o, wo_p, wo_t, d_own)
        proj, g, g_p, _, _, d_wo, wk_p, wv_p, part, far, d_gq, d_gk = attn_bwd_call(
            tp_size, q, k, q_rot, k_rot, v, d_attn, o_t, o32, lse, gains, cos_tab, sin_tab, ss, part, far, d_full, w_q, w_k, w_v, wq_p)
        d_y, d_wq, d_wk, d_wv = dy_dw_call(tp_size, g, g_p, w_q, w_k, w_v, wq_p, wk_p, wv_p, y_full, part, far)
        x_out, d_x, d_mod, d_gq, d_gk, d_wq, d_wk, d_wv, d_wo = token_call(
            x_loc, dy_loc, proj, d_y, m_block, e_loc, b_o, d_gq, d_gk, (d_wq, d_wk, d_wv, d_wo))
        d_e = all_sum_call(tp_size, d_mod.reshape(tp_size, -1, HEAD_DIM)).reshape(nb, 3, dim)
        return x_out, d_x, d_e, jnp.sum(d_e, axis=0), d_wq, d_wk, d_wv, d_wo, d_gq, d_gk

    in_specs = (P('dp', 'tp', None), P('dp', None, None), P(None, None), P(None, 'tp'), P('tp'), P(None, 'tp'), P('tp'),
                P(None, 'tp'), P('tp'), P('tp', None), P(None), P('tp'), P('tp'), P('dp', None), P('dp', 'tp', None))
    out_specs = (P('dp', 'tp', None), P('dp', 'tp', None), P('dp', None, None), P('dp', None), P('dp', 'tp'), P('dp', 'tp'),
                 P('dp', 'tp'), P(('dp', 'tp'), None), P(('dp', 'tp')), P(('dp', 'tp')))
    return jax.shard_map(device_step, mesh=mesh, in_specs=in_specs, out_specs=out_specs, check_vma=False)
```
